32 devices in a mesh: cells: 8 (over z, x), views: 4 (over y, core).
Axes of the slice: x: 2, y: 2, z: 4, core: 2. Of those that a mesh axis runs over, the one named last changes fastest.
Arguments:
- params: float32 [59, 16384], P(None, 'cells'), may hold values from -5 to 4, as said below
- first_moment: float32 [59, 16384], P(None, 'cells'), may hold values from -0.6 to 0.6
- second_moment: float32 [59, 16384], P(None, 'cells'), may hold values from 1e-12 to 0.05
- cameras: float32 [4, 6], P('views'), may hold values from -0.004 to 0.004
- visible: int32 [4, 16384], P('views', 'cells'), may hold values from 0 to 1, as said below
- send_plan: int32 [4, 8, 8, 256], P('views', 'cells'), may hold values from -1 to 2047, as said below
- tile_lists: int32 [4, 32, 512], P('views', 'cells'), may hold values from -1 to 2047, as said below
- target: float32 [4, 3, 8192], P('views', None, 'cells'), may hold values from 0 to 1
Outputs:
- updated_params: float32 [59, 16384], P(None, 'cells')
- updated_first: float32 [59, 16384], P(None, 'cells')
- updated_second: float32 [59, 16384], P(None, 'cells')
The draws below stay inside these ranges and needn't reach their ends.
Inputs may be any that keep to these rules, and one draw needn't show every extreme that they name: `params`: rows 0 to 2 hold a Gaussian's mean, 3 to 5 the logarithms of its scales, 6 to 9 a rotation quaternion whose first component is at least 0.6, 10 its opacity logit, 11 to 58 its spherical-harmonic coefficients; every Gaussian lies at depth 2 or more before every camera. In each view, between a quarter and three quarters of each owner's block of 2048 Gaussians are visible. Every row of an owner's block of 2048 Gaussians belongs to exactly one rendering device, 256 rows to each device; send_plan[v, s, d, :] lists exactly the rows of owner s that belong to device d and are visible in view v, live entries first, then -1; in every view some device receives 256 rows from every owner. `tile_lists`: tile t is rendered on device t // 4; an entry e stands for send_plan[v, e // 256, t // 4, e % 256], which is live; live entries come first, ordered by increasing params[2] of their Gaussians, then -1; some tile of each view has 512 live entries.
All inputs are finite; a program needn't handle non-finite values.
Results may differ from the reference program's by a relative error of at most 0.0003.
Values sent between devices are 32-bit elements; how exact they have to be, the bound alone decides.
A program may use at most 64 MiB of HBM per device.

```python
import jax
import jax.numpy as jnp
from jax import lax

G_DEV = 2048
TILES_DEV = 4
L = 512
TILE_COLS = 32
ADAM_STEP = 1000
CAP = 256
VIEWS = 4
OWNERS = 8
GAUSSIANS = 16384
TILES = 32
N_CELLS = 8
N_VIEWS = 4


def draw_scene(key):
    block_cols = TILE_COLS // 4
    block_high = 4 * TILES_DEV
    hot_rows = (L + OWNERS - 1) // OWNERS
    widest = min(27, (block_high - 1) // 2)
    reach_span = widest - 5
    shape_rows = (OWNERS, G_DEV)
    local_ids = jnp.arange(G_DEV, dtype=jnp.int32)
    placement = jnp.argsort(jax.random.randint(jax.random.fold_in(key, 301), shape_rows, 0, 4096) * G_DEV + local_ids[None, :], axis=-1).astype(jnp.int32)
    home_owner = placement // CAP
    within = placement % CAP
    edge_splat = (within == CAP - 1) & (within >= hot_rows) & (home_owner < block_cols)
    hot_tile = jax.random.randint(jax.random.fold_in(key, 302), (OWNERS,), 0, TILES_DEV)
    random_tile = jax.random.randint(jax.random.fold_in(key, 303), shape_rows, 0, TILES_DEV)
    aim_tile = jnp.where(within < hot_rows, hot_tile[home_owner], random_tile)
    aim_across = 16 * (aim_tile % 4) + jax.random.randint(jax.random.fold_in(key, 304), shape_rows, 0, 16)
    aim_down = 16 * (aim_tile // 4) + jax.random.randint(jax.random.fold_in(key, 305), shape_rows, 0, 16)
    reach = 6 + jnp.minimum(jax.random.randint(jax.random.fold_in(key, 306), shape_rows, 0, reach_span), jax.random.randint(jax.random.fold_in(key, 307), shape_rows, 0, reach_span))
    centre_across = jnp.clip(aim_across, reach, 63 - reach)
    centre_down = jnp.clip(aim_down, reach, block_high - 1 - reach)
    first_col = jnp.where(edge_splat, (aim_across - 28) // 16, (centre_across - reach) // 16)
    last_col = jnp.where(edge_splat, (aim_across + 28) // 16, (centre_across + reach) // 16)
    first_row = jnp.where(edge_splat, 0, (centre_down - reach) // 16)
    last_row = jnp.where(edge_splat, 0, (centre_down + reach) // 16)
    pixel_across = 64 * (home_owner % block_cols) + jnp.where(edge_splat, aim_across, centre_across)
    pixel_down = jnp.where(edge_splat, -48, block_high * (home_owner // block_cols) + centre_down)
    depth_keys = jax.random.randint(jax.random.fold_in(key, 308), (GAUSSIANS,), 0, 1024) * GAUSSIANS + jnp.arange(GAUSSIANS, dtype=jnp.int32)
    depth_rank = jnp.argsort(depth_keys).astype(jnp.int32).reshape(OWNERS, G_DEV)
    front_owner = jax.random.randint(jax.random.fold_in(key, 309), (VIEWS, 1, 1), 0, OWNERS)
    drawn = jax.random.randint(jax.random.fold_in(key, 310), (VIEWS, OWNERS, 1), G_DEV // 4, 3 * G_DEV // 4 + 1)
    noise = jax.random.randint(jax.random.fold_in(key, 311), (VIEWS, OWNERS, G_DEV), 0, 1024)
    scores = jnp.where(home_owner[None] == front_owner, 0, 1024 * G_DEV) + noise * G_DEV + local_ids[None, None, :]
    ranks = jnp.argsort(jnp.argsort(scores, axis=-1), axis=-1)
    seen = ranks < drawn
    visible = seen.astype(jnp.int32).reshape(VIEWS, GAUSSIANS)
    home_rows = jnp.argsort(placement, axis=-1).astype(jnp.int32)
    seen_home = jnp.take_along_axis(seen, jnp.broadcast_to(home_rows[None], (VIEWS, OWNERS, G_DEV)), axis=2).reshape(VIEWS, OWNERS, OWNERS, CAP)
    rows_home = jnp.broadcast_to(home_rows.reshape(1, OWNERS, OWNERS, CAP), (VIEWS, OWNERS, OWNERS, CAP))
    slot_ids = jnp.arange(CAP, dtype=jnp.int32)
    compact = jnp.argsort(jnp.where(seen_home, slot_ids, CAP + slot_ids), axis=-1)
    plan = jnp.where(jnp.take_along_axis(seen_home, compact, axis=3), jnp.take_along_axis(rows_home, compact, axis=3), -1).astype(jnp.int32)
    safe_rows = jnp.maximum(plan, 0)
    sources = jnp.arange(OWNERS, dtype=jnp.int32)[None, :, None, None]

    def per_slot(table):
        return jnp.transpose(table[sources, safe_rows], (0, 2, 1, 3)).reshape(VIEWS, OWNERS, 1, OWNERS * CAP)
    live = jnp.transpose(plan >= 0, (0, 2, 1, 3)).reshape(VIEWS, OWNERS, 1, OWNERS * CAP)
    tile_local = jnp.arange(TILES_DEV, dtype=jnp.int32)[None, None, :, None]
    tile_across = tile_local % 4
    tile_down = tile_local // 4
    meets = live & (per_slot(first_col) <= tile_across) & (per_slot(last_col) >= tile_across) & (per_slot(first_row) <= tile_down) & (per_slot(last_row) >= tile_down)
    slot_all = jnp.arange(OWNERS * CAP, dtype=jnp.int32)
    edge_ints = edge_splat.astype(jnp.int32)
    sort_key = jnp.where(meets, per_slot(depth_rank) + GAUSSIANS * (1 - per_slot(edge_ints)), 2 * GAUSSIANS + slot_all)
    order = jnp.argsort(sort_key, axis=-1)[..., :L].astype(jnp.int32)
    best = jnp.take_along_axis(sort_key, order, axis=-1)
    lists = jnp.where(best < 2 * GAUSSIANS, order, -1).astype(jnp.int32).reshape(VIEWS, OWNERS * TILES_DEV, L)
    return (visible, plan, lists, pixel_across, pixel_down, reach, depth_rank, edge_ints)


def draw_visible(key, part):
    return draw_scene(key)[0]


def draw_send_plan(key, part):
    return draw_scene(key)[1]


def draw_tile_lists(key, part):
    return draw_scene(key)[2]


def draw_params(key, part):
    scene = draw_scene(key)
    half_width = TILE_COLS * 8.0
    rows_pix = TILES // TILE_COLS * 16
    edge_splat = scene[7].reshape(GAUSSIANS) > 0
    rank_part = (scene[6].reshape(GAUSSIANS).astype(jnp.float32) + 0.5) / GAUSSIANS
    across = (scene[3].reshape(GAUSSIANS).astype(jnp.float32) + 0.5 - half_width) / half_width
    down = (scene[4].reshape(GAUSSIANS).astype(jnp.float32) + 0.5 - rows_pix * 0.5) / half_width
    depth = jnp.where(edge_splat, 2.05 + 0.4 * rank_part, 2.5 + 1.5 * rank_part)
    sigma_pix = (scene[5].reshape(GAUSSIANS).astype(jnp.float32) - 3.0) / 3.0
    jitter = jax.random.uniform(jax.random.fold_in(key, 201), (3, GAUSSIANS), jnp.float32, -0.15, 0.15)
    drawn_scale = jnp.log(sigma_pix * depth / half_width)[None, :] + jitter
    edge_scale = jnp.log(48.0 / half_width * depth / (5.4 * jnp.sqrt(1.0 + down * down)))
    log_scale = jnp.where(edge_splat[None, :], jnp.broadcast_to(edge_scale[None, :], (3, GAUSSIANS)), drawn_scale)
    quat_first = jax.random.uniform(jax.random.fold_in(key, 204), (1, GAUSSIANS), jnp.float32, 0.6, 1.2)
    quat_rest = jax.random.uniform(jax.random.fold_in(key, 205), (3, GAUSSIANS), jnp.float32, -1.0, 1.0)
    logit = jax.random.uniform(jax.random.fold_in(key, 206), (1, GAUSSIANS), jnp.float32, -3.5, -1.0)
    constant_part = jax.random.uniform(jax.random.fold_in(key, 207), (3, GAUSSIANS), jnp.float32, -1.5, 1.5)
    higher = jnp.clip(0.3 * jax.random.normal(jax.random.fold_in(key, 208), (45, GAUSSIANS), jnp.float32), -1.5, 1.5)
    edge_logit = jax.random.uniform(jax.random.fold_in(key, 211), (1, GAUSSIANS), jnp.float32, -1.5, -1.0)
    logit = jnp.where(edge_splat[None, :], edge_logit, logit)
    means = jnp.stack([across * depth, down * depth, depth])
    return jnp.concatenate([means, log_scale, quat_first, quat_rest, logit, constant_part, higher], axis=0)


def draw_moments(key):
    edge_splat = draw_scene(key)[7].reshape(GAUSSIANS) > 0
    faint_second = jnp.exp(jax.random.uniform(jax.random.fold_in(key, 402), (59, GAUSSIANS), jnp.float32, -27.631021, -25.328436))
    drawn_second = jnp.exp(jax.random.uniform(jax.random.fold_in(key, 403), (59, GAUSSIANS), jnp.float32, -6.9077553, -2.9957323))
    second = jnp.where(edge_splat[None, :], faint_second, drawn_second)
    drawn_first = jnp.clip(0.1 * jax.random.normal(jax.random.fold_in(key, 404), (59, GAUSSIANS), jnp.float32), -0.6, 0.6)
    faint_first = 0.3 * jnp.sqrt(faint_second) * jnp.clip(jax.random.normal(jax.random.fold_in(key, 405), (59, GAUSSIANS), jnp.float32), -2.0, 2.0)
    first = jnp.where(edge_splat[None, :], faint_first, drawn_first)
    return (first, second)


def draw_first_moment(key, part):
    return draw_moments(key)[0]


def draw_second_moment(key, part):
    return draw_moments(key)[1]


def levels(stream_key, extent, cuts, least, largest):
    level = 1.0
    for position, blocks in cuts:
        draws = jax.random.uniform(jax.random.fold_in(jax.random.fold_in(stream_key, 6), position), (blocks,), jnp.float32, least / len(cuts), largest / len(cuts))
        level = level * jnp.repeat(jnp.exp(draws), extent[position] // blocks).reshape((-1,) + (1,) * (len(extent) - 1 - position))
    return level


def setup_inputs(seed: int = 0) -> dict:
    keys = jax.random.split(jax.random.key(seed), 9)
    params = draw_params(jax.random.fold_in(keys[8], 71), 0)
    first_moment = draw_first_moment(jax.random.fold_in(keys[8], 71), 0)
    second_moment = draw_second_moment(jax.random.fold_in(keys[8], 71), 0)
    cameras = jnp.clip(jax.random.uniform(keys[3], (VIEWS, 6), jnp.float32, -0.004, 0.004) * levels(keys[3], (VIEWS, 6), ((0, 4),), -0.4, 0.0), -0.004, 0.004)
    visible = draw_visible(jax.random.fold_in(keys[8], 71), 0)
    send_plan = draw_send_plan(jax.random.fold_in(keys[8], 71), 0)
    tile_lists = draw_tile_lists(jax.random.fold_in(keys[8], 71), 0)
    target = jnp.clip(1.0 * jax.random.uniform(keys[7], (VIEWS, 3, TILES * 256), jnp.float32) ** levels(keys[7], (VIEWS, 3, TILES * 256), ((0, 4), (2, 8)), -0.2, 0.2), 0.0, 1.0)
    return {"params": params, "first_moment": first_moment, "second_moment": second_moment, "cameras": cameras, "visible": visible, "send_plan": send_plan, "tile_lists": tile_lists, "target": target}


harmonic_zero = 0.28209479177387814
harmonic_one = 0.4886025119029199
harmonic_two = (1.0925484305920792, -1.0925484305920792, 0.31539156525252005, -1.0925484305920792, 0.5462742152960396)
harmonic_three = (-0.5900435899266435, 2.890611442640554, -0.4570457994644658, 0.3731763325901154, -0.4570457994644658, 1.445305721320277, -0.5900435899266435)

def harmonics(across, upward, onward):
    across_sq = across * across
    upward_sq = upward * upward
    onward_sq = onward * onward
    return jnp.stack([harmonic_zero * jnp.ones_like(across), -harmonic_one * upward, harmonic_one * onward, -harmonic_one * across, harmonic_two[0] * across * upward, harmonic_two[1] * upward * onward, harmonic_two[2] * (2.0 * onward_sq - across_sq - upward_sq), harmonic_two[3] * across * onward, harmonic_two[4] * (across_sq - upward_sq), harmonic_three[0] * upward * (3.0 * across_sq - upward_sq), harmonic_three[1] * across * upward * onward, harmonic_three[2] * upward * (4.0 * onward_sq - across_sq - upward_sq), harmonic_three[3] * onward * (2.0 * onward_sq - 3.0 * across_sq - 3.0 * upward_sq), harmonic_three[4] * across * (4.0 * onward_sq - across_sq - upward_sq), harmonic_three[5] * onward * (across_sq - upward_sq), harmonic_three[6] * across * (across_sq - 3.0 * upward_sq)])

def camera_rotation(angles):
    cos_roll, sin_roll = (jnp.cos(angles[0]), jnp.sin(angles[0]))
    cos_pitch, sin_pitch = (jnp.cos(angles[1]), jnp.sin(angles[1]))
    cos_yaw, sin_yaw = (jnp.cos(angles[2]), jnp.sin(angles[2]))
    naught = jnp.zeros_like(cos_roll)
    unit_one = jnp.ones_like(cos_roll)
    roll = jnp.stack([jnp.stack([unit_one, naught, naught]), jnp.stack([naught, cos_roll, -sin_roll]), jnp.stack([naught, sin_roll, cos_roll])])
    pitch = jnp.stack([jnp.stack([cos_pitch, naught, sin_pitch]), jnp.stack([naught, unit_one, naught]), jnp.stack([-sin_pitch, naught, cos_pitch])])
    yawing = jnp.stack([jnp.stack([cos_yaw, -sin_yaw, naught]), jnp.stack([sin_yaw, cos_yaw, naught]), jnp.stack([naught, naught, unit_one])])
    inner_turn = jnp.dot(pitch, roll, precision=lax.Precision.HIGHEST)
    return jnp.dot(yawing, inner_turn, precision=lax.Precision.HIGHEST)

def project(values, camera):
    turn = camera_rotation(camera[0:3])
    offset = values[0:3] - camera[3:6][:, None]
    in_view = jnp.dot(turn, offset, precision=lax.Precision.HIGHEST)
    inv_depth = 1.0 / in_view[2]
    screen_col = in_view[0] * inv_depth
    screen_row = in_view[1] * inv_depth
    scales = jnp.exp(values[3:6])
    quat = values[6:10] / jnp.sqrt(lax.optimization_barrier(jnp.sum(values[6:10] * values[6:10], axis=0, keepdims=True)))
    quat_w, quat_x, quat_y, quat_z = (quat[0], quat[1], quat[2], quat[3])
    spin = [[1.0 - 2.0 * (quat_y * quat_y + quat_z * quat_z), 2.0 * (quat_x * quat_y - quat_w * quat_z), 2.0 * (quat_x * quat_z + quat_w * quat_y)], [2.0 * (quat_x * quat_y + quat_w * quat_z), 1.0 - 2.0 * (quat_x * quat_x + quat_z * quat_z), 2.0 * (quat_y * quat_z - quat_w * quat_x)], [2.0 * (quat_x * quat_z - quat_w * quat_y), 2.0 * (quat_y * quat_z + quat_w * quat_x), 1.0 - 2.0 * (quat_x * quat_x + quat_y * quat_y)]]
    basis_cam = []
    for outer_index in range(3):
        row_terms = []
        for col_index in range(3):
            entry = turn[outer_index, 0] * spin[0][col_index]
            for mid_index in range(1, 3):
                entry = entry + turn[outer_index, mid_index] * spin[mid_index][col_index]
            row_terms.append(entry * scales[col_index])
        basis_cam.append(row_terms)
    jac_top = [(basis_cam[0][col_index] - screen_col * basis_cam[2][col_index]) * inv_depth for col_index in range(3)]
    jac_low = [(basis_cam[1][col_index] - screen_row * basis_cam[2][col_index]) * inv_depth for col_index in range(3)]
    sigma_a = jac_top[0] * jac_top[0] + jac_top[1] * jac_top[1] + jac_top[2] * jac_top[2]
    sigma_b = jac_top[0] * jac_low[0] + jac_top[1] * jac_low[1] + jac_top[2] * jac_low[2]
    sigma_c = jac_low[0] * jac_low[0] + jac_low[1] * jac_low[1] + jac_low[2] * jac_low[2]
    determinant = sigma_a * sigma_c - sigma_b * sigma_b
    opacity = jax.nn.sigmoid(values[10])
    distance = jnp.sqrt(lax.optimization_barrier(jnp.sum(offset * offset, axis=0)))
    unit_dir = offset / distance
    basis = harmonics(unit_dir[0], unit_dir[1], unit_dir[2])
    coeffs = values[11:59].reshape(16, 3, values.shape[1])
    colors = 0.5 + lax.optimization_barrier(jnp.sum(basis[:, None, :] * coeffs, axis=0))
    screen = jnp.stack([screen_col, screen_row, sigma_c / determinant, -sigma_b / determinant, sigma_a / determinant, opacity])
    return jnp.concatenate([screen, colors], axis=0)

def group_loss(pieces):
    features, live_mask, pixel_column, pixel_row, target_tile = pieces
    entries = live_mask.shape[1]
    delta_col = pixel_column[:, :, None] - features[0][:, None, :]
    delta_row = pixel_row[:, :, None] - features[1][:, None, :]
    power = -0.5 * (features[2][:, None, :] * delta_col * delta_col + 2.0 * features[3][:, None, :] * delta_col * delta_row + features[4][:, None, :] * delta_row * delta_row)
    alphas = features[5][:, None, :] * jnp.exp(power) * live_mask[:, None, :]
    log_keep = jnp.log(1.0 - alphas)
    earlier = (lax.broadcasted_iota(jnp.int32, (entries, entries), 0) < lax.broadcasted_iota(jnp.int32, (entries, entries), 1)).astype(jnp.float32)
    transmit = jnp.exp(jnp.einsum('bpl,lm->bpm', log_keep, earlier, precision=lax.Precision.HIGHEST))
    weights = alphas * transmit
    image = jnp.einsum('bpl,kbl->kbp', weights, features[6:9], precision=lax.Precision.HIGHEST)
    error = image - target_tile
    return jnp.sum(error * error)

def render_tiles(picked, live_mask, pixel_column, pixel_row, target_tile):
    groups = live_mask.shape[0] // 4
    entries = live_mask.shape[1]
    pixels = pixel_column.shape[1]
    stacked = (jnp.transpose(picked.reshape(picked.shape[0], groups, 4, entries), (1, 0, 2, 3)), live_mask.reshape(groups, 4, entries), pixel_column.reshape(groups, 4, pixels), pixel_row.reshape(groups, 4, pixels), jnp.transpose(target_tile.reshape(3, groups, 4, pixels), (1, 0, 2, 3)))
    return jnp.sum(lax.map(jax.checkpoint(group_loss), stacked))

def pixel_grid(first_tile, count, tiles_dev, rows_pix):
    tile_ids = first_tile + jnp.arange(count, dtype=jnp.int32)
    pixel_ids = jnp.arange(256, dtype=jnp.int32)
    block_cols = TILE_COLS // 4
    owner_ids = tile_ids // tiles_dev
    local_ids = tile_ids % tiles_dev
    tile_col = 4 * (owner_ids % block_cols) + local_ids % 4
    tile_row = tiles_dev // 4 * (owner_ids // block_cols) + local_ids // 4
    half_width = TILE_COLS * 8.0
    column = (tile_col[:, None] * 16 + pixel_ids[None, :] % 16).astype(jnp.float32)
    row_pos = (tile_row[:, None] * 16 + pixel_ids[None, :] // 16).astype(jnp.float32)
    return ((column + 0.5 - half_width) / half_width, (row_pos + 0.5 - rows_pix * 0.5) / half_width)

def adam_update(params, first_moment, second_moment, gradient, counts):
    row_ids = lax.broadcasted_iota(jnp.int32, params.shape, 0)
    rates = jnp.where(row_ids < 6, 0.01, jnp.where(row_ids < 10, 0.005, jnp.where(row_ids < 11, 0.05, jnp.where(row_ids < 14, 0.0025, 0.000125))))
    first_new = 0.9 * first_moment + 0.1 * gradient
    second = 0.999 * second_moment + 0.001 * gradient * gradient
    bias_one = 1.0 - 0.9 ** ADAM_STEP
    bias_two = 1.0 - 0.999 ** ADAM_STEP
    stride = rates * (first_new / bias_one) / (jnp.sqrt(second / bias_two) + 1e-08)
    seen_mask = counts > 0.0
    return (jnp.where(seen_mask, params - stride, params), jnp.where(seen_mask, first_new, first_moment), jnp.where(seen_mask, second, second_moment))

def reference(params, first_moment, second_moment, cameras, visible, send_plan, tile_lists, target):
    tiles_all = tile_lists.shape[1]
    tiles_dev = tiles_all // N_CELLS
    capacity = send_plan.shape[3]
    block = params.shape[1] // N_CELLS
    rows_pix = tiles_all // TILE_COLS * 16
    pixel_column, pixel_row = pixel_grid(0, tiles_all, tiles_dev, rows_pix)
    device_of = (jnp.arange(tiles_all, dtype=jnp.int32) // tiles_dev)[:, None]

    def view_loss(values, view_index):
        features = project(values, cameras[view_index])
        lists = tile_lists[view_index]
        live_mask = (lists >= 0).astype(jnp.float32)
        slot_ids = jnp.maximum(lists, 0)
        source = slot_ids // capacity
        column = slot_ids % capacity
        local_row = send_plan[view_index][source, device_of, column]
        global_row = (source * block + jnp.maximum(local_row, 0)).astype(jnp.int32)
        picked = jnp.take(features, global_row, axis=1)
        target_tile = target[view_index].reshape(3, tiles_all, 256)
        return render_tiles(picked, live_mask, pixel_column, pixel_row, target_tile)

    def total_loss(values):
        total = jnp.zeros((), jnp.float32)
        for view_index in range(N_VIEWS):
            total = total + view_loss(values, view_index)
        return total
    gradient = jax.grad(total_loss)(params)
    counts = lax.optimization_barrier(jnp.sum(visible.astype(jnp.float32), axis=0, keepdims=True))
    new_params, new_first, new_second = adam_update(params, first_moment, second_moment, gradient, counts)
    return (new_params, new_first, new_second)
```

```python
import functools

import jax
import jax.numpy as jnp
from jax import lax
from jax.experimental import pallas as pl
from jax.experimental.pallas import tpu as pltpu
from jax.sharding import PartitionSpec as P

TILE_COLS = 32
ADAM_STEP = 1000


harmonic_zero = 0.28209479177387814
harmonic_one = 0.4886025119029199
harmonic_two = (
    1.0925484305920792,
    -1.0925484305920792,
    0.31539156525252005,
    -1.0925484305920792,
    0.5462742152960396,
)
harmonic_three = (
    -0.5900435899266435,
    2.890611442640554,
    -0.4570457994644658,
    0.3731763325901154,
    -0.4570457994644658,
    1.445305721320277,
    -0.5900435899266435,
)


def harmonics(across, upward, onward):
    across_sq = across * across
    upward_sq = upward * upward
    onward_sq = onward * onward
    return jnp.stack(
        [
            harmonic_zero * jnp.ones_like(across),
            -harmonic_one * upward,
            harmonic_one * onward,
            -harmonic_one * across,
            harmonic_two[0] * across * upward,
            harmonic_two[1] * upward * onward,
            harmonic_two[2] * (2.0 * onward_sq - across_sq - upward_sq),
            harmonic_two[3] * across * onward,
            harmonic_two[4] * (across_sq - upward_sq),
            harmonic_three[0] * upward * (3.0 * across_sq - upward_sq),
            harmonic_three[1] * across * upward * onward,
            harmonic_three[2] * upward * (4.0 * onward_sq - across_sq - upward_sq),
            harmonic_three[3] * onward * (2.0 * onward_sq - 3.0 * across_sq - 3.0 * upward_sq),
            harmonic_three[4] * across * (4.0 * onward_sq - across_sq - upward_sq),
            harmonic_three[5] * onward * (across_sq - upward_sq),
            harmonic_three[6] * across * (across_sq - 3.0 * upward_sq),
        ]
    )


def camera_rotation(angles):
    cos_roll, sin_roll = (jnp.cos(angles[0]), jnp.sin(angles[0]))
    cos_pitch, sin_pitch = (jnp.cos(angles[1]), jnp.sin(angles[1]))
    cos_yaw, sin_yaw = (jnp.cos(angles[2]), jnp.sin(angles[2]))
    naught = jnp.zeros_like(cos_roll)
    unit_one = jnp.ones_like(cos_roll)
    roll = jnp.stack(
        [
            jnp.stack([unit_one, naught, naught]),
            jnp.stack([naught, cos_roll, -sin_roll]),
            jnp.stack([naught, sin_roll, cos_roll]),
        ]
    )
    pitch = jnp.stack(
        [
            jnp.stack([cos_pitch, naught, sin_pitch]),
            jnp.stack([naught, unit_one, naught]),
            jnp.stack([-sin_pitch, naught, cos_pitch]),
        ]
    )
    yawing = jnp.stack(
        [
            jnp.stack([cos_yaw, -sin_yaw, naught]),
            jnp.stack([sin_yaw, cos_yaw, naught]),
            jnp.stack([naught, naught, unit_one]),
        ]
    )
    inner_turn = jnp.dot(pitch, roll, precision=lax.Precision.HIGHEST)
    return jnp.dot(yawing, inner_turn, precision=lax.Precision.HIGHEST)


def project(values, camera):
    turn = camera_rotation(camera[0:3])
    offset = values[0:3] - camera[3:6][:, None]
    in_view = jnp.dot(turn, offset, precision=lax.Precision.HIGHEST)
    inv_depth = 1.0 / in_view[2]
    screen_col = in_view[0] * inv_depth
    screen_row = in_view[1] * inv_depth
    scales = jnp.exp(values[3:6])
    quat = values[6:10] / jnp.sqrt(jnp.sum(values[6:10] * values[6:10], axis=0, keepdims=True))
    quat_w, quat_x, quat_y, quat_z = (quat[0], quat[1], quat[2], quat[3])
    spin = [
        [
            1.0 - 2.0 * (quat_y * quat_y + quat_z * quat_z),
            2.0 * (quat_x * quat_y - quat_w * quat_z),
            2.0 * (quat_x * quat_z + quat_w * quat_y),
        ],
        [
            2.0 * (quat_x * quat_y + quat_w * quat_z),
            1.0 - 2.0 * (quat_x * quat_x + quat_z * quat_z),
            2.0 * (quat_y * quat_z - quat_w * quat_x),
        ],
        [
            2.0 * (quat_x * quat_z - quat_w * quat_y),
            2.0 * (quat_y * quat_z + quat_w * quat_x),
            1.0 - 2.0 * (quat_x * quat_x + quat_y * quat_y),
        ],
    ]
    basis_cam = []
    for outer_index in range(3):
        row_terms = []
        for col_index in range(3):
            entry = turn[outer_index, 0] * spin[0][col_index]
            for mid_index in range(1, 3):
                entry = entry + turn[outer_index, mid_index] * spin[mid_index][col_index]
            row_terms.append(entry * scales[col_index])
        basis_cam.append(row_terms)
    jac_top = [
        (basis_cam[0][col_index] - screen_col * basis_cam[2][col_index]) * inv_depth
        for col_index in range(3)
    ]
    jac_low = [
        (basis_cam[1][col_index] - screen_row * basis_cam[2][col_index]) * inv_depth
        for col_index in range(3)
    ]
    sigma_a = jac_top[0] * jac_top[0] + jac_top[1] * jac_top[1] + jac_top[2] * jac_top[2]
    sigma_b = jac_top[0] * jac_low[0] + jac_top[1] * jac_low[1] + jac_top[2] * jac_low[2]
    sigma_c = jac_low[0] * jac_low[0] + jac_low[1] * jac_low[1] + jac_low[2] * jac_low[2]
    determinant = sigma_a * sigma_c - sigma_b * sigma_b
    opacity = jax.nn.sigmoid(values[10])
    distance = jnp.sqrt(jnp.sum(offset * offset, axis=0))
    unit_dir = offset / distance
    basis = harmonics(unit_dir[0], unit_dir[1], unit_dir[2])
    coeffs = values[11:59].reshape(16, 3, values.shape[1])
    colors = 0.5 + jnp.sum(basis[:, None, :] * coeffs, axis=0)
    screen = jnp.stack(
        [
            screen_col,
            screen_row,
            sigma_c / determinant,
            -sigma_b / determinant,
            sigma_a / determinant,
            opacity,
        ]
    )
    return jnp.concatenate([screen, colors], axis=0)


def group_loss(pieces):
    features, live_mask, pixel_column, pixel_row, target_tile = pieces
    entries = live_mask.shape[1]
    delta_col = pixel_column[:, :, None] - features[0][:, None, :]
    delta_row = pixel_row[:, :, None] - features[1][:, None, :]
    power = -0.5 * (
        features[2][:, None, :] * delta_col * delta_col
        + 2.0 * features[3][:, None, :] * delta_col * delta_row
        + features[4][:, None, :] * delta_row * delta_row
    )
    alphas = features[5][:, None, :] * jnp.exp(power) * live_mask[:, None, :]
    log_keep = jnp.log(1.0 - alphas)
    earlier = (
        lax.broadcasted_iota(jnp.int32, (entries, entries), 0)
        < lax.broadcasted_iota(jnp.int32, (entries, entries), 1)
    ).astype(jnp.float32)
    transmit = jnp.exp(
        jnp.einsum("bpl,lm->bpm", log_keep, earlier, precision=lax.Precision.HIGHEST)
    )
    weights = alphas * transmit
    image = jnp.einsum("bpl,kbl->kbp", weights, features[6:9], precision=lax.Precision.HIGHEST)
    error = image - target_tile
    return jnp.sum(error * error)


def render_tiles(picked, live_mask, pixel_column, pixel_row, target_tile):
    groups = live_mask.shape[0] // 4
    entries = live_mask.shape[1]
    pixels = pixel_column.shape[1]
    stacked = (
        jnp.transpose(picked.reshape(picked.shape[0], groups, 4, entries), (1, 0, 2, 3)),
        live_mask.reshape(groups, 4, entries),
        pixel_column.reshape(groups, 4, pixels),
        pixel_row.reshape(groups, 4, pixels),
        jnp.transpose(target_tile.reshape(3, groups, 4, pixels), (1, 0, 2, 3)),
    )
    return jnp.sum(lax.map(jax.checkpoint(group_loss), stacked))


def pixel_grid(first_tile, count, tiles_dev, rows_pix):
    tile_ids = first_tile + jnp.arange(count, dtype=jnp.int32)
    pixel_ids = jnp.arange(256, dtype=jnp.int32)
    block_cols = TILE_COLS // 4
    owner_ids = tile_ids // tiles_dev
    local_ids = tile_ids % tiles_dev
    tile_col = 4 * (owner_ids % block_cols) + local_ids % 4
    tile_row = tiles_dev // 4 * (owner_ids // block_cols) + local_ids // 4
    half_width = TILE_COLS * 8.0
    column = (tile_col[:, None] * 16 + pixel_ids[None, :] % 16).astype(jnp.float32)
    row_pos = (tile_row[:, None] * 16 + pixel_ids[None, :] // 16).astype(jnp.float32)
    return ((column + 0.5 - half_width) / half_width, (row_pos + 0.5 - rows_pix * 0.5) / half_width)


def adam_update(params, first_moment, second_moment, gradient, counts):
    row_ids = lax.broadcasted_iota(jnp.int32, params.shape, 0)
    rates = jnp.where(
        row_ids < 6,
        0.01,
        jnp.where(
            row_ids < 10,
            0.005,
            jnp.where(row_ids < 11, 0.05, jnp.where(row_ids < 14, 0.0025, 0.000125)),
        ),
    )
    first_new = 0.9 * first_moment + 0.1 * gradient
    second = 0.999 * second_moment + 0.001 * gradient * gradient
    bias_one = 1.0 - 0.9**ADAM_STEP
    bias_two = 1.0 - 0.999**ADAM_STEP
    stride = rates * (first_new / bias_one) / (jnp.sqrt(second / bias_two) + 1e-08)
    seen_mask = counts > 0.0
    return (
        jnp.where(seen_mask, params - stride, params),
        jnp.where(seen_mask, first_new, first_moment),
        jnp.where(seen_mask, second, second_moment),
    )


def shards(params, first_moment, second_moment, cameras, visible, send_plan, tile_lists, target):
    cells = lax.axis_size("cells")
    camera = cameras[0]
    plan_rows = send_plan[0, 0]
    capacity = plan_rows.shape[1]
    sent_live = (plan_rows >= 0)[None]
    sent_rows = jnp.maximum(plan_rows, 0)
    lists = tile_lists[0]
    tiles_here = lists.shape[0]
    live_mask = (lists >= 0).astype(jnp.float32)
    slot_ids = jnp.maximum(lists, 0)
    rows_pix = tiles_here * cells // TILE_COLS * 16
    pixel_column, pixel_row = pixel_grid(
        lax.axis_index("cells") * tiles_here, tiles_here, tiles_here, rows_pix
    )
    target_tile = target[0].reshape(3, tiles_here, 256)
    block = params.shape[1]

    def image_loss(table):
        picked = jnp.take(table, slot_ids, axis=1)
        return render_tiles(picked, live_mask, pixel_column, pixel_row, target_tile)

    def own_projection(values):
        return project(values, camera)

    features, project_pull = jax.vjp(own_projection, params)
    outgoing = jnp.take(features, sent_rows, axis=1)
    incoming = lax.all_to_all(outgoing, "cells", split_axis=1, concat_axis=1, tiled=True)
    loss_value, pullback = jax.vjp(
        image_loss, incoming.reshape(features.shape[0], cells * capacity)
    )
    table_grad = pullback(jnp.ones((), jnp.float32))[0]
    returned = lax.all_to_all(
        table_grad.reshape(features.shape[0], cells, capacity),
        "cells",
        split_axis=1,
        concat_axis=1,
        tiled=True,
    )
    kept = jnp.where(sent_live, returned, 0.0)
    gradient = project_pull(
        jnp.zeros((features.shape[0], block), jnp.float32).at[:, sent_rows].add(kept)
    )[0]
    seen_here = visible.astype(jnp.float32)
    total_grad, counts = lax.psum((gradient, seen_here), "views")
    new_params, new_first, new_second = adam_update(
        params, first_moment, second_moment, total_grad, counts
    )
    return (new_params, new_first, new_second)

LANES = 128
PAD_ROWS = 64
FEATS = 9


def project_rows(rows, turn, centre):
    offset = [rows[i] - centre[i] for i in range(3)]
    in_view = [
        turn[i][0] * offset[0] + turn[i][1] * offset[1] + turn[i][2] * offset[2] for i in range(3)
    ]
    inv_depth = 1.0 / in_view[2]
    screen_col = in_view[0] * inv_depth
    screen_row = in_view[1] * inv_depth
    scales = [jnp.exp(rows[3 + i]) for i in range(3)]
    raw = rows[6:10]
    norm = jnp.sqrt(raw[0] * raw[0] + raw[1] * raw[1] + raw[2] * raw[2] + raw[3] * raw[3])
    inv_norm = 1.0 / norm
    quat_w, quat_x, quat_y, quat_z = [item * inv_norm for item in raw]
    spin = [
        [
            1.0 - 2.0 * (quat_y * quat_y + quat_z * quat_z),
            2.0 * (quat_x * quat_y - quat_w * quat_z),
            2.0 * (quat_x * quat_z + quat_w * quat_y),
        ],
        [
            2.0 * (quat_x * quat_y + quat_w * quat_z),
            1.0 - 2.0 * (quat_x * quat_x + quat_z * quat_z),
            2.0 * (quat_y * quat_z - quat_w * quat_x),
        ],
        [
            2.0 * (quat_x * quat_z - quat_w * quat_y),
            2.0 * (quat_y * quat_z + quat_w * quat_x),
            1.0 - 2.0 * (quat_x * quat_x + quat_y * quat_y),
        ],
    ]
    basis_cam = [
        [
            (turn[i][0] * spin[0][j] + turn[i][1] * spin[1][j] + turn[i][2] * spin[2][j])
            * scales[j]
            for j in range(3)
        ]
        for i in range(3)
    ]
    top = [(basis_cam[0][j] - screen_col * basis_cam[2][j]) * inv_depth for j in range(3)]
    low = [(basis_cam[1][j] - screen_row * basis_cam[2][j]) * inv_depth for j in range(3)]
    sigma_a = top[0] * top[0] + top[1] * top[1] + top[2] * top[2]
    sigma_b = top[0] * low[0] + top[1] * low[1] + top[2] * low[2]
    sigma_c = low[0] * low[0] + low[1] * low[1] + low[2] * low[2]
    inv_det = 1.0 / (sigma_a * sigma_c - sigma_b * sigma_b)
    opacity = 1.0 / (1.0 + jnp.exp(-rows[10]))
    inv_dist = 1.0 / jnp.sqrt(offset[0] * offset[0] + offset[1] * offset[1] + offset[2] * offset[2])
    x, y, z = [item * inv_dist for item in offset]
    xx, yy, zz = x * x, y * y, z * z
    basis = [
        None,
        -harmonic_one * y,
        harmonic_one * z,
        -harmonic_one * x,
        harmonic_two[0] * x * y,
        harmonic_two[1] * y * z,
        harmonic_two[2] * (2.0 * zz - xx - yy),
        harmonic_two[3] * x * z,
        harmonic_two[4] * (xx - yy),
        harmonic_three[0] * y * (3.0 * xx - yy),
        harmonic_three[1] * x * y * z,
        harmonic_three[2] * y * (4.0 * zz - xx - yy),
        harmonic_three[3] * z * (2.0 * zz - 3.0 * xx - 3.0 * yy),
        harmonic_three[4] * x * (4.0 * zz - xx - yy),
        harmonic_three[5] * z * (xx - yy),
        harmonic_three[6] * x * (xx - 3.0 * yy),
    ]
    colors = []
    for k in range(3):
        total = harmonic_zero * rows[11 + k]
        for j in range(1, 16):
            total = total + basis[j] * rows[11 + 3 * j + k]
        colors.append(0.5 + total)
    return (
        screen_col,
        screen_row,
        sigma_c * inv_det,
        -sigma_b * inv_det,
        sigma_a * inv_det,
        opacity,
        *colors,
    )


def camera_terms(cam):
    cosines, sines = jnp.cos(cam), jnp.sin(cam)
    cr, cp, cy = [cosines[:, i : i + 1] for i in range(3)]
    sr, sp, sy = [sines[:, i : i + 1] for i in range(3)]
    turn = [
        [cy * cp, cy * sp * sr - sy * cr, cy * sp * cr + sy * sr],
        [sy * cp, sy * sp * sr + cy * cr, sy * sp * cr - cy * sr],
        [-sp, cp * sr, cp * cr],
    ]
    centre = [cam[:, 3 + i : 4 + i] for i in range(3)]
    return turn, centre


def stage_rows(params_ref, staged):
    count, block = params_ref.shape
    for b in range(block // LANES):
        staged[b * PAD_ROWS : b * PAD_ROWS + count, :] = params_ref[:, b * LANES : (b + 1) * LANES]


def lane_pick(source, lanes):
    return jnp.take_along_axis(source, lanes, axis=1, mode="promise_in_bounds")


def gather_eight(load, blocks, index):
    index = jnp.maximum(index, 0)
    lanes, block = index & (LANES - 1), index >> 7
    total = lane_pick(load(0), lanes)
    for b in range(1, blocks):
        total = jnp.where(block == b, lane_pick(load(b), lanes), total)
    return total


def split_three(x):
    first = x.astype(jnp.bfloat16).astype(jnp.float32)
    rest = x - first
    second = rest.astype(jnp.bfloat16).astype(jnp.float32)
    return first, second, rest - second


def scatter_fill(g, index, lhs, hot, start):
    width = g.shape[1]
    parts = jnp.concatenate(split_three(g), axis=0)
    high, low = index >> 7, index & (LANES - 1)
    blocks = lhs.shape[0] // parts.shape[0]
    size = parts.shape[0]
    for b in range(blocks):
        lhs[b * size : (b + 1) * size, pl.ds(start, width)] = jnp.where(
            high == b, parts, 0.0
        ).astype(jnp.bfloat16)
    lane_ids = lax.broadcasted_iota(jnp.int32, (LANES, width), 0)
    hot[:, pl.ds(start, width)] = jnp.where(lane_ids == low, 1.0, 0.0).astype(jnp.bfloat16)


def scatter_finish(lhs, hot):
    out = lax.dot_general(
        lhs[...], hot[...], (((1,), (1,)), ((), ())), preferred_element_type=jnp.float32
    )
    blocks = lhs.shape[0] // 48
    return [
        out[48 * b : 48 * b + 16] + out[48 * b + 16 : 48 * b + 32] + out[48 * b + 32 : 48 * b + 48]
        for b in range(blocks)
    ]


def project_kernel(params_ref, cam_ref, plan_ref, out_ref, staged, table, last, order):
    count, block = params_ref.shape
    blocks = block // LANES
    halves = plan_ref.shape[1] // LANES
    stage_rows(params_ref, staged)
    turn, centre = camera_terms(cam_ref[...])
    for part in range(blocks // 8):
        base = part * 8 * PAD_ROWS
        rows = [staged[pl.ds(base + r, 8, stride=PAD_ROWS), :] for r in range(count)]
        feats = project_rows(rows, turn, centre)
        for f in range(8):
            table[pl.ds(part * 64 + f, 8, stride=8), :] = feats[f]
        last[part * 8 : part * 8 + 8, :] = feats[8]
    slots = plan_ref.shape[0] * halves
    for o in range(slots):
        d, h = divmod(o, halves)
        row = plan_ref[d : d + 1, h * LANES : (h + 1) * LANES]
        order[o : o + 1, :] = row
        out_ref[d, 8 * h : 8 * h + 8, :] = gather_eight(
            lambda b: table[8 * b : 8 * b + 8, :], blocks, jnp.broadcast_to(row, (8, LANES))
        )
    for p in range(slots // 8):
        picked = gather_eight(
            lambda b: jnp.broadcast_to(last[b : b + 1, :], (8, LANES)),
            blocks,
            order[8 * p : 8 * p + 8, :],
        )
        for i in range(8 // halves):
            out_ref[8 // halves * p + i, 8 * halves :, :] = picked[i * halves : (i + 1) * halves]


def render_kernel(
    cells, recv_ref, lists_ref, target_ref, out_ref,
    order, picks, wanted, before, after, alpha_s, trans_s, flow_s, parts_s, pair_s, lhs, hot,
):
    tiles, entries = lists_ref.shape
    owners, packed, _ = recv_ref.shape
    halves = packed // FEATS
    blocks = owners * halves
    quarters = entries // LANES
    me = lax.axis_index("cells")
    rows_pix = tiles * cells // TILE_COLS * 16
    half_width = TILE_COLS * 8.0
    wanted[...] = jnp.transpose(
        jnp.concatenate(
            [target_ref[k] for k in range(3)] + [jnp.zeros((5, target_ref.shape[2]), jnp.float32)],
            axis=0,
        )
    )
    row_ids = lax.broadcasted_iota(jnp.int32, (entries, entries), 0)
    col_ids = lax.broadcasted_iota(jnp.int32, (entries, entries), 1)
    before[...] = jnp.where(row_ids < col_ids, 1.0, 0.0).astype(jnp.bfloat16)
    after[...] = jnp.where(row_ids > col_ids, 1.0, 0.0).astype(jnp.bfloat16)

    def load_main(b):
        s, h = divmod(b, halves)
        return recv_ref[s, 8 * h : 8 * h + 8, :]

    def load_last(b):
        s, h = divmod(b, halves)
        return jnp.broadcast_to(recv_ref[s, 8 * halves + h : 8 * halves + h + 1, :], (8, LANES))

    slots = tiles * quarters
    for o in range(slots):
        t, q = divmod(o, quarters)
        row = lists_ref[t : t + 1, q * LANES : (q + 1) * LANES]
        order[o : o + 1, :] = row
        picks[t, 0:8, q * LANES : (q + 1) * LANES] = gather_eight(
            load_main, blocks, jnp.broadcast_to(row, (8, LANES))
        )
    for p in range(slots // 8):
        picked = gather_eight(load_last, blocks, order[8 * p : 8 * p + 8, :])
        for i in range(8):
            t, q = divmod(8 * p + i, quarters)
            picks[t, 8:9, q * LANES : (q + 1) * LANES] = picked[i : i + 1]

    def one_tile(t, carry):
        def feature(f):
            return picks[t, f : f + 1, :]

        listed = lists_ref[pl.ds(t, 1), :]
        opacity = jnp.where(listed >= 0, feature(5), 0.0)
        tile_col = 4 * lax.rem(me, TILE_COLS // 4) + lax.rem(t, 4)
        tile_row = tiles // 4 * lax.div(me, TILE_COLS // 4) + lax.div(t, 4)
        across = (lax.broadcasted_iota(jnp.int32, (16, entries), 0) + tile_col * 16).astype(jnp.float32)
        delta_col = (across + 0.5 - half_width) * (1.0 / half_width) - feature(0)
        square_term = -0.5 * feature(2) * delta_col * delta_col
        cross_term = -feature(3) * delta_col
        row_scale = -0.5 * feature(4)

        def delta_row_at(r):
            down = (jnp.full((1, entries), tile_row * 16 + r, jnp.int32)).astype(jnp.float32)
            return (down + 0.5 - rows_pix * 0.5) * (1.0 / half_width) - feature(1)

        def put_parts(r, x):
            first = x.astype(jnp.bfloat16)
            parts_s[pl.ds(r * 16, 16), :] = first
            parts_s[pl.ds(256 + r * 16, 16), :] = (x - first.astype(jnp.float32)).astype(jnp.bfloat16)

        def forward(r, carry):
            delta_row = delta_row_at(r)
            power = square_term + cross_term * delta_row + row_scale * delta_row * delta_row
            alpha = opacity * jnp.exp(power)
            alpha_s[pl.ds(r * 16, 16), :] = alpha
            put_parts(r, jnp.log(1.0 - alpha))
            return carry

        lax.fori_loop(0, 16, forward, 0, unroll=4)
        sums = jnp.dot(parts_s[...], before[...], preferred_element_type=jnp.float32)
        trans_s[...] = jnp.exp(sums[0:256] + sums[256:512])

        def errors_of(r, carry):
            weight = alpha_s[pl.ds(r * 16, 16), :] * trans_s[pl.ds(r * 16, 16), :]
            where = pl.ds(t * 256 + r * 16, 16)
            values = [jnp.sum(weight * feature(6 + k), axis=1, keepdims=True) for k in range(3)]
            lane = lax.broadcasted_iota(jnp.int32, (16, 8), 1)
            image = jnp.where(lane == 0, values[0], jnp.where(lane == 1, values[1], values[2]))
            wanted[where, :] = 2.0 * (image - wanted[where, :])
            return carry

        lax.fori_loop(0, 16, errors_of, 0, unroll=8)

        def colors_of(r, carry):
            weight = alpha_s[pl.ds(r * 16, 16), :] * trans_s[pl.ds(r * 16, 16), :]
            errors = wanted[pl.ds(t * 256 + r * 16, 16), :]
            slope = 0.0
            sums = []
            for k in range(3):
                error = errors[:, k : k + 1]
                slope = slope + error * feature(6 + k)
                sums.append(carry[k] + error * weight)
            flow = weight * slope
            flow_s[pl.ds(r * 16, 16), :] = flow
            put_parts(r, flow)
            return tuple(sums)

        empty = jnp.zeros((16, entries), jnp.float32)
        color_sums = lax.fori_loop(0, 16, colors_of, (empty, empty, empty), unroll=4)
        sums = jnp.dot(parts_s[...], after[...], preferred_element_type=jnp.float32)
        trans_s[...] = sums[0:256] + sums[256:512]

        def backward(r, carry):
            delta_row = delta_row_at(r)
            alpha = alpha_s[pl.ds(r * 16, 16), :]
            slope = flow_s[pl.ds(r * 16, 16), :] - alpha / (1.0 - alpha) * trans_s[pl.ds(r * 16, 16), :]
            return (
                carry[0] + slope,
                carry[1] + slope * delta_row,
                carry[2] + slope * (delta_row * delta_row),
            )

        plain, tilted, bent = lax.fori_loop(0, 16, backward, (empty, empty, empty), unroll=4)

        def fold(x):
            return jnp.sum(x, axis=0, keepdims=True)

        moved = plain * delta_col
        pair_s[...] = jnp.concatenate(
            [
                fold(plain),
                fold(moved),
                fold(tilted),
                fold(moved * delta_col),
                fold(tilted * delta_col),
                fold(bent),
                fold(color_sums[0]),
                fold(color_sums[1]),
                fold(color_sums[2]),
                jnp.zeros((7, entries), jnp.float32),
            ],
            axis=0,
        )
        scatter_fill(pair_s[...], listed, lhs, hot, pl.multiple_of(t * entries, entries))
        return carry

    lax.fori_loop(0, tiles, one_tile, 0)
    for b, piece in enumerate(scatter_finish(lhs, hot)):
        s, h = divmod(b, halves)
        out_ref[s, 8 * h : 8 * h + 8, :] = piece[0:8]
        out_ref[s, 8 * halves + h : 8 * halves + h + 1, :] = piece[8:9]


def owner_rows(back_ref, plan_ref, out_ref, lhs, hot, spread):
    devices, packed, _ = back_ref.shape
    halves = packed // FEATS
    for d in range(devices):
        main = jnp.concatenate([back_ref[d, 8 * h : 8 * h + 8, :] for h in range(halves)], axis=1)
        last = jnp.concatenate(
            [back_ref[d, 8 * halves + h : 8 * halves + h + 1, :] for h in range(halves)], axis=1
        )
        g = jnp.concatenate([main, last, jnp.zeros((7, halves * LANES), jnp.float32)], axis=0)
        scatter_fill(g, plan_ref[d : d + 1, :], lhs, hot, d * halves * LANES)
    pieces = scatter_finish(lhs, hot)
    blocks = len(pieces)
    for b, piece in enumerate(pieces):
        spread[16 * b : 16 * b + 16, :] = piece
    for f in range(FEATS):
        out_ref[f * blocks : (f + 1) * blocks, :] = spread[pl.ds(f, blocks, stride=16), :]


def main_kernel(
    params_ref, cam_ref, plan_ref, visible_ref, lists_ref, target_ref, shared_ref,
    staged, table, last, plan_order, outgoing, incoming, back, returned, mine, extra,
    order, picks, wanted, before, after, alpha_s, trans_s, flow_s, parts_s, pair_s, lhs, hot,
    own_lhs, own_hot, spread,
    send_one, recv_one, send_two, recv_two, send_three, recv_three, send_four, recv_four, local_sem,
):
    cells, views = lax.axis_size("cells"), lax.axis_size("views")
    cell, view = lax.axis_index("cells"), lax.axis_index("views")
    blocks = params_ref.shape[1] // LANES
    grads = FEATS * blocks
    barrier = pltpu.get_barrier_semaphore()

    def greet(axis, me, size):
        for k in range(1, size):
            pl.semaphore_signal(
                barrier,
                inc=1,
                device_id={axis: lax.rem(me + k, size)},
                device_id_type=pl.DeviceIdType.MESH,
            )

    def send_all(axis, me, size, source, dest, send_sem, recv_sem):
        copies = []
        for k in range(1, size):
            peer = lax.rem(me + k, size)
            copy = pltpu.make_async_remote_copy(
                src_ref=source(peer),
                dst_ref=dest(me),
                send_sem=send_sem.at[k - 1],
                recv_sem=recv_sem.at[k - 1],
                device_id={axis: peer},
                device_id_type=pl.DeviceIdType.MESH,
            )
            copy.start()
            copies.append(copy)
        return copies

    greet("cells", cell, cells)
    greet("views", view, views)
    for b in range(blocks):
        extra[b : b + 1, :] = visible_ref[:, b * LANES : (b + 1) * LANES].astype(jnp.float32)
    extra[blocks : blocks + 8, :] = jnp.broadcast_to(
        jnp.concatenate([cam_ref[...], jnp.zeros((1, LANES - 6), jnp.float32)], axis=1), (8, LANES)
    )
    project_kernel(params_ref, cam_ref, plan_ref, outgoing, staged, table, last, plan_order)
    pl.semaphore_wait(barrier, cells + views - 2)

    first = send_all(
        "cells", cell, cells, lambda p: outgoing.at[p], lambda p: incoming.at[p], send_one, recv_one
    )
    keep = pltpu.make_async_copy(outgoing.at[cell], incoming.at[cell], local_sem.at[0])
    keep.start()
    fourth = send_all(
        "views", view, views,
        lambda p: extra, lambda p: shared_ref.at[p, grads : grads + blocks + 8, :],
        send_four, recv_four,
    )
    keep_extra = pltpu.make_async_copy(
        extra, shared_ref.at[view, grads : grads + blocks + 8, :], local_sem.at[1]
    )
    keep_extra.start()
    keep.wait()
    for copy in first:
        copy.wait()
    render_kernel(
        cells, incoming, lists_ref, target_ref, back,
        order, picks, wanted, before, after, alpha_s, trans_s, flow_s, parts_s, pair_s, lhs, hot,
    )
    second = send_all(
        "cells", cell, cells, lambda p: back.at[p], lambda p: returned.at[p], send_two, recv_two
    )
    keep = pltpu.make_async_copy(back.at[cell], returned.at[cell], local_sem.at[2])
    keep.start()
    keep.wait()
    for copy in second:
        copy.wait()
    owner_rows(returned, plan_ref, mine, own_lhs, own_hot, spread)
    third = send_all(
        "views", view, views,
        lambda p: mine, lambda p: shared_ref.at[p, 0:grads, :],
        send_three, recv_three,
    )
    keep = pltpu.make_async_copy(mine, shared_ref.at[view, 0:grads, :], local_sem.at[3])
    keep.start()
    keep.wait()
    keep_extra.wait()
    for copy in fourth:
        copy.wait()
    for copy in third:
        copy.wait()


def update_kernel(params_ref, first_ref, second_ref, shared_ref, new_ref, new_first_ref, new_second_ref, staged, grads):
    count, block = params_ref.shape
    blocks = block // LANES
    views = shared_ref.shape[0]
    stage_rows(params_ref, staged)
    grads[...] = jnp.zeros_like(grads)

    def one_part(step, carry):
        part, view = lax.div(step, views), lax.rem(step, views)
        base = part * (8 * PAD_ROWS)
        start = pl.multiple_of(part * 8, 8)
        cam = shared_ref[view, (FEATS + 1) * blocks : (FEATS + 1) * blocks + 1, :]
        turn, centre = camera_terms(cam)
        rows = tuple(staged[pl.ds(base + r, 8, stride=PAD_ROWS), :] for r in range(count))
        feats, pull = jax.vjp(lambda *items: project_rows(items, turn, centre), *rows)
        got = [shared_ref[view, pl.ds(f * blocks + start, 8), :] for f in range(FEATS)]
        slopes = (
            feats[2] * got[1] + feats[3] * got[2],
            feats[3] * got[1] + feats[4] * got[2],
            -0.5 * got[3],
            -got[4],
            -0.5 * got[5],
            got[0] / feats[5],
            got[6],
            got[7],
            got[8],
        )
        for r, item in enumerate(pull(slopes)):
            where = pl.ds(base + r, 8, stride=PAD_ROWS)
            grads[where, :] = grads[where, :] + item
        return carry

    lax.fori_loop(0, blocks // 8 * views, one_part, 0)
    row_ids = lax.broadcasted_iota(jnp.int32, (count, LANES), 0)
    rates = jnp.where(
        row_ids < 6,
        0.01,
        jnp.where(
            row_ids < 10,
            0.005,
            jnp.where(row_ids < 11, 0.05, jnp.where(row_ids < 14, 0.0025, 0.000125)),
        ),
    )
    bias_one = 1.0 - 0.9**ADAM_STEP
    bias_two = 1.0 - 0.999**ADAM_STEP
    for b in range(blocks):
        span = slice(b * LANES, (b + 1) * LANES)
        gradient = grads[b * PAD_ROWS : b * PAD_ROWS + count, :]
        params, first, second = params_ref[:, span], first_ref[:, span], second_ref[:, span]
        counts = shared_ref[0, FEATS * blocks + b : FEATS * blocks + b + 1, :]
        for view in range(1, views):
            counts = counts + shared_ref[view, FEATS * blocks + b : FEATS * blocks + b + 1, :]
        seen = jnp.broadcast_to(counts, params.shape) > 0.0
        first_new = 0.9 * first + 0.1 * gradient
        second_new = 0.999 * second + 0.001 * gradient * gradient
        stride = rates * (first_new / bias_one) / (jnp.sqrt(second_new / bias_two) + 1e-08)
        new_ref[:, span] = jnp.where(seen, params - stride, params)
        new_first_ref[:, span] = jnp.where(seen, first_new, first)
        new_second_ref[:, span] = jnp.where(seen, second_new, second)


def fused_shards(params, first_moment, second_moment, cameras, visible, send_plan, tile_lists, target):
    cells, views = lax.axis_size("cells"), lax.axis_size("views")
    count, block = params.shape
    blocks = block // LANES
    plan = send_plan[0, 0]
    lists = tile_lists[0]
    tiles, entries = lists.shape
    halves = plan.shape[1] // LANES
    slots = cells * halves
    f32, bf16 = jnp.float32, jnp.bfloat16
    packet = pltpu.VMEM((cells, FEATS * halves, LANES), f32)
    dma = pltpu.SemaphoreType.DMA
    shared = pl.pallas_call(
        main_kernel,
        out_shape=jax.ShapeDtypeStruct((views, (FEATS + 1) * blocks + 8, LANES), f32),
        out_specs=pl.BlockSpec(memory_space=pltpu.VMEM),
        scratch_shapes=[
            pltpu.VMEM((blocks * PAD_ROWS, LANES), f32),
            pltpu.VMEM((blocks * 8, LANES), f32),
            pltpu.VMEM((blocks, LANES), f32),
            pltpu.VMEM((slots, LANES), jnp.int32),
            packet, packet, packet, packet,
            pltpu.VMEM((FEATS * blocks, LANES), f32),
            pltpu.VMEM((blocks + 8, LANES), f32),
            pltpu.VMEM((tiles * entries // LANES, LANES), jnp.int32),
            pltpu.VMEM((tiles, 16, entries), f32),
            pltpu.VMEM((tiles * 256, 8), f32),
            pltpu.VMEM((entries, entries), bf16),
            pltpu.VMEM((entries, entries), bf16),
            pltpu.VMEM((256, entries), f32),
            pltpu.VMEM((256, entries), f32),
            pltpu.VMEM((256, entries), f32),
            pltpu.VMEM((512, entries), bf16),
            pltpu.VMEM((16, entries), f32),
            pltpu.VMEM((slots * 48, tiles * entries), bf16),
            pltpu.VMEM((LANES, tiles * entries), bf16),
            pltpu.VMEM((blocks * 48, slots * LANES), bf16),
            pltpu.VMEM((LANES, slots * LANES), bf16),
            pltpu.VMEM((blocks * 16, LANES), f32),
            dma((cells - 1,)), dma((cells - 1,)), dma((cells - 1,)), dma((cells - 1,)),
            dma((views - 1,)), dma((views - 1,)), dma((views - 1,)), dma((views - 1,)),
            dma((4,)),
        ],
        compiler_params=pltpu.CompilerParams(collective_id=0, has_side_effects=True),
    )(params, cameras, plan, visible, lists, jnp.transpose(target, (1, 0, 2)))
    like = jax.ShapeDtypeStruct(params.shape, f32)
    return tuple(
        pl.pallas_call(
            update_kernel,
            out_shape=(like, like, like),
            scratch_shapes=[
                pltpu.VMEM((blocks * PAD_ROWS, LANES), f32),
                pltpu.VMEM((blocks * PAD_ROWS, LANES), f32),
            ],
        )(params, first_moment, second_moment, shared)
    )


def local_shards(params, first_moment, second_moment, cameras, visible, send_plan, tile_lists, target):
    capacity = send_plan.shape[3]
    tiles, entries = tile_lists.shape[1:]
    halves = capacity // LANES
    fits = (
        capacity % LANES == 0
        and params.shape[1] % (8 * LANES) == 0
        and entries % LANES == 0
        and 8 % max(halves, 1) == 0
        and lax.axis_size("cells") * halves % 8 == 0
        and tiles * entries // LANES % 8 == 0
        and tiles * entries <= 4096
        and tiles % 4 == 0
    )
    body = fused_shards if fits else shards
    return body(params, first_moment, second_moment, cameras, visible, send_plan, tile_lists, target)


def solution(mesh):
    in_specs = (
        P(None, "cells"),
        P(None, "cells"),
        P(None, "cells"),
        P("views", None),
        P("views", "cells"),
        P("views", "cells", None, None),
        P("views", "cells", None),
        P("views", None, "cells"),
    )
    out_specs = (P(None, "cells"), P(None, "cells"), P(None, "cells"))
    return jax.shard_map(local_shards, mesh=mesh, in_specs=in_specs, out_specs=out_specs, check_vma=False)
```

```python
import functools

import jax
import jax.numpy as jnp
from jax import lax
from jax.experimental import pallas as pl
from jax.experimental.pallas import tpu as pltpu
from jax.sharding import PartitionSpec as P

TILE_COLS = 32
ADAM_STEP = 1000


harmonic_zero = 0.28209479177387814
harmonic_one = 0.4886025119029199
harmonic_two = (
    1.0925484305920792,
    -1.0925484305920792,
    0.31539156525252005,
    -1.0925484305920792,
    0.5462742152960396,
)
harmonic_three = (
    -0.5900435899266435,
    2.890611442640554,
    -0.4570457994644658,
    0.3731763325901154,
    -0.4570457994644658,
    1.445305721320277,
    -0.5900435899266435,
)


def harmonics(across, upward, onward):
    across_sq = across * across
    upward_sq = upward * upward
    onward_sq = onward * onward
    return jnp.stack(
        [
            harmonic_zero * jnp.ones_like(across),
            -harmonic_one * upward,
            harmonic_one * onward,
            -harmonic_one * across,
            harmonic_two[0] * across * upward,
            harmonic_two[1] * upward * onward,
            harmonic_two[2] * (2.0 * onward_sq - across_sq - upward_sq),
            harmonic_two[3] * across * onward,
            harmonic_two[4] * (across_sq - upward_sq),
            harmonic_three[0] * upward * (3.0 * across_sq - upward_sq),
            harmonic_three[1] * across * upward * onward,
            harmonic_three[2] * upward * (4.0 * onward_sq - across_sq - upward_sq),
            harmonic_three[3] * onward * (2.0 * onward_sq - 3.0 * across_sq - 3.0 * upward_sq),
            harmonic_three[4] * across * (4.0 * onward_sq - across_sq - upward_sq),
            harmonic_three[5] * onward * (across_sq - upward_sq),
            harmonic_three[6] * across * (across_sq - 3.0 * upward_sq),
        ]
    )


def camera_rotation(angles):
    cos_roll, sin_roll = (jnp.cos(angles[0]), jnp.sin(angles[0]))
    cos_pitch, sin_pitch = (jnp.cos(angles[1]), jnp.sin(angles[1]))
    cos_yaw, sin_yaw = (jnp.cos(angles[2]), jnp.sin(angles[2]))
    naught = jnp.zeros_like(cos_roll)
    unit_one = jnp.ones_like(cos_roll)
    roll = jnp.stack(
        [
            jnp.stack([unit_one, naught, naught]),
            jnp.stack([naught, cos_roll, -sin_roll]),
            jnp.stack([naught, sin_roll, cos_roll]),
        ]
    )
    pitch = jnp.stack(
        [
            jnp.stack([cos_pitch, naught, sin_pitch]),
            jnp.stack([naught, unit_one, naught]),
            jnp.stack([-sin_pitch, naught, cos_pitch]),
        ]
    )
    yawing = jnp.stack(
        [
            jnp.stack([cos_yaw, -sin_yaw, naught]),
            jnp.stack([sin_yaw, cos_yaw, naught]),
            jnp.stack([naught, naught, unit_one]),
        ]
    )
    inner_turn = jnp.dot(pitch, roll, precision=lax.Precision.HIGHEST)
    return jnp.dot(yawing, inner_turn, precision=lax.Precision.HIGHEST)


def project(values, camera):
    turn = camera_rotation(camera[0:3])
    offset = values[0:3] - camera[3:6][:, None]
    in_view = jnp.dot(turn, offset, precision=lax.Precision.HIGHEST)
    inv_depth = 1.0 / in_view[2]
    screen_col = in_view[0] * inv_depth
    screen_row = in_view[1] * inv_depth
    scales = jnp.exp(values[3:6])
    quat = values[6:10] / jnp.sqrt(jnp.sum(values[6:10] * values[6:10], axis=0, keepdims=True))
    quat_w, quat_x, quat_y, quat_z = (quat[0], quat[1], quat[2], quat[3])
    spin = [
        [
            1.0 - 2.0 * (quat_y * quat_y + quat_z * quat_z),
            2.0 * (quat_x * quat_y - quat_w * quat_z),
            2.0 * (quat_x * quat_z + quat_w * quat_y),
        ],
        [
            2.0 * (quat_x * quat_y + quat_w * quat_z),
            1.0 - 2.0 * (quat_x * quat_x + quat_z * quat_z),
            2.0 * (quat_y * quat_z - quat_w * quat_x),
        ],
        [
            2.0 * (quat_x * quat_z - quat_w * quat_y),
            2.0 * (quat_y * quat_z + quat_w * quat_x),
            1.0 - 2.0 * (quat_x * quat_x + quat_y * quat_y),
        ],
    ]
    basis_cam = []
    for outer_index in range(3):
        row_terms = []
        for col_index in range(3):
            entry = turn[outer_index, 0] * spin[0][col_index]
            for mid_index in range(1, 3):
                entry = entry + turn[outer_index, mid_index] * spin[mid_index][col_index]
            row_terms.append(entry * scales[col_index])
        basis_cam.append(row_terms)
    jac_top = [
        (basis_cam[0][col_index] - screen_col * basis_cam[2][col_index]) * inv_depth
        for col_index in range(3)
    ]
    jac_low = [
        (basis_cam[1][col_index] - screen_row * basis_cam[2][col_index]) * inv_depth
        for col_index in range(3)
    ]
    sigma_a = jac_top[0] * jac_top[0] + jac_top[1] * jac_top[1] + jac_top[2] * jac_top[2]
    sigma_b = jac_top[0] * jac_low[0] + jac_top[1] * jac_low[1] + jac_top[2] * jac_low[2]
    sigma_c = jac_low[0] * jac_low[0] + jac_low[1] * jac_low[1] + jac_low[2] * jac_low[2]
    determinant = sigma_a * sigma_c - sigma_b * sigma_b
    opacity = jax.nn.sigmoid(values[10])
    distance = jnp.sqrt(jnp.sum(offset * offset, axis=0))
    unit_dir = offset / distance
    basis = harmonics(unit_dir[0], unit_dir[1], unit_dir[2])
    coeffs = values[11:59].reshape(16, 3, values.shape[1])
    colors = 0.5 + jnp.sum(basis[:, None, :] * coeffs, axis=0)
    screen = jnp.stack(
        [
            screen_col,
            screen_row,
            sigma_c / determinant,
            -sigma_b / determinant,
            sigma_a / determinant,
            opacity,
        ]
    )
    return jnp.concatenate([screen, colors], axis=0)


def group_loss(pieces):
    features, live_mask, pixel_column, pixel_row, target_tile = pieces
    entries = live_mask.shape[1]
    delta_col = pixel_column[:, :, None] - features[0][:, None, :]
    delta_row = pixel_row[:, :, None] - features[1][:, None, :]
    power = -0.5 * (
        features[2][:, None, :] * delta_col * delta_col
        + 2.0 * features[3][:, None, :] * delta_col * delta_row
        + features[4][:, None, :] * delta_row * delta_row
    )
    alphas = features[5][:, None, :] * jnp.exp(power) * live_mask[:, None, :]
    log_keep = jnp.log(1.0 - alphas)
    earlier = (
        lax.broadcasted_iota(jnp.int32, (entries, entries), 0)
        < lax.broadcasted_iota(jnp.int32, (entries, entries), 1)
    ).astype(jnp.float32)
    transmit = jnp.exp(
        jnp.einsum("bpl,lm->bpm", log_keep, earlier, precision=lax.Precision.HIGHEST)
    )
    weights = alphas * transmit
    image = jnp.einsum("bpl,kbl->kbp", weights, features[6:9], precision=lax.Precision.HIGHEST)
    error = image - target_tile
    return jnp.sum(error * error)


def render_tiles(picked, live_mask, pixel_column, pixel_row, target_tile):
    groups = live_mask.shape[0] // 4
    entries = live_mask.shape[1]
    pixels = pixel_column.shape[1]
    stacked = (
        jnp.transpose(picked.reshape(picked.shape[0], groups, 4, entries), (1, 0, 2, 3)),
        live_mask.reshape(groups, 4, entries),
        pixel_column.reshape(groups, 4, pixels),
        pixel_row.reshape(groups, 4, pixels),
        jnp.transpose(target_tile.reshape(3, groups, 4, pixels), (1, 0, 2, 3)),
    )
    return jnp.sum(lax.map(jax.checkpoint(group_loss), stacked))


def pixel_grid(first_tile, count, tiles_dev, rows_pix):
    tile_ids = first_tile + jnp.arange(count, dtype=jnp.int32)
    pixel_ids = jnp.arange(256, dtype=jnp.int32)
    block_cols = TILE_COLS // 4
    owner_ids = tile_ids // tiles_dev
    local_ids = tile_ids % tiles_dev
    tile_col = 4 * (owner_ids % block_cols) + local_ids % 4
    tile_row = tiles_dev // 4 * (owner_ids // block_cols) + local_ids // 4
    half_width = TILE_COLS * 8.0
    column = (tile_col[:, None] * 16 + pixel_ids[None, :] % 16).astype(jnp.float32)
    row_pos = (tile_row[:, None] * 16 + pixel_ids[None, :] // 16).astype(jnp.float32)
    return ((column + 0.5 - half_width) / half_width, (row_pos + 0.5 - rows_pix * 0.5) / half_width)


def adam_update(params, first_moment, second_moment, gradient, counts):
    row_ids = lax.broadcasted_iota(jnp.int32, params.shape, 0)
    rates = jnp.where(
        row_ids < 6,
        0.01,
        jnp.where(
            row_ids < 10,
            0.005,
            jnp.where(row_ids < 11, 0.05, jnp.where(row_ids < 14, 0.0025, 0.000125)),
        ),
    )
    first_new = 0.9 * first_moment + 0.1 * gradient
    second = 0.999 * second_moment + 0.001 * gradient * gradient
    bias_one = 1.0 - 0.9**ADAM_STEP
    bias_two = 1.0 - 0.999**ADAM_STEP
    stride = rates * (first_new / bias_one) / (jnp.sqrt(second / bias_two) + 1e-08)
    seen_mask = counts > 0.0
    return (
        jnp.where(seen_mask, params - stride, params),
        jnp.where(seen_mask, first_new, first_moment),
        jnp.where(seen_mask, second, second_moment),
    )


def shards(params, first_moment, second_moment, cameras, visible, send_plan, tile_lists, target):
    cells = lax.axis_size("cells")
    camera = cameras[0]
    plan_rows = send_plan[0, 0]
    capacity = plan_rows.shape[1]
    sent_live = (plan_rows >= 0)[None]
    sent_rows = jnp.maximum(plan_rows, 0)
    lists = tile_lists[0]
    tiles_here = lists.shape[0]
    live_mask = (lists >= 0).astype(jnp.float32)
    slot_ids = jnp.maximum(lists, 0)
    rows_pix = tiles_here * cells // TILE_COLS * 16
    pixel_column, pixel_row = pixel_grid(
        lax.axis_index("cells") * tiles_here, tiles_here, tiles_here, rows_pix
    )
    target_tile = target[0].reshape(3, tiles_here, 256)
    block = params.shape[1]

    def image_loss(table):
        picked = jnp.take(table, slot_ids, axis=1)
        return render_tiles(picked, live_mask, pixel_column, pixel_row, target_tile)

    def own_projection(values):
        return project(values, camera)

    features, project_pull = jax.vjp(own_projection, params)
    outgoing = jnp.take(features, sent_rows, axis=1)
    incoming = lax.all_to_all(outgoing, "cells", split_axis=1, concat_axis=1, tiled=True)
    loss_value, pullback = jax.vjp(
        image_loss, incoming.reshape(features.shape[0], cells * capacity)
    )
    table_grad = pullback(jnp.ones((), jnp.float32))[0]
    returned = lax.all_to_all(
        table_grad.reshape(features.shape[0], cells, capacity),
        "cells",
        split_axis=1,
        concat_axis=1,
        tiled=True,
    )
    kept = jnp.where(sent_live, returned, 0.0)
    gradient = project_pull(
        jnp.zeros((features.shape[0], block), jnp.float32).at[:, sent_rows].add(kept)
    )[0]
    seen_here = visible.astype(jnp.float32)
    total_grad, counts = lax.psum((gradient, seen_here), "views")
    new_params, new_first, new_second = adam_update(
        params, first_moment, second_moment, total_grad, counts
    )
    return (new_params, new_first, new_second)

LANES = 128
PAD_ROWS = 64
FEATS = 9


def project_rows(rows, turn, centre):
    offset = [rows[i] - centre[i] for i in range(3)]
    in_view = [
        turn[i][0] * offset[0] + turn[i][1] * offset[1] + turn[i][2] * offset[2] for i in range(3)
    ]
    inv_depth = 1.0 / in_view[2]
    screen_col = in_view[0] * inv_depth
    screen_row = in_view[1] * inv_depth
    scales = [jnp.exp(rows[3 + i]) for i in range(3)]
    raw = rows[6:10]
    norm = jnp.sqrt(raw[0] * raw[0] + raw[1] * raw[1] + raw[2] * raw[2] + raw[3] * raw[3])
    inv_norm = 1.0 / norm
    quat_w, quat_x, quat_y, quat_z = [item * inv_norm for item in raw]
    spin = [
        [
            1.0 - 2.0 * (quat_y * quat_y + quat_z * quat_z),
            2.0 * (quat_x * quat_y - quat_w * quat_z),
            2.0 * (quat_x * quat_z + quat_w * quat_y),
        ],
        [
            2.0 * (quat_x * quat_y + quat_w * quat_z),
            1.0 - 2.0 * (quat_x * quat_x + quat_z * quat_z),
            2.0 * (quat_y * quat_z - quat_w * quat_x),
        ],
        [
            2.0 * (quat_x * quat_z - quat_w * quat_y),
            2.0 * (quat_y * quat_z + quat_w * quat_x),
            1.0 - 2.0 * (quat_x * quat_x + quat_y * quat_y),
        ],
    ]
    basis_cam = [
        [
            (turn[i][0] * spin[0][j] + turn[i][1] * spin[1][j] + turn[i][2] * spin[2][j])
            * scales[j]
            for j in range(3)
        ]
        for i in range(3)
    ]
    top = [(basis_cam[0][j] - screen_col * basis_cam[2][j]) * inv_depth for j in range(3)]
    low = [(basis_cam[1][j] - screen_row * basis_cam[2][j]) * inv_depth for j in range(3)]
    sigma_a = top[0] * top[0] + top[1] * top[1] + top[2] * top[2]
    sigma_b = top[0] * low[0] + top[1] * low[1] + top[2] * low[2]
    sigma_c = low[0] * low[0] + low[1] * low[1] + low[2] * low[2]
    inv_det = 1.0 / (sigma_a * sigma_c - sigma_b * sigma_b)
    opacity = 1.0 / (1.0 + jnp.exp(-rows[10]))
    inv_dist = 1.0 / jnp.sqrt(offset[0] * offset[0] + offset[1] * offset[1] + offset[2] * offset[2])
    x, y, z = [item * inv_dist for item in offset]
    xx, yy, zz = x * x, y * y, z * z
    basis = [
        None,
        -harmonic_one * y,
        harmonic_one * z,
        -harmonic_one * x,
        harmonic_two[0] * x * y,
        harmonic_two[1] * y * z,
        harmonic_two[2] * (2.0 * zz - xx - yy),
        harmonic_two[3] * x * z,
        harmonic_two[4] * (xx - yy),
        harmonic_three[0] * y * (3.0 * xx - yy),
        harmonic_three[1] * x * y * z,
        harmonic_three[2] * y * (4.0 * zz - xx - yy),
        harmonic_three[3] * z * (2.0 * zz - 3.0 * xx - 3.0 * yy),
        harmonic_three[4] * x * (4.0 * zz - xx - yy),
        harmonic_three[5] * z * (xx - yy),
        harmonic_three[6] * x * (xx - 3.0 * yy),
    ]
    colors = []
    for k in range(3):
        total = harmonic_zero * rows[11 + k]
        for j in range(1, 16):
            total = total + basis[j] * rows[11 + 3 * j + k]
        colors.append(0.5 + total)
    return (
        screen_col,
        screen_row,
        sigma_c * inv_det,
        -sigma_b * inv_det,
        sigma_a * inv_det,
        opacity,
        *colors,
    )


def camera_terms(cam):
    cosines, sines = jnp.cos(cam), jnp.sin(cam)
    cr, cp, cy = [cosines[:, i : i + 1] for i in range(3)]
    sr, sp, sy = [sines[:, i : i + 1] for i in range(3)]
    turn = [
        [cy * cp, cy * sp * sr - sy * cr, cy * sp * cr + sy * sr],
        [sy * cp, sy * sp * sr + cy * cr, sy * sp * cr - cy * sr],
        [-sp, cp * sr, cp * cr],
    ]
    centre = [cam[:, 3 + i : 4 + i] for i in range(3)]
    return turn, centre

def fill_dense(params_ref, dense):
    count, block = params_ref.shape
    for b in range(block // LANES):
        part, line = divmod(b, 8)
        for r in range(0, count, 8):
            size = min(8, count - r)
            where = pl.ds((part * PAD_ROWS + r) * 8 + line, size, stride=8)
            dense[where, :] = params_ref[r : r + size, b * LANES : (b + 1) * LANES]


def dense_rows(dense, part, count):
    return [
        dense[pl.ds(pl.multiple_of((part * PAD_ROWS + r) * 8, 8), 8), :] for r in range(count)
    ]


def lane_pick(source, lanes):
    return jnp.take_along_axis(source, lanes, axis=1, mode="promise_in_bounds")


def gather_eight(load, blocks, index):
    index = jnp.maximum(index, 0)
    lanes, block = index & (LANES - 1), index >> 7
    total = lane_pick(load(0), lanes)
    for b in range(1, blocks):
        total = jnp.where(block == b, lane_pick(load(b), lanes), total)
    return total


def split_three(x):
    first = x.astype(jnp.bfloat16).astype(jnp.float32)
    rest = x - first
    second = rest.astype(jnp.bfloat16).astype(jnp.float32)
    return first, second, rest - second


def fill_hot(hot, index, start, bits):
    row_ids = lax.broadcasted_iota(jnp.int32, (hot.shape[0], LANES), 0)
    low = index & ((1 << bits) - 1)
    hot[:, start : start + LANES] = jnp.where(row_ids == low, 1.0, 0.0).astype(jnp.bfloat16)


def fill_values(lhs, main, last, index, start, bits):
    parts = jnp.concatenate(
        [*split_three(main), *split_three(last), jnp.zeros((5, LANES), jnp.float32)], axis=0
    )
    high = jnp.broadcast_to(index >> bits, parts.shape)
    for b in range(lhs.shape[0] // 32):
        lhs[32 * b : 32 * b + 32, pl.ds(start, LANES)] = jnp.where(high == b, parts, 0.0).astype(
            jnp.bfloat16
        )


def scatter_finish(lhs, hot):
    out = lax.dot_general(
        lhs[...], hot[...], (((1,), (1,)), ((), ())), preferred_element_type=jnp.float32
    )
    pieces = []
    for b in range(lhs.shape[0] // 32):
        rows = out[32 * b : 32 * b + 32]
        pieces.append(
            (rows[0:8] + rows[8:16] + rows[16:24], rows[24:25] + rows[25:26] + rows[26:27])
        )
    return pieces


def send_features(feat_parts, plan_ref, out_ref, table, last, order):
    halves = plan_ref.shape[1] // LANES
    blocks = last.shape[0]
    for part, feats in enumerate(feat_parts):
        for f in range(8):
            table[pl.ds(part * 64 + f, 8, stride=8), :] = feats[f]
        last[part * 8 : part * 8 + 8, :] = feats[8]
    slots = plan_ref.shape[0] * halves
    for o in range(slots):
        d, h = divmod(o, halves)
        row = plan_ref[d : d + 1, h * LANES : (h + 1) * LANES]
        order[o : o + 1, :] = row
        out_ref[d, 8 * h : 8 * h + 8, :] = gather_eight(
            lambda b: table[8 * b : 8 * b + 8, :], blocks, jnp.broadcast_to(row, (8, LANES))
        )
    for p in range(slots // 8):
        picked = gather_eight(
            lambda b: jnp.broadcast_to(last[b : b + 1, :], (8, LANES)),
            blocks,
            order[8 * p : 8 * p + 8, :],
        )
        for i in range(8 // halves):
            out_ref[8 // halves * p + i, 8 * halves :, :] = picked[i * halves : (i + 1) * halves]


def pixel_terms():
    lane = lax.broadcasted_iota(jnp.int32, (8, LANES), 1)
    inner = lane & 31
    tile = lane >> 5
    x = (inner & 15).astype(jnp.float32) - 7.5
    step = (inner >> 4).astype(jnp.float32) - 0.5
    return tile, x, step


def render_setup(lists_ref, target_ref, order, wanted, basis, slopes, hot, bits):
    tiles, entries = lists_ref.shape
    quarters = entries // LANES
    for q in range(quarters):
        order[q * tiles : (q + 1) * tiles, :] = lists_ref[:, q * LANES : (q + 1) * LANES]
    sub = lax.broadcasted_iota(jnp.int32, (8, LANES), 0)
    lane = lax.broadcasted_iota(jnp.int32, (8, LANES), 1)
    tile, x, step = pixel_terms()
    shifted = 32 * (sub & 3) + (lane & 31)
    for k in range(3):
        total = jnp.zeros((8, LANES), jnp.float32)
        for r in range(8):
            row = jnp.broadcast_to(target_ref[k, :, r * LANES : (r + 1) * LANES], (8, LANES))
            here = (tile == r // 2) & ((sub >> 2) == r % 2)
            total = jnp.where(here, lane_pick(row, shifted), total)
        wanted[8 * k : 8 * k + 8, :] = total
    for g in range(LANES // 8):
        row = sub + 8 * g
        coef = (row * 43) >> 9
        mine = tile == (row & 3)

        def column(j, *terms):
            total = jnp.zeros((8, LANES), jnp.float32)
            for c, value in terms:
                total = jnp.where(coef == c, value, total)
            total = jnp.where(mine, total, 0.0)
            basis[8 * g : 8 * g + 8, j * LANES : (j + 1) * LANES] = total

        column(0, (0, x * x), (1, x * step), (2, step * step), (3, x), (4, step), (5, 1.0))
        column(1, (1, x), (2, 2.0 * step), (4, 1.0))
        column(2, (2, 1.0))
        for k in range(3):
            column(3 + k, (6 + k, 1.0))
    mine = tile == (sub & 3)
    blank = jnp.zeros((LANES, LANES), jnp.bfloat16)
    for s in range(8):
        y = step + (2.0 * s - 7.0)
        rows = [jnp.ones_like(x), x, y, x * x, x * y, y * y]
        rows = jnp.concatenate(
            [jnp.where(mine, item, 0.0) for item in rows] + [jnp.zeros((80, LANES), jnp.float32)],
            axis=0,
        ).astype(jnp.bfloat16)
        for part in range(2):
            start = (part * 8 + s) * 2 * LANES
            slopes[:, start : start + LANES] = rows
            slopes[:, start + LANES : start + 2 * LANES] = blank
    for o in range(tiles * quarters):
        fill_hot(hot, order[o : o + 1, :], o * LANES, bits)


def render_rest(
    cells, recv_ref, order, wanted, back_ref,
    coefs, tables, basis, alpha_s, weight_s, slope_s, joint, slopes, moved, pairs, lhs, hot, bits,
):
    owners, packed, _ = recv_ref.shape
    halves = packed // FEATS
    blocks = owners * halves
    tiles = 4
    quarters = order.shape[0] // tiles
    entries = quarters * LANES
    me = lax.axis_index("cells")
    rows_pix = tiles * cells // TILE_COLS * 16
    half_width = TILE_COLS * 8.0
    inv_width = 1.0 / half_width
    log_two = 1.4426950408889634
    sub = lax.broadcasted_iota(jnp.int32, (8, LANES), 0)
    local = sub & 3
    tile_col = 4 * lax.rem(me, TILE_COLS // 4) + local
    tile_row = lax.div(me, TILE_COLS // 4)
    centre_col = (16 * tile_col + 8).astype(jnp.float32) - half_width
    centre_row = (jnp.full((8, LANES), 16 * tile_row + 8, jnp.int32)).astype(
        jnp.float32
    ) - rows_pix * 0.5

    def load(f):
        def get(b):
            s, h = divmod(b, halves)
            r = 8 * h + f if f < 8 else 8 * halves + h
            return jnp.broadcast_to(recv_ref[s, r : r + 1, :], (8, LANES))

        return get

    for p in range(quarters // 2):
        index = order[8 * p : 8 * p + 8, :]
        feats = [gather_eight(load(f), blocks, index) for f in range(FEATS)]
        off_col = feats[0] * half_width - centre_col
        off_row = feats[1] * half_width - centre_row
        moved[16 * p : 16 * p + 8, :] = off_col
        moved[16 * p + 8 : 16 * p + 16, :] = off_row
        square = feats[2] * (-0.5 * log_two * inv_width * inv_width)
        cross = feats[3] * (-log_two * inv_width * inv_width)
        bend = feats[4] * (-0.5 * log_two * inv_width * inv_width)
        faint = jnp.maximum(jnp.log(feats[5]) * log_two, -1e30)
        along = square * off_col + cross * off_row
        level = along * off_col + bend * off_row * off_row + jnp.where(index >= 0, faint, -1e30)
        terms = [
            square,
            cross,
            bend,
            -(along + square * off_col),
            -(2.0 * bend * off_row + cross * off_col),
            level,
            feats[6],
            feats[7],
            feats[8],
        ]
        for c, term in enumerate(terms):
            for i, piece in enumerate(split_three(term)):
                row = (3 * c + i) * tiles
                for q in range(2):
                    start = (2 * p + q) * LANES
                    coefs[start + row : start + row + tiles, :] = piece[4 * q : 4 * q + 4]
    for q in range(quarters):
        coefs[q * LANES + 108 : (q + 1) * LANES, :] = jnp.zeros((LANES - 108, LANES), jnp.float32)
    weights = basis[...].astype(jnp.bfloat16)
    for q in range(quarters):
        span = slice(q * LANES, (q + 1) * LANES)
        turned = jnp.transpose(coefs[span, :]).astype(jnp.bfloat16)
        result = jnp.dot(turned, weights, preferred_element_type=jnp.float32)
        for j in range(6):
            tables[j, span, :] = result[:, j * LANES : (j + 1) * LANES]

    height = (2 * sub - 7).astype(jnp.float32)

    def table(l, j):
        return jnp.broadcast_to(tables[j, pl.ds(l, 1), :], (8, LANES))

    def forward(l, carry):
        trans, red, green, blue = carry
        power = table(l, 0) + height * (table(l, 1) + height * table(l, 2))
        alpha = jnp.exp2(power)
        weight = alpha * trans
        where = pl.ds(pl.multiple_of(l * 8, 8), 8)
        alpha_s[where, :] = alpha
        weight_s[where, :] = weight
        return (
            trans * (1.0 - alpha),
            red + weight * table(l, 3),
            green + weight * table(l, 4),
            blue + weight * table(l, 5),
        )

    zero = jnp.zeros((8, LANES), jnp.float32)
    _, red, green, blue = lax.fori_loop(
        0, entries, forward, (jnp.ones((8, LANES), jnp.float32), zero, zero, zero), unroll=16
    )
    errors = [2.0 * (item - wanted[8 * k : 8 * k + 8, :]) for k, item in enumerate((red, green, blue))]
    wanted[0:8, :], wanted[8:16, :], wanted[16:24, :] = errors
    tile, _, _ = pixel_terms()
    mine = tile == local
    for s in range(8):
        tops, lows = [], []
        for k in range(3):
            row = jnp.broadcast_to(wanted[8 * k + s : 8 * k + s + 1, :], (8, LANES))
            row = jnp.where(mine, row, 0.0)
            top = row.astype(jnp.bfloat16).astype(jnp.float32)
            tops.append(top)
            lows.append(row - top)
        tops = jnp.concatenate(tops + lows, axis=0).astype(jnp.bfloat16)
        start = s * 2 * LANES + LANES
        slopes[48:96, start : start + LANES] = tops
        start = start + 16 * LANES
        slopes[48:72, start : start + LANES] = tops[0:24]

    def backward(i, behind):
        l = entries - 1 - i
        where = pl.ds(pl.multiple_of(l * 8, 8), 8)
        slope = errors[0] * table(l, 3) + errors[1] * table(l, 4) + errors[2] * table(l, 5)
        above = slope - behind
        slope_s[where, :] = weight_s[where, :] * above
        return behind + alpha_s[where, :] * above

    lax.fori_loop(0, entries, backward, zero, unroll=16)

    def relay(c, carry):
        rows = pl.ds(pl.multiple_of(c * 16, 16), 16)
        for s in range(8):
            for part, source in enumerate((slope_s, weight_s)):
                item = source[pl.ds(c * 128 + s, 16, stride=8), :]
                top = item.astype(jnp.bfloat16)
                start = s * 2 * LANES + part * LANES
                joint[rows, start : start + LANES] = top
                start = start + 16 * LANES
                joint[rows, start : start + LANES] = (item - top.astype(jnp.float32)).astype(
                    jnp.bfloat16
                )
        return carry

    lax.fori_loop(0, entries // 16, relay, 0, unroll=2)
    sums = lax.dot_general(
        joint[...], slopes[...], (((1,), (1,)), ((), ())), preferred_element_type=jnp.float32
    )
    turned = [jnp.transpose(sums[q * LANES : (q + 1) * LANES]) for q in range(quarters)]
    for p in range(quarters // 2):
        off_col = moved[16 * p : 16 * p + 8, :]
        off_row = moved[16 * p + 8 : 16 * p + 16, :]

        def quantity(j):
            span = slice(8 * j, 8 * j + 8)
            return jnp.where(sub < 4, turned[2 * p][span], turned[2 * p + 1][span])

        plain, across, down = quantity(0), quantity(1), quantity(2)
        near_col = across - off_col * plain
        near_row = down - off_row * plain
        rows = [
            plain,
            near_col * inv_width,
            near_row * inv_width,
            (quantity(3) - off_col * (across + near_col)) * (inv_width * inv_width),
            (quantity(4) - off_col * down - off_row * near_col) * (inv_width * inv_width),
            (quantity(5) - off_row * (down + near_row)) * (inv_width * inv_width),
            *[quantity(6 + k) + quantity(9 + k) for k in range(3)],
        ]
        for f, item in enumerate(rows):
            pairs[pl.ds(p * 128 + f, 8, stride=16), :] = item
    for o in range(tiles * quarters):
        fill_values(
            lhs,
            pairs[o * 16 : o * 16 + 8, :],
            pairs[o * 16 + 8 : o * 16 + 9, :],
            order[o : o + 1, :],
            o * LANES,
            bits,
        )
    for s, (main, last) in enumerate(scatter_finish(lhs, hot)):
        for h in range(halves):
            span = slice(h * LANES, (h + 1) * LANES)
            back_ref[s, 8 * h : 8 * h + 8, :] = main[:, span]
            back_ref[s, 8 * halves + h : 8 * halves + h + 1, :] = last[:, span]


def main_kernel(
    params_ref, cam_ref, plan_ref, visible_ref, lists_ref, target_ref, out_ref,
    held, dense, table, last, plan_order, outgoing, incoming, back, returned, mine, extra, extras, shared,
    order, wanted, basis, coefs, tables, alpha_s, weight_s, slope_s, joint, slopes, moved, pairs,
    lhs, hot, own_lhs, own_hot,
    send_one, recv_one, send_two, recv_two, send_three, recv_three, send_four, recv_four, local_sem,
):
    cells, views = lax.axis_size("cells"), lax.axis_size("views")
    cell, view = lax.axis_index("cells"), lax.axis_index("views")
    count, block = params_ref.shape
    blocks = block // LANES
    capacity = plan_ref.shape[1]
    halves = capacity // LANES
    bits = capacity.bit_length() - 1
    fetch = pltpu.make_async_copy(params_ref, held, local_sem.at[0])
    fetch.start()
    barrier = pltpu.get_barrier_semaphore()

    def greet(axis, me, size):
        for k in range(1, size):
            pl.semaphore_signal(
                barrier,
                inc=1,
                device_id={axis: lax.rem(me + k, size)},
                device_id_type=pl.DeviceIdType.MESH,
            )

    def send_all(axis, me, size, source, dest, send_sem, recv_sem):
        copies = []
        for k in range(1, size):
            peer = lax.rem(me + k, size)
            copy = pltpu.make_async_remote_copy(
                src_ref=source(peer),
                dst_ref=dest(me),
                send_sem=send_sem.at[k - 1],
                recv_sem=recv_sem.at[k - 1],
                device_id={axis: peer},
                device_id_type=pl.DeviceIdType.MESH,
            )
            copy.start()
            copies.append(copy)
        return copies

    greet("cells", cell, cells)
    greet("views", view, views)
    for b in range(blocks):
        extra[b : b + 1, :] = visible_ref[:, b * LANES : (b + 1) * LANES].astype(jnp.float32)
    turn, centre = camera_terms(cam_ref[...])
    known = [*turn[0], *turn[1], *turn[2], *centre]
    lane = lax.broadcasted_iota(jnp.int32, (8, LANES), 1)
    line = jnp.zeros((8, LANES), jnp.float32)
    for i, item in enumerate(known):
        line = jnp.where(lane == i, jnp.broadcast_to(item, (8, LANES)), line)
    extra[blocks : blocks + 8, :] = line
    fetch.wait()
    fill_dense(held, dense)
    feat_parts = [
        project_rows(dense_rows(dense, part, count), turn, centre) for part in range(blocks // 8)
    ]
    send_features(feat_parts, plan_ref, outgoing, table, last, plan_order)
    pl.semaphore_wait(barrier, cells + views - 2)

    first = send_all(
        "cells", cell, cells, lambda p: outgoing.at[p], lambda p: incoming.at[p], send_one, recv_one
    )
    fourth = send_all(
        "views", view, views, lambda p: extra, lambda p: extras.at[p], send_four, recv_four
    )
    incoming[cell] = outgoing[cell]
    extras[view] = extra[...]
    render_setup(lists_ref, target_ref, order, wanted, basis, slopes, hot, bits)
    for copy in first:
        copy.wait()
    render_rest(
        cells, incoming, order, wanted, back,
        coefs, tables, basis, alpha_s, weight_s, slope_s, joint, slopes, moved, pairs, lhs, hot, bits,
    )
    second = send_all(
        "cells", cell, cells, lambda p: back.at[p], lambda p: returned.at[p], send_two, recv_two
    )
    returned[cell] = back[cell]
    wide = own_hot.shape[0].bit_length() - 1
    for o in range(cells * halves):
        d, h = divmod(o, halves)
        fill_hot(own_hot, plan_ref[d : d + 1, h * LANES : (h + 1) * LANES], o * LANES, wide)
    for copy in second:
        copy.wait()
    for o in range(cells * halves):
        d, h = divmod(o, halves)
        fill_values(
            own_lhs,
            returned[d, 8 * h : 8 * h + 8, :],
            returned[d, 8 * halves + h : 8 * halves + h + 1, :],
            plan_ref[d : d + 1, h * LANES : (h + 1) * LANES],
            o * LANES,
            wide,
        )
    for g, (main, tip) in enumerate(scatter_finish(own_lhs, own_hot)):
        for i in range(2):
            span = slice(i * LANES, (i + 1) * LANES)
            for f in range(8):
                mine[f * blocks + 2 * g + i : f * blocks + 2 * g + i + 1, :] = main[f : f + 1, span]
            mine[8 * blocks + 2 * g + i : 8 * blocks + 2 * g + i + 1, :] = tip[:, span]
    third = send_all(
        "views", view, views, lambda p: mine, lambda p: shared.at[p], send_three, recv_three
    )
    for copy in fourth:
        copy.wait()
    counts = extras[0, 0:blocks, :]
    for v in range(1, views):
        counts = counts + extras[v, 0:blocks, :]
    grads = blocks * PAD_ROWS
    out_ref[grads : grads + blocks, :] = counts

    def pull_view(fresh, source, lines):
        known = [jnp.broadcast_to(lines[:, i : i + 1], (8, LANES)) for i in range(12)]
        turn = [known[0:3], known[3:6], known[6:9]]
        centre = known[9:12]

        def one_part(part, carry):
            rows = dense_rows(dense, part, count)
            feats, pull = jax.vjp(lambda *items: project_rows(items, turn, centre), *rows)
            got = [
                source[pl.ds(pl.multiple_of(f * blocks + part * 8, 8), 8), :] for f in range(FEATS)
            ]
            wanted_slopes = (
                feats[2] * got[1] + feats[3] * got[2],
                feats[3] * got[1] + feats[4] * got[2],
                -0.5 * got[3],
                -got[4],
                -0.5 * got[5],
                got[0] / feats[5],
                got[6],
                got[7],
                got[8],
            )
            for r, item in enumerate(pull(wanted_slopes)):
                where = pl.ds(pl.multiple_of((part * PAD_ROWS + r) * 8, 8), 8)
                out_ref[where, :] = item if fresh else out_ref[where, :] + item
            return carry

        lax.fori_loop(0, blocks // 8, one_part, 0)

    pull_view(True, mine, extra[blocks : blocks + 1, :])
    for k in range(1, views):
        third[views - 1 - k].wait()
        origin = lax.rem(view + k, views)
        pull_view(False, shared.at[origin], extras[origin, blocks : blocks + 1, :])


def update_kernel(params_ref, first_ref, second_ref, grads_ref, new_ref, new_first_ref, new_second_ref):
    count, block = params_ref.shape
    blocks = block // LANES
    row_ids = lax.broadcasted_iota(jnp.int32, (8, LANES), 0)
    bias_one = 1.0 - 0.9**ADAM_STEP
    bias_two = 1.0 - 0.999**ADAM_STEP
    for b in range(blocks):
        span = slice(b * LANES, (b + 1) * LANES)
        part, line = divmod(b, 8)
        counts = grads_ref[blocks * PAD_ROWS + b : blocks * PAD_ROWS + b + 1, :]
        for r in range(0, count, 8):
            size = min(8, count - r)
            rows = slice(r, r + size)
            gradient = grads_ref[pl.ds((part * PAD_ROWS + r) * 8 + line, size, stride=8), :]
            if r >= 16:
                rates = 0.000125
            else:
                ids = row_ids[0:size] + r
                rates = jnp.where(
                    ids < 6,
                    0.01,
                    jnp.where(
                        ids < 10,
                        0.005,
                        jnp.where(ids < 11, 0.05, jnp.where(ids < 14, 0.0025, 0.000125)),
                    ),
                )
            params, first, second = params_ref[rows, span], first_ref[rows, span], second_ref[rows, span]
            seen = jnp.broadcast_to(counts, params.shape) > 0.0
            first_new = 0.9 * first + 0.1 * gradient
            second_new = 0.999 * second + 0.001 * gradient * gradient
            stride = rates * (first_new / bias_one) / (jnp.sqrt(second_new / bias_two) + 1e-08)
            new_ref[rows, span] = jnp.where(seen, params - stride, params)
            new_first_ref[rows, span] = jnp.where(seen, first_new, first)
            new_second_ref[rows, span] = jnp.where(seen, second_new, second)


def fused_shards(params, first_moment, second_moment, cameras, visible, send_plan, tile_lists, target):
    cells, views = lax.axis_size("cells"), lax.axis_size("views")
    count, block = params.shape
    blocks = block // LANES
    plan = send_plan[0, 0]
    lists = tile_lists[0]
    tiles, entries = lists.shape
    capacity = plan.shape[1]
    halves = capacity // LANES
    slots = cells * halves
    f32, bf16 = jnp.float32, jnp.bfloat16
    packet = pltpu.VMEM((cells, FEATS * halves, LANES), f32)
    dma = pltpu.SemaphoreType.DMA
    vmem = pl.BlockSpec(memory_space=pltpu.VMEM)
    grads = pl.pallas_call(
        main_kernel,
        out_shape=jax.ShapeDtypeStruct((blocks * PAD_ROWS + blocks, LANES), f32),
        in_specs=[pl.BlockSpec(memory_space=pl.ANY), vmem, vmem, vmem, vmem, vmem],
        out_specs=vmem,
        scratch_shapes=[
            pltpu.VMEM((count, block), f32),
            pltpu.VMEM((blocks * PAD_ROWS, LANES), f32),
            pltpu.VMEM((blocks * 8, LANES), f32),
            pltpu.VMEM((blocks, LANES), f32),
            pltpu.VMEM((slots, LANES), jnp.int32),
            packet, packet, packet, packet,
            pltpu.VMEM((FEATS * blocks, LANES), f32),
            pltpu.VMEM((blocks + 8, LANES), f32),
            pltpu.VMEM((views, blocks + 8, LANES), f32),
            pltpu.VMEM((views, FEATS * blocks, LANES), f32),
            pltpu.VMEM((tiles * entries // LANES, LANES), jnp.int32),
            pltpu.VMEM((24, LANES), f32),
            pltpu.VMEM((LANES, 6 * LANES), f32),
            pltpu.VMEM((entries, LANES), f32),
            pltpu.VMEM((6, entries, LANES), f32),
            pltpu.VMEM((entries * 8, LANES), f32),
            pltpu.VMEM((entries * 8, LANES), f32),
            pltpu.VMEM((entries * 8, LANES), f32),
            pltpu.VMEM((entries, 32 * LANES), bf16),
            pltpu.VMEM((LANES, 32 * LANES), bf16),
            pltpu.VMEM((entries // LANES * 8, LANES), f32),
            pltpu.VMEM((tiles * entries // LANES * 16, LANES), f32),
            pltpu.VMEM((cells * 32, tiles * entries), bf16),
            pltpu.VMEM((capacity, tiles * entries), bf16),
            pltpu.VMEM((blocks // 2 * 32, slots * LANES), bf16),
            pltpu.VMEM((2 * LANES, slots * LANES), bf16),
            dma((cells - 1,)), dma((cells - 1,)), dma((cells - 1,)), dma((cells - 1,)),
            dma((views - 1,)), dma((views - 1,)), dma((views - 1,)), dma((views - 1,)),
            dma((1,)),
        ],
        compiler_params=pltpu.CompilerParams(collective_id=0, has_side_effects=True),
    )(params, cameras, plan, visible, lists, jnp.transpose(target, (1, 0, 2)))
    like = jax.ShapeDtypeStruct(params.shape, f32)
    return tuple(
        pl.pallas_call(update_kernel, out_shape=(like, like, like))(
            params, first_moment, second_moment, grads
        )
    )


def local_shards(params, first_moment, second_moment, cameras, visible, send_plan, tile_lists, target):
    capacity = send_plan.shape[3]
    tiles, entries = tile_lists.shape[1:]
    halves = capacity // LANES
    fits = (
        capacity % LANES == 0
        and params.shape[1] % (8 * LANES) == 0
        and entries % (2 * LANES) == 0
        and 8 % max(halves, 1) == 0
        and lax.axis_size("cells") * halves % 8 == 0
        and tiles * entries <= 4096
        and tiles == 4
    )
    body = fused_shards if fits else shards
    return body(params, first_moment, second_moment, cameras, visible, send_plan, tile_lists, target)


def solution(mesh):
    in_specs = (
        P(None, "cells"),
        P(None, "cells"),
        P(None, "cells"),
        P("views", None),
        P("views", "cells"),
        P("views", "cells", None, None),
        P("views", "cells", None),
        P("views", None, "cells"),
    )
    out_specs = (P(None, "cells"), P(None, "cells"), P(None, "cells"))
    return jax.shard_map(local_shards, mesh=mesh, in_specs=in_specs, out_specs=out_specs, check_vma=False)
```

```python
import functools

import jax
import jax.numpy as jnp
from jax import lax
from jax.experimental import pallas as pl
from jax.experimental.pallas import tpu as pltpu
from jax.sharding import PartitionSpec as P

TILE_COLS = 32
ADAM_STEP = 1000


harmonic_zero = 0.28209479177387814
harmonic_one = 0.4886025119029199
harmonic_two = (
    1.0925484305920792,
    -1.0925484305920792,
    0.31539156525252005,
    -1.0925484305920792,
    0.5462742152960396,
)
harmonic_three = (
    -0.5900435899266435,
    2.890611442640554,
    -0.4570457994644658,
    0.3731763325901154,
    -0.4570457994644658,
    1.445305721320277,
    -0.5900435899266435,
)


def harmonics(across, upward, onward):
    across_sq = across * across
    upward_sq = upward * upward
    onward_sq = onward * onward
    return jnp.stack(
        [
            harmonic_zero * jnp.ones_like(across),
            -harmonic_one * upward,
            harmonic_one * onward,
            -harmonic_one * across,
            harmonic_two[0] * across * upward,
            harmonic_two[1] * upward * onward,
            harmonic_two[2] * (2.0 * onward_sq - across_sq - upward_sq),
            harmonic_two[3] * across * onward,
            harmonic_two[4] * (across_sq - upward_sq),
            harmonic_three[0] * upward * (3.0 * across_sq - upward_sq),
            harmonic_three[1] * across * upward * onward,
            harmonic_three[2] * upward * (4.0 * onward_sq - across_sq - upward_sq),
            harmonic_three[3] * onward * (2.0 * onward_sq - 3.0 * across_sq - 3.0 * upward_sq),
            harmonic_three[4] * across * (4.0 * onward_sq - across_sq - upward_sq),
            harmonic_three[5] * onward * (across_sq - upward_sq),
            harmonic_three[6] * across * (across_sq - 3.0 * upward_sq),
        ]
    )


def camera_rotation(angles):
    cos_roll, sin_roll = (jnp.cos(angles[0]), jnp.sin(angles[0]))
    cos_pitch, sin_pitch = (jnp.cos(angles[1]), jnp.sin(angles[1]))
    cos_yaw, sin_yaw = (jnp.cos(angles[2]), jnp.sin(angles[2]))
    naught = jnp.zeros_like(cos_roll)
    unit_one = jnp.ones_like(cos_roll)
    roll = jnp.stack(
        [
            jnp.stack([unit_one, naught, naught]),
            jnp.stack([naught, cos_roll, -sin_roll]),
            jnp.stack([naught, sin_roll, cos_roll]),
        ]
    )
    pitch = jnp.stack(
        [
            jnp.stack([cos_pitch, naught, sin_pitch]),
            jnp.stack([naught, unit_one, naught]),
            jnp.stack([-sin_pitch, naught, cos_pitch]),
        ]
    )
    yawing = jnp.stack(
        [
            jnp.stack([cos_yaw, -sin_yaw, naught]),
            jnp.stack([sin_yaw, cos_yaw, naught]),
            jnp.stack([naught, naught, unit_one]),
        ]
    )
    inner_turn = jnp.dot(pitch, roll, precision=lax.Precision.HIGHEST)
    return jnp.dot(yawing, inner_turn, precision=lax.Precision.HIGHEST)


def project(values, camera):
    turn = camera_rotation(camera[0:3])
    offset = values[0:3] - camera[3:6][:, None]
    in_view = jnp.dot(turn, offset, precision=lax.Precision.HIGHEST)
    inv_depth = 1.0 / in_view[2]
    screen_col = in_view[0] * inv_depth
    screen_row = in_view[1] * inv_depth
    scales = jnp.exp(values[3:6])
    quat = values[6:10] / jnp.sqrt(jnp.sum(values[6:10] * values[6:10], axis=0, keepdims=True))
    quat_w, quat_x, quat_y, quat_z = (quat[0], quat[1], quat[2], quat[3])
    spin = [
        [
            1.0 - 2.0 * (quat_y * quat_y + quat_z * quat_z),
            2.0 * (quat_x * quat_y - quat_w * quat_z),
            2.0 * (quat_x * quat_z + quat_w * quat_y),
        ],
        [
            2.0 * (quat_x * quat_y + quat_w * quat_z),
            1.0 - 2.0 * (quat_x * quat_x + quat_z * quat_z),
            2.0 * (quat_y * quat_z - quat_w * quat_x),
        ],
        [
            2.0 * (quat_x * quat_z - quat_w * quat_y),
            2.0 * (quat_y * quat_z + quat_w * quat_x),
            1.0 - 2.0 * (quat_x * quat_x + quat_y * quat_y),
        ],
    ]
    basis_cam = []
    for outer_index in range(3):
        row_terms = []
        for col_index in range(3):
            entry = turn[outer_index, 0] * spin[0][col_index]
            for mid_index in range(1, 3):
                entry = entry + turn[outer_index, mid_index] * spin[mid_index][col_index]
            row_terms.append(entry * scales[col_index])
        basis_cam.append(row_terms)
    jac_top = [
        (basis_cam[0][col_index] - screen_col * basis_cam[2][col_index]) * inv_depth
        for col_index in range(3)
    ]
    jac_low = [
        (basis_cam[1][col_index] - screen_row * basis_cam[2][col_index]) * inv_depth
        for col_index in range(3)
    ]
    sigma_a = jac_top[0] * jac_top[0] + jac_top[1] * jac_top[1] + jac_top[2] * jac_top[2]
    sigma_b = jac_top[0] * jac_low[0] + jac_top[1] * jac_low[1] + jac_top[2] * jac_low[2]
    sigma_c = jac_low[0] * jac_low[0] + jac_low[1] * jac_low[1] + jac_low[2] * jac_low[2]
    determinant = sigma_a * sigma_c - sigma_b * sigma_b
    opacity = jax.nn.sigmoid(values[10])
    distance = jnp.sqrt(jnp.sum(offset * offset, axis=0))
    unit_dir = offset / distance
    basis = harmonics(unit_dir[0], unit_dir[1], unit_dir[2])
    coeffs = values[11:59].reshape(16, 3, values.shape[1])
    colors = 0.5 + jnp.sum(basis[:, None, :] * coeffs, axis=0)
    screen = jnp.stack(
        [
            screen_col,
            screen_row,
            sigma_c / determinant,
            -sigma_b / determinant,
            sigma_a / determinant,
            opacity,
        ]
    )
    return jnp.concatenate([screen, colors], axis=0)


def group_loss(pieces):
    features, live_mask, pixel_column, pixel_row, target_tile = pieces
    entries = live_mask.shape[1]
    delta_col = pixel_column[:, :, None] - features[0][:, None, :]
    delta_row = pixel_row[:, :, None] - features[1][:, None, :]
    power = -0.5 * (
        features[2][:, None, :] * delta_col * delta_col
        + 2.0 * features[3][:, None, :] * delta_col * delta_row
        + features[4][:, None, :] * delta_row * delta_row
    )
    alphas = features[5][:, None, :] * jnp.exp(power) * live_mask[:, None, :]
    log_keep = jnp.log(1.0 - alphas)
    earlier = (
        lax.broadcasted_iota(jnp.int32, (entries, entries), 0)
        < lax.broadcasted_iota(jnp.int32, (entries, entries), 1)
    ).astype(jnp.float32)
    transmit = jnp.exp(
        jnp.einsum("bpl,lm->bpm", log_keep, earlier, precision=lax.Precision.HIGHEST)
    )
    weights = alphas * transmit
    image = jnp.einsum("bpl,kbl->kbp", weights, features[6:9], precision=lax.Precision.HIGHEST)
    error = image - target_tile
    return jnp.sum(error * error)


def render_tiles(picked, live_mask, pixel_column, pixel_row, target_tile):
    groups = live_mask.shape[0] // 4
    entries = live_mask.shape[1]
    pixels = pixel_column.shape[1]
    stacked = (
        jnp.transpose(picked.reshape(picked.shape[0], groups, 4, entries), (1, 0, 2, 3)),
        live_mask.reshape(groups, 4, entries),
        pixel_column.reshape(groups, 4, pixels),
        pixel_row.reshape(groups, 4, pixels),
        jnp.transpose(target_tile.reshape(3, groups, 4, pixels), (1, 0, 2, 3)),
    )
    return jnp.sum(lax.map(jax.checkpoint(group_loss), stacked))


def pixel_grid(first_tile, count, tiles_dev, rows_pix):
    tile_ids = first_tile + jnp.arange(count, dtype=jnp.int32)
    pixel_ids = jnp.arange(256, dtype=jnp.int32)
    block_cols = TILE_COLS // 4
    owner_ids = tile_ids // tiles_dev
    local_ids = tile_ids % tiles_dev
    tile_col = 4 * (owner_ids % block_cols) + local_ids % 4
    tile_row = tiles_dev // 4 * (owner_ids // block_cols) + local_ids // 4
    half_width = TILE_COLS * 8.0
    column = (tile_col[:, None] * 16 + pixel_ids[None, :] % 16).astype(jnp.float32)
    row_pos = (tile_row[:, None] * 16 + pixel_ids[None, :] // 16).astype(jnp.float32)
    return ((column + 0.5 - half_width) / half_width, (row_pos + 0.5 - rows_pix * 0.5) / half_width)


def adam_update(params, first_moment, second_moment, gradient, counts):
    row_ids = lax.broadcasted_iota(jnp.int32, params.shape, 0)
    rates = jnp.where(
        row_ids < 6,
        0.01,
        jnp.where(
            row_ids < 10,
            0.005,
            jnp.where(row_ids < 11, 0.05, jnp.where(row_ids < 14, 0.0025, 0.000125)),
        ),
    )
    first_new = 0.9 * first_moment + 0.1 * gradient
    second = 0.999 * second_moment + 0.001 * gradient * gradient
    bias_one = 1.0 - 0.9**ADAM_STEP
    bias_two = 1.0 - 0.999**ADAM_STEP
    stride = rates * (first_new / bias_one) / (jnp.sqrt(second / bias_two) + 1e-08)
    seen_mask = counts > 0.0
    return (
        jnp.where(seen_mask, params - stride, params),
        jnp.where(seen_mask, first_new, first_moment),
        jnp.where(seen_mask, second, second_moment),
    )


def shards(params, first_moment, second_moment, cameras, visible, send_plan, tile_lists, target):
    cells = lax.axis_size("cells")
    camera = cameras[0]
    plan_rows = send_plan[0, 0]
    capacity = plan_rows.shape[1]
    sent_live = (plan_rows >= 0)[None]
    sent_rows = jnp.maximum(plan_rows, 0)
    lists = tile_lists[0]
    tiles_here = lists.shape[0]
    live_mask = (lists >= 0).astype(jnp.float32)
    slot_ids = jnp.maximum(lists, 0)
    rows_pix = tiles_here * cells // TILE_COLS * 16
    pixel_column, pixel_row = pixel_grid(
        lax.axis_index("cells") * tiles_here, tiles_here, tiles_here, rows_pix
    )
    target_tile = target[0].reshape(3, tiles_here, 256)
    block = params.shape[1]

    def image_loss(table):
        picked = jnp.take(table, slot_ids, axis=1)
        return render_tiles(picked, live_mask, pixel_column, pixel_row, target_tile)

    def own_projection(values):
        return project(values, camera)

    features, project_pull = jax.vjp(own_projection, params)
    outgoing = jnp.take(features, sent_rows, axis=1)
    incoming = lax.all_to_all(outgoing, "cells", split_axis=1, concat_axis=1, tiled=True)
    loss_value, pullback = jax.vjp(
        image_loss, incoming.reshape(features.shape[0], cells * capacity)
    )
    table_grad = pullback(jnp.ones((), jnp.float32))[0]
    returned = lax.all_to_all(
        table_grad.reshape(features.shape[0], cells, capacity),
        "cells",
        split_axis=1,
        concat_axis=1,
        tiled=True,
    )
    kept = jnp.where(sent_live, returned, 0.0)
    gradient = project_pull(
        jnp.zeros((features.shape[0], block), jnp.float32).at[:, sent_rows].add(kept)
    )[0]
    seen_here = visible.astype(jnp.float32)
    total_grad, counts = lax.psum((gradient, seen_here), "views")
    new_params, new_first, new_second = adam_update(
        params, first_moment, second_moment, total_grad, counts
    )
    return (new_params, new_first, new_second)

LANES = 128
PAD_ROWS = 64
FEATS = 9


def project_rows(rows, turn, centre):
    offset = [rows[i] - centre[i] for i in range(3)]
    in_view = [
        turn[i][0] * offset[0] + turn[i][1] * offset[1] + turn[i][2] * offset[2] for i in range(3)
    ]
    inv_depth = 1.0 / in_view[2]
    screen_col = in_view[0] * inv_depth
    screen_row = in_view[1] * inv_depth
    scales = [jnp.exp(rows[3 + i]) for i in range(3)]
    raw = rows[6:10]
    norm = jnp.sqrt(raw[0] * raw[0] + raw[1] * raw[1] + raw[2] * raw[2] + raw[3] * raw[3])
    inv_norm = 1.0 / norm
    quat_w, quat_x, quat_y, quat_z = [item * inv_norm for item in raw]
    spin = [
        [
            1.0 - 2.0 * (quat_y * quat_y + quat_z * quat_z),
            2.0 * (quat_x * quat_y - quat_w * quat_z),
            2.0 * (quat_x * quat_z + quat_w * quat_y),
        ],
        [
            2.0 * (quat_x * quat_y + quat_w * quat_z),
            1.0 - 2.0 * (quat_x * quat_x + quat_z * quat_z),
            2.0 * (quat_y * quat_z - quat_w * quat_x),
        ],
        [
            2.0 * (quat_x * quat_z - quat_w * quat_y),
            2.0 * (quat_y * quat_z + quat_w * quat_x),
            1.0 - 2.0 * (quat_x * quat_x + quat_y * quat_y),
        ],
    ]
    basis_cam = [
        [
            (turn[i][0] * spin[0][j] + turn[i][1] * spin[1][j] + turn[i][2] * spin[2][j])
            * scales[j]
            for j in range(3)
        ]
        for i in range(3)
    ]
    top = [(basis_cam[0][j] - screen_col * basis_cam[2][j]) * inv_depth for j in range(3)]
    low = [(basis_cam[1][j] - screen_row * basis_cam[2][j]) * inv_depth for j in range(3)]
    sigma_a = top[0] * top[0] + top[1] * top[1] + top[2] * top[2]
    sigma_b = top[0] * low[0] + top[1] * low[1] + top[2] * low[2]
    sigma_c = low[0] * low[0] + low[1] * low[1] + low[2] * low[2]
    inv_det = 1.0 / (sigma_a * sigma_c - sigma_b * sigma_b)
    opacity = 1.0 / (1.0 + jnp.exp(-rows[10]))
    inv_dist = 1.0 / jnp.sqrt(offset[0] * offset[0] + offset[1] * offset[1] + offset[2] * offset[2])
    x, y, z = [item * inv_dist for item in offset]
    xx, yy, zz = x * x, y * y, z * z
    basis = [
        None,
        -harmonic_one * y,
        harmonic_one * z,
        -harmonic_one * x,
        harmonic_two[0] * x * y,
        harmonic_two[1] * y * z,
        harmonic_two[2] * (2.0 * zz - xx - yy),
        harmonic_two[3] * x * z,
        harmonic_two[4] * (xx - yy),
        harmonic_three[0] * y * (3.0 * xx - yy),
        harmonic_three[1] * x * y * z,
        harmonic_three[2] * y * (4.0 * zz - xx - yy),
        harmonic_three[3] * z * (2.0 * zz - 3.0 * xx - 3.0 * yy),
        harmonic_three[4] * x * (4.0 * zz - xx - yy),
        harmonic_three[5] * z * (xx - yy),
        harmonic_three[6] * x * (xx - 3.0 * yy),
    ]
    colors = []
    for k in range(3):
        total = harmonic_zero * rows[11 + k]
        for j in range(1, 16):
            total = total + basis[j] * rows[11 + 3 * j + k]
        colors.append(0.5 + total)
    return (
        screen_col,
        screen_row,
        sigma_c * inv_det,
        -sigma_b * inv_det,
        sigma_a * inv_det,
        opacity,
        *colors,
    )


def camera_terms(cam):
    cosines, sines = jnp.cos(cam), jnp.sin(cam)
    cr, cp, cy = [cosines[:, i : i + 1] for i in range(3)]
    sr, sp, sy = [sines[:, i : i + 1] for i in range(3)]
    turn = [
        [cy * cp, cy * sp * sr - sy * cr, cy * sp * cr + sy * sr],
        [sy * cp, sy * sp * sr + cy * cr, sy * sp * cr - cy * sr],
        [-sp, cp * sr, cp * cr],
    ]
    centre = [cam[:, 3 + i : 4 + i] for i in range(3)]
    return turn, centre

MAIN_VMEM = 40 * 2**20
UPDATE_VMEM = 16 * 2**20
UNROLL = 1


def fill_dense(params_ref, dense):
    count, block = params_ref.shape
    for b in range(block // LANES):
        part, line = divmod(b, 8)
        for r in range(0, count, 8):
            size = min(8, count - r)
            where = pl.ds((part * PAD_ROWS + r) * 8 + line, size, stride=8)
            dense[where, :] = params_ref[r : r + size, b * LANES : (b + 1) * LANES]


def dense_rows(dense, part, count):
    return [
        dense[pl.ds(pl.multiple_of((part * PAD_ROWS + r) * 8, 8), 8), :] for r in range(count)
    ]


def lane_pick(source, lanes):
    return jnp.take_along_axis(source, lanes, axis=1, mode="promise_in_bounds")


def gather_eight(load, blocks, index):
    index = jnp.maximum(index, 0)
    lanes, block = index & (LANES - 1), index >> 7
    total = lane_pick(load(0), lanes)
    for b in range(1, blocks):
        total = jnp.where(block == b, lane_pick(load(b), lanes), total)
    return total


def split_three(x):
    first = x.astype(jnp.bfloat16).astype(jnp.float32)
    rest = x - first
    second = rest.astype(jnp.bfloat16).astype(jnp.float32)
    return first, second, rest - second


def fill_hot(hot, index, start, bits):
    row_ids = lax.broadcasted_iota(jnp.int32, (hot.shape[0], LANES), 0)
    low = index & ((1 << bits) - 1)
    hot[:, start : start + LANES] = jnp.where(row_ids == low, 1.0, 0.0).astype(jnp.bfloat16)


def fill_values(lhs, main, last, index, start, bits):
    parts = jnp.concatenate(
        [*split_three(main), *split_three(last), jnp.zeros((5, LANES), jnp.float32)], axis=0
    )
    high = jnp.broadcast_to(index >> bits, parts.shape)
    for b in range(lhs.shape[0] // 32):
        lhs[32 * b : 32 * b + 32, pl.ds(start, LANES)] = jnp.where(high == b, parts, 0.0).astype(
            jnp.bfloat16
        )


def scatter_finish(lhs, hot):
    out = lax.dot_general(
        lhs[...], hot[...], (((1,), (1,)), ((), ())), preferred_element_type=jnp.float32
    )
    pieces = []
    for b in range(lhs.shape[0] // 32):
        rows = out[32 * b : 32 * b + 32]
        pieces.append(
            (rows[0:8] + rows[8:16] + rows[16:24], rows[24:25] + rows[25:26] + rows[26:27])
        )
    return pieces


def send_features(feat_parts, plan_ref, out_ref, table, last, order):
    halves = plan_ref.shape[1] // LANES
    blocks = last.shape[0]
    for part, feats in enumerate(feat_parts):
        for f in range(8):
            table[pl.ds(part * 64 + f, 8, stride=8), :] = feats[f]
        last[part * 8 : part * 8 + 8, :] = feats[8]
    slots = plan_ref.shape[0] * halves
    for o in range(slots):
        d, h = divmod(o, halves)
        row = plan_ref[d : d + 1, h * LANES : (h + 1) * LANES]
        order[o : o + 1, :] = row
        out_ref[d, 8 * h : 8 * h + 8, :] = gather_eight(
            lambda b: table[8 * b : 8 * b + 8, :], blocks, jnp.broadcast_to(row, (8, LANES))
        )
    for p in range(slots // 8):
        picked = gather_eight(
            lambda b: jnp.broadcast_to(last[b : b + 1, :], (8, LANES)),
            blocks,
            order[8 * p : 8 * p + 8, :],
        )
        for i in range(8 // halves):
            out_ref[8 // halves * p + i, 8 * halves :, :] = picked[i * halves : (i + 1) * halves]


def pixel_terms():
    lane = lax.broadcasted_iota(jnp.int32, (8, LANES), 1)
    inner = lane & 31
    tile = lane >> 5
    x = (inner & 15).astype(jnp.float32) - 7.5
    step = (inner >> 4).astype(jnp.float32) - 0.5
    return tile, x, step


def render_setup(lists_ref, target_ref, order, wanted, basis, plan_sums, hot, bits):
    tiles, entries = lists_ref.shape
    quarters = entries // LANES
    for q in range(quarters):
        order[q * tiles : (q + 1) * tiles, :] = lists_ref[:, q * LANES : (q + 1) * LANES]
    sub = lax.broadcasted_iota(jnp.int32, (8, LANES), 0)
    lane = lax.broadcasted_iota(jnp.int32, (8, LANES), 1)
    tile, x, step = pixel_terms()
    shifted = 32 * (sub & 3) + (lane & 31)
    for k in range(3):
        total = jnp.zeros((8, LANES), jnp.float32)
        for r in range(8):
            row = jnp.broadcast_to(target_ref[k, :, r * LANES : (r + 1) * LANES], (8, LANES))
            here = (tile == r // 2) & ((sub >> 2) == r % 2)
            total = jnp.where(here, lane_pick(row, shifted), total)
        wanted[8 * k : 8 * k + 8, :] = total
    for g in range(LANES // 8):
        row = sub + 8 * g
        coef = (row * 43) >> 9
        mine = tile == (row & 3)

        def column(j, *terms):
            total = jnp.zeros((8, LANES), jnp.float32)
            for c, value in terms:
                total = jnp.where(coef == c, value, total)
            total = jnp.where(mine, total, 0.0)
            basis[8 * g : 8 * g + 8, j * LANES : (j + 1) * LANES] = total

        column(0, (0, x * x), (1, x * step), (2, step * step), (3, x), (4, step), (5, 1.0))
        column(1, (1, x), (2, 2.0 * step), (4, 1.0))
        column(2, (2, 1.0))
        for k in range(3):
            column(3 + k, (6 + k, 1.0))
    mine = tile == (sub & 3)
    for s in range(8):
        y = step + (2.0 * s - 7.0)
        rows = [jnp.ones_like(x), x, y, x * x, x * y, y * y]
        rows = jnp.concatenate([jnp.where(mine, item, 0.0) for item in rows], axis=0)
        for part in range(2):
            start = (part * 8 + s) * LANES
            plan_sums[:, start : start + LANES] = rows.astype(jnp.bfloat16)
    for o in range(tiles * quarters):
        fill_hot(hot, order[o : o + 1, :], o * LANES, bits)


def render_rest(
    cells, copies, recv_ref, order, wanted, back_ref,
    coefs, tables, basis, alpha_s, weight_s, slope_s, joint_g, joint_w, plan_sums, error_sums,
    moved, pairs, lhs, hot, bits,
):
    owners, packed, _ = recv_ref.shape
    halves = packed // FEATS
    blocks = owners * halves
    tiles = 4
    quarters = order.shape[0] // tiles
    entries = quarters * LANES
    me = lax.axis_index("cells")
    rows_pix = tiles * cells // TILE_COLS * 16
    half_width = TILE_COLS * 8.0
    inv_width = 1.0 / half_width
    log_two = 1.4426950408889634
    sub = lax.broadcasted_iota(jnp.int32, (8, LANES), 0)
    local = sub & 3
    tile_col = 4 * lax.rem(me, TILE_COLS // 4) + local
    tile_row = lax.div(me, TILE_COLS // 4)
    centre_col = (16 * tile_col + 8).astype(jnp.float32) - half_width
    centre_row = (jnp.full((8, LANES), 16 * tile_row + 8, jnp.int32)).astype(
        jnp.float32
    ) - rows_pix * 0.5

    picked = [[None] * FEATS for _ in range(quarters // 2)]
    for k in range(owners):
        origin = lax.rem(me + owners - k, owners)
        if k:
            copies[k - 1].wait()
        for p in range(quarters // 2):
            index = jnp.maximum(order[8 * p : 8 * p + 8, :], 0)
            lanes, block = index & (LANES - 1), index >> 7
            for h in range(halves):
                here = block == origin * halves + h
                for f in range(FEATS):
                    r = 8 * h + f if f < 8 else 8 * halves + h
                    row = jnp.broadcast_to(recv_ref[origin, r : r + 1, :], (8, LANES))
                    item = lane_pick(row, lanes)
                    old = picked[p][f]
                    picked[p][f] = item if old is None else jnp.where(here, item, old)

    for p in range(quarters // 2):
        index = order[8 * p : 8 * p + 8, :]
        feats = picked[p]
        off_col = feats[0] * half_width - centre_col
        off_row = feats[1] * half_width - centre_row
        moved[16 * p : 16 * p + 8, :] = off_col
        moved[16 * p + 8 : 16 * p + 16, :] = off_row
        square = feats[2] * (-0.5 * log_two * inv_width * inv_width)
        cross = feats[3] * (-log_two * inv_width * inv_width)
        bend = feats[4] * (-0.5 * log_two * inv_width * inv_width)
        faint = jnp.maximum(jnp.log(feats[5]) * log_two, -1e30)
        along = square * off_col + cross * off_row
        level = along * off_col + bend * off_row * off_row + jnp.where(index >= 0, faint, -1e30)
        terms = [
            square,
            cross,
            bend,
            -(along + square * off_col),
            -(2.0 * bend * off_row + cross * off_col),
            level,
            feats[6],
            feats[7],
            feats[8],
        ]
        for c, term in enumerate(terms):
            for i, piece in enumerate(split_three(term)):
                row = (3 * c + i) * tiles
                for q in range(2):
                    start = (2 * p + q) * LANES
                    coefs[start + row : start + row + tiles, :] = piece[4 * q : 4 * q + 4]
    for q in range(quarters):
        coefs[q * LANES + 108 : (q + 1) * LANES, :] = jnp.zeros((LANES - 108, LANES), jnp.float32)
    weights = basis[...].astype(jnp.bfloat16)
    for q in range(quarters):
        span = slice(q * LANES, (q + 1) * LANES)
        turned = jnp.transpose(coefs[span, :]).astype(jnp.bfloat16)
        result = jnp.dot(turned, weights, preferred_element_type=jnp.float32)
        for j in range(6):
            tables[j, span, :] = result[:, j * LANES : (j + 1) * LANES]

    height = (2 * sub - 7).astype(jnp.float32)

    def table(l, j):
        return jnp.broadcast_to(tables[j, pl.ds(l, 1), :], (8, LANES))

    def relay(source, joint, c, s):
        item = source[pl.ds(c * 128 + s, 16, stride=8), :]
        top = item.astype(jnp.bfloat16)
        rows = pl.ds(pl.multiple_of(c * 16, 16), 16)
        joint[rows, s * LANES : (s + 1) * LANES] = top
        joint[rows, (8 + s) * LANES : (9 + s) * LANES] = (
            item - top.astype(jnp.float32)
        ).astype(jnp.bfloat16)

    def forward(c, carry, late):
        trans, red, green, blue = carry
        for i in range(16):
            l = c * 16 + i
            power = table(l, 0) + height * (table(l, 1) + height * table(l, 2))
            alpha = jnp.exp2(power)
            weight = alpha * trans
            where = pl.ds(pl.multiple_of(l * 8, 8), 8)
            alpha_s[where, :] = alpha
            weight_s[where, :] = weight
            trans = trans * (1.0 - alpha)
            red = red + weight * table(l, 3)
            green = green + weight * table(l, 4)
            blue = blue + weight * table(l, 5)
            if late and i % 2:
                relay(weight_s, joint_w, c - 1, i // 2)
        return trans, red, green, blue

    zero = jnp.zeros((8, LANES), jnp.float32)
    chunks = entries // 16
    carry = forward(0, (jnp.ones((8, LANES), jnp.float32), zero, zero, zero), False)
    carry = lax.fori_loop(1, chunks, lambda c, v: forward(c, v, True), carry, unroll=UNROLL)
    red, green, blue = carry[1:]
    for s in range(8):
        relay(weight_s, joint_w, chunks - 1, s)
    errors = [2.0 * (item - wanted[8 * k : 8 * k + 8, :]) for k, item in enumerate((red, green, blue))]
    wanted[0:8, :], wanted[8:16, :], wanted[16:24, :] = errors
    tile, _, _ = pixel_terms()
    mine = tile == local
    for s in range(8):
        tops, lows = [], []
        for k in range(3):
            row = jnp.broadcast_to(wanted[8 * k + s : 8 * k + s + 1, :], (8, LANES))
            row = jnp.where(mine, row, 0.0)
            top = row.astype(jnp.bfloat16).astype(jnp.float32)
            tops.append(top)
            lows.append(row - top)
        blank = [jnp.zeros((24, LANES), jnp.float32)]
        start = s * LANES
        error_sums[:, start : start + LANES] = jnp.concatenate(tops + lows, axis=0).astype(jnp.bfloat16)
        start = (8 + s) * LANES
        error_sums[:, start : start + LANES] = jnp.concatenate(tops + blank, axis=0).astype(jnp.bfloat16)

    def backward(c, behind, late):
        for i in range(15, -1, -1):
            l = c * 16 + i
            where = pl.ds(pl.multiple_of(l * 8, 8), 8)
            slope = errors[0] * table(l, 3) + errors[1] * table(l, 4) + errors[2] * table(l, 5)
            alpha = alpha_s[where, :]
            slope_s[where, :] = weight_s[where, :] * (slope - behind)
            behind = (1.0 - alpha) * behind + alpha * slope
            if late and i % 2:
                relay(slope_s, joint_g, c + 1, i // 2)
        return behind

    behind = backward(chunks - 1, zero, False)
    lax.fori_loop(
        1, chunks, lambda i, v: backward(chunks - 1 - i, v, True), behind, unroll=UNROLL
    )
    for s in range(8):
        relay(slope_s, joint_g, 0, s)
    over = (((1,), (1,)), ((), ()))
    turned = lax.dot_general(
        plan_sums[...], joint_g[...], over, preferred_element_type=jnp.float32
    )
    tinted = lax.dot_general(
        error_sums[...], joint_w[...], over, preferred_element_type=jnp.float32
    )
    for p in range(quarters // 2):
        off_col = moved[16 * p : 16 * p + 8, :]
        off_row = moved[16 * p + 8 : 16 * p + 16, :]

        def quantity(j):
            source, r = (turned, j) if j < 6 else (tinted, j - 6)
            rows = source[8 * r : 8 * r + 8]
            start = 2 * p * LANES
            return jnp.where(
                sub < 4, rows[:, start : start + LANES], rows[:, start + LANES : start + 2 * LANES]
            )

        plain, across, down = quantity(0), quantity(1), quantity(2)
        near_col = across - off_col * plain
        near_row = down - off_row * plain
        rows = [
            plain,
            near_col * inv_width,
            near_row * inv_width,
            (quantity(3) - off_col * (across + near_col)) * (inv_width * inv_width),
            (quantity(4) - off_col * down - off_row * near_col) * (inv_width * inv_width),
            (quantity(5) - off_row * (down + near_row)) * (inv_width * inv_width),
            *[quantity(6 + k) + quantity(9 + k) for k in range(3)],
        ]
        for f, item in enumerate(rows):
            pairs[pl.ds(p * 128 + f, 8, stride=16), :] = item
    for o in range(tiles * quarters):
        fill_values(
            lhs,
            pairs[o * 16 : o * 16 + 8, :],
            pairs[o * 16 + 8 : o * 16 + 9, :],
            order[o : o + 1, :],
            o * LANES,
            bits,
        )
    for s, (main, last) in enumerate(scatter_finish(lhs, hot)):
        for h in range(halves):
            span = slice(h * LANES, (h + 1) * LANES)
            back_ref[s, 8 * h : 8 * h + 8, :] = main[:, span]
            back_ref[s, 8 * halves + h : 8 * halves + h + 1, :] = last[:, span]


def main_kernel(
    params_in, cam_in, plan_in, visible_in, lists_in, target_in, out_ref,
    params_ref, cam_ref, plan_ref, visible_ref, lists_ref, target_ref, dense, table, last, plan_order, outgoing, incoming, back, returned, mine, extra, extras, shared,
    order, wanted, basis, coefs, tables, alpha_s, weight_s, slope_s, joint_g, joint_w,
    plan_sums, error_sums, moved, pairs, lhs, hot, own_lhs, own_hot,
    send_one, recv_one, send_two, recv_two, send_three, recv_three, send_four, recv_four, local_sem,
):
    cells, views = lax.axis_size("cells"), lax.axis_size("views")
    cell, view = lax.axis_index("cells"), lax.axis_index("views")
    count, block = params_ref.shape
    blocks = block // LANES
    capacity = plan_ref.shape[1]
    halves = capacity // LANES
    bits = capacity.bit_length() - 1
    fetches = [
        pltpu.make_async_copy(source, dest, local_sem.at[i])
        for i, (source, dest) in enumerate(
            (
                (params_in, params_ref),
                (cam_in, cam_ref),
                (plan_in, plan_ref),
                (visible_in, visible_ref),
                (lists_in, lists_ref),
                (target_in, target_ref),
            )
        )
    ]
    for fetch in fetches:
        fetch.start()
    barrier = pltpu.get_barrier_semaphore()

    def greet(axis, me, size):
        for k in range(1, size):
            pl.semaphore_signal(
                barrier,
                inc=1,
                device_id={axis: lax.rem(me + k, size)},
                device_id_type=pl.DeviceIdType.MESH,
            )

    def send_all(axis, me, size, source, dest, send_sem, recv_sem):
        copies = []
        for k in range(1, size):
            peer = lax.rem(me + k, size)
            copy = pltpu.make_async_remote_copy(
                src_ref=source(peer),
                dst_ref=dest(me),
                send_sem=send_sem.at[k - 1],
                recv_sem=recv_sem.at[k - 1],
                device_id={axis: peer},
                device_id_type=pl.DeviceIdType.MESH,
            )
            copy.start()
            copies.append(copy)
        return copies

    greet("cells", cell, cells)
    greet("views", view, views)
    fetches[1].wait()
    turn, centre = camera_terms(cam_ref[...])
    known = [*turn[0], *turn[1], *turn[2], *centre]
    lane = lax.broadcasted_iota(jnp.int32, (8, LANES), 1)
    line = jnp.zeros((8, LANES), jnp.float32)
    for i, item in enumerate(known):
        line = jnp.where(lane == i, jnp.broadcast_to(item, (8, LANES)), line)
    extra[blocks : blocks + 8, :] = line
    fetches[3].wait()
    for b in range(blocks):
        extra[b : b + 1, :] = visible_ref[:, b * LANES : (b + 1) * LANES].astype(jnp.float32)
    fetches[0].wait()
    fill_dense(params_ref, dense)
    feat_parts = [
        project_rows(dense_rows(dense, part, count), turn, centre) for part in range(blocks // 8)
    ]
    fetches[2].wait()
    send_features(feat_parts, plan_ref, outgoing, table, last, plan_order)
    pl.semaphore_wait(barrier, cells + views - 2)

    first = send_all(
        "cells", cell, cells, lambda p: outgoing.at[p], lambda p: incoming.at[p], send_one, recv_one
    )
    fourth = send_all(
        "views", view, views, lambda p: extra, lambda p: extras.at[p], send_four, recv_four
    )
    incoming[cell] = outgoing[cell]
    extras[view] = extra[...]
    fetches[4].wait()
    fetches[5].wait()
    render_setup(lists_ref, target_ref, order, wanted, basis, plan_sums, hot, bits)
    render_rest(
        cells, first, incoming, order, wanted, back,
        coefs, tables, basis, alpha_s, weight_s, slope_s, joint_g, joint_w, plan_sums, error_sums,
        moved, pairs, lhs, hot, bits,
    )
    second = send_all(
        "cells", cell, cells, lambda p: back.at[p], lambda p: returned.at[p], send_two, recv_two
    )
    returned[cell] = back[cell]
    wide = own_hot.shape[0].bit_length() - 1
    for o in range(cells * halves):
        d, h = divmod(o, halves)
        fill_hot(own_hot, plan_ref[d : d + 1, h * LANES : (h + 1) * LANES], o * LANES, wide)
    for copy in second:
        copy.wait()
    for o in range(cells * halves):
        d, h = divmod(o, halves)
        fill_values(
            own_lhs,
            returned[d, 8 * h : 8 * h + 8, :],
            returned[d, 8 * halves + h : 8 * halves + h + 1, :],
            plan_ref[d : d + 1, h * LANES : (h + 1) * LANES],
            o * LANES,
            wide,
        )
    for g, (main, tip) in enumerate(scatter_finish(own_lhs, own_hot)):
        for i in range(2):
            span = slice(i * LANES, (i + 1) * LANES)
            for f in range(8):
                mine[f * blocks + 2 * g + i : f * blocks + 2 * g + i + 1, :] = main[f : f + 1, span]
            mine[8 * blocks + 2 * g + i : 8 * blocks + 2 * g + i + 1, :] = tip[:, span]
    third = send_all(
        "views", view, views, lambda p: mine, lambda p: shared.at[p], send_three, recv_three
    )
    for copy in fourth:
        copy.wait()
    counts = extras[0, 0:blocks, :]
    for v in range(1, views):
        counts = counts + extras[v, 0:blocks, :]
    grads = blocks * PAD_ROWS
    out_ref[grads : grads + blocks, :] = counts

    def pull_view(fresh, source, lines):
        known = [jnp.broadcast_to(lines[:, i : i + 1], (8, LANES)) for i in range(12)]
        turn = [known[0:3], known[3:6], known[6:9]]
        centre = known[9:12]

        def one_part(part, carry):
            rows = dense_rows(dense, part, count)
            feats, pull = jax.vjp(lambda *items: project_rows(items, turn, centre), *rows)
            got = [
                source[pl.ds(pl.multiple_of(f * blocks + part * 8, 8), 8), :] for f in range(FEATS)
            ]
            wanted_slopes = (
                feats[2] * got[1] + feats[3] * got[2],
                feats[3] * got[1] + feats[4] * got[2],
                -0.5 * got[3],
                -got[4],
                -0.5 * got[5],
                got[0] / feats[5],
                got[6],
                got[7],
                got[8],
            )
            for r, item in enumerate(pull(wanted_slopes)):
                where = pl.ds(pl.multiple_of((part * PAD_ROWS + r) * 8, 8), 8)
                out_ref[where, :] = item if fresh else out_ref[where, :] + item
            return carry

        lax.fori_loop(0, blocks // 8, one_part, 0)

    pull_view(True, mine, extra[blocks : blocks + 1, :])
    for k in range(1, views):
        third[views - 1 - k].wait()
        origin = lax.rem(view + k, views)
        pull_view(False, shared.at[origin], extras[origin, blocks : blocks + 1, :])


def update_kernel(params_ref, first_ref, second_ref, grads_ref, new_ref, new_first_ref, new_second_ref):
    count, block = params_ref.shape
    blocks = block // LANES
    row_ids = lax.broadcasted_iota(jnp.int32, (8, LANES), 0)
    bias_one = 1.0 - 0.9**ADAM_STEP
    bias_two = 1.0 - 0.999**ADAM_STEP
    for b in range(blocks):
        span = slice(b * LANES, (b + 1) * LANES)
        part, line = divmod(b, 8)
        counts = grads_ref[blocks * PAD_ROWS + b : blocks * PAD_ROWS + b + 1, :]
        for r in range(0, count, 8):
            size = min(8, count - r)
            rows = slice(r, r + size)
            gradient = grads_ref[pl.ds((part * PAD_ROWS + r) * 8 + line, size, stride=8), :]
            if r >= 16:
                rates = 0.000125
            else:
                ids = row_ids[0:size] + r
                rates = jnp.where(
                    ids < 6,
                    0.01,
                    jnp.where(
                        ids < 10,
                        0.005,
                        jnp.where(ids < 11, 0.05, jnp.where(ids < 14, 0.0025, 0.000125)),
                    ),
                )
            params, first, second = params_ref[rows, span], first_ref[rows, span], second_ref[rows, span]
            seen = jnp.broadcast_to(counts, params.shape) > 0.0
            first_new = 0.9 * first + 0.1 * gradient
            second_new = 0.999 * second + 0.001 * gradient * gradient
            stride = rates * (first_new / bias_one) / (jnp.sqrt(second_new / bias_two) + 1e-08)
            new_ref[rows, span] = jnp.where(seen, params - stride, params)
            new_first_ref[rows, span] = jnp.where(seen, first_new, first)
            new_second_ref[rows, span] = jnp.where(seen, second_new, second)


def fused_shards(params, first_moment, second_moment, cameras, visible, send_plan, tile_lists, target):
    cells, views = lax.axis_size("cells"), lax.axis_size("views")
    count, block = params.shape
    blocks = block // LANES
    plan = send_plan[0, 0]
    lists = tile_lists[0]
    tiles, entries = lists.shape
    capacity = plan.shape[1]
    halves = capacity // LANES
    slots = cells * halves
    f32, bf16 = jnp.float32, jnp.bfloat16
    packet = pltpu.VMEM((cells, FEATS * halves, LANES), f32)
    dma = pltpu.SemaphoreType.DMA
    vmem = pl.BlockSpec(memory_space=pltpu.VMEM)
    grads = pl.pallas_call(
        main_kernel,
        out_shape=jax.ShapeDtypeStruct((blocks * PAD_ROWS + blocks, LANES), f32),
        in_specs=[pl.BlockSpec(memory_space=pltpu.HBM)] * 6,
        out_specs=vmem,
        scratch_shapes=[
            pltpu.VMEM((count, block), f32),
            pltpu.VMEM(cameras.shape, f32),
            pltpu.VMEM(plan.shape, jnp.int32),
            pltpu.VMEM(visible.shape, jnp.int32),
            pltpu.VMEM(lists.shape, jnp.int32),
            pltpu.VMEM((3, 1, target.shape[2]), f32),
            pltpu.VMEM((blocks * PAD_ROWS, LANES), f32),
            pltpu.VMEM((blocks * 8, LANES), f32),
            pltpu.VMEM((blocks, LANES), f32),
            pltpu.VMEM((slots, LANES), jnp.int32),
            packet, packet, packet, packet,
            pltpu.VMEM((FEATS * blocks, LANES), f32),
            pltpu.VMEM((blocks + 8, LANES), f32),
            pltpu.VMEM((views, blocks + 8, LANES), f32),
            pltpu.VMEM((views, FEATS * blocks, LANES), f32),
            pltpu.VMEM((tiles * entries // LANES, LANES), jnp.int32),
            pltpu.VMEM((24, LANES), f32),
            pltpu.VMEM((LANES, 6 * LANES), f32),
            pltpu.VMEM((entries, LANES), f32),
            pltpu.VMEM((6, entries, LANES), f32),
            pltpu.VMEM((entries * 8, LANES), f32),
            pltpu.VMEM((entries * 8, LANES), f32),
            pltpu.VMEM((entries * 8, LANES), f32),
            pltpu.VMEM((entries, 16 * LANES), bf16),
            pltpu.VMEM((entries, 16 * LANES), bf16),
            pltpu.VMEM((48, 16 * LANES), bf16),
            pltpu.VMEM((48, 16 * LANES), bf16),
            pltpu.VMEM((entries // LANES * 8, LANES), f32),
            pltpu.VMEM((tiles * entries // LANES * 16, LANES), f32),
            pltpu.VMEM((cells * 32, tiles * entries), bf16),
            pltpu.VMEM((capacity, tiles * entries), bf16),
            pltpu.VMEM((blocks // 2 * 32, slots * LANES), bf16),
            pltpu.VMEM((2 * LANES, slots * LANES), bf16),
            dma((cells - 1,)), dma((cells - 1,)), dma((cells - 1,)), dma((cells - 1,)),
            dma((views - 1,)), dma((views - 1,)), dma((views - 1,)), dma((views - 1,)),
            dma((6,)),
        ],
        compiler_params=pltpu.CompilerParams(
            collective_id=0, has_side_effects=True, vmem_limit_bytes=MAIN_VMEM
        ),
        cost_estimate=pl.CostEstimate(
            flops=4096 * tiles * 256 * entries,
            bytes_accessed=4 * count * block,
            transcendentals=tiles * 256 * entries,
        ),
    )(
        *[
            pltpu.with_memory_space_constraint(item, pltpu.HBM)
            for item in (params, cameras, plan, visible, lists, jnp.transpose(target, (1, 0, 2)))
        ]
    )
    like = jax.ShapeDtypeStruct(params.shape, f32)
    return tuple(
        pl.pallas_call(
            update_kernel,
            out_shape=(like, like, like),
            compiler_params=pltpu.CompilerParams(vmem_limit_bytes=UPDATE_VMEM),
        )(params, first_moment, second_moment, grads)
    )


def local_shards(params, first_moment, second_moment, cameras, visible, send_plan, tile_lists, target):
    capacity = send_plan.shape[3]
    tiles, entries = tile_lists.shape[1:]
    halves = capacity // LANES
    fits = (
        capacity % LANES == 0
        and params.shape[1] % (8 * LANES) == 0
        and entries % (2 * LANES) == 0
        and 8 % max(halves, 1) == 0
        and lax.axis_size("cells") * halves % 8 == 0
        and tiles * entries <= 4096
        and tiles == 4
    )
    body = fused_shards if fits else shards
    return body(params, first_moment, second_moment, cameras, visible, send_plan, tile_lists, target)


def solution(mesh):
    in_specs = (
        P(None, "cells"),
        P(None, "cells"),
        P(None, "cells"),
        P("views", None),
        P("views", "cells"),
        P("views", "cells", None, None),
        P("views", "cells", None),
        P("views", None, "cells"),
    )
    out_specs = (P(None, "cells"), P(None, "cells"), P(None, "cells"))
    return jax.shard_map(local_shards, mesh=mesh, in_specs=in_specs, out_specs=out_specs, check_vma=False)
```

```python
import functools

import jax
import jax.numpy as jnp
from jax import lax
from jax.experimental import pallas as pl
from jax.experimental.pallas import tpu as pltpu
from jax.sharding import PartitionSpec as P

TILE_COLS = 32
ADAM_STEP = 1000


harmonic_zero = 0.28209479177387814
harmonic_one = 0.4886025119029199
harmonic_two = (
    1.0925484305920792,
    -1.0925484305920792,
    0.31539156525252005,
    -1.0925484305920792,
    0.5462742152960396,
)
harmonic_three = (
    -0.5900435899266435,
    2.890611442640554,
    -0.4570457994644658,
    0.3731763325901154,
    -0.4570457994644658,
    1.445305721320277,
    -0.5900435899266435,
)


def harmonics(across, upward, onward):
    across_sq = across * across
    upward_sq = upward * upward
    onward_sq = onward * onward
    return jnp.stack(
        [
            harmonic_zero * jnp.ones_like(across),
            -harmonic_one * upward,
            harmonic_one * onward,
            -harmonic_one * across,
            harmonic_two[0] * across * upward,
            harmonic_two[1] * upward * onward,
            harmonic_two[2] * (2.0 * onward_sq - across_sq - upward_sq),
            harmonic_two[3] * across * onward,
            harmonic_two[4] * (across_sq - upward_sq),
            harmonic_three[0] * upward * (3.0 * across_sq - upward_sq),
            harmonic_three[1] * across * upward * onward,
            harmonic_three[2] * upward * (4.0 * onward_sq - across_sq - upward_sq),
            harmonic_three[3] * onward * (2.0 * onward_sq - 3.0 * across_sq - 3.0 * upward_sq),
            harmonic_three[4] * across * (4.0 * onward_sq - across_sq - upward_sq),
            harmonic_three[5] * onward * (across_sq - upward_sq),
            harmonic_three[6] * across * (across_sq - 3.0 * upward_sq),
        ]
    )


def camera_rotation(angles):
    cos_roll, sin_roll = (jnp.cos(angles[0]), jnp.sin(angles[0]))
    cos_pitch, sin_pitch = (jnp.cos(angles[1]), jnp.sin(angles[1]))
    cos_yaw, sin_yaw = (jnp.cos(angles[2]), jnp.sin(angles[2]))
    naught = jnp.zeros_like(cos_roll)
    unit_one = jnp.ones_like(cos_roll)
    roll = jnp.stack(
        [
            jnp.stack([unit_one, naught, naught]),
            jnp.stack([naught, cos_roll, -sin_roll]),
            jnp.stack([naught, sin_roll, cos_roll]),
        ]
    )
    pitch = jnp.stack(
        [
            jnp.stack([cos_pitch, naught, sin_pitch]),
            jnp.stack([naught, unit_one, naught]),
            jnp.stack([-sin_pitch, naught, cos_pitch]),
        ]
    )
    yawing = jnp.stack(
        [
            jnp.stack([cos_yaw, -sin_yaw, naught]),
            jnp.stack([sin_yaw, cos_yaw, naught]),
            jnp.stack([naught, naught, unit_one]),
        ]
    )
    inner_turn = jnp.dot(pitch, roll, precision=lax.Precision.HIGHEST)
    return jnp.dot(yawing, inner_turn, precision=lax.Precision.HIGHEST)


def project(values, camera):
    turn = camera_rotation(camera[0:3])
    offset = values[0:3] - camera[3:6][:, None]
    in_view = jnp.dot(turn, offset, precision=lax.Precision.HIGHEST)
    inv_depth = 1.0 / in_view[2]
    screen_col = in_view[0] * inv_depth
    screen_row = in_view[1] * inv_depth
    scales = jnp.exp(values[3:6])
    quat = values[6:10] / jnp.sqrt(jnp.sum(values[6:10] * values[6:10], axis=0, keepdims=True))
    quat_w, quat_x, quat_y, quat_z = (quat[0], quat[1], quat[2], quat[3])
    spin = [
        [
            1.0 - 2.0 * (quat_y * quat_y + quat_z * quat_z),
            2.0 * (quat_x * quat_y - quat_w * quat_z),
            2.0 * (quat_x * quat_z + quat_w * quat_y),
        ],
        [
            2.0 * (quat_x * quat_y + quat_w * quat_z),
            1.0 - 2.0 * (quat_x * quat_x + quat_z * quat_z),
            2.0 * (quat_y * quat_z - quat_w * quat_x),
        ],
        [
            2.0 * (quat_x * quat_z - quat_w * quat_y),
            2.0 * (quat_y * quat_z + quat_w * quat_x),
            1.0 - 2.0 * (quat_x * quat_x + quat_y * quat_y),
        ],
    ]
    basis_cam = []
    for outer_index in range(3):
        row_terms = []
        for col_index in range(3):
            entry = turn[outer_index, 0] * spin[0][col_index]
            for mid_index in range(1, 3):
                entry = entry + turn[outer_index, mid_index] * spin[mid_index][col_index]
            row_terms.append(entry * scales[col_index])
        basis_cam.append(row_terms)
    jac_top = [
        (basis_cam[0][col_index] - screen_col * basis_cam[2][col_index]) * inv_depth
        for col_index in range(3)
    ]
    jac_low = [
        (basis_cam[1][col_index] - screen_row * basis_cam[2][col_index]) * inv_depth
        for col_index in range(3)
    ]
    sigma_a = jac_top[0] * jac_top[0] + jac_top[1] * jac_top[1] + jac_top[2] * jac_top[2]
    sigma_b = jac_top[0] * jac_low[0] + jac_top[1] * jac_low[1] + jac_top[2] * jac_low[2]
    sigma_c = jac_low[0] * jac_low[0] + jac_low[1] * jac_low[1] + jac_low[2] * jac_low[2]
    determinant = sigma_a * sigma_c - sigma_b * sigma_b
    opacity = jax.nn.sigmoid(values[10])
    distance = jnp.sqrt(jnp.sum(offset * offset, axis=0))
    unit_dir = offset / distance
    basis = harmonics(unit_dir[0], unit_dir[1], unit_dir[2])
    coeffs = values[11:59].reshape(16, 3, values.shape[1])
    colors = 0.5 + jnp.sum(basis[:, None, :] * coeffs, axis=0)
    screen = jnp.stack(
        [
            screen_col,
            screen_row,
            sigma_c / determinant,
            -sigma_b / determinant,
            sigma_a / determinant,
            opacity,
        ]
    )
    return jnp.concatenate([screen, colors], axis=0)


def group_loss(pieces):
    features, live_mask, pixel_column, pixel_row, target_tile = pieces
    entries = live_mask.shape[1]
    delta_col = pixel_column[:, :, None] - features[0][:, None, :]
    delta_row = pixel_row[:, :, None] - features[1][:, None, :]
    power = -0.5 * (
        features[2][:, None, :] * delta_col * delta_col
        + 2.0 * features[3][:, None, :] * delta_col * delta_row
        + features[4][:, None, :] * delta_row * delta_row
    )
    alphas = features[5][:, None, :] * jnp.exp(power) * live_mask[:, None, :]
    log_keep = jnp.log(1.0 - alphas)
    earlier = (
        lax.broadcasted_iota(jnp.int32, (entries, entries), 0)
        < lax.broadcasted_iota(jnp.int32, (entries, entries), 1)
    ).astype(jnp.float32)
    transmit = jnp.exp(
        jnp.einsum("bpl,lm->bpm", log_keep, earlier, precision=lax.Precision.HIGHEST)
    )
    weights = alphas * transmit
    image = jnp.einsum("bpl,kbl->kbp", weights, features[6:9], precision=lax.Precision.HIGHEST)
    error = image - target_tile
    return jnp.sum(error * error)


def render_tiles(picked, live_mask, pixel_column, pixel_row, target_tile):
    groups = live_mask.shape[0] // 4
    entries = live_mask.shape[1]
    pixels = pixel_column.shape[1]
    stacked = (
        jnp.transpose(picked.reshape(picked.shape[0], groups, 4, entries), (1, 0, 2, 3)),
        live_mask.reshape(groups, 4, entries),
        pixel_column.reshape(groups, 4, pixels),
        pixel_row.reshape(groups, 4, pixels),
        jnp.transpose(target_tile.reshape(3, groups, 4, pixels), (1, 0, 2, 3)),
    )
    return jnp.sum(lax.map(jax.checkpoint(group_loss), stacked))


def pixel_grid(first_tile, count, tiles_dev, rows_pix):
    tile_ids = first_tile + jnp.arange(count, dtype=jnp.int32)
    pixel_ids = jnp.arange(256, dtype=jnp.int32)
    block_cols = TILE_COLS // 4
    owner_ids = tile_ids // tiles_dev
    local_ids = tile_ids % tiles_dev
    tile_col = 4 * (owner_ids % block_cols) + local_ids % 4
    tile_row = tiles_dev // 4 * (owner_ids // block_cols) + local_ids // 4
    half_width = TILE_COLS * 8.0
    column = (tile_col[:, None] * 16 + pixel_ids[None, :] % 16).astype(jnp.float32)
    row_pos = (tile_row[:, None] * 16 + pixel_ids[None, :] // 16).astype(jnp.float32)
    return ((column + 0.5 - half_width) / half_width, (row_pos + 0.5 - rows_pix * 0.5) / half_width)


def adam_update(params, first_moment, second_moment, gradient, counts):
    row_ids = lax.broadcasted_iota(jnp.int32, params.shape, 0)
    rates = jnp.where(
        row_ids < 6,
        0.01,
        jnp.where(
            row_ids < 10,
            0.005,
            jnp.where(row_ids < 11, 0.05, jnp.where(row_ids < 14, 0.0025, 0.000125)),
        ),
    )
    first_new = 0.9 * first_moment + 0.1 * gradient
    second = 0.999 * second_moment + 0.001 * gradient * gradient
    bias_one = 1.0 - 0.9**ADAM_STEP
    bias_two = 1.0 - 0.999**ADAM_STEP
    stride = rates * (first_new / bias_one) / (jnp.sqrt(second / bias_two) + 1e-08)
    seen_mask = counts > 0.0
    return (
        jnp.where(seen_mask, params - stride, params),
        jnp.where(seen_mask, first_new, first_moment),
        jnp.where(seen_mask, second, second_moment),
    )


def shards(params, first_moment, second_moment, cameras, visible, send_plan, tile_lists, target):
    cells = lax.axis_size("cells")
    camera = cameras[0]
    plan_rows = send_plan[0, 0]
    capacity = plan_rows.shape[1]
    sent_live = (plan_rows >= 0)[None]
    sent_rows = jnp.maximum(plan_rows, 0)
    lists = tile_lists[0]
    tiles_here = lists.shape[0]
    live_mask = (lists >= 0).astype(jnp.float32)
    slot_ids = jnp.maximum(lists, 0)
    rows_pix = tiles_here * cells // TILE_COLS * 16
    pixel_column, pixel_row = pixel_grid(
        lax.axis_index("cells") * tiles_here, tiles_here, tiles_here, rows_pix
    )
    target_tile = target[0].reshape(3, tiles_here, 256)
    block = params.shape[1]

    def image_loss(table):
        picked = jnp.take(table, slot_ids, axis=1)
        return render_tiles(picked, live_mask, pixel_column, pixel_row, target_tile)

    def own_projection(values):
        return project(values, camera)

    features, project_pull = jax.vjp(own_projection, params)
    outgoing = jnp.take(features, sent_rows, axis=1)
    incoming = lax.all_to_all(outgoing, "cells", split_axis=1, concat_axis=1, tiled=True)
    loss_value, pullback = jax.vjp(
        image_loss, incoming.reshape(features.shape[0], cells * capacity)
    )
    table_grad = pullback(jnp.ones((), jnp.float32))[0]
    returned = lax.all_to_all(
        table_grad.reshape(features.shape[0], cells, capacity),
        "cells",
        split_axis=1,
        concat_axis=1,
        tiled=True,
    )
    kept = jnp.where(sent_live, returned, 0.0)
    gradient = project_pull(
        jnp.zeros((features.shape[0], block), jnp.float32).at[:, sent_rows].add(kept)
    )[0]
    seen_here = visible.astype(jnp.float32)
    total_grad, counts = lax.psum((gradient, seen_here), "views")
    new_params, new_first, new_second = adam_update(
        params, first_moment, second_moment, total_grad, counts
    )
    return (new_params, new_first, new_second)

LANES = 128
PAD_ROWS = 64
FEATS = 9


def project_rows(rows, turn, centre):
    offset = [rows[i] - centre[i] for i in range(3)]
    in_view = [
        turn[i][0] * offset[0] + turn[i][1] * offset[1] + turn[i][2] * offset[2] for i in range(3)
    ]
    inv_depth = 1.0 / in_view[2]
    screen_col = in_view[0] * inv_depth
    screen_row = in_view[1] * inv_depth
    scales = [jnp.exp(rows[3 + i]) for i in range(3)]
    raw = rows[6:10]
    norm = jnp.sqrt(raw[0] * raw[0] + raw[1] * raw[1] + raw[2] * raw[2] + raw[3] * raw[3])
    inv_norm = 1.0 / norm
    quat_w, quat_x, quat_y, quat_z = [item * inv_norm for item in raw]
    spin = [
        [
            1.0 - 2.0 * (quat_y * quat_y + quat_z * quat_z),
            2.0 * (quat_x * quat_y - quat_w * quat_z),
            2.0 * (quat_x * quat_z + quat_w * quat_y),
        ],
        [
            2.0 * (quat_x * quat_y + quat_w * quat_z),
            1.0 - 2.0 * (quat_x * quat_x + quat_z * quat_z),
            2.0 * (quat_y * quat_z - quat_w * quat_x),
        ],
        [
            2.0 * (quat_x * quat_z - quat_w * quat_y),
            2.0 * (quat_y * quat_z + quat_w * quat_x),
            1.0 - 2.0 * (quat_x * quat_x + quat_y * quat_y),
        ],
    ]
    basis_cam = [
        [
            (turn[i][0] * spin[0][j] + turn[i][1] * spin[1][j] + turn[i][2] * spin[2][j])
            * scales[j]
            for j in range(3)
        ]
        for i in range(3)
    ]
    top = [(basis_cam[0][j] - screen_col * basis_cam[2][j]) * inv_depth for j in range(3)]
    low = [(basis_cam[1][j] - screen_row * basis_cam[2][j]) * inv_depth for j in range(3)]
    sigma_a = top[0] * top[0] + top[1] * top[1] + top[2] * top[2]
    sigma_b = top[0] * low[0] + top[1] * low[1] + top[2] * low[2]
    sigma_c = low[0] * low[0] + low[1] * low[1] + low[2] * low[2]
    inv_det = 1.0 / (sigma_a * sigma_c - sigma_b * sigma_b)
    opacity = 1.0 / (1.0 + jnp.exp(-rows[10]))
    inv_dist = 1.0 / jnp.sqrt(offset[0] * offset[0] + offset[1] * offset[1] + offset[2] * offset[2])
    x, y, z = [item * inv_dist for item in offset]
    xx, yy, zz = x * x, y * y, z * z
    basis = [
        None,
        -harmonic_one * y,
        harmonic_one * z,
        -harmonic_one * x,
        harmonic_two[0] * x * y,
        harmonic_two[1] * y * z,
        harmonic_two[2] * (2.0 * zz - xx - yy),
        harmonic_two[3] * x * z,
        harmonic_two[4] * (xx - yy),
        harmonic_three[0] * y * (3.0 * xx - yy),
        harmonic_three[1] * x * y * z,
        harmonic_three[2] * y * (4.0 * zz - xx - yy),
        harmonic_three[3] * z * (2.0 * zz - 3.0 * xx - 3.0 * yy),
        harmonic_three[4] * x * (4.0 * zz - xx - yy),
        harmonic_three[5] * z * (xx - yy),
        harmonic_three[6] * x * (xx - 3.0 * yy),
    ]
    colors = []
    for k in range(3):
        total = harmonic_zero * rows[11 + k]
        for j in range(1, 16):
            total = total + basis[j] * rows[11 + 3 * j + k]
        colors.append(0.5 + total)
    return (
        screen_col,
        screen_row,
        sigma_c * inv_det,
        -sigma_b * inv_det,
        sigma_a * inv_det,
        opacity,
        *colors,
    )


def camera_terms(cam):
    cosines, sines = jnp.cos(cam), jnp.sin(cam)
    cr, cp, cy = [cosines[:, i : i + 1] for i in range(3)]
    sr, sp, sy = [sines[:, i : i + 1] for i in range(3)]
    turn = [
        [cy * cp, cy * sp * sr - sy * cr, cy * sp * cr + sy * sr],
        [sy * cp, sy * sp * sr + cy * cr, sy * sp * cr - cy * sr],
        [-sp, cp * sr, cp * cr],
    ]
    centre = [cam[:, 3 + i : 4 + i] for i in range(3)]
    return turn, centre

MAIN_VMEM = 40 * 2**20
UPDATE_VMEM = 16 * 2**20


def fill_dense(params_ref, dense):
    count, block = params_ref.shape
    for b in range(block // LANES):
        part, line = divmod(b, 8)
        for r in range(0, count, 8):
            size = min(8, count - r)
            where = pl.ds((part * PAD_ROWS + r) * 8 + line, size, stride=8)
            dense[where, :] = params_ref[r : r + size, b * LANES : (b + 1) * LANES]


def dense_rows(dense, part, count):
    return [
        dense[(part * PAD_ROWS + r) * 8 : (part * PAD_ROWS + r) * 8 + 8, :] for r in range(count)
    ]


def lane_pick(source, lanes):
    return jnp.take_along_axis(source, lanes, axis=1, mode="promise_in_bounds")


def gather_eight(load, blocks, index):
    index = jnp.maximum(index, 0)
    lanes, block = index & (LANES - 1), index >> 7
    total = lane_pick(load(0), lanes)
    for b in range(1, blocks):
        total = jnp.where(block == b, lane_pick(load(b), lanes), total)
    return total


def split_three(x):
    first = x.astype(jnp.bfloat16).astype(jnp.float32)
    rest = x - first
    second = rest.astype(jnp.bfloat16).astype(jnp.float32)
    return first, second, rest - second


def fill_hot(hot, index, start, bits):
    row_ids = lax.broadcasted_iota(jnp.int32, (hot.shape[0], LANES), 0)
    low = index & ((1 << bits) - 1)
    hot[:, start : start + LANES] = jnp.where(row_ids == low, 1.0, 0.0).astype(jnp.bfloat16)


def split_two(x):
    first = x.astype(jnp.bfloat16).astype(jnp.float32)
    return first, x - first


def fill_values(lhs, main, last, index, start, bits):
    groups = lhs.shape[0] // 18
    span = slice(start, start + LANES)
    parts = jnp.concatenate(split_two(main), axis=0)
    tips = [jnp.broadcast_to(item, (8, LANES)) for item in split_two(last)]
    high = jnp.broadcast_to(index >> bits, (16, LANES))
    sub = lax.broadcasted_iota(jnp.int32, (8, LANES), 0)
    for b in range(groups):
        lhs[16 * b : 16 * b + 16, span] = jnp.where(high == b, parts, 0.0).astype(jnp.bfloat16)
    for g in range(groups // 8):
        here = high[0:8] == sub + 8 * g
        rows = jnp.concatenate([jnp.where(here, item, 0.0) for item in tips], axis=0)
        row = 16 * groups + 16 * g
        lhs[row : row + 16, span] = rows.astype(jnp.bfloat16)


def scatter_dot(lhs, hot, rows):
    return lax.dot_general(
        lhs[rows], hot[...], (((1,), (1,)), ((), ())), preferred_element_type=jnp.float32
    )


def scatter_main(lhs, hot, first, last):
    out = scatter_dot(lhs, hot, slice(16 * first, 16 * last))
    return [out[16 * b : 16 * b + 8] + out[16 * b + 8 : 16 * b + 16] for b in range(last - first)]


def scatter_tips(lhs, hot):
    groups = lhs.shape[0] // 18
    out = scatter_dot(lhs, hot, slice(16 * groups, 18 * groups))
    return [
        out[16 * (b // 8) + b % 8 : 16 * (b // 8) + b % 8 + 1]
        + out[16 * (b // 8) + 8 + b % 8 : 16 * (b // 8) + 9 + b % 8]
        for b in range(groups)
    ]


def send_features(feat_parts, plan_ref, out_ref, table, last, order):
    halves = plan_ref.shape[1] // LANES
    blocks = last.shape[0]
    for part, feats in enumerate(feat_parts):
        for f in range(8):
            table[pl.ds(part * 64 + f, 8, stride=8), :] = feats[f]
        last[part * 8 : part * 8 + 8, :] = feats[8]
    slots = plan_ref.shape[0] * halves
    for o in range(slots):
        d, h = divmod(o, halves)
        row = plan_ref[d : d + 1, h * LANES : (h + 1) * LANES]
        order[o : o + 1, :] = row
        out_ref[d, 8 * h : 8 * h + 8, :] = gather_eight(
            lambda b: table[8 * b : 8 * b + 8, :], blocks, jnp.broadcast_to(row, (8, LANES))
        )
    for p in range(slots // 8):
        picked = gather_eight(
            lambda b: jnp.broadcast_to(last[b : b + 1, :], (8, LANES)),
            blocks,
            order[8 * p : 8 * p + 8, :],
        )
        for i in range(8 // halves):
            out_ref[8 // halves * p + i, 8 * halves :, :] = picked[i * halves : (i + 1) * halves]


def pixel_terms():
    lane = lax.broadcasted_iota(jnp.int32, (8, LANES), 1)
    inner = lane & 31
    tile = lane >> 5
    x = (inner & 15).astype(jnp.float32) - 7.5
    step = (inner >> 4).astype(jnp.float32) - 0.5
    return tile, x, step


def render_setup(lists_ref, target_ref, order, wanted, basis, plan_sums, hot, bits):
    tiles, entries = lists_ref.shape
    quarters = entries // LANES
    for q in range(quarters):
        order[q * tiles : (q + 1) * tiles, :] = lists_ref[:, q * LANES : (q + 1) * LANES]
    sub = lax.broadcasted_iota(jnp.int32, (8, LANES), 0)
    lane = lax.broadcasted_iota(jnp.int32, (8, LANES), 1)
    tile, x, step = pixel_terms()
    shifted = 32 * (sub & 3) + (lane & 31)
    for k in range(3):
        total = jnp.zeros((8, LANES), jnp.float32)
        for r in range(8):
            row = jnp.broadcast_to(target_ref[k, :, r * LANES : (r + 1) * LANES], (8, LANES))
            here = (tile == r // 2) & ((sub >> 2) == r % 2)
            total = jnp.where(here, lane_pick(row, shifted), total)
        wanted[8 * k : 8 * k + 8, :] = total
    for g in range(LANES // 8):
        row = sub + 8 * g
        coef = (row * 43) >> 9
        mine = tile == (row & 3)

        def column(j, *terms):
            total = jnp.zeros((8, LANES), jnp.float32)
            for c, value in terms:
                total = jnp.where(coef == c, value, total)
            total = jnp.where(mine, total, 0.0)
            basis[8 * g : 8 * g + 8, j * LANES : (j + 1) * LANES] = total

        column(0, (0, x * x), (1, x * step), (2, step * step), (3, x), (4, step), (5, 1.0))
        column(1, (1, x), (2, 2.0 * step), (4, 1.0))
        column(2, (2, 1.0))
        for k in range(3):
            column(3 + k, (6 + k, 1.0))
    mine = tile == (sub & 3)
    for s in range(8):
        y = step + (2.0 * s - 7.0)
        rows = [jnp.ones_like(x), x, y, x * x, x * y, y * y]
        rows = jnp.concatenate([jnp.where(mine, item, 0.0) for item in rows], axis=0)
        for part in range(2):
            start = (part * 8 + s) * LANES
            plan_sums[:, start : start + LANES] = rows.astype(jnp.bfloat16)
    for o in range(tiles * quarters):
        fill_hot(hot, order[o : o + 1, :], o * LANES, bits)


def render_rest(
    cells, copies, recv_ref, order, wanted, back_ref,
    coefs, tables, basis, alpha_s, weight_s, slope_s, joint_g, joint_w, plan_sums, error_sums,
    turned, tinted, moved, pairs, lhs, hot, bits,
):
    owners, packed, _ = recv_ref.shape
    halves = packed // FEATS
    blocks = owners * halves
    tiles = 4
    quarters = order.shape[0] // tiles
    entries = quarters * LANES
    me = lax.axis_index("cells")
    rows_pix = tiles * cells // TILE_COLS * 16
    half_width = TILE_COLS * 8.0
    inv_width = 1.0 / half_width
    log_two = 1.4426950408889634
    sub = lax.broadcasted_iota(jnp.int32, (8, LANES), 0)
    local = sub & 3
    tile_col = 4 * lax.rem(me, TILE_COLS // 4) + local
    tile_row = lax.div(me, TILE_COLS // 4)
    centre_col = (16 * tile_col + 8).astype(jnp.float32) - half_width
    centre_row = (jnp.full((8, LANES), 16 * tile_row + 8, jnp.int32)).astype(
        jnp.float32
    ) - rows_pix * 0.5

    picked = [[None] * FEATS for _ in range(quarters // 2)]
    for k in range(owners):
        origin = lax.rem(me + owners - k, owners)
        if k:
            copies[k - 1].wait()
        for p in range(quarters // 2):
            index = jnp.maximum(order[8 * p : 8 * p + 8, :], 0)
            lanes, block = index & (LANES - 1), index >> 7
            for h in range(halves):
                here = block == origin * halves + h
                for f in range(FEATS):
                    r = 8 * h + f if f < 8 else 8 * halves + h
                    row = jnp.broadcast_to(recv_ref[origin, r : r + 1, :], (8, LANES))
                    item = lane_pick(row, lanes)
                    old = picked[p][f]
                    picked[p][f] = item if old is None else jnp.where(here, item, old)

    for p in range(quarters // 2):
        index = order[8 * p : 8 * p + 8, :]
        feats = picked[p]
        off_col = feats[0] * half_width - centre_col
        off_row = feats[1] * half_width - centre_row
        moved[16 * p : 16 * p + 8, :] = off_col
        moved[16 * p + 8 : 16 * p + 16, :] = off_row
        square = feats[2] * (-0.5 * log_two * inv_width * inv_width)
        cross = feats[3] * (-log_two * inv_width * inv_width)
        bend = feats[4] * (-0.5 * log_two * inv_width * inv_width)
        faint = jnp.maximum(jnp.log(feats[5]) * log_two, -1e30)
        along = square * off_col + cross * off_row
        level = along * off_col + bend * off_row * off_row + jnp.where(index >= 0, faint, -1e30)
        terms = [
            square,
            cross,
            bend,
            -(along + square * off_col),
            -(2.0 * bend * off_row + cross * off_col),
            level,
            feats[6],
            feats[7],
            feats[8],
        ]
        for c, term in enumerate(terms):
            for i, piece in enumerate(split_three(term)):
                row = (3 * c + i) * tiles
                for q in range(2):
                    start = (2 * p + q) * LANES
                    coefs[start + row : start + row + tiles, :] = piece[4 * q : 4 * q + 4]
    for q in range(quarters):
        coefs[q * LANES + 108 : (q + 1) * LANES, :] = jnp.zeros((LANES - 108, LANES), jnp.float32)
    weights = basis[...].astype(jnp.bfloat16)
    for q in range(quarters):
        span = slice(q * LANES, (q + 1) * LANES)
        columns = jnp.transpose(coefs[span, :]).astype(jnp.bfloat16)
        result = jnp.dot(columns, weights, preferred_element_type=jnp.float32)
        for j in range(6):
            tables[j, span, :] = result[:, j * LANES : (j + 1) * LANES]

    height = (2 * sub - 7).astype(jnp.float32)

    def table(l, j):
        return jnp.broadcast_to(tables[j, pl.ds(l, 1), :], (8, LANES))

    def relay(source, base, joint, q, c, s):
        item = source[pl.ds(base + c * 128 + s, 16, stride=8), :]
        top = item.astype(jnp.bfloat16)
        rows = pl.ds(pl.multiple_of(q * LANES, LANES) + c * 16, 16)
        joint[rows, s * LANES : (s + 1) * LANES] = top
        joint[rows, (8 + s) * LANES : (9 + s) * LANES] = (
            item - top.astype(jnp.float32)
        ).astype(jnp.bfloat16)

    chunks = LANES // 16

    def forward(q, carry):
        trans, red, green, blue = carry
        base = pl.multiple_of(q * 8 * LANES, 8 * LANES)
        first = pl.multiple_of(q * LANES, LANES)
        for c in range(chunks):
            for i in range(16):
                l = first + (c * 16 + i)
                where = pl.ds(base + (c * 16 + i) * 8, 8)
                power = table(l, 0) + height * (table(l, 1) + height * table(l, 2))
                alpha = jnp.exp2(power)
                weight = alpha * trans
                alpha_s[where, :] = alpha
                weight_s[where, :] = weight
                trans = trans * (1.0 - alpha)
                red = red + weight * table(l, 3)
                green = green + weight * table(l, 4)
                blue = blue + weight * table(l, 5)
                if c and i % 2:
                    relay(weight_s, base, joint_w, q, c - 1, i // 2)
        for s in range(8):
            relay(weight_s, base, joint_w, q, chunks - 1, s)
        return trans, red, green, blue

    zero = jnp.zeros((8, LANES), jnp.float32)
    carry = lax.fori_loop(
        0, quarters, forward, (jnp.ones((8, LANES), jnp.float32), zero, zero, zero)
    )
    red, green, blue = carry[1:]
    errors = [2.0 * (item - wanted[8 * k : 8 * k + 8, :]) for k, item in enumerate((red, green, blue))]
    wanted[0:8, :], wanted[8:16, :], wanted[16:24, :] = errors
    tile, _, _ = pixel_terms()
    mine = tile == local
    for s in range(8):
        tops, lows = [], []
        for k in range(3):
            row = jnp.broadcast_to(wanted[8 * k + s : 8 * k + s + 1, :], (8, LANES))
            row = jnp.where(mine, row, 0.0)
            top = row.astype(jnp.bfloat16).astype(jnp.float32)
            tops.append(top)
            lows.append(row - top)
        blank = [jnp.zeros((24, LANES), jnp.float32)]
        start = s * LANES
        error_sums[:, start : start + LANES] = jnp.concatenate(tops + lows, axis=0).astype(jnp.bfloat16)
        start = (8 + s) * LANES
        error_sums[:, start : start + LANES] = jnp.concatenate(tops + blank, axis=0).astype(jnp.bfloat16)

    def sum_pixels(factors, joint, result, q):
        span = pl.ds(pl.multiple_of(q * LANES, LANES), LANES)
        result[:, span] = lax.dot_general(
            factors[...],
            joint[span, :],
            (((1,), (1,)), ((), ())),
            preferred_element_type=jnp.float32,
        )

    def backward(q, behind, late):
        base = pl.multiple_of(q * 8 * LANES, 8 * LANES)
        first = pl.multiple_of(q * LANES, LANES)
        sum_pixels(error_sums, joint_w, tinted, q)
        if late:
            sum_pixels(plan_sums, joint_g, turned, q + 1)
        for c in range(chunks - 1, -1, -1):
            for i in range(15, -1, -1):
                l = first + (c * 16 + i)
                where = pl.ds(base + (c * 16 + i) * 8, 8)
                slope = errors[0] * table(l, 3) + errors[1] * table(l, 4) + errors[2] * table(l, 5)
                alpha = alpha_s[where, :]
                slope_s[(c * 16 + i) * 8 : (c * 16 + i) * 8 + 8, :] = weight_s[where, :] * (
                    slope - behind
                )
                behind = (1.0 - alpha) * behind + alpha * slope
                if c < chunks - 1 and i % 2:
                    relay(slope_s, 0, joint_g, q, c + 1, i // 2)
        for s in range(8):
            relay(slope_s, 0, joint_g, q, 0, s)
        return behind

    behind = backward(quarters - 1, zero, False)
    lax.fori_loop(1, quarters, lambda i, v: backward(quarters - 1 - i, v, True), behind)
    sum_pixels(plan_sums, joint_g, turned, 0)
    for p in range(quarters // 2):
        off_col = moved[16 * p : 16 * p + 8, :]
        off_row = moved[16 * p + 8 : 16 * p + 16, :]

        def quantity(j):
            source, r = (turned, j) if j < 6 else (tinted, j - 6)
            rows = slice(8 * r, 8 * r + 8)
            start = 2 * p * LANES
            return jnp.where(
                sub < 4,
                source[rows, start : start + LANES],
                source[rows, start + LANES : start + 2 * LANES],
            )

        plain, across, down = quantity(0), quantity(1), quantity(2)
        near_col = across - off_col * plain
        near_row = down - off_row * plain
        rows = [
            plain,
            near_col * inv_width,
            near_row * inv_width,
            (quantity(3) - off_col * (across + near_col)) * (inv_width * inv_width),
            (quantity(4) - off_col * down - off_row * near_col) * (inv_width * inv_width),
            (quantity(5) - off_row * (down + near_row)) * (inv_width * inv_width),
            *[quantity(6 + k) + quantity(9 + k) for k in range(3)],
        ]
        for f, item in enumerate(rows):
            pairs[pl.ds(p * 128 + f, 8, stride=16), :] = item
    for o in range(tiles * quarters):
        fill_values(
            lhs,
            pairs[o * 16 : o * 16 + 8, :],
            pairs[o * 16 + 8 : o * 16 + 9, :],
            order[o : o + 1, :],
            o * LANES,
            bits,
        )
    for s, (main, last) in enumerate(zip(scatter_main(lhs, hot, 0, owners), scatter_tips(lhs, hot))):
        for h in range(halves):
            span = slice(h * LANES, (h + 1) * LANES)
            back_ref[s, 8 * h : 8 * h + 8, :] = main[:, span]
            back_ref[s, 8 * halves + h : 8 * halves + h + 1, :] = last[:, span]


def main_kernel(
    params_in, cam_in, plan_in, visible_in, lists_in, target_in, out_ref,
    params_ref, cam_ref, plan_ref, visible_ref, lists_ref, target_ref, dense, table, last, plan_order, outgoing, incoming, back, returned, mine, extra, extras, shared,
    order, wanted, basis, coefs, tables, alpha_s, weight_s, slope_s, joint_g, joint_w,
    plan_sums, error_sums, turned, tinted, moved, pairs, lhs, hot, own_lhs, own_hot,
    send_one, recv_one, send_two, recv_two, send_three, recv_three, send_four, recv_four, local_sem,
):
    cells, views = lax.axis_size("cells"), lax.axis_size("views")
    cell, view = lax.axis_index("cells"), lax.axis_index("views")
    count, block = params_ref.shape
    blocks = block // LANES
    capacity = plan_ref.shape[1]
    halves = capacity // LANES
    bits = capacity.bit_length() - 1
    fetches = [
        pltpu.make_async_copy(source, dest, local_sem.at[i])
        for i, (source, dest) in enumerate(
            (
                (params_in, params_ref),
                (cam_in, cam_ref),
                (plan_in, plan_ref),
                (visible_in, visible_ref),
                (lists_in, lists_ref),
                (target_in, target_ref),
            )
        )
    ]
    for fetch in fetches:
        fetch.start()
    barrier = pltpu.get_barrier_semaphore()

    def greet(axis, me, size):
        for k in range(1, size):
            pl.semaphore_signal(
                barrier,
                inc=1,
                device_id={axis: lax.rem(me + k, size)},
                device_id_type=pl.DeviceIdType.MESH,
            )

    def send_all(axis, me, size, source, dest, send_sem, recv_sem):
        copies = []
        for k in range(1, size):
            peer = lax.rem(me + k, size)
            copy = pltpu.make_async_remote_copy(
                src_ref=source(peer),
                dst_ref=dest(me),
                send_sem=send_sem.at[k - 1],
                recv_sem=recv_sem.at[k - 1],
                device_id={axis: peer},
                device_id_type=pl.DeviceIdType.MESH,
            )
            copy.start()
            copies.append(copy)
        return copies

    greet("cells", cell, cells)
    greet("views", view, views)
    fetches[1].wait()
    turn, centre = camera_terms(cam_ref[...])
    known = [*turn[0], *turn[1], *turn[2], *centre]
    lane = lax.broadcasted_iota(jnp.int32, (8, LANES), 1)
    line = jnp.zeros((8, LANES), jnp.float32)
    for i, item in enumerate(known):
        line = jnp.where(lane == i, jnp.broadcast_to(item, (8, LANES)), line)
    extra[blocks : blocks + 8, :] = line
    fetches[3].wait()
    for b in range(blocks):
        extra[b : b + 1, :] = visible_ref[:, b * LANES : (b + 1) * LANES].astype(jnp.float32)
    fetches[0].wait()
    fill_dense(params_ref, dense)
    feat_parts = [
        project_rows(dense_rows(dense, part, count), turn, centre) for part in range(blocks // 8)
    ]
    fetches[2].wait()
    send_features(feat_parts, plan_ref, outgoing, table, last, plan_order)
    pl.semaphore_wait(barrier, cells + views - 2)

    first = send_all(
        "cells", cell, cells, lambda p: outgoing.at[p], lambda p: incoming.at[p], send_one, recv_one
    )
    fourth = send_all(
        "views", view, views, lambda p: extra, lambda p: extras.at[p], send_four, recv_four
    )
    incoming[cell] = outgoing[cell]
    extras[view] = extra[...]
    fetches[4].wait()
    fetches[5].wait()
    render_setup(lists_ref, target_ref, order, wanted, basis, plan_sums, hot, bits)
    render_rest(
        cells, first, incoming, order, wanted, back,
        coefs, tables, basis, alpha_s, weight_s, slope_s, joint_g, joint_w, plan_sums, error_sums,
        turned, tinted, moved, pairs, lhs, hot, bits,
    )
    second = send_all(
        "cells", cell, cells, lambda p: back.at[p], lambda p: returned.at[p], send_two, recv_two
    )
    returned[cell] = back[cell]
    wide = own_hot.shape[0].bit_length() - 1
    spots = []
    for k in range(cells):
        origin = lax.rem(cell + cells - k, cells)
        for h in range(halves):
            row = plan_order[pl.ds(origin * halves + h, 1), :]
            fill_hot(own_hot, row, (k * halves + h) * LANES, wide)
            spots.append((k, h, origin, row))
    for k, h, origin, row in spots:
        if k and h == 0:
            second[k - 1].wait()
        fill_values(
            own_lhs,
            returned[origin, 8 * h : 8 * h + 8, :],
            returned[origin, 8 * halves + h : 8 * halves + h + 1, :],
            row,
            (k * halves + h) * LANES,
            wide,
        )
    tips = scatter_tips(own_lhs, own_hot)
    parts = blocks // 8
    third = []
    for part in range(parts):
        for g, main in enumerate(scatter_main(own_lhs, own_hot, 4 * part, 4 * part + 4)):
            for i in range(2):
                span = slice(i * LANES, (i + 1) * LANES)
                for f in range(8):
                    mine[part, f * 8 + 2 * g + i : f * 8 + 2 * g + i + 1, :] = main[f : f + 1, span]
                mine[part, 64 + 2 * g + i : 64 + 2 * g + i + 1, :] = tips[4 * part + g][:, span]
        third.append(
            send_all(
                "views", view, views,
                lambda p: mine.at[part], lambda p: shared.at[p, part],
                send_three.at[part], recv_three.at[part],
            )
        )
    for copy in fourth:
        copy.wait()
    counts = extras[0, 0:blocks, :]
    for v in range(1, views):
        counts = counts + extras[v, 0:blocks, :]
    grads = blocks * PAD_ROWS
    out_ref[grads : grads + blocks, :] = counts

    def pull_view(fresh, part, source, lines):
        known = [jnp.broadcast_to(lines[:, i : i + 1], (8, LANES)) for i in range(12)]
        turn = [known[0:3], known[3:6], known[6:9]]
        centre = known[9:12]
        rows = dense_rows(dense, part, count)
        feats, pull = jax.vjp(lambda *items: project_rows(items, turn, centre), *rows)
        got = [source[8 * f : 8 * f + 8, :] for f in range(FEATS)]
        pulled = pull(
            (
                feats[2] * got[1] + feats[3] * got[2],
                feats[3] * got[1] + feats[4] * got[2],
                -0.5 * got[3],
                -got[4],
                -0.5 * got[5],
                got[0] / feats[5],
                got[6],
                got[7],
                got[8],
            )
        )
        for r, item in enumerate(pulled):
            where = slice((part * PAD_ROWS + r) * 8, (part * PAD_ROWS + r) * 8 + 8)
            out_ref[where, :] = item if fresh else out_ref[where, :] + item

    for part in range(parts):
        pull_view(True, part, mine.at[part], extra[blocks : blocks + 1, :])
    for part in range(parts):
        for k in range(1, views):
            third[part][views - 1 - k].wait()
            origin = lax.rem(view + k, views)
            pull_view(False, part, shared.at[origin, part], extras[origin, blocks : blocks + 1, :])


def update_kernel(params_ref, first_ref, second_ref, grads_ref, new_ref, new_first_ref, new_second_ref):
    count, block = params_ref.shape
    blocks = block // LANES
    row_ids = lax.broadcasted_iota(jnp.int32, (8, LANES), 0)
    bias_one = 1.0 - 0.9**ADAM_STEP
    bias_two = 1.0 - 0.999**ADAM_STEP
    for b in range(blocks):
        span = slice(b * LANES, (b + 1) * LANES)
        part, line = divmod(b, 8)
        counts = grads_ref[blocks * PAD_ROWS + b : blocks * PAD_ROWS + b + 1, :]
        for r in range(0, count, 8):
            size = min(8, count - r)
            rows = slice(r, r + size)
            gradient = grads_ref[pl.ds((part * PAD_ROWS + r) * 8 + line, size, stride=8), :]
            if r >= 16:
                rates = 0.000125
            else:
                ids = row_ids[0:size] + r
                rates = jnp.where(
                    ids < 6,
                    0.01,
                    jnp.where(
                        ids < 10,
                        0.005,
                        jnp.where(ids < 11, 0.05, jnp.where(ids < 14, 0.0025, 0.000125)),
                    ),
                )
            params, first, second = params_ref[rows, span], first_ref[rows, span], second_ref[rows, span]
            seen = jnp.broadcast_to(counts, params.shape) > 0.0
            first_new = 0.9 * first + 0.1 * gradient
            second_new = 0.999 * second + 0.001 * gradient * gradient
            stride = rates * (first_new / bias_one) / (jnp.sqrt(second_new / bias_two) + 1e-08)
            new_ref[rows, span] = jnp.where(seen, params - stride, params)
            new_first_ref[rows, span] = jnp.where(seen, first_new, first)
            new_second_ref[rows, span] = jnp.where(seen, second_new, second)


def fused_shards(params, first_moment, second_moment, cameras, visible, send_plan, tile_lists, target):
    cells, views = lax.axis_size("cells"), lax.axis_size("views")
    count, block = params.shape
    blocks = block // LANES
    plan = send_plan[0, 0]
    lists = tile_lists[0]
    tiles, entries = lists.shape
    capacity = plan.shape[1]
    halves = capacity // LANES
    slots = cells * halves
    f32, bf16 = jnp.float32, jnp.bfloat16
    packet = pltpu.VMEM((cells, FEATS * halves, LANES), f32)
    dma = pltpu.SemaphoreType.DMA
    vmem = pl.BlockSpec(memory_space=pltpu.VMEM)
    grads = pl.pallas_call(
        main_kernel,
        out_shape=jax.ShapeDtypeStruct((blocks * PAD_ROWS + blocks, LANES), f32),
        in_specs=[pl.BlockSpec(memory_space=pltpu.HBM)] * 6,
        out_specs=vmem,
        scratch_shapes=[
            pltpu.VMEM((count, block), f32),
            pltpu.VMEM(cameras.shape, f32),
            pltpu.VMEM(plan.shape, jnp.int32),
            pltpu.VMEM(visible.shape, jnp.int32),
            pltpu.VMEM(lists.shape, jnp.int32),
            pltpu.VMEM((3, 1, target.shape[2]), f32),
            pltpu.VMEM((blocks * PAD_ROWS, LANES), f32),
            pltpu.VMEM((blocks * 8, LANES), f32),
            pltpu.VMEM((blocks, LANES), f32),
            pltpu.VMEM((slots, LANES), jnp.int32),
            packet, packet, packet, packet,
            pltpu.VMEM((blocks // 8, FEATS * 8, LANES), f32),
            pltpu.VMEM((blocks + 8, LANES), f32),
            pltpu.VMEM((views, blocks + 8, LANES), f32),
            pltpu.VMEM((views, blocks // 8, FEATS * 8, LANES), f32),
            pltpu.VMEM((tiles * entries // LANES, LANES), jnp.int32),
            pltpu.VMEM((24, LANES), f32),
            pltpu.VMEM((LANES, 6 * LANES), f32),
            pltpu.VMEM((entries, LANES), f32),
            pltpu.VMEM((6, entries, LANES), f32),
            pltpu.VMEM((entries * 8, LANES), f32),
            pltpu.VMEM((entries * 8, LANES), f32),
            pltpu.VMEM((8 * LANES, LANES), f32),
            pltpu.VMEM((entries, 16 * LANES), bf16),
            pltpu.VMEM((entries, 16 * LANES), bf16),
            pltpu.VMEM((48, 16 * LANES), bf16),
            pltpu.VMEM((48, 16 * LANES), bf16),
            pltpu.VMEM((48, entries), f32),
            pltpu.VMEM((48, entries), f32),
            pltpu.VMEM((entries // LANES * 8, LANES), f32),
            pltpu.VMEM((tiles * entries // LANES * 16, LANES), f32),
            pltpu.VMEM((cells * 18, tiles * entries), bf16),
            pltpu.VMEM((capacity, tiles * entries), bf16),
            pltpu.VMEM((blocks // 2 * 18, slots * LANES), bf16),
            pltpu.VMEM((2 * LANES, slots * LANES), bf16),
            dma((cells - 1,)), dma((cells - 1,)), dma((cells - 1,)), dma((cells - 1,)),
            dma((blocks // 8, views - 1)), dma((blocks // 8, views - 1)), dma((views - 1,)), dma((views - 1,)),
            dma((6,)),
        ],
        compiler_params=pltpu.CompilerParams(
            collective_id=0, has_side_effects=True, vmem_limit_bytes=MAIN_VMEM
        ),
        cost_estimate=pl.CostEstimate(
            flops=4096 * tiles * 256 * entries,
            bytes_accessed=4 * count * block,
            transcendentals=tiles * 256 * entries,
        ),
    )(
        *[
            pltpu.with_memory_space_constraint(item, pltpu.HBM)
            for item in (params, cameras, plan, visible, lists, jnp.transpose(target, (1, 0, 2)))
        ]
    )
    like = jax.ShapeDtypeStruct(params.shape, f32)
    return tuple(
        pl.pallas_call(
            update_kernel,
            out_shape=(like, like, like),
            compiler_params=pltpu.CompilerParams(vmem_limit_bytes=UPDATE_VMEM),
        )(params, first_moment, second_moment, grads)
    )


def local_shards(params, first_moment, second_moment, cameras, visible, send_plan, tile_lists, target):
    capacity = send_plan.shape[3]
    tiles, entries = tile_lists.shape[1:]
    halves = capacity // LANES
    fits = (
        capacity % LANES == 0
        and params.shape[1] % (16 * LANES) == 0
        and entries % (2 * LANES) == 0
        and 8 % max(halves, 1) == 0
        and lax.axis_size("cells") % 8 == 0
        and tiles * entries <= 4096
        and tiles == 4
    )
    body = fused_shards if fits else shards
    return body(params, first_moment, second_moment, cameras, visible, send_plan, tile_lists, target)


def solution(mesh):
    in_specs = (
        P(None, "cells"),
        P(None, "cells"),
        P(None, "cells"),
        P("views", None),
        P("views", "cells"),
        P("views", "cells", None, None),
        P("views", "cells", None),
        P("views", None, "cells"),
    )
    out_specs = (P(None, "cells"), P(None, "cells"), P(None, "cells"))
    return jax.shard_map(local_shards, mesh=mesh, in_specs=in_specs, out_specs=out_specs, check_vma=False)
```

```python
import functools

import jax
import jax.numpy as jnp
from jax import lax
from jax.experimental import pallas as pl
from jax.experimental.pallas import tpu as pltpu
from jax.sharding import PartitionSpec as P

TILE_COLS = 32
ADAM_STEP = 1000


harmonic_zero = 0.28209479177387814
harmonic_one = 0.4886025119029199
harmonic_two = (
    1.0925484305920792,
    -1.0925484305920792,
    0.31539156525252005,
    -1.0925484305920792,
    0.5462742152960396,
)
harmonic_three = (
    -0.5900435899266435,
    2.890611442640554,
    -0.4570457994644658,
    0.3731763325901154,
    -0.4570457994644658,
    1.445305721320277,
    -0.5900435899266435,
)


def harmonics(across, upward, onward):
    across_sq = across * across
    upward_sq = upward * upward
    onward_sq = onward * onward
    return jnp.stack(
        [
            harmonic_zero * jnp.ones_like(across),
            -harmonic_one * upward,
            harmonic_one * onward,
            -harmonic_one * across,
            harmonic_two[0] * across * upward,
            harmonic_two[1] * upward * onward,
            harmonic_two[2] * (2.0 * onward_sq - across_sq - upward_sq),
            harmonic_two[3] * across * onward,
            harmonic_two[4] * (across_sq - upward_sq),
            harmonic_three[0] * upward * (3.0 * across_sq - upward_sq),
            harmonic_three[1] * across * upward * onward,
            harmonic_three[2] * upward * (4.0 * onward_sq - across_sq - upward_sq),
            harmonic_three[3] * onward * (2.0 * onward_sq - 3.0 * across_sq - 3.0 * upward_sq),
            harmonic_three[4] * across * (4.0 * onward_sq - across_sq - upward_sq),
            harmonic_three[5] * onward * (across_sq - upward_sq),
            harmonic_three[6] * across * (across_sq - 3.0 * upward_sq),
        ]
    )


def camera_rotation(angles):
    cos_roll, sin_roll = (jnp.cos(angles[0]), jnp.sin(angles[0]))
    cos_pitch, sin_pitch = (jnp.cos(angles[1]), jnp.sin(angles[1]))
    cos_yaw, sin_yaw = (jnp.cos(angles[2]), jnp.sin(angles[2]))
    naught = jnp.zeros_like(cos_roll)
    unit_one = jnp.ones_like(cos_roll)
    roll = jnp.stack(
        [
            jnp.stack([unit_one, naught, naught]),
            jnp.stack([naught, cos_roll, -sin_roll]),
            jnp.stack([naught, sin_roll, cos_roll]),
        ]
    )
    pitch = jnp.stack(
        [
            jnp.stack([cos_pitch, naught, sin_pitch]),
            jnp.stack([naught, unit_one, naught]),
            jnp.stack([-sin_pitch, naught, cos_pitch]),
        ]
    )
    yawing = jnp.stack(
        [
            jnp.stack([cos_yaw, -sin_yaw, naught]),
            jnp.stack([sin_yaw, cos_yaw, naught]),
            jnp.stack([naught, naught, unit_one]),
        ]
    )
    inner_turn = jnp.dot(pitch, roll, precision=lax.Precision.HIGHEST)
    return jnp.dot(yawing, inner_turn, precision=lax.Precision.HIGHEST)


def project(values, camera):
    turn = camera_rotation(camera[0:3])
    offset = values[0:3] - camera[3:6][:, None]
    in_view = jnp.dot(turn, offset, precision=lax.Precision.HIGHEST)
    inv_depth = 1.0 / in_view[2]
    screen_col = in_view[0] * inv_depth
    screen_row = in_view[1] * inv_depth
    scales = jnp.exp(values[3:6])
    quat = values[6:10] / jnp.sqrt(jnp.sum(values[6:10] * values[6:10], axis=0, keepdims=True))
    quat_w, quat_x, quat_y, quat_z = (quat[0], quat[1], quat[2], quat[3])
    spin = [
        [
            1.0 - 2.0 * (quat_y * quat_y + quat_z * quat_z),
            2.0 * (quat_x * quat_y - quat_w * quat_z),
            2.0 * (quat_x * quat_z + quat_w * quat_y),
        ],
        [
            2.0 * (quat_x * quat_y + quat_w * quat_z),
            1.0 - 2.0 * (quat_x * quat_x + quat_z * quat_z),
            2.0 * (quat_y * quat_z - quat_w * quat_x),
        ],
        [
            2.0 * (quat_x * quat_z - quat_w * quat_y),
            2.0 * (quat_y * quat_z + quat_w * quat_x),
            1.0 - 2.0 * (quat_x * quat_x + quat_y * quat_y),
        ],
    ]
    basis_cam = []
    for outer_index in range(3):
        row_terms = []
        for col_index in range(3):
            entry = turn[outer_index, 0] * spin[0][col_index]
            for mid_index in range(1, 3):
                entry = entry + turn[outer_index, mid_index] * spin[mid_index][col_index]
            row_terms.append(entry * scales[col_index])
        basis_cam.append(row_terms)
    jac_top = [
        (basis_cam[0][col_index] - screen_col * basis_cam[2][col_index]) * inv_depth
        for col_index in range(3)
    ]
    jac_low = [
        (basis_cam[1][col_index] - screen_row * basis_cam[2][col_index]) * inv_depth
        for col_index in range(3)
    ]
    sigma_a = jac_top[0] * jac_top[0] + jac_top[1] * jac_top[1] + jac_top[2] * jac_top[2]
    sigma_b = jac_top[0] * jac_low[0] + jac_top[1] * jac_low[1] + jac_top[2] * jac_low[2]
    sigma_c = jac_low[0] * jac_low[0] + jac_low[1] * jac_low[1] + jac_low[2] * jac_low[2]
    determinant = sigma_a * sigma_c - sigma_b * sigma_b
    opacity = jax.nn.sigmoid(values[10])
    distance = jnp.sqrt(jnp.sum(offset * offset, axis=0))
    unit_dir = offset / distance
    basis = harmonics(unit_dir[0], unit_dir[1], unit_dir[2])
    coeffs = values[11:59].reshape(16, 3, values.shape[1])
    colors = 0.5 + jnp.sum(basis[:, None, :] * coeffs, axis=0)
    screen = jnp.stack(
        [
            screen_col,
            screen_row,
            sigma_c / determinant,
            -sigma_b / determinant,
            sigma_a / determinant,
            opacity,
        ]
    )
    return jnp.concatenate([screen, colors], axis=0)


def group_loss(pieces):
    features, live_mask, pixel_column, pixel_row, target_tile = pieces
    entries = live_mask.shape[1]
    delta_col = pixel_column[:, :, None] - features[0][:, None, :]
    delta_row = pixel_row[:, :, None] - features[1][:, None, :]
    power = -0.5 * (
        features[2][:, None, :] * delta_col * delta_col
        + 2.0 * features[3][:, None, :] * delta_col * delta_row
        + features[4][:, None, :] * delta_row * delta_row
    )
    alphas = features[5][:, None, :] * jnp.exp(power) * live_mask[:, None, :]
    log_keep = jnp.log(1.0 - alphas)
    earlier = (
        lax.broadcasted_iota(jnp.int32, (entries, entries), 0)
        < lax.broadcasted_iota(jnp.int32, (entries, entries), 1)
    ).astype(jnp.float32)
    transmit = jnp.exp(
        jnp.einsum("bpl,lm->bpm", log_keep, earlier, precision=lax.Precision.HIGHEST)
    )
    weights = alphas * transmit
    image = jnp.einsum("bpl,kbl->kbp", weights, features[6:9], precision=lax.Precision.HIGHEST)
    error = image - target_tile
    return jnp.sum(error * error)


def render_tiles(picked, live_mask, pixel_column, pixel_row, target_tile):
    groups = live_mask.shape[0] // 4
    entries = live_mask.shape[1]
    pixels = pixel_column.shape[1]
    stacked = (
        jnp.transpose(picked.reshape(picked.shape[0], groups, 4, entries), (1, 0, 2, 3)),
        live_mask.reshape(groups, 4, entries),
        pixel_column.reshape(groups, 4, pixels),
        pixel_row.reshape(groups, 4, pixels),
        jnp.transpose(target_tile.reshape(3, groups, 4, pixels), (1, 0, 2, 3)),
    )
    return jnp.sum(lax.map(jax.checkpoint(group_loss), stacked))


def pixel_grid(first_tile, count, tiles_dev, rows_pix):
    tile_ids = first_tile + jnp.arange(count, dtype=jnp.int32)
    pixel_ids = jnp.arange(256, dtype=jnp.int32)
    block_cols = TILE_COLS // 4
    owner_ids = tile_ids // tiles_dev
    local_ids = tile_ids % tiles_dev
    tile_col = 4 * (owner_ids % block_cols) + local_ids % 4
    tile_row = tiles_dev // 4 * (owner_ids // block_cols) + local_ids // 4
    half_width = TILE_COLS * 8.0
    column = (tile_col[:, None] * 16 + pixel_ids[None, :] % 16).astype(jnp.float32)
    row_pos = (tile_row[:, None] * 16 + pixel_ids[None, :] // 16).astype(jnp.float32)
    return ((column + 0.5 - half_width) / half_width, (row_pos + 0.5 - rows_pix * 0.5) / half_width)


def adam_update(params, first_moment, second_moment, gradient, counts):
    row_ids = lax.broadcasted_iota(jnp.int32, params.shape, 0)
    rates = jnp.where(
        row_ids < 6,
        0.01,
        jnp.where(
            row_ids < 10,
            0.005,
            jnp.where(row_ids < 11, 0.05, jnp.where(row_ids < 14, 0.0025, 0.000125)),
        ),
    )
    first_new = 0.9 * first_moment + 0.1 * gradient
    second = 0.999 * second_moment + 0.001 * gradient * gradient
    bias_one = 1.0 - 0.9**ADAM_STEP
    bias_two = 1.0 - 0.999**ADAM_STEP
    stride = rates * (first_new / bias_one) / (jnp.sqrt(second / bias_two) + 1e-08)
    seen_mask = counts > 0.0
    return (
        jnp.where(seen_mask, params - stride, params),
        jnp.where(seen_mask, first_new, first_moment),
        jnp.where(seen_mask, second, second_moment),
    )


def shards(params, first_moment, second_moment, cameras, visible, send_plan, tile_lists, target):
    cells = lax.axis_size("cells")
    camera = cameras[0]
    plan_rows = send_plan[0, 0]
    capacity = plan_rows.shape[1]
    sent_live = (plan_rows >= 0)[None]
    sent_rows = jnp.maximum(plan_rows, 0)
    lists = tile_lists[0]
    tiles_here = lists.shape[0]
    live_mask = (lists >= 0).astype(jnp.float32)
    slot_ids = jnp.maximum(lists, 0)
    rows_pix = tiles_here * cells // TILE_COLS * 16
    pixel_column, pixel_row = pixel_grid(
        lax.axis_index("cells") * tiles_here, tiles_here, tiles_here, rows_pix
    )
    target_tile = target[0].reshape(3, tiles_here, 256)
    block = params.shape[1]

    def image_loss(table):
        picked = jnp.take(table, slot_ids, axis=1)
        return render_tiles(picked, live_mask, pixel_column, pixel_row, target_tile)

    def own_projection(values):
        return project(values, camera)

    features, project_pull = jax.vjp(own_projection, params)
    outgoing = jnp.take(features, sent_rows, axis=1)
    incoming = lax.all_to_all(outgoing, "cells", split_axis=1, concat_axis=1, tiled=True)
    loss_value, pullback = jax.vjp(
        image_loss, incoming.reshape(features.shape[0], cells * capacity)
    )
    table_grad = pullback(jnp.ones((), jnp.float32))[0]
    returned = lax.all_to_all(
        table_grad.reshape(features.shape[0], cells, capacity),
        "cells",
        split_axis=1,
        concat_axis=1,
        tiled=True,
    )
    kept = jnp.where(sent_live, returned, 0.0)
    gradient = project_pull(
        jnp.zeros((features.shape[0], block), jnp.float32).at[:, sent_rows].add(kept)
    )[0]
    seen_here = visible.astype(jnp.float32)
    total_grad, counts = lax.psum((gradient, seen_here), "views")
    new_params, new_first, new_second = adam_update(
        params, first_moment, second_moment, total_grad, counts
    )
    return (new_params, new_first, new_second)

LANES = 128
PAD_ROWS = 64
FEATS = 9


def project_rows(rows, turn, centre):
    offset = [rows[i] - centre[i] for i in range(3)]
    in_view = [
        turn[i][0] * offset[0] + turn[i][1] * offset[1] + turn[i][2] * offset[2] for i in range(3)
    ]
    inv_depth = 1.0 / in_view[2]
    screen_col = in_view[0] * inv_depth
    screen_row = in_view[1] * inv_depth
    scales = [jnp.exp(rows[3 + i]) for i in range(3)]
    raw = rows[6:10]
    norm = jnp.sqrt(raw[0] * raw[0] + raw[1] * raw[1] + raw[2] * raw[2] + raw[3] * raw[3])
    inv_norm = 1.0 / norm
    quat_w, quat_x, quat_y, quat_z = [item * inv_norm for item in raw]
    spin = [
        [
            1.0 - 2.0 * (quat_y * quat_y + quat_z * quat_z),
            2.0 * (quat_x * quat_y - quat_w * quat_z),
            2.0 * (quat_x * quat_z + quat_w * quat_y),
        ],
        [
            2.0 * (quat_x * quat_y + quat_w * quat_z),
            1.0 - 2.0 * (quat_x * quat_x + quat_z * quat_z),
            2.0 * (quat_y * quat_z - quat_w * quat_x),
        ],
        [
            2.0 * (quat_x * quat_z - quat_w * quat_y),
            2.0 * (quat_y * quat_z + quat_w * quat_x),
            1.0 - 2.0 * (quat_x * quat_x + quat_y * quat_y),
        ],
    ]
    basis_cam = [
        [
            (turn[i][0] * spin[0][j] + turn[i][1] * spin[1][j] + turn[i][2] * spin[2][j])
            * scales[j]
            for j in range(3)
        ]
        for i in range(3)
    ]
    top = [(basis_cam[0][j] - screen_col * basis_cam[2][j]) * inv_depth for j in range(3)]
    low = [(basis_cam[1][j] - screen_row * basis_cam[2][j]) * inv_depth for j in range(3)]
    sigma_a = top[0] * top[0] + top[1] * top[1] + top[2] * top[2]
    sigma_b = top[0] * low[0] + top[1] * low[1] + top[2] * low[2]
    sigma_c = low[0] * low[0] + low[1] * low[1] + low[2] * low[2]
    inv_det = 1.0 / (sigma_a * sigma_c - sigma_b * sigma_b)
    opacity = 1.0 / (1.0 + jnp.exp(-rows[10]))
    inv_dist = 1.0 / jnp.sqrt(offset[0] * offset[0] + offset[1] * offset[1] + offset[2] * offset[2])
    x, y, z = [item * inv_dist for item in offset]
    xx, yy, zz = x * x, y * y, z * z
    basis = [
        None,
        -harmonic_one * y,
        harmonic_one * z,
        -harmonic_one * x,
        harmonic_two[0] * x * y,
        harmonic_two[1] * y * z,
        harmonic_two[2] * (2.0 * zz - xx - yy),
        harmonic_two[3] * x * z,
        harmonic_two[4] * (xx - yy),
        harmonic_three[0] * y * (3.0 * xx - yy),
        harmonic_three[1] * x * y * z,
        harmonic_three[2] * y * (4.0 * zz - xx - yy),
        harmonic_three[3] * z * (2.0 * zz - 3.0 * xx - 3.0 * yy),
        harmonic_three[4] * x * (4.0 * zz - xx - yy),
        harmonic_three[5] * z * (xx - yy),
        harmonic_three[6] * x * (xx - 3.0 * yy),
    ]
    colors = []
    for k in range(3):
        total = harmonic_zero * rows[11 + k]
        for j in range(1, 16):
            total = total + basis[j] * rows[11 + 3 * j + k]
        colors.append(0.5 + total)
    return (
        screen_col,
        screen_row,
        sigma_c * inv_det,
        -sigma_b * inv_det,
        sigma_a * inv_det,
        opacity,
        *colors,
    )


def camera_terms(cam):
    cosines, sines = jnp.cos(cam), jnp.sin(cam)
    cr, cp, cy = [cosines[:, i : i + 1] for i in range(3)]
    sr, sp, sy = [sines[:, i : i + 1] for i in range(3)]
    turn = [
        [cy * cp, cy * sp * sr - sy * cr, cy * sp * cr + sy * sr],
        [sy * cp, sy * sp * sr + cy * cr, sy * sp * cr - cy * sr],
        [-sp, cp * sr, cp * cr],
    ]
    centre = [cam[:, 3 + i : 4 + i] for i in range(3)]
    return turn, centre

MAIN_VMEM = 40 * 2**20
UPDATE_VMEM = 16 * 2**20


def fill_dense(params_ref, dense):
    count, block = params_ref.shape
    for b in range(block // LANES):
        part, line = divmod(b, 8)
        for r in range(0, count, 8):
            size = min(8, count - r)
            where = pl.ds((part * PAD_ROWS + r) * 8 + line, size, stride=8)
            dense[where, :] = params_ref[r : r + size, b * LANES : (b + 1) * LANES]


def dense_rows(dense, part, count):
    return [
        dense[(part * PAD_ROWS + r) * 8 : (part * PAD_ROWS + r) * 8 + 8, :] for r in range(count)
    ]


def lane_pick(source, lanes):
    return jnp.take_along_axis(source, lanes, axis=1, mode="promise_in_bounds")


def gather_eight(load, blocks, index):
    index = jnp.maximum(index, 0)
    lanes, block = index & (LANES - 1), index >> 7
    total = lane_pick(load(0), lanes)
    for b in range(1, blocks):
        total = jnp.where(block == b, lane_pick(load(b), lanes), total)
    return total


def split_three(x):
    first = x.astype(jnp.bfloat16).astype(jnp.float32)
    rest = x - first
    second = rest.astype(jnp.bfloat16).astype(jnp.float32)
    return first, second, rest - second


def fill_hot(hot, index, start, bits):
    row_ids = lax.broadcasted_iota(jnp.int32, (hot.shape[0], LANES), 0)
    low = index & ((1 << bits) - 1)
    hot[:, start : start + LANES] = jnp.where(row_ids == low, 1.0, 0.0).astype(jnp.bfloat16)


def split_two(x):
    first = x.astype(jnp.bfloat16).astype(jnp.float32)
    return first, x - first


def fill_values(lhs, main, last, index, start, bits):
    groups = lhs.shape[0] // 18
    span = slice(start, start + LANES)
    parts = jnp.concatenate(split_two(main), axis=0)
    tips = [jnp.broadcast_to(item, (8, LANES)) for item in split_two(last)]
    high = jnp.broadcast_to(index >> bits, (16, LANES))
    sub = lax.broadcasted_iota(jnp.int32, (8, LANES), 0)
    for b in range(groups):
        lhs[16 * b : 16 * b + 16, span] = jnp.where(high == b, parts, 0.0).astype(jnp.bfloat16)
    for g in range(groups // 8):
        here = high[0:8] == sub + 8 * g
        rows = jnp.concatenate([jnp.where(here, item, 0.0) for item in tips], axis=0)
        row = 16 * groups + 16 * g
        lhs[row : row + 16, span] = rows.astype(jnp.bfloat16)


def scatter_dot(lhs, hot, rows):
    return lax.dot_general(
        lhs[rows], hot[...], (((1,), (1,)), ((), ())), preferred_element_type=jnp.float32
    )


def scatter_main(lhs, hot, first, last):
    out = scatter_dot(lhs, hot, slice(16 * first, 16 * last))
    return [out[16 * b : 16 * b + 8] + out[16 * b + 8 : 16 * b + 16] for b in range(last - first)]


def scatter_tips(lhs, hot):
    groups = lhs.shape[0] // 18
    out = scatter_dot(lhs, hot, slice(16 * groups, 18 * groups))
    return [
        out[16 * (b // 8) + b % 8 : 16 * (b // 8) + b % 8 + 1]
        + out[16 * (b // 8) + 8 + b % 8 : 16 * (b // 8) + 9 + b % 8]
        for b in range(groups)
    ]


def stage_features(feat_parts, plan_ref, table, last, order, tips):
    halves = plan_ref.shape[1] // LANES
    blocks = last.shape[0]
    for part, feats in enumerate(feat_parts):
        for f in range(8):
            table[pl.ds(part * 64 + f, 8, stride=8), :] = feats[f]
        last[part * 8 : part * 8 + 8, :] = feats[8]
    slots = plan_ref.shape[0] * halves
    for o in range(slots):
        d, h = divmod(o, halves)
        order[o : o + 1, :] = plan_ref[d : d + 1, h * LANES : (h + 1) * LANES]
    for p in range(slots // 8):
        tips[8 * p : 8 * p + 8, :] = gather_eight(
            lambda b: jnp.broadcast_to(last[b : b + 1, :], (8, LANES)),
            blocks,
            order[8 * p : 8 * p + 8, :],
        )


def pack_features(d, halves, table, order, tips, out_ref):
    blocks = table.shape[0] // 8
    for h in range(halves):
        row = pl.ds(d * halves + h, 1)
        out_ref[d, 8 * h : 8 * h + 8, :] = gather_eight(
            lambda b: table[8 * b : 8 * b + 8, :],
            blocks,
            jnp.broadcast_to(order[row, :], (8, LANES)),
        )
        out_ref[d, 8 * halves + h : 8 * halves + h + 1, :] = tips[row, :]


def pixel_terms():
    lane = lax.broadcasted_iota(jnp.int32, (8, LANES), 1)
    inner = lane & 31
    tile = lane >> 5
    x = (inner & 15).astype(jnp.float32) - 7.5
    step = (inner >> 4).astype(jnp.float32) - 0.5
    return tile, x, step


def render_setup(lists_ref, target_ref, order, wanted, basis, plan_sums, hot, bits):
    tiles, entries = lists_ref.shape
    quarters = entries // LANES
    for q in range(quarters):
        order[q * tiles : (q + 1) * tiles, :] = lists_ref[:, q * LANES : (q + 1) * LANES]
    sub = lax.broadcasted_iota(jnp.int32, (8, LANES), 0)
    lane = lax.broadcasted_iota(jnp.int32, (8, LANES), 1)
    tile, x, step = pixel_terms()
    shifted = 32 * (sub & 3) + (lane & 31)
    for k in range(3):
        total = jnp.zeros((8, LANES), jnp.float32)
        for r in range(8):
            row = jnp.broadcast_to(target_ref[k, :, r * LANES : (r + 1) * LANES], (8, LANES))
            here = (tile == r // 2) & ((sub >> 2) == r % 2)
            total = jnp.where(here, lane_pick(row, shifted), total)
        wanted[8 * k : 8 * k + 8, :] = total
    for g in range(LANES // 8):
        row = sub + 8 * g
        coef = (row * 43) >> 9
        mine = tile == (row & 3)

        def column(j, *terms):
            total = jnp.zeros((8, LANES), jnp.float32)
            for c, value in terms:
                total = jnp.where(coef == c, value, total)
            total = jnp.where(mine, total, 0.0)
            basis[8 * g : 8 * g + 8, j * LANES : (j + 1) * LANES] = total

        column(0, (0, x * x), (1, x * step), (2, step * step), (3, x), (4, step), (5, 1.0))
        column(1, (1, x), (2, 2.0 * step), (4, 1.0))
        column(2, (2, 1.0))
        for k in range(3):
            column(3 + k, (6 + k, 1.0))
    mine = tile == (sub & 3)
    for s in range(8):
        y = step + (2.0 * s - 7.0)
        rows = [jnp.ones_like(x), x, y, x * x, x * y, y * y]
        rows = jnp.concatenate([jnp.where(mine, item, 0.0) for item in rows], axis=0)
        for part in range(2):
            start = (part * 8 + s) * LANES
            plan_sums[:, start : start + LANES] = rows.astype(jnp.bfloat16)
    for o in range(tiles * quarters):
        fill_hot(hot, order[o : o + 1, :], o * LANES, bits)


def render_rest(
    cells, others, receive, recv_ref, order, wanted, back_ref,
    coefs, tables, basis, alpha_s, weight_s, slope_s, joint_g, joint_w, plan_sums, error_sums,
    turned, tinted, moved, pairs, lhs, hot, bits,
):
    owners, packed, _ = recv_ref.shape
    halves = packed // FEATS
    blocks = owners * halves
    tiles = 4
    quarters = order.shape[0] // tiles
    entries = quarters * LANES
    me = lax.axis_index("cells")
    rows_pix = tiles * cells // TILE_COLS * 16
    half_width = TILE_COLS * 8.0
    inv_width = 1.0 / half_width
    log_two = 1.4426950408889634
    sub = lax.broadcasted_iota(jnp.int32, (8, LANES), 0)
    local = sub & 3
    tile_col = 4 * lax.rem(me, TILE_COLS // 4) + local
    tile_row = lax.div(me, TILE_COLS // 4)
    centre_col = (16 * tile_col + 8).astype(jnp.float32) - half_width
    centre_row = (jnp.full((8, LANES), 16 * tile_row + 8, jnp.int32)).astype(
        jnp.float32
    ) - rows_pix * 0.5

    picked = [[None] * FEATS for _ in range(quarters // 2)]
    for k in range(owners):
        origin = others[-k] if k else me
        if k:
            receive(origin)
        for p in range(quarters // 2):
            index = jnp.maximum(order[8 * p : 8 * p + 8, :], 0)
            lanes, block = index & (LANES - 1), index >> 7
            for h in range(halves):
                here = block == origin * halves + h
                for f in range(FEATS):
                    r = 8 * h + f if f < 8 else 8 * halves + h
                    row = jnp.broadcast_to(recv_ref[origin, r : r + 1, :], (8, LANES))
                    item = lane_pick(row, lanes)
                    old = picked[p][f]
                    picked[p][f] = item if old is None else jnp.where(here, item, old)

    for p in range(quarters // 2):
        index = order[8 * p : 8 * p + 8, :]
        feats = picked[p]
        off_col = feats[0] * half_width - centre_col
        off_row = feats[1] * half_width - centre_row
        moved[16 * p : 16 * p + 8, :] = off_col
        moved[16 * p + 8 : 16 * p + 16, :] = off_row
        square = feats[2] * (-0.5 * log_two * inv_width * inv_width)
        cross = feats[3] * (-log_two * inv_width * inv_width)
        bend = feats[4] * (-0.5 * log_two * inv_width * inv_width)
        faint = jnp.maximum(jnp.log(feats[5]) * log_two, -1e30)
        along = square * off_col + cross * off_row
        level = along * off_col + bend * off_row * off_row + jnp.where(index >= 0, faint, -1e30)
        terms = [
            square,
            cross,
            bend,
            -(along + square * off_col),
            -(2.0 * bend * off_row + cross * off_col),
            level,
            feats[6],
            feats[7],
            feats[8],
        ]
        for c, term in enumerate(terms):
            for i, piece in enumerate(split_three(term)):
                row = (3 * c + i) * tiles
                for q in range(2):
                    start = (2 * p + q) * LANES
                    coefs[start + row : start + row + tiles, :] = piece[4 * q : 4 * q + 4]
    for q in range(quarters):
        coefs[q * LANES + 108 : (q + 1) * LANES, :] = jnp.zeros((LANES - 108, LANES), jnp.float32)
    weights = basis[...].astype(jnp.bfloat16)
    for q in range(quarters):
        span = slice(q * LANES, (q + 1) * LANES)
        columns = jnp.transpose(coefs[span, :]).astype(jnp.bfloat16)
        result = jnp.dot(columns, weights, preferred_element_type=jnp.float32)
        for j in range(6):
            tables[j, span, :] = result[:, j * LANES : (j + 1) * LANES]

    height = (2 * sub - 7).astype(jnp.float32)

    def table(l, j):
        return jnp.broadcast_to(tables[j, pl.ds(l, 1), :], (8, LANES))

    def relay(source, base, joint, q, c, s):
        item = source[pl.ds(base + c * 128 + s, 16, stride=8), :]
        top = item.astype(jnp.bfloat16)
        rows = pl.ds(pl.multiple_of(q * LANES, LANES) + c * 16, 16)
        joint[rows, s * LANES : (s + 1) * LANES] = top
        joint[rows, (8 + s) * LANES : (9 + s) * LANES] = (
            item - top.astype(jnp.float32)
        ).astype(jnp.bfloat16)

    chunks = LANES // 16

    def forward(q, carry):
        trans, red, green, blue = carry
        base = pl.multiple_of(q * 8 * LANES, 8 * LANES)
        first = pl.multiple_of(q * LANES, LANES)
        for c in range(chunks):
            for i in range(16):
                l = first + (c * 16 + i)
                where = pl.ds(base + (c * 16 + i) * 8, 8)
                power = table(l, 0) + height * (table(l, 1) + height * table(l, 2))
                alpha = jnp.exp2(power)
                weight = alpha * trans
                alpha_s[where, :] = alpha
                weight_s[where, :] = weight
                trans = trans * (1.0 - alpha)
                red = red + weight * table(l, 3)
                green = green + weight * table(l, 4)
                blue = blue + weight * table(l, 5)
                if c and i % 2:
                    relay(weight_s, base, joint_w, q, c - 1, i // 2)
        for s in range(8):
            relay(weight_s, base, joint_w, q, chunks - 1, s)
        return trans, red, green, blue

    zero = jnp.zeros((8, LANES), jnp.float32)
    carry = lax.fori_loop(
        0, quarters, forward, (jnp.ones((8, LANES), jnp.float32), zero, zero, zero)
    )
    red, green, blue = carry[1:]
    errors = [2.0 * (item - wanted[8 * k : 8 * k + 8, :]) for k, item in enumerate((red, green, blue))]
    wanted[0:8, :], wanted[8:16, :], wanted[16:24, :] = errors
    tile, _, _ = pixel_terms()
    mine = tile == local
    for s in range(8):
        tops, lows = [], []
        for k in range(3):
            row = jnp.broadcast_to(wanted[8 * k + s : 8 * k + s + 1, :], (8, LANES))
            row = jnp.where(mine, row, 0.0)
            top = row.astype(jnp.bfloat16).astype(jnp.float32)
            tops.append(top)
            lows.append(row - top)
        blank = [jnp.zeros((24, LANES), jnp.float32)]
        start = s * LANES
        error_sums[:, start : start + LANES] = jnp.concatenate(tops + lows, axis=0).astype(jnp.bfloat16)
        start = (8 + s) * LANES
        error_sums[:, start : start + LANES] = jnp.concatenate(tops + blank, axis=0).astype(jnp.bfloat16)

    def sum_pixels(factors, joint, result, q):
        span = pl.ds(pl.multiple_of(q * LANES, LANES), LANES)
        result[:, span] = lax.dot_general(
            factors[...],
            joint[span, :],
            (((1,), (1,)), ((), ())),
            preferred_element_type=jnp.float32,
        )

    def backward(q, behind, late):
        base = pl.multiple_of(q * 8 * LANES, 8 * LANES)
        first = pl.multiple_of(q * LANES, LANES)
        sum_pixels(error_sums, joint_w, tinted, q)
        if late:
            sum_pixels(plan_sums, joint_g, turned, q + 1)
        for c in range(chunks - 1, -1, -1):
            for i in range(15, -1, -1):
                l = first + (c * 16 + i)
                where = pl.ds(base + (c * 16 + i) * 8, 8)
                slope = errors[0] * table(l, 3) + errors[1] * table(l, 4) + errors[2] * table(l, 5)
                alpha = alpha_s[where, :]
                slope_s[(c * 16 + i) * 8 : (c * 16 + i) * 8 + 8, :] = weight_s[where, :] * (
                    slope - behind
                )
                behind = (1.0 - alpha) * behind + alpha * slope
                if c < chunks - 1 and i % 2:
                    relay(slope_s, 0, joint_g, q, c + 1, i // 2)
        for s in range(8):
            relay(slope_s, 0, joint_g, q, 0, s)
        return behind

    behind = backward(quarters - 1, zero, False)
    lax.fori_loop(1, quarters, lambda i, v: backward(quarters - 1 - i, v, True), behind)
    sum_pixels(plan_sums, joint_g, turned, 0)
    for p in range(quarters // 2):
        off_col = moved[16 * p : 16 * p + 8, :]
        off_row = moved[16 * p + 8 : 16 * p + 16, :]

        def quantity(j):
            source, r = (turned, j) if j < 6 else (tinted, j - 6)
            rows = slice(8 * r, 8 * r + 8)
            start = 2 * p * LANES
            return jnp.where(
                sub < 4,
                source[rows, start : start + LANES],
                source[rows, start + LANES : start + 2 * LANES],
            )

        plain, across, down = quantity(0), quantity(1), quantity(2)
        near_col = across - off_col * plain
        near_row = down - off_row * plain
        rows = [
            plain,
            near_col * inv_width,
            near_row * inv_width,
            (quantity(3) - off_col * (across + near_col)) * (inv_width * inv_width),
            (quantity(4) - off_col * down - off_row * near_col) * (inv_width * inv_width),
            (quantity(5) - off_row * (down + near_row)) * (inv_width * inv_width),
            *[quantity(6 + k) + quantity(9 + k) for k in range(3)],
        ]
        for f, item in enumerate(rows):
            pairs[pl.ds(p * 128 + f, 8, stride=16), :] = item
    for o in range(tiles * quarters):
        fill_values(
            lhs,
            pairs[o * 16 : o * 16 + 8, :],
            pairs[o * 16 + 8 : o * 16 + 9, :],
            order[o : o + 1, :],
            o * LANES,
            bits,
        )
    for s, (main, last) in enumerate(zip(scatter_main(lhs, hot, 0, owners), scatter_tips(lhs, hot))):
        for h in range(halves):
            span = slice(h * LANES, (h + 1) * LANES)
            back_ref[s, 8 * h : 8 * h + 8, :] = main[:, span]
            back_ref[s, 8 * halves + h : 8 * halves + h + 1, :] = last[:, span]


def main_kernel(
    params_in, cam_in, plan_in, visible_in, lists_in, target_in, out_ref,
    params_ref, cam_ref, plan_ref, visible_ref, lists_ref, target_ref, dense, table, last, plan_order, outgoing, incoming, back, returned, mine, extra, extras, relayed, plans, tips,
    order, wanted, basis, coefs, tables, alpha_s, weight_s, slope_s, joint_g, joint_w,
    plan_sums, error_sums, turned, tinted, moved, pairs, lhs, hot, own_lhs, own_hot,
    send_one, recv_one, send_two, recv_two, send_three, recv_three, send_four, recv_four, local_sem,
):
    cells, views = lax.axis_size("cells"), lax.axis_size("views")
    cell, view = lax.axis_index("cells"), lax.axis_index("views")
    count, block = params_ref.shape
    blocks = block // LANES
    capacity = plan_ref.shape[1]
    halves = capacity // LANES
    bits = capacity.bit_length() - 1
    fetches = [
        pltpu.make_async_copy(source, dest, local_sem.at[i])
        for i, (source, dest) in enumerate(
            (
                (params_in, params_ref),
                (cam_in, cam_ref),
                (plan_in, plan_ref),
                (visible_in, visible_ref),
                (lists_in, lists_ref),
                (target_in, target_ref),
            )
        )
    ]
    for fetch in fetches:
        fetch.start()
    barrier = pltpu.get_barrier_semaphore()

    def greet(axis, me, size):
        for k in range(1, size):
            pl.semaphore_signal(
                barrier,
                inc=1,
                device_id={axis: lax.rem(me + k, size)},
                device_id_type=pl.DeviceIdType.MESH,
            )

    far = lax.div(cell, 4)
    depth, side = lax.div(cell, 2), lax.rem(cell, 2)
    others = [
        2 * d + e
        for d in (3 - 3 * far, 2 - far, 1 - depth + 4 * far)
        for e in (1 - side, side)
    ] + [2 * depth + 1 - side]
    twin = view + 1 - 2 * lax.rem(view, 2)
    across = lax.rem(view + 2, views)
    mates = [twin, across, lax.rem(twin + 2, views)]

    def send(axis, peer, source, dest, send_sem, recv_sem):
        copy = pltpu.make_async_remote_copy(
            src_ref=source,
            dst_ref=dest,
            send_sem=send_sem,
            recv_sem=recv_sem,
            device_id={axis: peer},
            device_id_type=pl.DeviceIdType.MESH,
        )
        copy.start()
        return copy

    def receiver(buffer, sems):
        def receive(origin):
            pltpu.make_async_remote_copy(
                src_ref=buffer.at[origin],
                dst_ref=buffer.at[origin],
                send_sem=sems.at[origin],
                recv_sem=sems.at[origin],
                device_id={"cells": origin},
                device_id_type=pl.DeviceIdType.MESH,
            ).wait_recv()

        return receive

    receive_one = receiver(incoming, recv_one)
    receive_two = receiver(returned, recv_two)
    greet("cells", cell, cells)
    greet("views", view, views)
    fetches[1].wait()
    turn, centre = camera_terms(cam_ref[...])
    known = [*turn[0], *turn[1], *turn[2], *centre]
    lane = lax.broadcasted_iota(jnp.int32, (8, LANES), 1)
    line = jnp.zeros((8, LANES), jnp.float32)
    for i, item in enumerate(known):
        line = jnp.where(lane == i, jnp.broadcast_to(item, (8, LANES)), line)
    extra[blocks : blocks + 8, :] = line
    fetches[3].wait()
    for b in range(blocks):
        extra[b : b + 1, :] = visible_ref[:, b * LANES : (b + 1) * LANES].astype(jnp.float32)
    fetches[0].wait()
    fill_dense(params_ref, dense)
    feat_parts = [
        project_rows(dense_rows(dense, part, count), turn, centre) for part in range(blocks // 8)
    ]
    fetches[2].wait()
    stage_features(feat_parts, plan_ref, table, last, plan_order, tips)
    slots = cells * halves
    for o in range(slots // 8):
        extra[blocks + 8 + 8 * o : blocks + 16 + 8 * o, :] = plan_order[8 * o : 8 * o + 8, :].astype(
            jnp.float32
        )
    pl.semaphore_wait(barrier, cells + views - 2)

    sent = []
    for i, peer in enumerate(others):
        pack_features(peer, halves, table, plan_order, tips, outgoing)
        sent.append(
            send(
                "cells", peer, outgoing.at[peer], incoming.at[cell],
                send_one.at[i], recv_one.at[cell],
            )
        )
    early = [
        send(
            "views", mate, extra, extras.at[view], send_four.at[j], recv_four.at[j]
        )
        for j, mate in enumerate(mates)
    ]
    pack_features(cell, halves, table, plan_order, tips, incoming)
    fetches[4].wait()
    fetches[5].wait()
    render_setup(lists_ref, target_ref, order, wanted, basis, plan_sums, hot, bits)
    wide = own_hot.shape[1].bit_length() - 1
    arrivals = [cell] + others[::-1]

    def know_plan(v, rows):
        for k, origin in enumerate(arrivals):
            for h in range(halves):
                o = k * halves + h
                row = rows[pl.ds(blocks + 8 + origin * halves + h, 1), :].astype(jnp.int32)
                plans[v, o : o + 1, :] = row
                fill_hot(own_hot.at[v], row, o * LANES, wide)

    know_plan(0, extra)
    for j, mate in enumerate(mates):
        early[j].wait()
        know_plan(j + 1, extras.at[mate])
    render_rest(
        cells, others, receive_one, incoming, order, wanted, back,
        coefs, tables, basis, alpha_s, weight_s, slope_s, joint_g, joint_w, plan_sums, error_sums,
        turned, tinted, moved, pairs, lhs, hot, bits,
    )
    sent += [
        send(
            "cells", peer, back.at[peer], returned.at[cell], send_two.at[i], recv_two.at[cell]
        )
        for i, peer in enumerate(others)
    ]

    def forward(k, source, origin):
        return [
            send(
                "views", mate, source, relayed.at[view, origin],
                send_three.at[k, j], recv_three.at[k, j],
            )
            for j, mate in enumerate(mates)
        ]

    relays = [forward(0, back.at[cell], cell)]
    counts = extra[0:blocks, :]
    for mate in mates:
        counts = counts + extras[mate, 0:blocks, :]
    grads = blocks * PAD_ROWS
    out_ref[grads : grads + blocks, :] = counts
    parts = blocks // 8
    pulls = []
    for v in range(views):
        lines = extras.at[mates[v - 1]] if v else extra
        known = [
            jnp.broadcast_to(lines[blocks : blocks + 1, i : i + 1], (8, LANES)) for i in range(12)
        ]
        for part in range(parts):
            pulls.append(
                jax.vjp(
                    lambda *items: project_rows(items, [known[0:3], known[3:6], known[6:9]], known[9:12]),
                    *dense_rows(dense, part, count),
                )
            )
    for k in range(1, cells):
        receive_two(arrivals[k])
        relays.append(forward(k, returned.at[arrivals[k]], arrivals[k]))

    def fill(v, k, packet):
        for h in range(halves):
            o = k * halves + h
            fill_values(
                own_lhs.at[v],
                packet[8 * h : 8 * h + 8, :],
                packet[8 * halves + h : 8 * halves + h + 1, :],
                plans[v, o : o + 1, :],
                o * LANES,
                wide,
            )

    over = (((1,), (1,)), ((), ()))

    def scatter(v, span):
        return lax.dot_general(
            own_lhs[v, :, span], own_hot[v, :, span], over, preferred_element_type=jnp.float32
        )

    def pull_view(v, out):
        groups = own_lhs.shape[1] // 18
        for g in range(groups):
            part, line = divmod(2 * g, 8)
            main = out[16 * g : 16 * g + 8] + out[16 * g + 8 : 16 * g + 16]
            row = 16 * groups + 16 * (g // 8) + g % 8
            tip = out[row : row + 1] + out[row + 8 : row + 9]
            for i in range(2):
                span = slice(i * LANES, (i + 1) * LANES)
                mine[v, part, pl.ds(line + i, 8, stride=8), :] = main[:, span]
                mine[v, part, 64 + line + i : 65 + line + i, :] = tip[:, span]
        for part in range(parts):
            feats, pull = pulls[v * parts + part]
            got = [mine[v, part, 8 * f : 8 * f + 8, :] for f in range(FEATS)]
            pulled = pull(
                (
                    feats[2] * got[1] + feats[3] * got[2],
                    feats[3] * got[1] + feats[4] * got[2],
                    -0.5 * got[3],
                    -got[4],
                    -0.5 * got[5],
                    got[0] / feats[5],
                    got[6],
                    got[7],
                    got[8],
                )
            )
            for r, item in enumerate(pulled):
                where = slice((part * PAD_ROWS + r) * 8, (part * PAD_ROWS + r) * 8 + 8)
                out_ref[where, :] = out_ref[where, :] + item if v else item

    for k in range(cells):
        fill(0, k, returned.at[arrivals[k]] if k else back.at[cell])
    pull_view(0, scatter(0, slice(0, slots * LANES)))
    half = slots // 2 * LANES
    for group in ((0,), (1, 2)):
        starts = []
        for k in range(cells):
            for j in group:
                relays[k][j].wait()
                fill(j + 1, k, relayed.at[mates[j], arrivals[k]])
            if k == cells // 2 - 1:
                starts = [scatter(j + 1, slice(0, half)) for j in group]
        for j, start in zip(group, starts):
            pull_view(j + 1, start + scatter(j + 1, slice(half, slots * LANES)))
    for copy in sent:
        copy.wait_send()


def update_kernel(params_ref, first_ref, second_ref, grads_ref, new_ref, new_first_ref, new_second_ref):
    count, block = params_ref.shape
    blocks = block // LANES
    row_ids = lax.broadcasted_iota(jnp.int32, (8, LANES), 0)
    bias_one = 1.0 - 0.9**ADAM_STEP
    bias_two = 1.0 - 0.999**ADAM_STEP
    for b in range(blocks):
        span = slice(b * LANES, (b + 1) * LANES)
        part, line = divmod(b, 8)
        counts = grads_ref[blocks * PAD_ROWS + b : blocks * PAD_ROWS + b + 1, :]
        for r in range(0, count, 8):
            size = min(8, count - r)
            rows = slice(r, r + size)
            gradient = grads_ref[pl.ds((part * PAD_ROWS + r) * 8 + line, size, stride=8), :]
            if r >= 16:
                rates = 0.000125
            else:
                ids = row_ids[0:size] + r
                rates = jnp.where(
                    ids < 6,
                    0.01,
                    jnp.where(
                        ids < 10,
                        0.005,
                        jnp.where(ids < 11, 0.05, jnp.where(ids < 14, 0.0025, 0.000125)),
                    ),
                )
            params, first, second = params_ref[rows, span], first_ref[rows, span], second_ref[rows, span]
            seen = jnp.broadcast_to(counts, params.shape) > 0.0
            first_new = 0.9 * first + 0.1 * gradient
            second_new = 0.999 * second + 0.001 * gradient * gradient
            stride = rates * (first_new / bias_one) / (jnp.sqrt(second_new / bias_two) + 1e-08)
            new_ref[rows, span] = jnp.where(seen, params - stride, params)
            new_first_ref[rows, span] = jnp.where(seen, first_new, first)
            new_second_ref[rows, span] = jnp.where(seen, second_new, second)


def fused_shards(params, first_moment, second_moment, cameras, visible, send_plan, tile_lists, target):
    cells, views = lax.axis_size("cells"), lax.axis_size("views")
    count, block = params.shape
    blocks = block // LANES
    plan = send_plan[0, 0]
    lists = tile_lists[0]
    tiles, entries = lists.shape
    capacity = plan.shape[1]
    halves = capacity // LANES
    slots = cells * halves
    f32, bf16 = jnp.float32, jnp.bfloat16
    packet = pltpu.VMEM((cells, FEATS * halves, LANES), f32)
    dma = pltpu.SemaphoreType.DMA
    vmem = pl.BlockSpec(memory_space=pltpu.VMEM)
    grads = pl.pallas_call(
        main_kernel,
        out_shape=jax.ShapeDtypeStruct((blocks * PAD_ROWS + blocks, LANES), f32),
        in_specs=[pl.BlockSpec(memory_space=pltpu.HBM)] * 6,
        out_specs=vmem,
        scratch_shapes=[
            pltpu.VMEM((count, block), f32),
            pltpu.VMEM(cameras.shape, f32),
            pltpu.VMEM(plan.shape, jnp.int32),
            pltpu.VMEM(visible.shape, jnp.int32),
            pltpu.VMEM(lists.shape, jnp.int32),
            pltpu.VMEM((3, 1, target.shape[2]), f32),
            pltpu.VMEM((blocks * PAD_ROWS, LANES), f32),
            pltpu.VMEM((blocks * 8, LANES), f32),
            pltpu.VMEM((blocks, LANES), f32),
            pltpu.VMEM((slots, LANES), jnp.int32),
            packet, packet, packet, packet,
            pltpu.VMEM((views, blocks // 8, FEATS * 8, LANES), f32),
            pltpu.VMEM((blocks + 8 + slots, LANES), f32),
            pltpu.VMEM((views, blocks + 8 + slots, LANES), f32),
            pltpu.VMEM((views, cells, FEATS * halves, LANES), f32),
            pltpu.VMEM((views, slots, LANES), jnp.int32),
            pltpu.VMEM((slots, LANES), f32),
            pltpu.VMEM((tiles * entries // LANES, LANES), jnp.int32),
            pltpu.VMEM((24, LANES), f32),
            pltpu.VMEM((LANES, 6 * LANES), f32),
            pltpu.VMEM((entries, LANES), f32),
            pltpu.VMEM((6, entries, LANES), f32),
            pltpu.VMEM((entries * 8, LANES), f32),
            pltpu.VMEM((entries * 8, LANES), f32),
            pltpu.VMEM((8 * LANES, LANES), f32),
            pltpu.VMEM((entries, 16 * LANES), bf16),
            pltpu.VMEM((entries, 16 * LANES), bf16),
            pltpu.VMEM((48, 16 * LANES), bf16),
            pltpu.VMEM((48, 16 * LANES), bf16),
            pltpu.VMEM((48, entries), f32),
            pltpu.VMEM((48, entries), f32),
            pltpu.VMEM((entries // LANES * 8, LANES), f32),
            pltpu.VMEM((tiles * entries // LANES * 16, LANES), f32),
            pltpu.VMEM((cells * 18, tiles * entries), bf16),
            pltpu.VMEM((capacity, tiles * entries), bf16),
            pltpu.VMEM((views, blocks // 2 * 18, slots * LANES), bf16),
            pltpu.VMEM((views, 2 * LANES, slots * LANES), bf16),
            dma((cells - 1,)), dma((cells,)), dma((cells - 1,)), dma((cells,)),
            dma((cells, views - 1)), dma((cells, views - 1)), dma((views - 1,)), dma((views - 1,)),
            dma((6,)),
        ],
        compiler_params=pltpu.CompilerParams(
            collective_id=0,
            has_side_effects=True,
            vmem_limit_bytes=MAIN_VMEM,
        ),
        cost_estimate=pl.CostEstimate(
            flops=4096 * tiles * 256 * entries,
            bytes_accessed=4 * count * block,
            transcendentals=tiles * 256 * entries,
        ),
    )(
        *[
            pltpu.with_memory_space_constraint(item, pltpu.HBM)
            for item in (params, cameras, plan, visible, lists, jnp.transpose(target, (1, 0, 2)))
        ]
    )
    like = jax.ShapeDtypeStruct(params.shape, f32)
    return tuple(
        pl.pallas_call(
            update_kernel,
            out_shape=(like, like, like),
            compiler_params=pltpu.CompilerParams(vmem_limit_bytes=UPDATE_VMEM),
        )(params, first_moment, second_moment, grads)
    )


def local_shards(params, first_moment, second_moment, cameras, visible, send_plan, tile_lists, target):
    capacity = send_plan.shape[3]
    tiles, entries = tile_lists.shape[1:]
    halves = capacity // LANES
    fits = (
        capacity % LANES == 0
        and params.shape[1] % (16 * LANES) == 0
        and entries % (2 * LANES) == 0
        and 8 % max(halves, 1) == 0
        and lax.axis_size("cells") == 8
        and lax.axis_size("views") == 4
        and tiles * entries <= 4096
        and tiles == 4
    )
    body = fused_shards if fits else shards
    return body(params, first_moment, second_moment, cameras, visible, send_plan, tile_lists, target)


def solution(mesh):
    in_specs = (
        P(None, "cells"),
        P(None, "cells"),
        P(None, "cells"),
        P("views", None),
        P("views", "cells"),
        P("views", "cells", None, None),
        P("views", "cells", None),
        P("views", None, "cells"),
    )
    out_specs = (P(None, "cells"), P(None, "cells"), P(None, "cells"))
    return jax.shard_map(local_shards, mesh=mesh, in_specs=in_specs, out_specs=out_specs, check_vma=False)
```

```python
import functools

import jax
import jax.numpy as jnp
from jax import lax
from jax.experimental import pallas as pl
from jax.experimental.pallas import tpu as pltpu
from jax.sharding import PartitionSpec as P

TILE_COLS = 32
ADAM_STEP = 1000


harmonic_zero = 0.28209479177387814
harmonic_one = 0.4886025119029199
harmonic_two = (
    1.0925484305920792,
    -1.0925484305920792,
    0.31539156525252005,
    -1.0925484305920792,
    0.5462742152960396,
)
harmonic_three = (
    -0.5900435899266435,
    2.890611442640554,
    -0.4570457994644658,
    0.3731763325901154,
    -0.4570457994644658,
    1.445305721320277,
    -0.5900435899266435,
)


def harmonics(across, upward, onward):
    across_sq = across * across
    upward_sq = upward * upward
    onward_sq = onward * onward
    return jnp.stack(
        [
            harmonic_zero * jnp.ones_like(across),
            -harmonic_one * upward,
            harmonic_one * onward,
            -harmonic_one * across,
            harmonic_two[0] * across * upward,
            harmonic_two[1] * upward * onward,
            harmonic_two[2] * (2.0 * onward_sq - across_sq - upward_sq),
            harmonic_two[3] * across * onward,
            harmonic_two[4] * (across_sq - upward_sq),
            harmonic_three[0] * upward * (3.0 * across_sq - upward_sq),
            harmonic_three[1] * across * upward * onward,
            harmonic_three[2] * upward * (4.0 * onward_sq - across_sq - upward_sq),
            harmonic_three[3] * onward * (2.0 * onward_sq - 3.0 * across_sq - 3.0 * upward_sq),
            harmonic_three[4] * across * (4.0 * onward_sq - across_sq - upward_sq),
            harmonic_three[5] * onward * (across_sq - upward_sq),
            harmonic_three[6] * across * (across_sq - 3.0 * upward_sq),
        ]
    )


def camera_rotation(angles):
    cos_roll, sin_roll = (jnp.cos(angles[0]), jnp.sin(angles[0]))
    cos_pitch, sin_pitch = (jnp.cos(angles[1]), jnp.sin(angles[1]))
    cos_yaw, sin_yaw = (jnp.cos(angles[2]), jnp.sin(angles[2]))
    naught = jnp.zeros_like(cos_roll)
    unit_one = jnp.ones_like(cos_roll)
    roll = jnp.stack(
        [
            jnp.stack([unit_one, naught, naught]),
            jnp.stack([naught, cos_roll, -sin_roll]),
            jnp.stack([naught, sin_roll, cos_roll]),
        ]
    )
    pitch = jnp.stack(
        [
            jnp.stack([cos_pitch, naught, sin_pitch]),
            jnp.stack([naught, unit_one, naught]),
            jnp.stack([-sin_pitch, naught, cos_pitch]),
        ]
    )
    yawing = jnp.stack(
        [
            jnp.stack([cos_yaw, -sin_yaw, naught]),
            jnp.stack([sin_yaw, cos_yaw, naught]),
            jnp.stack([naught, naught, unit_one]),
        ]
    )
    inner_turn = jnp.dot(pitch, roll, precision=lax.Precision.HIGHEST)
    return jnp.dot(yawing, inner_turn, precision=lax.Precision.HIGHEST)


def project(values, camera):
    turn = camera_rotation(camera[0:3])
    offset = values[0:3] - camera[3:6][:, None]
    in_view = jnp.dot(turn, offset, precision=lax.Precision.HIGHEST)
    inv_depth = 1.0 / in_view[2]
    screen_col = in_view[0] * inv_depth
    screen_row = in_view[1] * inv_depth
    scales = jnp.exp(values[3:6])
    quat = values[6:10] / jnp.sqrt(jnp.sum(values[6:10] * values[6:10], axis=0, keepdims=True))
    quat_w, quat_x, quat_y, quat_z = (quat[0], quat[1], quat[2], quat[3])
    spin = [
        [
            1.0 - 2.0 * (quat_y * quat_y + quat_z * quat_z),
            2.0 * (quat_x * quat_y - quat_w * quat_z),
            2.0 * (quat_x * quat_z + quat_w * quat_y),
        ],
        [
            2.0 * (quat_x * quat_y + quat_w * quat_z),
            1.0 - 2.0 * (quat_x * quat_x + quat_z * quat_z),
            2.0 * (quat_y * quat_z - quat_w * quat_x),
        ],
        [
            2.0 * (quat_x * quat_z - quat_w * quat_y),
            2.0 * (quat_y * quat_z + quat_w * quat_x),
            1.0 - 2.0 * (quat_x * quat_x + quat_y * quat_y),
        ],
    ]
    basis_cam = []
    for outer_index in range(3):
        row_terms = []
        for col_index in range(3):
            entry = turn[outer_index, 0] * spin[0][col_index]
            for mid_index in range(1, 3):
                entry = entry + turn[outer_index, mid_index] * spin[mid_index][col_index]
            row_terms.append(entry * scales[col_index])
        basis_cam.append(row_terms)
    jac_top = [
        (basis_cam[0][col_index] - screen_col * basis_cam[2][col_index]) * inv_depth
        for col_index in range(3)
    ]
    jac_low = [
        (basis_cam[1][col_index] - screen_row * basis_cam[2][col_index]) * inv_depth
        for col_index in range(3)
    ]
    sigma_a = jac_top[0] * jac_top[0] + jac_top[1] * jac_top[1] + jac_top[2] * jac_top[2]
    sigma_b = jac_top[0] * jac_low[0] + jac_top[1] * jac_low[1] + jac_top[2] * jac_low[2]
    sigma_c = jac_low[0] * jac_low[0] + jac_low[1] * jac_low[1] + jac_low[2] * jac_low[2]
    determinant = sigma_a * sigma_c - sigma_b * sigma_b
    opacity = jax.nn.sigmoid(values[10])
    distance = jnp.sqrt(jnp.sum(offset * offset, axis=0))
    unit_dir = offset / distance
    basis = harmonics(unit_dir[0], unit_dir[1], unit_dir[2])
    coeffs = values[11:59].reshape(16, 3, values.shape[1])
    colors = 0.5 + jnp.sum(basis[:, None, :] * coeffs, axis=0)
    screen = jnp.stack(
        [
            screen_col,
            screen_row,
            sigma_c / determinant,
            -sigma_b / determinant,
            sigma_a / determinant,
            opacity,
        ]
    )
    return jnp.concatenate([screen, colors], axis=0)


def group_loss(pieces):
    features, live_mask, pixel_column, pixel_row, target_tile = pieces
    entries = live_mask.shape[1]
    delta_col = pixel_column[:, :, None] - features[0][:, None, :]
    delta_row = pixel_row[:, :, None] - features[1][:, None, :]
    power = -0.5 * (
        features[2][:, None, :] * delta_col * delta_col
        + 2.0 * features[3][:, None, :] * delta_col * delta_row
        + features[4][:, None, :] * delta_row * delta_row
    )
    alphas = features[5][:, None, :] * jnp.exp(power) * live_mask[:, None, :]
    log_keep = jnp.log(1.0 - alphas)
    earlier = (
        lax.broadcasted_iota(jnp.int32, (entries, entries), 0)
        < lax.broadcasted_iota(jnp.int32, (entries, entries), 1)
    ).astype(jnp.float32)
    transmit = jnp.exp(
        jnp.einsum("bpl,lm->bpm", log_keep, earlier, precision=lax.Precision.HIGHEST)
    )
    weights = alphas * transmit
    image = jnp.einsum("bpl,kbl->kbp", weights, features[6:9], precision=lax.Precision.HIGHEST)
    error = image - target_tile
    return jnp.sum(error * error)


def render_tiles(picked, live_mask, pixel_column, pixel_row, target_tile):
    groups = live_mask.shape[0] // 4
    entries = live_mask.shape[1]
    pixels = pixel_column.shape[1]
    stacked = (
        jnp.transpose(picked.reshape(picked.shape[0], groups, 4, entries), (1, 0, 2, 3)),
        live_mask.reshape(groups, 4, entries),
        pixel_column.reshape(groups, 4, pixels),
        pixel_row.reshape(groups, 4, pixels),
        jnp.transpose(target_tile.reshape(3, groups, 4, pixels), (1, 0, 2, 3)),
    )
    return jnp.sum(lax.map(jax.checkpoint(group_loss), stacked))


def pixel_grid(first_tile, count, tiles_dev, rows_pix):
    tile_ids = first_tile + jnp.arange(count, dtype=jnp.int32)
    pixel_ids = jnp.arange(256, dtype=jnp.int32)
    block_cols = TILE_COLS // 4
    owner_ids = tile_ids // tiles_dev
    local_ids = tile_ids % tiles_dev
    tile_col = 4 * (owner_ids % block_cols) + local_ids % 4
    tile_row = tiles_dev // 4 * (owner_ids // block_cols) + local_ids // 4
    half_width = TILE_COLS * 8.0
    column = (tile_col[:, None] * 16 + pixel_ids[None, :] % 16).astype(jnp.float32)
    row_pos = (tile_row[:, None] * 16 + pixel_ids[None, :] // 16).astype(jnp.float32)
    return ((column + 0.5 - half_width) / half_width, (row_pos + 0.5 - rows_pix * 0.5) / half_width)


def adam_update(params, first_moment, second_moment, gradient, counts):
    row_ids = lax.broadcasted_iota(jnp.int32, params.shape, 0)
    rates = jnp.where(
        row_ids < 6,
        0.01,
        jnp.where(
            row_ids < 10,
            0.005,
            jnp.where(row_ids < 11, 0.05, jnp.where(row_ids < 14, 0.0025, 0.000125)),
        ),
    )
    first_new = 0.9 * first_moment + 0.1 * gradient
    second = 0.999 * second_moment + 0.001 * gradient * gradient
    bias_one = 1.0 - 0.9**ADAM_STEP
    bias_two = 1.0 - 0.999**ADAM_STEP
    stride = rates * (first_new / bias_one) / (jnp.sqrt(second / bias_two) + 1e-08)
    seen_mask = counts > 0.0
    return (
        jnp.where(seen_mask, params - stride, params),
        jnp.where(seen_mask, first_new, first_moment),
        jnp.where(seen_mask, second, second_moment),
    )


def shards(params, first_moment, second_moment, cameras, visible, send_plan, tile_lists, target):
    cells = lax.axis_size("cells")
    camera = cameras[0]
    plan_rows = send_plan[0, 0]
    capacity = plan_rows.shape[1]
    sent_live = (plan_rows >= 0)[None]
    sent_rows = jnp.maximum(plan_rows, 0)
    lists = tile_lists[0]
    tiles_here = lists.shape[0]
    live_mask = (lists >= 0).astype(jnp.float32)
    slot_ids = jnp.maximum(lists, 0)
    rows_pix = tiles_here * cells // TILE_COLS * 16
    pixel_column, pixel_row = pixel_grid(
        lax.axis_index("cells") * tiles_here, tiles_here, tiles_here, rows_pix
    )
    target_tile = target[0].reshape(3, tiles_here, 256)
    block = params.shape[1]

    def image_loss(table):
        picked = jnp.take(table, slot_ids, axis=1)
        return render_tiles(picked, live_mask, pixel_column, pixel_row, target_tile)

    def own_projection(values):
        return project(values, camera)

    features, project_pull = jax.vjp(own_projection, params)
    outgoing = jnp.take(features, sent_rows, axis=1)
    incoming = lax.all_to_all(outgoing, "cells", split_axis=1, concat_axis=1, tiled=True)
    loss_value, pullback = jax.vjp(
        image_loss, incoming.reshape(features.shape[0], cells * capacity)
    )
    table_grad = pullback(jnp.ones((), jnp.float32))[0]
    returned = lax.all_to_all(
        table_grad.reshape(features.shape[0], cells, capacity),
        "cells",
        split_axis=1,
        concat_axis=1,
        tiled=True,
    )
    kept = jnp.where(sent_live, returned, 0.0)
    gradient = project_pull(
        jnp.zeros((features.shape[0], block), jnp.float32).at[:, sent_rows].add(kept)
    )[0]
    seen_here = visible.astype(jnp.float32)
    total_grad, counts = lax.psum((gradient, seen_here), "views")
    new_params, new_first, new_second = adam_update(
        params, first_moment, second_moment, total_grad, counts
    )
    return (new_params, new_first, new_second)

LANES = 128
PAD_ROWS = 64
FEATS = 9


def project_rows(rows, turn, centre):
    offset = [rows[i] - centre[i] for i in range(3)]
    in_view = [
        turn[i][0] * offset[0] + turn[i][1] * offset[1] + turn[i][2] * offset[2] for i in range(3)
    ]
    inv_depth = 1.0 / in_view[2]
    screen_col = in_view[0] * inv_depth
    screen_row = in_view[1] * inv_depth
    scales = [jnp.exp(rows[3 + i]) for i in range(3)]
    raw = rows[6:10]
    norm = jnp.sqrt(raw[0] * raw[0] + raw[1] * raw[1] + raw[2] * raw[2] + raw[3] * raw[3])
    inv_norm = 1.0 / norm
    quat_w, quat_x, quat_y, quat_z = [item * inv_norm for item in raw]
    spin = [
        [
            1.0 - 2.0 * (quat_y * quat_y + quat_z * quat_z),
            2.0 * (quat_x * quat_y - quat_w * quat_z),
            2.0 * (quat_x * quat_z + quat_w * quat_y),
        ],
        [
            2.0 * (quat_x * quat_y + quat_w * quat_z),
            1.0 - 2.0 * (quat_x * quat_x + quat_z * quat_z),
            2.0 * (quat_y * quat_z - quat_w * quat_x),
        ],
        [
            2.0 * (quat_x * quat_z - quat_w * quat_y),
            2.0 * (quat_y * quat_z + quat_w * quat_x),
            1.0 - 2.0 * (quat_x * quat_x + quat_y * quat_y),
        ],
    ]
    basis_cam = [
        [
            (turn[i][0] * spin[0][j] + turn[i][1] * spin[1][j] + turn[i][2] * spin[2][j])
            * scales[j]
            for j in range(3)
        ]
        for i in range(3)
    ]
    top = [(basis_cam[0][j] - screen_col * basis_cam[2][j]) * inv_depth for j in range(3)]
    low = [(basis_cam[1][j] - screen_row * basis_cam[2][j]) * inv_depth for j in range(3)]
    sigma_a = top[0] * top[0] + top[1] * top[1] + top[2] * top[2]
    sigma_b = top[0] * low[0] + top[1] * low[1] + top[2] * low[2]
    sigma_c = low[0] * low[0] + low[1] * low[1] + low[2] * low[2]
    inv_det = 1.0 / (sigma_a * sigma_c - sigma_b * sigma_b)
    opacity = 1.0 / (1.0 + jnp.exp(-rows[10]))
    inv_dist = 1.0 / jnp.sqrt(offset[0] * offset[0] + offset[1] * offset[1] + offset[2] * offset[2])
    x, y, z = [item * inv_dist for item in offset]
    xx, yy, zz = x * x, y * y, z * z
    basis = [
        None,
        -harmonic_one * y,
        harmonic_one * z,
        -harmonic_one * x,
        harmonic_two[0] * x * y,
        harmonic_two[1] * y * z,
        harmonic_two[2] * (2.0 * zz - xx - yy),
        harmonic_two[3] * x * z,
        harmonic_two[4] * (xx - yy),
        harmonic_three[0] * y * (3.0 * xx - yy),
        harmonic_three[1] * x * y * z,
        harmonic_three[2] * y * (4.0 * zz - xx - yy),
        harmonic_three[3] * z * (2.0 * zz - 3.0 * xx - 3.0 * yy),
        harmonic_three[4] * x * (4.0 * zz - xx - yy),
        harmonic_three[5] * z * (xx - yy),
        harmonic_three[6] * x * (xx - 3.0 * yy),
    ]
    colors = []
    for k in range(3):
        total = harmonic_zero * rows[11 + k]
        for j in range(1, 16):
            total = total + basis[j] * rows[11 + 3 * j + k]
        colors.append(0.5 + total)
    return (
        screen_col,
        screen_row,
        sigma_c * inv_det,
        -sigma_b * inv_det,
        sigma_a * inv_det,
        opacity,
        *colors,
    )


def static_terms(rows):
    scales = [jnp.exp(item) for item in rows[3:6]]
    raw = rows[6:10]
    inv_norm = 1.0 / jnp.sqrt(
        raw[0] * raw[0] + raw[1] * raw[1] + raw[2] * raw[2] + raw[3] * raw[3]
    )
    quat = [item * inv_norm for item in raw]
    w, x, y, z = quat
    spin = [
        [1.0 - 2.0 * (y * y + z * z), 2.0 * (x * y - w * z), 2.0 * (x * z + w * y)],
        [2.0 * (x * y + w * z), 1.0 - 2.0 * (x * x + z * z), 2.0 * (y * z - w * x)],
        [2.0 * (x * z - w * y), 2.0 * (y * z + w * x), 1.0 - 2.0 * (x * x + y * y)],
    ]
    frame = [[spin[m][j] * scales[j] for j in range(3)] for m in range(3)]
    fade = 1.0 - 1.0 / (1.0 + jnp.exp(-rows[10]))
    return scales, inv_norm, quat, frame, fade


def moving_terms(rows, frame, turn, centre):
    offset = [rows[i] - centre[i] for i in range(3)]
    in_view = [
        turn[i][0] * offset[0] + turn[i][1] * offset[1] + turn[i][2] * offset[2] for i in range(3)
    ]
    inv = 1.0 / in_view[2]
    col, row = in_view[0] * inv, in_view[1] * inv
    cam = [
        [
            turn[i][0] * frame[0][j] + turn[i][1] * frame[1][j] + turn[i][2] * frame[2][j]
            for j in range(3)
        ]
        for i in range(3)
    ]
    top = [(cam[0][j] - col * cam[2][j]) * inv for j in range(3)]
    low = [(cam[1][j] - row * cam[2][j]) * inv for j in range(3)]
    sigma_a = top[0] * top[0] + top[1] * top[1] + top[2] * top[2]
    sigma_b = top[0] * low[0] + top[1] * low[1] + top[2] * low[2]
    sigma_c = low[0] * low[0] + low[1] * low[1] + low[2] * low[2]
    inv_det = 1.0 / (sigma_a * sigma_c - sigma_b * sigma_b)
    conic = (sigma_c * inv_det, -sigma_b * inv_det, sigma_a * inv_det)
    inv_dist = 1.0 / jnp.sqrt(offset[0] * offset[0] + offset[1] * offset[1] + offset[2] * offset[2])
    ray = [item * inv_dist for item in offset]
    return inv, col, row, cam[2], top, low, conic, inv_dist, ray


def pull_moving(rows, terms, turn, got):
    inv, col, row, deep, top, low, conic, inv_dist, ray = terms
    k0, k1, k2 = conic
    g0, half, g2 = -0.5 * got[3], -0.5 * got[4], -0.5 * got[5]
    p00, p01 = g0 * k0 + half * k1, g0 * k1 + half * k2
    p10, p11 = half * k0 + g2 * k1, half * k1 + g2 * k2
    d00 = -2.0 * (k0 * p00 + k1 * p10)
    d01 = -2.0 * (k0 * p01 + k1 * p11)
    d11 = -2.0 * (k1 * p01 + k2 * p11)
    d_top = [(d00 * top[j] + d01 * low[j]) * inv for j in range(3)]
    d_low = [(d01 * top[j] + d11 * low[j]) * inv for j in range(3)]
    d_cam = [d_top, d_low, [-(col * d_top[j] + row * d_low[j]) for j in range(3)]]
    d_col = k0 * got[1] + k1 * got[2]
    d_row = k1 * got[1] + k2 * got[2]
    d_depth = 0.0
    for j in range(3):
        d_col = d_col - d_top[j] * deep[j]
        d_row = d_row - d_low[j] * deep[j]
        d_depth = d_depth - (d_top[j] * top[j] + d_low[j] * low[j])
    d_view = [d_col * inv, d_row * inv]
    d_view.append(d_depth - (col * d_view[0] + row * d_view[1]))
    d_frame = [
        [turn[0][m] * d_cam[0][j] + turn[1][m] * d_cam[1][j] + turn[2][m] * d_cam[2][j] for j in range(3)]
        for m in range(3)
    ]
    x, y, z = ray
    xx, yy, zz = x * x, y * y, z * z
    xy, yz, xz = x * y, y * z, x * z
    h1, h2, h3 = harmonic_one, harmonic_two, harmonic_three
    outer = 4.0 * zz - xx - yy
    basis = [
        None,
        -h1 * y,
        h1 * z,
        -h1 * x,
        h2[0] * xy,
        h2[1] * yz,
        h2[2] * (2.0 * zz - xx - yy),
        h2[3] * xz,
        h2[4] * (xx - yy),
        h3[0] * y * (3.0 * xx - yy),
        h3[1] * xy * z,
        h3[2] * y * outer,
        h3[3] * z * (2.0 * zz - 3.0 * xx - 3.0 * yy),
        h3[4] * x * outer,
        h3[5] * z * (xx - yy),
        h3[6] * x * (xx - 3.0 * yy),
    ]
    tint = got[6:9]
    d_shade = [harmonic_zero * item for item in tint]
    d_shade += [basis[j] * tint[k] for j in range(1, 16) for k in range(3)]
    e = [None] + [
        tint[0] * rows[11 + 3 * j] + tint[1] * rows[12 + 3 * j] + tint[2] * rows[13 + 3 * j]
        for j in range(1, 16)
    ]
    gx = (
        -h1 * e[3]
        + y * (h2[0] * e[4] + (6.0 * h3[0]) * (x * e[9]) - (2.0 * h3[2]) * (x * e[11]))
        + z * (h2[3] * e[7] + h3[1] * (y * e[10]))
        + x * ((-2.0 * h2[2]) * e[6] + (2.0 * h2[4]) * e[8])
        + xz * ((-6.0 * h3[3]) * e[12] + (2.0 * h3[5]) * e[14])
        + (h3[4] * (outer - 2.0 * xx)) * e[13]
        + ((3.0 * h3[6]) * (xx - yy)) * e[15]
    )
    gy = (
        -h1 * e[1]
        + x * (h2[0] * e[4] - (2.0 * h3[4]) * (y * e[13]) - (6.0 * h3[6]) * (y * e[15]))
        + z * (h2[1] * e[5] + h3[1] * (x * e[10]))
        + y * ((-2.0 * h2[2]) * e[6] - (2.0 * h2[4]) * e[8])
        + yz * ((-6.0 * h3[3]) * e[12] - (2.0 * h3[5]) * e[14])
        + ((3.0 * h3[0]) * (xx - yy)) * e[9]
        + (h3[2] * (outer - 2.0 * yy)) * e[11]
    )
    gz = (
        h1 * e[2]
        + y * (h2[1] * e[5] + h3[1] * (x * e[10]) + (8.0 * h3[2]) * (z * e[11]))
        + x * (h2[3] * e[7] + (8.0 * h3[4]) * (z * e[13]))
        + (4.0 * h2[2]) * (z * e[6])
        + ((3.0 * h3[3]) * (2.0 * zz - xx - yy)) * e[12]
        + (h3[5] * (xx - yy)) * e[14]
    )
    along = x * gx + y * gy + z * gz
    d_ray = [(gx - x * along) * inv_dist, (gy - y * along) * inv_dist, (gz - z * along) * inv_dist]
    d_place = [
        turn[0][i] * d_view[0] + turn[1][i] * d_view[1] + turn[2][i] * d_view[2] + d_ray[i]
        for i in range(3)
    ]
    return [*d_place, *d_frame[0], *d_frame[1], *d_frame[2], got[0]], d_shade


def pull_static(static, sums):
    scales, inv_norm, quat, frame, fade = static
    d_frame = [sums[3:6], sums[6:9], sums[9:12]]
    d_scale = [
        d_frame[0][j] * frame[0][j] + d_frame[1][j] * frame[1][j] + d_frame[2][j] * frame[2][j]
        for j in range(3)
    ]
    d = [[d_frame[m][j] * scales[j] for j in range(3)] for m in range(3)]
    w, x, y, z = quat
    d_quat = [
        2.0 * (z * (d[1][0] - d[0][1]) + y * (d[0][2] - d[2][0]) + x * (d[2][1] - d[1][2])),
        2.0 * (y * (d[0][1] + d[1][0]) + z * (d[0][2] + d[2][0]) + w * (d[2][1] - d[1][2]) - 2.0 * x * (d[1][1] + d[2][2])),
        2.0 * (x * (d[0][1] + d[1][0]) + w * (d[0][2] - d[2][0]) + z * (d[1][2] + d[2][1]) - 2.0 * y * (d[0][0] + d[2][2])),
        2.0 * (w * (d[1][0] - d[0][1]) + x * (d[0][2] + d[2][0]) + y * (d[1][2] + d[2][1]) - 2.0 * z * (d[0][0] + d[1][1])),
    ]
    along = w * d_quat[0] + x * d_quat[1] + y * d_quat[2] + z * d_quat[3]
    d_raw = [(d_quat[i] - quat[i] * along) * inv_norm for i in range(4)]
    return [*sums[0:3], *d_scale, *d_raw, fade * sums[12]]


def camera_terms(cam):
    cosines, sines = jnp.cos(cam), jnp.sin(cam)
    cr, cp, cy = [cosines[:, i : i + 1] for i in range(3)]
    sr, sp, sy = [sines[:, i : i + 1] for i in range(3)]
    turn = [
        [cy * cp, cy * sp * sr - sy * cr, cy * sp * cr + sy * sr],
        [sy * cp, sy * sp * sr + cy * cr, sy * sp * cr - cy * sr],
        [-sp, cp * sr, cp * cr],
    ]
    centre = [cam[:, 3 + i : 4 + i] for i in range(3)]
    return turn, centre

MAIN_VMEM = 40 * 2**20
UPDATE_VMEM = 16 * 2**20


def fill_dense(params_ref, dense):
    count, block = params_ref.shape
    for b in range(block // LANES):
        part, line = divmod(b, 8)
        for r in range(0, count, 8):
            size = min(8, count - r)
            where = pl.ds((part * PAD_ROWS + r) * 8 + line, size, stride=8)
            dense[where, :] = params_ref[r : r + size, b * LANES : (b + 1) * LANES]


def dense_rows(dense, part, count):
    return [
        dense[(part * PAD_ROWS + r) * 8 : (part * PAD_ROWS + r) * 8 + 8, :] for r in range(count)
    ]


def lane_pick(source, lanes):
    return jnp.take_along_axis(source, lanes, axis=1, mode="promise_in_bounds")


def gather_eight(load, blocks, index):
    index = jnp.maximum(index, 0)
    lanes, block = index & (LANES - 1), index >> 7
    total = lane_pick(load(0), lanes)
    for b in range(1, blocks):
        total = jnp.where(block == b, lane_pick(load(b), lanes), total)
    return total


def split_three(x):
    first = x.astype(jnp.bfloat16).astype(jnp.float32)
    rest = x - first
    second = rest.astype(jnp.bfloat16).astype(jnp.float32)
    return first, second, rest - second


def fill_hot(hot, index, start, bits):
    shape = (hot.shape[0], LANES)
    row_ids = lax.broadcasted_iota(jnp.int32, shape, 0).astype(jnp.float32).astype(jnp.bfloat16)
    low = (index & ((1 << bits) - 1)).astype(jnp.float32).astype(jnp.bfloat16)
    one, none = jnp.ones(shape, jnp.bfloat16), jnp.zeros(shape, jnp.bfloat16)
    hot[:, start : start + LANES] = jnp.where(row_ids == jnp.broadcast_to(low, shape), one, none)


def split_two(x):
    first = x.astype(jnp.bfloat16).astype(jnp.float32)
    return first, x - first


def fill_values(lhs, main, last, index, start, bits):
    groups = lhs.shape[0] // 18
    span = slice(start, start + LANES)
    parts = jnp.concatenate(split_two(main), axis=0)
    tips = [jnp.broadcast_to(item, (8, LANES)) for item in split_two(last)]
    high = jnp.broadcast_to(index >> bits, (16, LANES))
    sub = lax.broadcasted_iota(jnp.int32, (8, LANES), 0)
    for b in range(groups):
        lhs[16 * b : 16 * b + 16, span] = jnp.where(high == b, parts, 0.0).astype(jnp.bfloat16)
    for g in range(groups // 8):
        here = high[0:8] == sub + 8 * g
        rows = jnp.concatenate([jnp.where(here, item, 0.0) for item in tips], axis=0)
        row = 16 * groups + 16 * g
        lhs[row : row + 16, span] = rows.astype(jnp.bfloat16)


def scatter_dot(lhs, hot, rows):
    return lax.dot_general(
        lhs[rows], hot[...], (((1,), (1,)), ((), ())), preferred_element_type=jnp.float32
    )


def scatter_main(lhs, hot, first, last):
    out = scatter_dot(lhs, hot, slice(16 * first, 16 * last))
    return [out[16 * b : 16 * b + 8] + out[16 * b + 8 : 16 * b + 16] for b in range(last - first)]


def scatter_tips(lhs, hot):
    groups = lhs.shape[0] // 18
    out = scatter_dot(lhs, hot, slice(16 * groups, 18 * groups))
    return [
        out[16 * (b // 8) + b % 8 : 16 * (b // 8) + b % 8 + 1]
        + out[16 * (b // 8) + 8 + b % 8 : 16 * (b // 8) + 9 + b % 8]
        for b in range(groups)
    ]


def stage_features(feat_parts, plan_ref, table, last, order, tips):
    halves = plan_ref.shape[1] // LANES
    blocks = last.shape[0]
    for part, feats in enumerate(feat_parts):
        for f in range(8):
            table[pl.ds(part * 64 + f, 8, stride=8), :] = feats[f]
        last[part * 8 : part * 8 + 8, :] = feats[8]
    slots = plan_ref.shape[0] * halves
    for o in range(slots):
        d, h = divmod(o, halves)
        order[o : o + 1, :] = plan_ref[d : d + 1, h * LANES : (h + 1) * LANES]
    for p in range(slots // 8):
        tips[8 * p : 8 * p + 8, :] = gather_eight(
            lambda b: jnp.broadcast_to(last[b : b + 1, :], (8, LANES)),
            blocks,
            order[8 * p : 8 * p + 8, :],
        )


def pack_features(d, halves, table, order, tips, out_ref):
    blocks = table.shape[0] // 8
    for h in range(halves):
        row = pl.ds(d * halves + h, 1)
        out_ref[d, 8 * h : 8 * h + 8, :] = gather_eight(
            lambda b: table[8 * b : 8 * b + 8, :],
            blocks,
            jnp.broadcast_to(order[row, :], (8, LANES)),
        )
        out_ref[d, 8 * halves + h : 8 * halves + h + 1, :] = tips[row, :]


def pixel_terms():
    lane = lax.broadcasted_iota(jnp.int32, (8, LANES), 1)
    inner = lane & 31
    tile = lane >> 5
    x = (inner & 15).astype(jnp.float32) - 7.5
    step = (inner >> 4).astype(jnp.float32) - 0.5
    return tile, x, step


def render_setup(lists_ref, target_ref, order, wanted, basis, plan_sums, hot, bits):
    tiles, entries = lists_ref.shape
    quarters = entries // LANES
    for q in range(quarters):
        order[q * tiles : (q + 1) * tiles, :] = lists_ref[:, q * LANES : (q + 1) * LANES]
    sub = lax.broadcasted_iota(jnp.int32, (8, LANES), 0)
    lane = lax.broadcasted_iota(jnp.int32, (8, LANES), 1)
    tile, x, step = pixel_terms()
    shifted = 32 * (sub & 3) + (lane & 31)
    for k in range(3):
        total = jnp.zeros((8, LANES), jnp.float32)
        for r in range(8):
            row = jnp.broadcast_to(target_ref[k, :, r * LANES : (r + 1) * LANES], (8, LANES))
            here = (tile == r // 2) & ((sub >> 2) == r % 2)
            total = jnp.where(here, lane_pick(row, shifted), total)
        wanted[8 * k : 8 * k + 8, :] = total
    for g in range(LANES // 8):
        row = sub + 8 * g
        coef = (row * 43) >> 9
        mine = tile == (row & 3)

        def column(j, *terms):
            total = jnp.zeros((8, LANES), jnp.float32)
            for c, value in terms:
                total = jnp.where(coef == c, value, total)
            total = jnp.where(mine, total, 0.0)
            basis[8 * g : 8 * g + 8, j * LANES : (j + 1) * LANES] = total

        column(0, (0, x * x), (1, x * step), (2, step * step), (3, x), (4, step), (5, 1.0))
        column(1, (1, x), (2, 2.0 * step), (4, 1.0))
        column(2, (2, 1.0))
        for k in range(3):
            column(3 + k, (6 + k, 1.0))
    mine = tile == (sub & 3)
    for s in range(8):
        y = step + (2.0 * s - 7.0)
        rows = [jnp.ones_like(x), x, y, x * x, x * y, y * y]
        rows = jnp.concatenate([jnp.where(mine, item, 0.0) for item in rows], axis=0)
        for part in range(2):
            start = (part * 8 + s) * LANES
            plan_sums[:, start : start + LANES] = rows.astype(jnp.bfloat16)
    for o in range(tiles * quarters):
        fill_hot(hot, order[o : o + 1, :], o * LANES, bits)


def render_rest(
    cells, others, receive, recv_ref, order, wanted, back_ref,
    coefs, tables, basis, alpha_s, weight_s, slope_s, joint_g, joint_w, plan_sums, error_sums,
    turned, tinted, moved, pairs, lhs, hot, bits,
):
    owners, packed, _ = recv_ref.shape
    halves = packed // FEATS
    blocks = owners * halves
    tiles = 4
    quarters = order.shape[0] // tiles
    entries = quarters * LANES
    me = lax.axis_index("cells")
    rows_pix = tiles * cells // TILE_COLS * 16
    half_width = TILE_COLS * 8.0
    inv_width = 1.0 / half_width
    log_two = 1.4426950408889634
    sub = lax.broadcasted_iota(jnp.int32, (8, LANES), 0)
    local = sub & 3
    tile_col = 4 * lax.rem(me, TILE_COLS // 4) + local
    tile_row = lax.div(me, TILE_COLS // 4)
    centre_col = (16 * tile_col + 8).astype(jnp.float32) - half_width
    centre_row = (jnp.full((8, LANES), 16 * tile_row + 8, jnp.int32)).astype(
        jnp.float32
    ) - rows_pix * 0.5

    picked = [[None] * FEATS for _ in range(quarters // 2)]
    for k in range(owners):
        origin = others[-k] if k else me
        if k:
            receive(origin)
        for p in range(quarters // 2):
            index = jnp.maximum(order[8 * p : 8 * p + 8, :], 0)
            lanes, block = index & (LANES - 1), index >> 7
            for h in range(halves):
                here = block == origin * halves + h
                for f in range(FEATS):
                    r = 8 * h + f if f < 8 else 8 * halves + h
                    row = jnp.broadcast_to(recv_ref[origin, r : r + 1, :], (8, LANES))
                    item = lane_pick(row, lanes)
                    old = picked[p][f]
                    picked[p][f] = item if old is None else jnp.where(here, item, old)

    for p in range(quarters // 2):
        index = order[8 * p : 8 * p + 8, :]
        feats = picked[p]
        off_col = feats[0] * half_width - centre_col
        off_row = feats[1] * half_width - centre_row
        moved[16 * p : 16 * p + 8, :] = off_col
        moved[16 * p + 8 : 16 * p + 16, :] = off_row
        square = feats[2] * (-0.5 * log_two * inv_width * inv_width)
        cross = feats[3] * (-log_two * inv_width * inv_width)
        bend = feats[4] * (-0.5 * log_two * inv_width * inv_width)
        faint = jnp.maximum(jnp.log(feats[5]) * log_two, -1e30)
        along = square * off_col + cross * off_row
        level = along * off_col + bend * off_row * off_row + jnp.where(index >= 0, faint, -1e30)
        terms = [
            square,
            cross,
            bend,
            -(along + square * off_col),
            -(2.0 * bend * off_row + cross * off_col),
            level,
            feats[6],
            feats[7],
            feats[8],
        ]
        for c, term in enumerate(terms):
            for i, piece in enumerate(split_three(term)):
                row = (3 * c + i) * tiles
                for q in range(2):
                    start = (2 * p + q) * LANES
                    coefs[start + row : start + row + tiles, :] = piece[4 * q : 4 * q + 4]
    for q in range(quarters):
        coefs[q * LANES + 108 : (q + 1) * LANES, :] = jnp.zeros((LANES - 108, LANES), jnp.float32)
    weights = basis[...].astype(jnp.bfloat16)
    for q in range(quarters):
        span = slice(q * LANES, (q + 1) * LANES)
        columns = jnp.transpose(coefs[span, :]).astype(jnp.bfloat16)
        result = jnp.dot(columns, weights, preferred_element_type=jnp.float32)
        for j in range(6):
            tables[j, span, :] = result[:, j * LANES : (j + 1) * LANES]

    height = (2 * sub - 7).astype(jnp.float32)

    def table(l, j):
        return jnp.broadcast_to(tables[j, pl.ds(l, 1), :], (8, LANES))

    def relay(source, base, joint, q, c, s):
        item = source[pl.ds(base + c * 128 + s, 16, stride=8), :]
        top = item.astype(jnp.bfloat16)
        rows = pl.ds(pl.multiple_of(q * LANES, LANES) + c * 16, 16)
        joint[rows, s * LANES : (s + 1) * LANES] = top
        joint[rows, (8 + s) * LANES : (9 + s) * LANES] = (
            item - top.astype(jnp.float32)
        ).astype(jnp.bfloat16)

    chunks = LANES // 16

    def forward(q, carry):
        trans, red, green, blue = carry
        base = pl.multiple_of(q * 8 * LANES, 8 * LANES)
        first = pl.multiple_of(q * LANES, LANES)
        for c in range(chunks):
            for i in range(16):
                l = first + (c * 16 + i)
                where = pl.ds(base + (c * 16 + i) * 8, 8)
                power = table(l, 0) + height * (table(l, 1) + height * table(l, 2))
                alpha = jnp.exp2(power)
                weight = alpha * trans
                alpha_s[where, :] = alpha
                weight_s[where, :] = weight
                trans = trans * (1.0 - alpha)
                red = red + weight * table(l, 3)
                green = green + weight * table(l, 4)
                blue = blue + weight * table(l, 5)
                if c and i % 2:
                    relay(weight_s, base, joint_w, q, c - 1, i // 2)
        for s in range(8):
            relay(weight_s, base, joint_w, q, chunks - 1, s)
        return trans, red, green, blue

    zero = jnp.zeros((8, LANES), jnp.float32)
    carry = lax.fori_loop(
        0, quarters, forward, (jnp.ones((8, LANES), jnp.float32), zero, zero, zero)
    )
    red, green, blue = carry[1:]
    errors = [2.0 * (item - wanted[8 * k : 8 * k + 8, :]) for k, item in enumerate((red, green, blue))]
    wanted[0:8, :], wanted[8:16, :], wanted[16:24, :] = errors
    tile, _, _ = pixel_terms()
    mine = tile == local
    for s in range(8):
        tops, lows = [], []
        for k in range(3):
            row = jnp.broadcast_to(wanted[8 * k + s : 8 * k + s + 1, :], (8, LANES))
            row = jnp.where(mine, row, 0.0)
            top = row.astype(jnp.bfloat16).astype(jnp.float32)
            tops.append(top)
            lows.append(row - top)
        blank = [jnp.zeros((24, LANES), jnp.float32)]
        start = s * LANES
        error_sums[:, start : start + LANES] = jnp.concatenate(tops + lows, axis=0).astype(jnp.bfloat16)
        start = (8 + s) * LANES
        error_sums[:, start : start + LANES] = jnp.concatenate(tops + blank, axis=0).astype(jnp.bfloat16)

    def sum_pixels(factors, joint, result, q):
        span = pl.ds(pl.multiple_of(q * LANES, LANES), LANES)
        result[:, span] = lax.dot_general(
            factors[...],
            joint[span, :],
            (((1,), (1,)), ((), ())),
            preferred_element_type=jnp.float32,
        )

    def backward(q, behind, late):
        base = pl.multiple_of(q * 8 * LANES, 8 * LANES)
        first = pl.multiple_of(q * LANES, LANES)
        sum_pixels(error_sums, joint_w, tinted, q)
        if late:
            sum_pixels(plan_sums, joint_g, turned, q + 1)
        for c in range(chunks - 1, -1, -1):
            for i in range(15, -1, -1):
                l = first + (c * 16 + i)
                where = pl.ds(base + (c * 16 + i) * 8, 8)
                slope = errors[0] * table(l, 3) + errors[1] * table(l, 4) + errors[2] * table(l, 5)
                alpha = alpha_s[where, :]
                slope_s[(c * 16 + i) * 8 : (c * 16 + i) * 8 + 8, :] = weight_s[where, :] * (
                    slope - behind
                )
                behind = (1.0 - alpha) * behind + alpha * slope
                if c < chunks - 1 and i % 2:
                    relay(slope_s, 0, joint_g, q, c + 1, i // 2)
        for s in range(8):
            relay(slope_s, 0, joint_g, q, 0, s)
        return behind

    behind = backward(quarters - 1, zero, False)
    lax.fori_loop(1, quarters, lambda i, v: backward(quarters - 1 - i, v, True), behind)
    sum_pixels(plan_sums, joint_g, turned, 0)
    for p in range(quarters // 2):
        off_col = moved[16 * p : 16 * p + 8, :]
        off_row = moved[16 * p + 8 : 16 * p + 16, :]

        def quantity(j):
            source, r = (turned, j) if j < 6 else (tinted, j - 6)
            rows = slice(8 * r, 8 * r + 8)
            start = 2 * p * LANES
            return jnp.where(
                sub < 4,
                source[rows, start : start + LANES],
                source[rows, start + LANES : start + 2 * LANES],
            )

        plain, across, down = quantity(0), quantity(1), quantity(2)
        near_col = across - off_col * plain
        near_row = down - off_row * plain
        rows = [
            plain,
            near_col * inv_width,
            near_row * inv_width,
            (quantity(3) - off_col * (across + near_col)) * (inv_width * inv_width),
            (quantity(4) - off_col * down - off_row * near_col) * (inv_width * inv_width),
            (quantity(5) - off_row * (down + near_row)) * (inv_width * inv_width),
            *[quantity(6 + k) + quantity(9 + k) for k in range(3)],
        ]
        for f, item in enumerate(rows):
            pairs[pl.ds(p * 128 + f, 8, stride=16), :] = item
    for o in range(tiles * quarters):
        fill_values(
            lhs,
            pairs[o * 16 : o * 16 + 8, :],
            pairs[o * 16 + 8 : o * 16 + 9, :],
            order[o : o + 1, :],
            o * LANES,
            bits,
        )
    for s, (main, last) in enumerate(zip(scatter_main(lhs, hot, 0, owners), scatter_tips(lhs, hot))):
        for h in range(halves):
            span = slice(h * LANES, (h + 1) * LANES)
            back_ref[s, 8 * h : 8 * h + 8, :] = main[:, span]
            back_ref[s, 8 * halves + h : 8 * halves + h + 1, :] = last[:, span]


def main_kernel(
    params_in, cam_in, plan_in, visible_in, lists_in, target_in, out_ref,
    params_ref, cam_ref, plan_ref, visible_ref, lists_ref, target_ref, dense, table, last, plan_order, outgoing, incoming, back, returned, extra, extras, relayed, tips,
    order, wanted, basis, coefs, tables, alpha_s, weight_s, slope_s, joint_g, joint_w,
    plan_sums, error_sums, turned, tinted, moved, pairs, lhs, hot, own_lhs, own_hot,
    send_one, recv_one, send_two, recv_two, send_three, recv_three, send_four, recv_four, local_sem,
):
    cells, views = lax.axis_size("cells"), lax.axis_size("views")
    cell, view = lax.axis_index("cells"), lax.axis_index("views")
    count, block = params_ref.shape
    blocks = block // LANES
    capacity = plan_ref.shape[1]
    halves = capacity // LANES
    bits = capacity.bit_length() - 1
    fetches = [
        pltpu.make_async_copy(source, dest, local_sem.at[i])
        for i, (source, dest) in enumerate(
            (
                (params_in, params_ref),
                (cam_in, cam_ref),
                (plan_in, plan_ref),
                (visible_in, visible_ref),
                (lists_in, lists_ref),
                (target_in, target_ref),
            )
        )
    ]
    for fetch in fetches:
        fetch.start()
    barrier = pltpu.get_barrier_semaphore()

    def greet(axis, me, size):
        for k in range(1, size):
            pl.semaphore_signal(
                barrier,
                inc=1,
                device_id={axis: lax.rem(me + k, size)},
                device_id_type=pl.DeviceIdType.MESH,
            )

    far = lax.div(cell, 4)
    depth, side = lax.div(cell, 2), lax.rem(cell, 2)
    others = [
        2 * d + e
        for d in (3 - 3 * far, 2 - far, 1 - depth + 4 * far)
        for e in (1 - side, side)
    ] + [2 * depth + 1 - side]
    twin = view + 1 - 2 * lax.rem(view, 2)
    across = lax.rem(view + 2, views)
    mates = [twin, across, lax.rem(twin + 2, views)]

    def send(axis, peer, source, dest, send_sem, recv_sem):
        copy = pltpu.make_async_remote_copy(
            src_ref=source,
            dst_ref=dest,
            send_sem=send_sem,
            recv_sem=recv_sem,
            device_id={axis: peer},
            device_id_type=pl.DeviceIdType.MESH,
        )
        copy.start()
        return copy

    def receiver(buffer, sems):
        def receive(origin):
            pltpu.make_async_remote_copy(
                src_ref=buffer.at[origin],
                dst_ref=buffer.at[origin],
                send_sem=sems.at[origin],
                recv_sem=sems.at[origin],
                device_id={"cells": origin},
                device_id_type=pl.DeviceIdType.MESH,
            ).wait_recv()

        return receive

    receive_one = receiver(incoming, recv_one)
    receive_two = receiver(returned, recv_two)
    greet("cells", cell, cells)
    greet("views", view, views)
    fetches[1].wait()
    turn, centre = camera_terms(cam_ref[...])
    known = [*turn[0], *turn[1], *turn[2], *centre]
    lane = lax.broadcasted_iota(jnp.int32, (8, LANES), 1)
    line = jnp.zeros((8, LANES), jnp.float32)
    for i, item in enumerate(known):
        line = jnp.where(lane == i, jnp.broadcast_to(item, (8, LANES)), line)
    extra[blocks : blocks + 8, :] = line
    fetches[3].wait()
    for b in range(blocks):
        extra[b : b + 1, :] = visible_ref[:, b * LANES : (b + 1) * LANES].astype(jnp.float32)
    fetches[0].wait()
    fill_dense(params_ref, dense)
    feat_parts = [
        project_rows(dense_rows(dense, part, count), turn, centre) for part in range(blocks // 8)
    ]
    fetches[2].wait()
    stage_features(feat_parts, plan_ref, table, last, plan_order, tips)
    pl.semaphore_wait(barrier, cells + views - 2)

    sent = []
    for i, peer in enumerate(others):
        pack_features(peer, halves, table, plan_order, tips, outgoing)
        sent.append(
            send(
                "cells", peer, outgoing.at[peer], incoming.at[cell],
                send_one.at[i], recv_one.at[cell],
            )
        )
    pack_features(cell, halves, table, plan_order, tips, incoming)
    fetches[4].wait()
    fetches[5].wait()
    render_setup(lists_ref, target_ref, order, wanted, basis, plan_sums, hot, bits)
    wide = own_hot.shape[0].bit_length() - 1
    arrivals = [cell] + others[::-1]
    slots = cells * halves
    sub = lax.broadcasted_iota(jnp.int32, (8, LANES), 0)
    count_lanes = lane.astype(jnp.float32)
    for o in range(slots):
        row = plan_order[o : o + 1, :]
        fill_hot(own_hot, row, o * LANES, wide)
        here = jnp.broadcast_to(row >> wide, (8, LANES)) == sub
        own_lhs[:, o * LANES : (o + 1) * LANES] = jnp.concatenate(
            [jnp.where(here, o + 1.0, 0.0), jnp.where(here, count_lanes, 0.0)], axis=0
        ).astype(jnp.bfloat16)
    inverse = lax.dot_general(
        own_lhs[...], own_hot[...], (((1,), (1,)), ((), ())), preferred_element_type=jnp.float32
    )
    for i in range(2):
        span = slice(i * LANES, (i + 1) * LANES)
        extra[pl.ds(blocks + 8 + i, 8, stride=2), :] = inverse[0:8, span]
        extra[pl.ds(2 * blocks + 8 + i, 8, stride=2), :] = inverse[8:16, span]
    early = [
        send("views", mate, extra, extras.at[view], send_four.at[j], recv_four.at[j])
        for j, mate in enumerate(mates)
    ]
    render_rest(
        cells, others, receive_one, incoming, order, wanted, back,
        coefs, tables, basis, alpha_s, weight_s, slope_s, joint_g, joint_w, plan_sums, error_sums,
        turned, tinted, moved, pairs, lhs, hot, bits,
    )
    sent += [
        send(
            "cells", peer, back.at[peer], returned.at[cell], send_two.at[i], recv_two.at[cell]
        )
        for i, peer in enumerate(others)
    ]

    def forward(k, source, origin):
        return [
            send(
                "views", mate, source, relayed.at[view, origin],
                send_three.at[k, j], recv_three.at[k, j],
            )
            for j, mate in enumerate(mates)
        ]

    relays = [forward(0, back.at[cell], cell)]
    for copy in early:
        copy.wait()
    counts = extra[0:blocks, :]
    for mate in mates:
        counts = counts + extras[mate, 0:blocks, :]
    grads = blocks * PAD_ROWS
    out_ref[grads : grads + blocks, :] = counts
    parts = blocks // 8
    seen = [extra] + [extras.at[mate] for mate in mates]
    rows_of = [dense_rows(dense, part, count) for part in range(parts)]
    statics = [static_terms(rows) for rows in rows_of]
    turns, terms = [], []
    for source in seen:
        known = [
            jnp.broadcast_to(source[blocks : blocks + 1, i : i + 1], (8, LANES)) for i in range(12)
        ]
        turns.append([known[0:3], known[3:6], known[6:9]])
        terms.append(
            [
                moving_terms(rows_of[part], statics[part][3], turns[-1], known[9:12])
                for part in range(parts)
            ]
        )
    for k in range(1, cells):
        receive_two(arrivals[k])
        relays.append(forward(k, returned.at[arrivals[k]], arrivals[k]))

    def collect(v, got, packet, origin):
        for part in range(parts):
            start = blocks + 8 + 8 * part
            block = seen[v][start : start + 8, :].astype(jnp.int32)
            lanes = seen[v][blocks + start : blocks + start + 8, :].astype(jnp.int32)
            for h in range(halves):
                here = block == origin * halves + h + 1
                for f in range(FEATS):
                    r = 8 * h + f if f < 8 else 8 * halves + h
                    item = lane_pick(jnp.broadcast_to(packet[r : r + 1, :], (8, LANES)), lanes)
                    got[part][f] = jnp.where(here, item, got[part][f])

    def nothing():
        return [[jnp.zeros((8, LANES), jnp.float32)] * FEATS for _ in range(parts)]

    totals = [None] * parts

    def pull_group(group, gots, last):
        for part in range(parts):
            sums, shades = None, None
            for v, got in zip(group, gots):
                moved_part, shade_part = pull_moving(
                    dense_rows(dense, part, count), terms[v][part], turns[v], got[part]
                )
                if sums is None:
                    sums, shades = moved_part, shade_part
                else:
                    sums = [a + b for a, b in zip(sums, moved_part)]
                    shades = [a + b for a, b in zip(shades, shade_part)]
            if totals[part] is not None:
                sums = [a + b for a, b in zip(sums, totals[part])]
            base = part * PAD_ROWS
            for r, item in enumerate(shades):
                where = slice((base + 11 + r) * 8, (base + 12 + r) * 8)
                out_ref[where, :] = item if totals[part] is None else out_ref[where, :] + item
            totals[part] = sums
            if last:
                for r, item in enumerate(pull_static(statics[part], sums)):
                    out_ref[(base + r) * 8 : (base + r + 1) * 8, :] = item

    got = nothing()
    for k in range(cells):
        collect(0, got, returned.at[arrivals[k]] if k else back.at[cell], arrivals[k])
    pull_group((0,), (got,), False)
    for group in ((1,), (2, 3)):
        gots = [nothing() for _ in group]
        for k in range(cells):
            for v, got in zip(group, gots):
                relays[k][v - 1].wait()
                collect(v, got, relayed.at[mates[v - 1], arrivals[k]], arrivals[k])
        pull_group(group, gots, 3 in group)
    for copy in sent:
        copy.wait_send()


def update_kernel(params_ref, first_ref, second_ref, grads_ref, new_ref, new_first_ref, new_second_ref):
    count, block = params_ref.shape
    blocks = block // LANES
    row_ids = lax.broadcasted_iota(jnp.int32, (8, LANES), 0)
    bias_one = 1.0 - 0.9**ADAM_STEP
    bias_two = 1.0 - 0.999**ADAM_STEP
    for b in range(blocks):
        span = slice(b * LANES, (b + 1) * LANES)
        part, line = divmod(b, 8)
        counts = grads_ref[blocks * PAD_ROWS + b : blocks * PAD_ROWS + b + 1, :]
        for r in range(0, count, 8):
            size = min(8, count - r)
            rows = slice(r, r + size)
            gradient = grads_ref[pl.ds((part * PAD_ROWS + r) * 8 + line, size, stride=8), :]
            if r >= 16:
                rates = 0.000125
            else:
                ids = row_ids[0:size] + r
                rates = jnp.where(
                    ids < 6,
                    0.01,
                    jnp.where(
                        ids < 10,
                        0.005,
                        jnp.where(ids < 11, 0.05, jnp.where(ids < 14, 0.0025, 0.000125)),
                    ),
                )
            params, first, second = params_ref[rows, span], first_ref[rows, span], second_ref[rows, span]
            seen = jnp.broadcast_to(counts, params.shape) > 0.0
            first_new = 0.9 * first + 0.1 * gradient
            second_new = 0.999 * second + 0.001 * gradient * gradient
            stride = rates * (first_new / bias_one) / (jnp.sqrt(second_new / bias_two) + 1e-08)
            new_ref[rows, span] = jnp.where(seen, params - stride, params)
            new_first_ref[rows, span] = jnp.where(seen, first_new, first)
            new_second_ref[rows, span] = jnp.where(seen, second_new, second)


def fused_shards(params, first_moment, second_moment, cameras, visible, send_plan, tile_lists, target):
    cells, views = lax.axis_size("cells"), lax.axis_size("views")
    count, block = params.shape
    blocks = block // LANES
    plan = send_plan[0, 0]
    lists = tile_lists[0]
    tiles, entries = lists.shape
    capacity = plan.shape[1]
    halves = capacity // LANES
    slots = cells * halves
    f32, bf16 = jnp.float32, jnp.bfloat16
    packet = pltpu.VMEM((cells, FEATS * halves, LANES), f32)
    dma = pltpu.SemaphoreType.DMA
    vmem = pl.BlockSpec(memory_space=pltpu.VMEM)
    grads = pl.pallas_call(
        main_kernel,
        out_shape=jax.ShapeDtypeStruct((blocks * PAD_ROWS + blocks, LANES), f32),
        in_specs=[pl.BlockSpec(memory_space=pltpu.HBM)] * 6,
        out_specs=vmem,
        scratch_shapes=[
            pltpu.VMEM((count, block), f32),
            pltpu.VMEM(cameras.shape, f32),
            pltpu.VMEM(plan.shape, jnp.int32),
            pltpu.VMEM(visible.shape, jnp.int32),
            pltpu.VMEM(lists.shape, jnp.int32),
            pltpu.VMEM((3, 1, target.shape[2]), f32),
            pltpu.VMEM((blocks * PAD_ROWS, LANES), f32),
            pltpu.VMEM((blocks * 8, LANES), f32),
            pltpu.VMEM((blocks, LANES), f32),
            pltpu.VMEM((slots, LANES), jnp.int32),
            packet, packet, packet, packet,
            pltpu.VMEM((3 * blocks + 8, LANES), f32),
            pltpu.VMEM((views, 3 * blocks + 8, LANES), f32),
            pltpu.VMEM((views, cells, FEATS * halves, LANES), f32),
            pltpu.VMEM((slots, LANES), f32),
            pltpu.VMEM((tiles * entries // LANES, LANES), jnp.int32),
            pltpu.VMEM((24, LANES), f32),
            pltpu.VMEM((LANES, 6 * LANES), f32),
            pltpu.VMEM((entries, LANES), f32),
            pltpu.VMEM((6, entries, LANES), f32),
            pltpu.VMEM((entries * 8, LANES), f32),
            pltpu.VMEM((entries * 8, LANES), f32),
            pltpu.VMEM((8 * LANES, LANES), f32),
            pltpu.VMEM((entries, 16 * LANES), bf16),
            pltpu.VMEM((entries, 16 * LANES), bf16),
            pltpu.VMEM((48, 16 * LANES), bf16),
            pltpu.VMEM((48, 16 * LANES), bf16),
            pltpu.VMEM((48, entries), f32),
            pltpu.VMEM((48, entries), f32),
            pltpu.VMEM((entries // LANES * 8, LANES), f32),
            pltpu.VMEM((tiles * entries // LANES * 16, LANES), f32),
            pltpu.VMEM((cells * 18, tiles * entries), bf16),
            pltpu.VMEM((capacity, tiles * entries), bf16),
            pltpu.VMEM((16, slots * LANES), bf16),
            pltpu.VMEM((2 * LANES, slots * LANES), bf16),
            dma((cells - 1,)), dma((cells,)), dma((cells - 1,)), dma((cells,)),
            dma((cells, views - 1)), dma((cells, views - 1)), dma((views - 1,)), dma((views - 1,)),
            dma((6,)),
        ],
        compiler_params=pltpu.CompilerParams(
            collective_id=0,
            has_side_effects=True,
            vmem_limit_bytes=MAIN_VMEM,
        ),
        cost_estimate=pl.CostEstimate(
            flops=4096 * tiles * 256 * entries,
            bytes_accessed=4 * count * block,
            transcendentals=tiles * 256 * entries,
        ),
    )(
        *[
            pltpu.with_memory_space_constraint(item, pltpu.HBM)
            for item in (params, cameras, plan, visible, lists, jnp.transpose(target, (1, 0, 2)))
        ]
    )
    like = jax.ShapeDtypeStruct(params.shape, f32)
    return tuple(
        pl.pallas_call(
            update_kernel,
            out_shape=(like, like, like),
            compiler_params=pltpu.CompilerParams(vmem_limit_bytes=UPDATE_VMEM),
        )(params, first_moment, second_moment, grads)
    )


def local_shards(params, first_moment, second_moment, cameras, visible, send_plan, tile_lists, target):
    capacity = send_plan.shape[3]
    tiles, entries = tile_lists.shape[1:]
    halves = capacity // LANES
    fits = (
        capacity % LANES == 0
        and params.shape[1] == 16 * LANES
        and entries % (2 * LANES) == 0
        and 8 % max(halves, 1) == 0
        and lax.axis_size("cells") == 8
        and lax.axis_size("views") == 4
        and tiles * entries <= 4096
        and tiles == 4
    )
    body = fused_shards if fits else shards
    return body(params, first_moment, second_moment, cameras, visible, send_plan, tile_lists, target)


def solution(mesh):
    in_specs = (
        P(None, "cells"),
        P(None, "cells"),
        P(None, "cells"),
        P("views", None),
        P("views", "cells"),
        P("views", "cells", None, None),
        P("views", "cells", None),
        P("views", None, "cells"),
    )
    out_specs = (P(None, "cells"), P(None, "cells"), P(None, "cells"))
    return jax.shard_map(local_shards, mesh=mesh, in_specs=in_specs, out_specs=out_specs, check_vma=False)
```

```python
import functools

import jax
import jax.numpy as jnp
from jax import lax
from jax.experimental import pallas as pl
from jax.experimental.pallas import tpu as pltpu
from jax.sharding import PartitionSpec as P

TILE_COLS = 32
ADAM_STEP = 1000


harmonic_zero = 0.28209479177387814
harmonic_one = 0.4886025119029199
harmonic_two = (
    1.0925484305920792,
    -1.0925484305920792,
    0.31539156525252005,
    -1.0925484305920792,
    0.5462742152960396,
)
harmonic_three = (
    -0.5900435899266435,
    2.890611442640554,
    -0.4570457994644658,
    0.3731763325901154,
    -0.4570457994644658,
    1.445305721320277,
    -0.5900435899266435,
)


def harmonics(across, upward, onward):
    across_sq = across * across
    upward_sq = upward * upward
    onward_sq = onward * onward
    return jnp.stack(
        [
            harmonic_zero * jnp.ones_like(across),
            -harmonic_one * upward,
            harmonic_one * onward,
            -harmonic_one * across,
            harmonic_two[0] * across * upward,
            harmonic_two[1] * upward * onward,
            harmonic_two[2] * (2.0 * onward_sq - across_sq - upward_sq),
            harmonic_two[3] * across * onward,
            harmonic_two[4] * (across_sq - upward_sq),
            harmonic_three[0] * upward * (3.0 * across_sq - upward_sq),
            harmonic_three[1] * across * upward * onward,
            harmonic_three[2] * upward * (4.0 * onward_sq - across_sq - upward_sq),
            harmonic_three[3] * onward * (2.0 * onward_sq - 3.0 * across_sq - 3.0 * upward_sq),
            harmonic_three[4] * across * (4.0 * onward_sq - across_sq - upward_sq),
            harmonic_three[5] * onward * (across_sq - upward_sq),
            harmonic_three[6] * across * (across_sq - 3.0 * upward_sq),
        ]
    )


def camera_rotation(angles):
    cos_roll, sin_roll = (jnp.cos(angles[0]), jnp.sin(angles[0]))
    cos_pitch, sin_pitch = (jnp.cos(angles[1]), jnp.sin(angles[1]))
    cos_yaw, sin_yaw = (jnp.cos(angles[2]), jnp.sin(angles[2]))
    naught = jnp.zeros_like(cos_roll)
    unit_one = jnp.ones_like(cos_roll)
    roll = jnp.stack(
        [
            jnp.stack([unit_one, naught, naught]),
            jnp.stack([naught, cos_roll, -sin_roll]),
            jnp.stack([naught, sin_roll, cos_roll]),
        ]
    )
    pitch = jnp.stack(
        [
            jnp.stack([cos_pitch, naught, sin_pitch]),
            jnp.stack([naught, unit_one, naught]),
            jnp.stack([-sin_pitch, naught, cos_pitch]),
        ]
    )
    yawing = jnp.stack(
        [
            jnp.stack([cos_yaw, -sin_yaw, naught]),
            jnp.stack([sin_yaw, cos_yaw, naught]),
            jnp.stack([naught, naught, unit_one]),
        ]
    )
    inner_turn = jnp.dot(pitch, roll, precision=lax.Precision.HIGHEST)
    return jnp.dot(yawing, inner_turn, precision=lax.Precision.HIGHEST)


def project(values, camera):
    turn = camera_rotation(camera[0:3])
    offset = values[0:3] - camera[3:6][:, None]
    in_view = jnp.dot(turn, offset, precision=lax.Precision.HIGHEST)
    inv_depth = 1.0 / in_view[2]
    screen_col = in_view[0] * inv_depth
    screen_row = in_view[1] * inv_depth
    scales = jnp.exp(values[3:6])
    quat = values[6:10] / jnp.sqrt(jnp.sum(values[6:10] * values[6:10], axis=0, keepdims=True))
    quat_w, quat_x, quat_y, quat_z = (quat[0], quat[1], quat[2], quat[3])
    spin = [
        [
            1.0 - 2.0 * (quat_y * quat_y + quat_z * quat_z),
            2.0 * (quat_x * quat_y - quat_w * quat_z),
            2.0 * (quat_x * quat_z + quat_w * quat_y),
        ],
        [
            2.0 * (quat_x * quat_y + quat_w * quat_z),
            1.0 - 2.0 * (quat_x * quat_x + quat_z * quat_z),
            2.0 * (quat_y * quat_z - quat_w * quat_x),
        ],
        [
            2.0 * (quat_x * quat_z - quat_w * quat_y),
            2.0 * (quat_y * quat_z + quat_w * quat_x),
            1.0 - 2.0 * (quat_x * quat_x + quat_y * quat_y),
        ],
    ]
    basis_cam = []
    for outer_index in range(3):
        row_terms = []
        for col_index in range(3):
            entry = turn[outer_index, 0] * spin[0][col_index]
            for mid_index in range(1, 3):
                entry = entry + turn[outer_index, mid_index] * spin[mid_index][col_index]
            row_terms.append(entry * scales[col_index])
        basis_cam.append(row_terms)
    jac_top = [
        (basis_cam[0][col_index] - screen_col * basis_cam[2][col_index]) * inv_depth
        for col_index in range(3)
    ]
    jac_low = [
        (basis_cam[1][col_index] - screen_row * basis_cam[2][col_index]) * inv_depth
        for col_index in range(3)
    ]
    sigma_a = jac_top[0] * jac_top[0] + jac_top[1] * jac_top[1] + jac_top[2] * jac_top[2]
    sigma_b = jac_top[0] * jac_low[0] + jac_top[1] * jac_low[1] + jac_top[2] * jac_low[2]
    sigma_c = jac_low[0] * jac_low[0] + jac_low[1] * jac_low[1] + jac_low[2] * jac_low[2]
    determinant = sigma_a * sigma_c - sigma_b * sigma_b
    opacity = jax.nn.sigmoid(values[10])
    distance = jnp.sqrt(jnp.sum(offset * offset, axis=0))
    unit_dir = offset / distance
    basis = harmonics(unit_dir[0], unit_dir[1], unit_dir[2])
    coeffs = values[11:59].reshape(16, 3, values.shape[1])
    colors = 0.5 + jnp.sum(basis[:, None, :] * coeffs, axis=0)
    screen = jnp.stack(
        [
            screen_col,
            screen_row,
            sigma_c / determinant,
            -sigma_b / determinant,
            sigma_a / determinant,
            opacity,
        ]
    )
    return jnp.concatenate([screen, colors], axis=0)


def group_loss(pieces):
    features, live_mask, pixel_column, pixel_row, target_tile = pieces
    entries = live_mask.shape[1]
    delta_col = pixel_column[:, :, None] - features[0][:, None, :]
    delta_row = pixel_row[:, :, None] - features[1][:, None, :]
    power = -0.5 * (
        features[2][:, None, :] * delta_col * delta_col
        + 2.0 * features[3][:, None, :] * delta_col * delta_row
        + features[4][:, None, :] * delta_row * delta_row
    )
    alphas = features[5][:, None, :] * jnp.exp(power) * live_mask[:, None, :]
    log_keep = jnp.log(1.0 - alphas)
    earlier = (
        lax.broadcasted_iota(jnp.int32, (entries, entries), 0)
        < lax.broadcasted_iota(jnp.int32, (entries, entries), 1)
    ).astype(jnp.float32)
    transmit = jnp.exp(
        jnp.einsum("bpl,lm->bpm", log_keep, earlier, precision=lax.Precision.HIGHEST)
    )
    weights = alphas * transmit
    image = jnp.einsum("bpl,kbl->kbp", weights, features[6:9], precision=lax.Precision.HIGHEST)
    error = image - target_tile
    return jnp.sum(error * error)


def render_tiles(picked, live_mask, pixel_column, pixel_row, target_tile):
    groups = live_mask.shape[0] // 4
    entries = live_mask.shape[1]
    pixels = pixel_column.shape[1]
    stacked = (
        jnp.transpose(picked.reshape(picked.shape[0], groups, 4, entries), (1, 0, 2, 3)),
        live_mask.reshape(groups, 4, entries),
        pixel_column.reshape(groups, 4, pixels),
        pixel_row.reshape(groups, 4, pixels),
        jnp.transpose(target_tile.reshape(3, groups, 4, pixels), (1, 0, 2, 3)),
    )
    return jnp.sum(lax.map(jax.checkpoint(group_loss), stacked))


def pixel_grid(first_tile, count, tiles_dev, rows_pix):
    tile_ids = first_tile + jnp.arange(count, dtype=jnp.int32)
    pixel_ids = jnp.arange(256, dtype=jnp.int32)
    block_cols = TILE_COLS // 4
    owner_ids = tile_ids // tiles_dev
    local_ids = tile_ids % tiles_dev
    tile_col = 4 * (owner_ids % block_cols) + local_ids % 4
    tile_row = tiles_dev // 4 * (owner_ids // block_cols) + local_ids // 4
    half_width = TILE_COLS * 8.0
    column = (tile_col[:, None] * 16 + pixel_ids[None, :] % 16).astype(jnp.float32)
    row_pos = (tile_row[:, None] * 16 + pixel_ids[None, :] // 16).astype(jnp.float32)
    return ((column + 0.5 - half_width) / half_width, (row_pos + 0.5 - rows_pix * 0.5) / half_width)


def adam_update(params, first_moment, second_moment, gradient, counts):
    row_ids = lax.broadcasted_iota(jnp.int32, params.shape, 0)
    rates = jnp.where(
        row_ids < 6,
        0.01,
        jnp.where(
            row_ids < 10,
            0.005,
            jnp.where(row_ids < 11, 0.05, jnp.where(row_ids < 14, 0.0025, 0.000125)),
        ),
    )
    first_new = 0.9 * first_moment + 0.1 * gradient
    second = 0.999 * second_moment + 0.001 * gradient * gradient
    bias_one = 1.0 - 0.9**ADAM_STEP
    bias_two = 1.0 - 0.999**ADAM_STEP
    stride = rates * (first_new / bias_one) / (jnp.sqrt(second / bias_two) + 1e-08)
    seen_mask = counts > 0.0
    return (
        jnp.where(seen_mask, params - stride, params),
        jnp.where(seen_mask, first_new, first_moment),
        jnp.where(seen_mask, second, second_moment),
    )


def shards(params, first_moment, second_moment, cameras, visible, send_plan, tile_lists, target):
    cells = lax.axis_size("cells")
    camera = cameras[0]
    plan_rows = send_plan[0, 0]
    capacity = plan_rows.shape[1]
    sent_live = (plan_rows >= 0)[None]
    sent_rows = jnp.maximum(plan_rows, 0)
    lists = tile_lists[0]
    tiles_here = lists.shape[0]
    live_mask = (lists >= 0).astype(jnp.float32)
    slot_ids = jnp.maximum(lists, 0)
    rows_pix = tiles_here * cells // TILE_COLS * 16
    pixel_column, pixel_row = pixel_grid(
        lax.axis_index("cells") * tiles_here, tiles_here, tiles_here, rows_pix
    )
    target_tile = target[0].reshape(3, tiles_here, 256)
    block = params.shape[1]

    def image_loss(table):
        picked = jnp.take(table, slot_ids, axis=1)
        return render_tiles(picked, live_mask, pixel_column, pixel_row, target_tile)

    def own_projection(values):
        return project(values, camera)

    features, project_pull = jax.vjp(own_projection, params)
    outgoing = jnp.take(features, sent_rows, axis=1)
    incoming = lax.all_to_all(outgoing, "cells", split_axis=1, concat_axis=1, tiled=True)
    loss_value, pullback = jax.vjp(
        image_loss, incoming.reshape(features.shape[0], cells * capacity)
    )
    table_grad = pullback(jnp.ones((), jnp.float32))[0]
    returned = lax.all_to_all(
        table_grad.reshape(features.shape[0], cells, capacity),
        "cells",
        split_axis=1,
        concat_axis=1,
        tiled=True,
    )
    kept = jnp.where(sent_live, returned, 0.0)
    gradient = project_pull(
        jnp.zeros((features.shape[0], block), jnp.float32).at[:, sent_rows].add(kept)
    )[0]
    seen_here = visible.astype(jnp.float32)
    total_grad, counts = lax.psum((gradient, seen_here), "views")
    new_params, new_first, new_second = adam_update(
        params, first_moment, second_moment, total_grad, counts
    )
    return (new_params, new_first, new_second)

LANES = 128
PAD_ROWS = 64
FEATS = 9


def project_rows(rows, turn, centre):
    offset = [rows[i] - centre[i] for i in range(3)]
    in_view = [
        turn[i][0] * offset[0] + turn[i][1] * offset[1] + turn[i][2] * offset[2] for i in range(3)
    ]
    inv_depth = 1.0 / in_view[2]
    screen_col = in_view[0] * inv_depth
    screen_row = in_view[1] * inv_depth
    scales = [jnp.exp(rows[3 + i]) for i in range(3)]
    raw = rows[6:10]
    norm = jnp.sqrt(raw[0] * raw[0] + raw[1] * raw[1] + raw[2] * raw[2] + raw[3] * raw[3])
    inv_norm = 1.0 / norm
    quat_w, quat_x, quat_y, quat_z = [item * inv_norm for item in raw]
    spin = [
        [
            1.0 - 2.0 * (quat_y * quat_y + quat_z * quat_z),
            2.0 * (quat_x * quat_y - quat_w * quat_z),
            2.0 * (quat_x * quat_z + quat_w * quat_y),
        ],
        [
            2.0 * (quat_x * quat_y + quat_w * quat_z),
            1.0 - 2.0 * (quat_x * quat_x + quat_z * quat_z),
            2.0 * (quat_y * quat_z - quat_w * quat_x),
        ],
        [
            2.0 * (quat_x * quat_z - quat_w * quat_y),
            2.0 * (quat_y * quat_z + quat_w * quat_x),
            1.0 - 2.0 * (quat_x * quat_x + quat_y * quat_y),
        ],
    ]
    basis_cam = [
        [
            (turn[i][0] * spin[0][j] + turn[i][1] * spin[1][j] + turn[i][2] * spin[2][j])
            * scales[j]
            for j in range(3)
        ]
        for i in range(3)
    ]
    top = [(basis_cam[0][j] - screen_col * basis_cam[2][j]) * inv_depth for j in range(3)]
    low = [(basis_cam[1][j] - screen_row * basis_cam[2][j]) * inv_depth for j in range(3)]
    sigma_a = top[0] * top[0] + top[1] * top[1] + top[2] * top[2]
    sigma_b = top[0] * low[0] + top[1] * low[1] + top[2] * low[2]
    sigma_c = low[0] * low[0] + low[1] * low[1] + low[2] * low[2]
    inv_det = 1.0 / (sigma_a * sigma_c - sigma_b * sigma_b)
    opacity = 1.0 / (1.0 + jnp.exp(-rows[10]))
    inv_dist = 1.0 / jnp.sqrt(offset[0] * offset[0] + offset[1] * offset[1] + offset[2] * offset[2])
    x, y, z = [item * inv_dist for item in offset]
    xx, yy, zz = x * x, y * y, z * z
    basis = [
        None,
        -harmonic_one * y,
        harmonic_one * z,
        -harmonic_one * x,
        harmonic_two[0] * x * y,
        harmonic_two[1] * y * z,
        harmonic_two[2] * (2.0 * zz - xx - yy),
        harmonic_two[3] * x * z,
        harmonic_two[4] * (xx - yy),
        harmonic_three[0] * y * (3.0 * xx - yy),
        harmonic_three[1] * x * y * z,
        harmonic_three[2] * y * (4.0 * zz - xx - yy),
        harmonic_three[3] * z * (2.0 * zz - 3.0 * xx - 3.0 * yy),
        harmonic_three[4] * x * (4.0 * zz - xx - yy),
        harmonic_three[5] * z * (xx - yy),
        harmonic_three[6] * x * (xx - 3.0 * yy),
    ]
    colors = []
    for k in range(3):
        total = harmonic_zero * rows[11 + k]
        for j in range(1, 16):
            total = total + basis[j] * rows[11 + 3 * j + k]
        colors.append(0.5 + total)
    return (
        screen_col,
        screen_row,
        sigma_c * inv_det,
        -sigma_b * inv_det,
        sigma_a * inv_det,
        opacity,
        *colors,
    )


def static_terms(rows):
    scales = [jnp.exp(item) for item in rows[3:6]]
    raw = rows[6:10]
    inv_norm = 1.0 / jnp.sqrt(
        raw[0] * raw[0] + raw[1] * raw[1] + raw[2] * raw[2] + raw[3] * raw[3]
    )
    quat = [item * inv_norm for item in raw]
    w, x, y, z = quat
    spin = [
        [1.0 - 2.0 * (y * y + z * z), 2.0 * (x * y - w * z), 2.0 * (x * z + w * y)],
        [2.0 * (x * y + w * z), 1.0 - 2.0 * (x * x + z * z), 2.0 * (y * z - w * x)],
        [2.0 * (x * z - w * y), 2.0 * (y * z + w * x), 1.0 - 2.0 * (x * x + y * y)],
    ]
    frame = [[spin[m][j] * scales[j] for j in range(3)] for m in range(3)]
    fade = 1.0 - 1.0 / (1.0 + jnp.exp(-rows[10]))
    return scales, inv_norm, quat, frame, fade


def moving_terms(rows, frame, turn, centre):
    offset = [rows[i] - centre[i] for i in range(3)]
    in_view = [
        turn[i][0] * offset[0] + turn[i][1] * offset[1] + turn[i][2] * offset[2] for i in range(3)
    ]
    inv = 1.0 / in_view[2]
    col, row = in_view[0] * inv, in_view[1] * inv
    cam = [
        [
            turn[i][0] * frame[0][j] + turn[i][1] * frame[1][j] + turn[i][2] * frame[2][j]
            for j in range(3)
        ]
        for i in range(3)
    ]
    top = [(cam[0][j] - col * cam[2][j]) * inv for j in range(3)]
    low = [(cam[1][j] - row * cam[2][j]) * inv for j in range(3)]
    sigma_a = top[0] * top[0] + top[1] * top[1] + top[2] * top[2]
    sigma_b = top[0] * low[0] + top[1] * low[1] + top[2] * low[2]
    sigma_c = low[0] * low[0] + low[1] * low[1] + low[2] * low[2]
    inv_det = 1.0 / (sigma_a * sigma_c - sigma_b * sigma_b)
    conic = (sigma_c * inv_det, -sigma_b * inv_det, sigma_a * inv_det)
    inv_dist = 1.0 / jnp.sqrt(offset[0] * offset[0] + offset[1] * offset[1] + offset[2] * offset[2])
    ray = [item * inv_dist for item in offset]
    return inv, col, row, cam[2], top, low, conic, inv_dist, ray


def pull_moving(rows, terms, turn, got):
    inv, col, row, deep, top, low, conic, inv_dist, ray = terms
    k0, k1, k2 = conic
    g0, half, g2 = -0.5 * got[3], -0.5 * got[4], -0.5 * got[5]
    p00, p01 = g0 * k0 + half * k1, g0 * k1 + half * k2
    p10, p11 = half * k0 + g2 * k1, half * k1 + g2 * k2
    d00 = -2.0 * (k0 * p00 + k1 * p10)
    d01 = -2.0 * (k0 * p01 + k1 * p11)
    d11 = -2.0 * (k1 * p01 + k2 * p11)
    d_top = [(d00 * top[j] + d01 * low[j]) * inv for j in range(3)]
    d_low = [(d01 * top[j] + d11 * low[j]) * inv for j in range(3)]
    d_cam = [d_top, d_low, [-(col * d_top[j] + row * d_low[j]) for j in range(3)]]
    d_col = k0 * got[1] + k1 * got[2]
    d_row = k1 * got[1] + k2 * got[2]
    d_depth = 0.0
    for j in range(3):
        d_col = d_col - d_top[j] * deep[j]
        d_row = d_row - d_low[j] * deep[j]
        d_depth = d_depth - (d_top[j] * top[j] + d_low[j] * low[j])
    d_view = [d_col * inv, d_row * inv]
    d_view.append(d_depth - (col * d_view[0] + row * d_view[1]))
    d_frame = [
        [turn[0][m] * d_cam[0][j] + turn[1][m] * d_cam[1][j] + turn[2][m] * d_cam[2][j] for j in range(3)]
        for m in range(3)
    ]
    x, y, z = ray
    xx, yy, zz = x * x, y * y, z * z
    xy, yz, xz = x * y, y * z, x * z
    h1, h2, h3 = harmonic_one, harmonic_two, harmonic_three
    outer = 4.0 * zz - xx - yy
    basis = [
        None,
        -h1 * y,
        h1 * z,
        -h1 * x,
        h2[0] * xy,
        h2[1] * yz,
        h2[2] * (2.0 * zz - xx - yy),
        h2[3] * xz,
        h2[4] * (xx - yy),
        h3[0] * y * (3.0 * xx - yy),
        h3[1] * xy * z,
        h3[2] * y * outer,
        h3[3] * z * (2.0 * zz - 3.0 * xx - 3.0 * yy),
        h3[4] * x * outer,
        h3[5] * z * (xx - yy),
        h3[6] * x * (xx - 3.0 * yy),
    ]
    tint = got[6:9]
    d_shade = [harmonic_zero * item for item in tint]
    d_shade += [basis[j] * tint[k] for j in range(1, 16) for k in range(3)]
    e = [None] + [
        tint[0] * rows[11 + 3 * j] + tint[1] * rows[12 + 3 * j] + tint[2] * rows[13 + 3 * j]
        for j in range(1, 16)
    ]
    gx = (
        -h1 * e[3]
        + y * (h2[0] * e[4] + (6.0 * h3[0]) * (x * e[9]) - (2.0 * h3[2]) * (x * e[11]))
        + z * (h2[3] * e[7] + h3[1] * (y * e[10]))
        + x * ((-2.0 * h2[2]) * e[6] + (2.0 * h2[4]) * e[8])
        + xz * ((-6.0 * h3[3]) * e[12] + (2.0 * h3[5]) * e[14])
        + (h3[4] * (outer - 2.0 * xx)) * e[13]
        + ((3.0 * h3[6]) * (xx - yy)) * e[15]
    )
    gy = (
        -h1 * e[1]
        + x * (h2[0] * e[4] - (2.0 * h3[4]) * (y * e[13]) - (6.0 * h3[6]) * (y * e[15]))
        + z * (h2[1] * e[5] + h3[1] * (x * e[10]))
        + y * ((-2.0 * h2[2]) * e[6] - (2.0 * h2[4]) * e[8])
        + yz * ((-6.0 * h3[3]) * e[12] - (2.0 * h3[5]) * e[14])
        + ((3.0 * h3[0]) * (xx - yy)) * e[9]
        + (h3[2] * (outer - 2.0 * yy)) * e[11]
    )
    gz = (
        h1 * e[2]
        + y * (h2[1] * e[5] + h3[1] * (x * e[10]) + (8.0 * h3[2]) * (z * e[11]))
        + x * (h2[3] * e[7] + (8.0 * h3[4]) * (z * e[13]))
        + (4.0 * h2[2]) * (z * e[6])
        + ((3.0 * h3[3]) * (2.0 * zz - xx - yy)) * e[12]
        + (h3[5] * (xx - yy)) * e[14]
    )
    along = x * gx + y * gy + z * gz
    d_ray = [(gx - x * along) * inv_dist, (gy - y * along) * inv_dist, (gz - z * along) * inv_dist]
    d_place = [
        turn[0][i] * d_view[0] + turn[1][i] * d_view[1] + turn[2][i] * d_view[2] + d_ray[i]
        for i in range(3)
    ]
    return [*d_place, *d_frame[0], *d_frame[1], *d_frame[2], got[0]], d_shade


def pull_static(static, sums):
    scales, inv_norm, quat, frame, fade = static
    d_frame = [sums[3:6], sums[6:9], sums[9:12]]
    d_scale = [
        d_frame[0][j] * frame[0][j] + d_frame[1][j] * frame[1][j] + d_frame[2][j] * frame[2][j]
        for j in range(3)
    ]
    d = [[d_frame[m][j] * scales[j] for j in range(3)] for m in range(3)]
    w, x, y, z = quat
    d_quat = [
        2.0 * (z * (d[1][0] - d[0][1]) + y * (d[0][2] - d[2][0]) + x * (d[2][1] - d[1][2])),
        2.0 * (y * (d[0][1] + d[1][0]) + z * (d[0][2] + d[2][0]) + w * (d[2][1] - d[1][2]) - 2.0 * x * (d[1][1] + d[2][2])),
        2.0 * (x * (d[0][1] + d[1][0]) + w * (d[0][2] - d[2][0]) + z * (d[1][2] + d[2][1]) - 2.0 * y * (d[0][0] + d[2][2])),
        2.0 * (w * (d[1][0] - d[0][1]) + x * (d[0][2] + d[2][0]) + y * (d[1][2] + d[2][1]) - 2.0 * z * (d[0][0] + d[1][1])),
    ]
    along = w * d_quat[0] + x * d_quat[1] + y * d_quat[2] + z * d_quat[3]
    d_raw = [(d_quat[i] - quat[i] * along) * inv_norm for i in range(4)]
    return [*sums[0:3], *d_scale, *d_raw, fade * sums[12]]


def camera_terms(cam):
    cosines, sines = jnp.cos(cam), jnp.sin(cam)
    cr, cp, cy = [cosines[:, i : i + 1] for i in range(3)]
    sr, sp, sy = [sines[:, i : i + 1] for i in range(3)]
    turn = [
        [cy * cp, cy * sp * sr - sy * cr, cy * sp * cr + sy * sr],
        [sy * cp, sy * sp * sr + cy * cr, sy * sp * cr - cy * sr],
        [-sp, cp * sr, cp * cr],
    ]
    centre = [cam[:, 3 + i : 4 + i] for i in range(3)]
    return turn, centre

MAIN_VMEM = 40 * 2**20
UPDATE_VMEM = 16 * 2**20
WAVES = 4


def fill_dense(params_ref, dense):
    count, block = params_ref.shape
    for b in range(block // LANES):
        part, line = divmod(b, 8)
        for r in range(0, count, 8):
            size = min(8, count - r)
            where = pl.ds((part * PAD_ROWS + r) * 8 + line, size, stride=8)
            dense[where, :] = params_ref[r : r + size, b * LANES : (b + 1) * LANES]


def dense_rows(dense, part, count):
    return [
        dense[(part * PAD_ROWS + r) * 8 : (part * PAD_ROWS + r) * 8 + 8, :] for r in range(count)
    ]


def lane_pick(source, lanes):
    return jnp.take_along_axis(source, lanes, axis=1, mode="promise_in_bounds")


def gather_eight(load, blocks, index):
    index = jnp.maximum(index, 0)
    lanes, block = index & (LANES - 1), index >> 7
    total = lane_pick(load(0), lanes)
    for b in range(1, blocks):
        total = jnp.where(block == b, lane_pick(load(b), lanes), total)
    return total


def split_three(x):
    first = x.astype(jnp.bfloat16).astype(jnp.float32)
    rest = x - first
    second = rest.astype(jnp.bfloat16).astype(jnp.float32)
    return first, second, rest - second


def fill_hot(hot, index, start, bits):
    shape = (hot.shape[0], LANES)
    row_ids = lax.broadcasted_iota(jnp.int32, shape, 0).astype(jnp.float32).astype(jnp.bfloat16)
    low = (index & ((1 << bits) - 1)).astype(jnp.float32).astype(jnp.bfloat16)
    one, none = jnp.ones(shape, jnp.bfloat16), jnp.zeros(shape, jnp.bfloat16)
    hot[:, start : start + LANES] = jnp.where(row_ids == jnp.broadcast_to(low, shape), one, none)


def split_two(x):
    first = x.astype(jnp.bfloat16).astype(jnp.float32)
    return first, x - first


def fill_values(lhs, main, last, index, start, bits):
    groups = lhs.shape[0] // 18
    span = slice(start, start + LANES)
    parts = jnp.concatenate(split_two(main), axis=0)
    tips = [jnp.broadcast_to(item, (8, LANES)) for item in split_two(last)]
    high = jnp.broadcast_to(index >> bits, (16, LANES))
    sub = lax.broadcasted_iota(jnp.int32, (8, LANES), 0)
    for b in range(groups):
        lhs[16 * b : 16 * b + 16, span] = jnp.where(high == b, parts, 0.0).astype(jnp.bfloat16)
    for g in range(groups // 8):
        here = high[0:8] == sub + 8 * g
        rows = jnp.concatenate([jnp.where(here, item, 0.0) for item in tips], axis=0)
        row = 16 * groups + 16 * g
        lhs[row : row + 16, span] = rows.astype(jnp.bfloat16)


def scatter_dot(lhs, hot, rows):
    return lax.dot_general(
        lhs[rows], hot[...], (((1,), (1,)), ((), ())), preferred_element_type=jnp.float32
    )


def scatter_main(lhs, hot, first, last):
    out = scatter_dot(lhs, hot, slice(16 * first, 16 * last))
    return [out[16 * b : 16 * b + 8] + out[16 * b + 8 : 16 * b + 16] for b in range(last - first)]


def scatter_tips(lhs, hot):
    groups = lhs.shape[0] // 18
    out = scatter_dot(lhs, hot, slice(16 * groups, 18 * groups))
    return [
        out[16 * (b // 8) + b % 8 : 16 * (b // 8) + b % 8 + 1]
        + out[16 * (b // 8) + 8 + b % 8 : 16 * (b // 8) + 9 + b % 8]
        for b in range(groups)
    ]


def stage_features(feat_parts, plan_ref, table, last, order, tips):
    halves = plan_ref.shape[1] // LANES
    blocks = last.shape[0]
    for part, feats in enumerate(feat_parts):
        for f in range(8):
            table[pl.ds(part * 64 + f, 8, stride=8), :] = feats[f]
        last[part * 8 : part * 8 + 8, :] = feats[8]
    slots = plan_ref.shape[0] * halves
    for o in range(slots):
        d, h = divmod(o, halves)
        order[o : o + 1, :] = plan_ref[d : d + 1, h * LANES : (h + 1) * LANES]
    for p in range(slots // 8):
        tips[8 * p : 8 * p + 8, :] = gather_eight(
            lambda b: jnp.broadcast_to(last[b : b + 1, :], (8, LANES)),
            blocks,
            order[8 * p : 8 * p + 8, :],
        )


def pack_features(d, halves, table, order, tips, out_ref):
    blocks = table.shape[0] // 8
    for h in range(halves):
        row = pl.ds(d * halves + h, 1)
        out_ref[d, 8 * h : 8 * h + 8, :] = gather_eight(
            lambda b: table[8 * b : 8 * b + 8, :],
            blocks,
            jnp.broadcast_to(order[row, :], (8, LANES)),
        )
        out_ref[d, 8 * halves + h : 8 * halves + h + 1, :] = tips[row, :]


def pixel_terms():
    lane = lax.broadcasted_iota(jnp.int32, (8, LANES), 1)
    inner = lane & 31
    tile = lane >> 5
    x = (inner & 15).astype(jnp.float32) - 7.5
    step = (inner >> 4).astype(jnp.float32) - 0.5
    return tile, x, step


def render_setup(lists_ref, target_ref, order, wanted, basis, plan_sums, hot, bits):
    tiles, entries = lists_ref.shape
    quarters = entries // LANES
    for q in range(quarters):
        order[q * tiles : (q + 1) * tiles, :] = lists_ref[:, q * LANES : (q + 1) * LANES]
    sub = lax.broadcasted_iota(jnp.int32, (8, LANES), 0)
    lane = lax.broadcasted_iota(jnp.int32, (8, LANES), 1)
    tile, x, step = pixel_terms()
    shifted = 32 * (sub & 3) + (lane & 31)
    for k in range(3):
        total = jnp.zeros((8, LANES), jnp.float32)
        for r in range(8):
            row = jnp.broadcast_to(target_ref[k, :, r * LANES : (r + 1) * LANES], (8, LANES))
            here = (tile == r // 2) & ((sub >> 2) == r % 2)
            total = jnp.where(here, lane_pick(row, shifted), total)
        wanted[8 * k : 8 * k + 8, :] = total
    for g in range(LANES // 8):
        row = sub + 8 * g
        coef = (row * 43) >> 9
        mine = tile == (row & 3)

        def column(j, *terms):
            total = jnp.zeros((8, LANES), jnp.float32)
            for c, value in terms:
                total = jnp.where(coef == c, value, total)
            total = jnp.where(mine, total, 0.0)
            basis[8 * g : 8 * g + 8, j * LANES : (j + 1) * LANES] = total

        column(0, (0, x * x), (1, x * step), (2, step * step), (3, x), (4, step), (5, 1.0))
        column(1, (1, x), (2, 2.0 * step), (4, 1.0))
        column(2, (2, 1.0))
        for k in range(3):
            column(3 + k, (6 + k, 1.0))
    mine = tile == (sub & 3)
    for s in range(8):
        y = step + (2.0 * s - 7.0)
        rows = [jnp.ones_like(x), x, y, x * x, x * y, y * y]
        rows = jnp.concatenate([jnp.where(mine, item, 0.0) for item in rows], axis=0)
        for part in range(2):
            start = (part * 8 + s) * LANES
            plan_sums[:, start : start + LANES] = rows.astype(jnp.bfloat16)
    for o in range(tiles * quarters):
        fill_hot(hot, order[o : o + 1, :], o * LANES, bits)


def render_rest(
    cells, others, receive, recv_ref, order, wanted, back_ref,
    coefs, tables, basis, alpha_s, weight_s, stages, joint_g, joint_w, plan_sums, error_sums,
    turned, tinted, moved, pairs, lhs, hot, bits,
):
    owners, packed, _ = recv_ref.shape
    halves = packed // FEATS
    blocks = owners * halves
    tiles = 4
    quarters = order.shape[0] // tiles
    entries = quarters * LANES
    me = lax.axis_index("cells")
    rows_pix = tiles * cells // TILE_COLS * 16
    half_width = TILE_COLS * 8.0
    inv_width = 1.0 / half_width
    log_two = 1.4426950408889634
    sub = lax.broadcasted_iota(jnp.int32, (8, LANES), 0)
    local = sub & 3
    tile_col = 4 * lax.rem(me, TILE_COLS // 4) + local
    tile_row = lax.div(me, TILE_COLS // 4)
    centre_col = (16 * tile_col + 8).astype(jnp.float32) - half_width
    centre_row = (jnp.full((8, LANES), 16 * tile_row + 8, jnp.int32)).astype(
        jnp.float32
    ) - rows_pix * 0.5

    picked = [[None] * FEATS for _ in range(quarters // 2)]
    for k in range(owners):
        origin = others[-k] if k else me
        if k:
            receive(origin)
        for p in range(quarters // 2):
            index = jnp.maximum(order[8 * p : 8 * p + 8, :], 0)
            lanes, block = index & (LANES - 1), index >> 7
            for h in range(halves):
                here = block == origin * halves + h
                for f in range(FEATS):
                    r = 8 * h + f if f < 8 else 8 * halves + h
                    row = jnp.broadcast_to(recv_ref[origin, r : r + 1, :], (8, LANES))
                    item = lane_pick(row, lanes)
                    old = picked[p][f]
                    picked[p][f] = item if old is None else jnp.where(here, item, old)

    for p in range(quarters // 2):
        index = order[8 * p : 8 * p + 8, :]
        feats = picked[p]
        off_col = feats[0] * half_width - centre_col
        off_row = feats[1] * half_width - centre_row
        moved[16 * p : 16 * p + 8, :] = off_col
        moved[16 * p + 8 : 16 * p + 16, :] = off_row
        square = feats[2] * (-0.5 * log_two * inv_width * inv_width)
        cross = feats[3] * (-log_two * inv_width * inv_width)
        bend = feats[4] * (-0.5 * log_two * inv_width * inv_width)
        faint = jnp.maximum(jnp.log(feats[5]) * log_two, -1e30)
        along = square * off_col + cross * off_row
        level = along * off_col + bend * off_row * off_row + jnp.where(index >= 0, faint, -1e30)
        terms = [
            square,
            cross,
            bend,
            -(along + square * off_col),
            -(2.0 * bend * off_row + cross * off_col),
            level,
            feats[6],
            feats[7],
            feats[8],
        ]
        for c, term in enumerate(terms):
            for i, piece in enumerate(split_three(term)):
                row = (3 * c + i) * tiles
                for q in range(2):
                    start = (2 * p + q) * LANES
                    coefs[start + row : start + row + tiles, :] = piece[4 * q : 4 * q + 4]
    for q in range(quarters):
        coefs[q * LANES + 108 : (q + 1) * LANES, :] = jnp.zeros((LANES - 108, LANES), jnp.float32)
    weights = basis[...].astype(jnp.bfloat16)
    for q in range(quarters):
        span = slice(q * LANES, (q + 1) * LANES)
        columns = jnp.transpose(coefs[span, :]).astype(jnp.bfloat16)
        result = jnp.dot(columns, weights, preferred_element_type=jnp.float32)
        for j in range(6):
            tables[j, span, :] = result[:, j * LANES : (j + 1) * LANES]

    height = (2 * sub - 7).astype(jnp.float32)

    def table(l, j):
        return jnp.broadcast_to(tables[j, pl.ds(l, 1), :], (8, LANES))

    def keep(stage, c, i, item):
        tile = (c * 16 + i // 8 * 8) * 8
        stage[pl.ds(tile + i % 8, 8, stride=8), :] = item

    def turn_over(stage, joint, q, s):
        item = jnp.transpose(
            jnp.concatenate([stage[t * 64 + s * 8 : t * 64 + s * 8 + 8, :] for t in range(16)], axis=0)
        )
        top = item.astype(jnp.bfloat16)
        span = pl.ds(pl.multiple_of(q * LANES, LANES), LANES)
        joint[s * LANES : (s + 1) * LANES, span] = top
        joint[(8 + s) * LANES : (9 + s) * LANES, span] = (
            item - top.astype(jnp.float32)
        ).astype(jnp.bfloat16)

    chunks = LANES // 16

    def forward(q, carry, stage, other):
        trans, red, green, blue = carry
        first = pl.multiple_of(q * LANES, LANES)
        base = pl.multiple_of(q * 8 * LANES, 8 * LANES)
        for c in range(chunks):
            for i in range(16):
                l = first + (c * 16 + i)
                where = pl.ds(base + (c * 16 + i) * 8, 8)
                power = table(l, 0) + height * (table(l, 1) + height * table(l, 2))
                alpha = jnp.exp2(power)
                weight = alpha * trans
                alpha_s[where, :] = alpha
                weight_s[where, :] = weight
                keep(stage, c, i, weight)
                trans = trans * (1.0 - alpha)
                red = red + weight * table(l, 3)
                green = green + weight * table(l, 4)
                blue = blue + weight * table(l, 5)
            turn_over(other, joint_w, q, c)
        return trans, red, green, blue

    zero = jnp.zeros((8, LANES), jnp.float32)
    even, odd = stages

    def forward_pair(i, carry):
        carry = forward(2 * i, carry, even, odd)
        return forward(2 * i + 1, carry, odd, even)

    carry = lax.fori_loop(
        0, quarters // 2, forward_pair, (jnp.ones((8, LANES), jnp.float32), zero, zero, zero)
    )
    for c in range(chunks):
        turn_over(odd, joint_w, quarters, c)
    red, green, blue = carry[1:]
    errors = [2.0 * (item - wanted[8 * k : 8 * k + 8, :]) for k, item in enumerate((red, green, blue))]
    wanted[0:8, :], wanted[8:16, :], wanted[16:24, :] = errors
    tile, _, _ = pixel_terms()
    mine = tile == local
    for s in range(8):
        tops, lows = [], []
        for k in range(3):
            row = jnp.broadcast_to(wanted[8 * k + s : 8 * k + s + 1, :], (8, LANES))
            row = jnp.where(mine, row, 0.0)
            top = row.astype(jnp.bfloat16).astype(jnp.float32)
            tops.append(top)
            lows.append(row - top)
        blank = [jnp.zeros((24, LANES), jnp.float32)]
        start = s * LANES
        error_sums[:, start : start + LANES] = jnp.concatenate(tops + lows, axis=0).astype(jnp.bfloat16)
        start = (8 + s) * LANES
        error_sums[:, start : start + LANES] = jnp.concatenate(tops + blank, axis=0).astype(jnp.bfloat16)

    def backward(q, behind, stage, other):
        first = pl.multiple_of(q * LANES, LANES)
        tinted[:, pl.ds(first, LANES)] = jnp.dot(
            error_sums[...],
            joint_w[:, pl.ds(first + LANES, LANES)],
            preferred_element_type=jnp.float32,
        )
        base = pl.multiple_of(q * 8 * LANES, 8 * LANES)
        for c in range(chunks - 1, -1, -1):
            for i in range(15, -1, -1):
                l = first + (c * 16 + i)
                where = pl.ds(base + (c * 16 + i) * 8, 8)
                slope = errors[0] * table(l, 3) + errors[1] * table(l, 4) + errors[2] * table(l, 5)
                alpha = alpha_s[where, :]
                keep(stage, c, i, weight_s[where, :] * (slope - behind))
                behind = (1.0 - alpha) * behind + alpha * slope
            turn_over(other, joint_g, q + 1, chunks - 1 - c)
        return behind

    def backward_pair(i, behind):
        q = quarters - 1 - 2 * i
        behind = backward(q, behind, odd, even)
        return backward(q - 1, behind, even, odd)

    lax.fori_loop(0, quarters // 2, backward_pair, zero)
    for c in range(chunks):
        turn_over(even, joint_g, 0, c)
    turned[...] = jnp.dot(
        plan_sums[...], joint_g[:, 0:entries], preferred_element_type=jnp.float32
    )
    for p in range(quarters // 2):
        off_col = moved[16 * p : 16 * p + 8, :]
        off_row = moved[16 * p + 8 : 16 * p + 16, :]

        def quantity(j):
            source, r = (turned, j) if j < 6 else (tinted, j - 6)
            rows = slice(8 * r, 8 * r + 8)
            start = 2 * p * LANES
            return jnp.where(
                sub < 4,
                source[rows, start : start + LANES],
                source[rows, start + LANES : start + 2 * LANES],
            )

        plain, across, down = quantity(0), quantity(1), quantity(2)
        near_col = across - off_col * plain
        near_row = down - off_row * plain
        rows = [
            plain,
            near_col * inv_width,
            near_row * inv_width,
            (quantity(3) - off_col * (across + near_col)) * (inv_width * inv_width),
            (quantity(4) - off_col * down - off_row * near_col) * (inv_width * inv_width),
            (quantity(5) - off_row * (down + near_row)) * (inv_width * inv_width),
            *[quantity(6 + k) + quantity(9 + k) for k in range(3)],
        ]
        for f, item in enumerate(rows):
            pairs[pl.ds(p * 128 + f, 8, stride=16), :] = item
    for o in range(tiles * quarters):
        fill_values(
            lhs,
            pairs[o * 16 : o * 16 + 8, :],
            pairs[o * 16 + 8 : o * 16 + 9, :],
            order[o : o + 1, :],
            o * LANES,
            bits,
        )
    for s, (main, last) in enumerate(zip(scatter_main(lhs, hot, 0, owners), scatter_tips(lhs, hot))):
        for h in range(halves):
            span = slice(h * LANES, (h + 1) * LANES)
            back_ref[s, 8 * h : 8 * h + 8, :] = main[:, span]
            back_ref[s, 8 * halves + h : 8 * halves + h + 1, :] = last[:, span]


def main_kernel(
    params_in, cam_in, plan_in, visible_in, lists_in, target_in, out_ref,
    params_ref, cam_ref, plan_ref, visible_ref, lists_ref, target_ref, dense, table, last, plan_order, outgoing, incoming, back, returned, extra, extras, relayed, tips,
    order, wanted, basis, coefs, tables, alpha_s, weight_s, stages, joint_g, joint_w,
    plan_sums, error_sums, turned, tinted, moved, pairs, lhs, hot, own_lhs, own_hot,
    send_one, recv_one, send_two, recv_two, send_three, recv_three, send_four, recv_four, local_sem,
):
    cells, views = lax.axis_size("cells"), lax.axis_size("views")
    cell, view = lax.axis_index("cells"), lax.axis_index("views")
    count, block = params_ref.shape
    blocks = block // LANES
    capacity = plan_ref.shape[1]
    halves = capacity // LANES
    bits = capacity.bit_length() - 1
    fetches = [
        pltpu.make_async_copy(source, dest, local_sem.at[i])
        for i, (source, dest) in enumerate(
            (
                (params_in, params_ref),
                (cam_in, cam_ref),
                (plan_in, plan_ref),
                (visible_in, visible_ref),
                (lists_in, lists_ref),
                (target_in, target_ref),
            )
        )
    ]
    for fetch in fetches:
        fetch.start()
    barrier = pltpu.get_barrier_semaphore()

    def greet(axis, me, size):
        for k in range(1, size):
            pl.semaphore_signal(
                barrier,
                inc=1,
                device_id={axis: lax.rem(me + k, size)},
                device_id_type=pl.DeviceIdType.MESH,
            )

    far = lax.div(cell, 4)
    depth, side = lax.div(cell, 2), lax.rem(cell, 2)
    others = [
        2 * d + e
        for d in (3 - 3 * far, 2 - far, 1 - depth + 4 * far)
        for e in (1 - side, side)
    ] + [2 * depth + 1 - side]
    twin = view + 1 - 2 * lax.rem(view, 2)
    across = lax.rem(view + 2, views)
    mates = [twin, across, lax.rem(twin + 2, views)]

    def send(axis, peer, source, dest, send_sem, recv_sem):
        copy = pltpu.make_async_remote_copy(
            src_ref=source,
            dst_ref=dest,
            send_sem=send_sem,
            recv_sem=recv_sem,
            device_id={axis: peer},
            device_id_type=pl.DeviceIdType.MESH,
        )
        copy.start()
        return copy

    def receiver(buffer, sems):
        def receive(origin):
            pltpu.make_async_remote_copy(
                src_ref=buffer.at[origin],
                dst_ref=buffer.at[origin],
                send_sem=sems.at[origin],
                recv_sem=sems.at[origin],
                device_id={"cells": origin},
                device_id_type=pl.DeviceIdType.MESH,
            ).wait_recv()

        return receive

    receive_one = receiver(incoming, recv_one)
    receive_two = receiver(returned, recv_two)
    greet("cells", cell, cells)
    greet("views", view, views)
    fetches[1].wait()
    turn, centre = camera_terms(cam_ref[...])
    known = [*turn[0], *turn[1], *turn[2], *centre]
    lane = lax.broadcasted_iota(jnp.int32, (8, LANES), 1)
    line = jnp.zeros((8, LANES), jnp.float32)
    for i, item in enumerate(known):
        line = jnp.where(lane == i, jnp.broadcast_to(item, (8, LANES)), line)
    extra[blocks : blocks + 8, :] = line
    fetches[3].wait()
    for b in range(blocks):
        extra[b : b + 1, :] = visible_ref[:, b * LANES : (b + 1) * LANES].astype(jnp.float32)
    fetches[0].wait()
    fill_dense(params_ref, dense)
    feat_parts = [
        project_rows(dense_rows(dense, part, count), turn, centre) for part in range(blocks // 8)
    ]
    fetches[2].wait()
    stage_features(feat_parts, plan_ref, table, last, plan_order, tips)
    pl.semaphore_wait(barrier, cells + views - 2)

    sent = []
    for i, peer in enumerate(others):
        pack_features(peer, halves, table, plan_order, tips, outgoing)
        sent.append(
            send(
                "cells", peer, outgoing.at[peer], incoming.at[cell],
                send_one.at[i], recv_one.at[cell],
            )
        )
    pack_features(cell, halves, table, plan_order, tips, incoming)
    fetches[4].wait()
    fetches[5].wait()
    render_setup(lists_ref, target_ref, order, wanted, basis, plan_sums, hot, bits)
    wide = own_hot.shape[0].bit_length() - 1
    arrivals = [cell] + others[::-1]
    slots = cells * halves
    sub = lax.broadcasted_iota(jnp.int32, (8, LANES), 0)
    count_lanes = lane.astype(jnp.float32)
    for o in range(slots):
        row = plan_order[o : o + 1, :]
        fill_hot(own_hot, row, o * LANES, wide)
        here = jnp.broadcast_to(row >> wide, (8, LANES)) == sub
        own_lhs[:, o * LANES : (o + 1) * LANES] = jnp.concatenate(
            [jnp.where(here, o + 1.0, 0.0), jnp.where(here, count_lanes, 0.0)], axis=0
        ).astype(jnp.bfloat16)
    inverse = lax.dot_general(
        own_lhs[...], own_hot[...], (((1,), (1,)), ((), ())), preferred_element_type=jnp.float32
    )
    for i in range(2):
        span = slice(i * LANES, (i + 1) * LANES)
        extra[pl.ds(blocks + 8 + i, 8, stride=2), :] = inverse[0:8, span]
        extra[pl.ds(2 * blocks + 8 + i, 8, stride=2), :] = inverse[8:16, span]
    early = [
        send("views", mate, extra, extras.at[view], send_four.at[j], recv_four.at[j])
        for j, mate in enumerate(mates)
    ]
    render_rest(
        cells, others, receive_one, incoming, order, wanted, back,
        coefs, tables, basis, alpha_s, weight_s, stages, joint_g, joint_w, plan_sums, error_sums,
        turned, tinted, moved, pairs, lhs, hot, bits,
    )
    sent += [
        send(
            "cells", peer, back.at[peer], returned.at[cell], send_two.at[i], recv_two.at[cell]
        )
        for i, peer in enumerate(others)
    ]

    def forward(k, source, origin):
        return [
            send(
                "views", mate, source, relayed.at[view, origin],
                send_three.at[k, j], recv_three.at[k, j],
            )
            for j, mate in enumerate(mates)
        ]

    relays = [forward(0, back.at[cell], cell)]
    for copy in early:
        copy.wait()
    counts = extra[0:blocks, :]
    for mate in mates:
        counts = counts + extras[mate, 0:blocks, :]
    grads = blocks * PAD_ROWS
    out_ref[grads : grads + blocks, :] = counts
    parts = blocks // 8
    seen = [extra] + [extras.at[mate] for mate in mates]
    rows_of = [dense_rows(dense, part, count) for part in range(parts)]
    statics = [static_terms(rows) for rows in rows_of]
    turns, terms = [], []
    for source in seen:
        known = [
            jnp.broadcast_to(source[blocks : blocks + 1, i : i + 1], (8, LANES)) for i in range(12)
        ]
        turns.append([known[0:3], known[3:6], known[6:9]])
        terms.append(
            [
                moving_terms(rows_of[part], statics[part][3], turns[-1], known[9:12])
                for part in range(parts)
            ]
        )
    for k in range(1, cells):
        receive_two(arrivals[k])
        relays.append(forward(k, returned.at[arrivals[k]], arrivals[k]))

    def collect(v, got, packet, origin):
        for part in range(parts):
            start = blocks + 8 + 8 * part
            block = seen[v][start : start + 8, :].astype(jnp.int32)
            lanes = seen[v][blocks + start : blocks + start + 8, :].astype(jnp.int32)
            for h in range(halves):
                here = block == origin * halves + h + 1
                for f in range(FEATS):
                    r = 8 * h + f if f < 8 else 8 * halves + h
                    item = lane_pick(jnp.broadcast_to(packet[r : r + 1, :], (8, LANES)), lanes)
                    got[part][f] = jnp.where(here, item, got[part][f])

    def nothing():
        return [[jnp.zeros((8, LANES), jnp.float32)] * FEATS for _ in range(parts)]

    totals = [None] * parts

    def pull_group(group, gots, last):
        for part in range(parts):
            sums, shades = None, None
            for v, got in zip(group, gots):
                moved_part, shade_part = pull_moving(
                    dense_rows(dense, part, count), terms[v][part], turns[v], got[part]
                )
                if sums is None:
                    sums, shades = moved_part, shade_part
                else:
                    sums = [a + b for a, b in zip(sums, moved_part)]
                    shades = [a + b for a, b in zip(shades, shade_part)]
            if totals[part] is not None:
                sums = [a + b for a, b in zip(sums, totals[part])]
            base = part * PAD_ROWS
            for r, item in enumerate(shades):
                where = slice((base + 11 + r) * 8, (base + 12 + r) * 8)
                out_ref[where, :] = item if totals[part] is None else out_ref[where, :] + item
            totals[part] = sums
            if last:
                for r, item in enumerate(pull_static(statics[part], sums)):
                    out_ref[(base + r) * 8 : (base + r + 1) * 8, :] = item

    got = nothing()
    for k in range(cells):
        collect(0, got, returned.at[arrivals[k]] if k else back.at[cell], arrivals[k])
    pull_group((0,), (got,), False)
    for group in ((1,), (2, 3)):
        gots = [nothing() for _ in group]
        for k in range(cells):
            for v, got in zip(group, gots):
                relays[k][v - 1].wait()
                collect(v, got, relayed.at[mates[v - 1], arrivals[k]], arrivals[k])
        pull_group(group, gots, 3 in group)
    for copy in sent:
        copy.wait_send()


def update_kernel(
    params_ref, first_ref, second_ref, grads_ref, new_out, new_first_out, new_second_out,
    new_ref, new_first_ref, new_second_ref, sems,
):
    count, block = params_ref.shape
    blocks = block // LANES
    row_ids = lax.broadcasted_iota(jnp.int32, (8, LANES), 0)
    scale_one = 1.0 / (1.0 - 0.9**ADAM_STEP)
    scale_two = 1.0 / (1.0 - 0.999**ADAM_STEP)
    copies = []
    group = blocks // WAVES
    for b in range(blocks):
        span = slice(b * LANES, (b + 1) * LANES)
        part, line = divmod(b, 8)
        counts = grads_ref[blocks * PAD_ROWS + b : blocks * PAD_ROWS + b + 1, :]
        for r in range(0, count, 8):
            size = min(8, count - r)
            rows = slice(r, r + size)
            gradient = grads_ref[pl.ds((part * PAD_ROWS + r) * 8 + line, size, stride=8), :]
            if r >= 16:
                rates = 0.000125 * scale_one
            else:
                ids = row_ids[0:size] + r
                rates = scale_one * jnp.where(
                    ids < 6,
                    0.01,
                    jnp.where(
                        ids < 10,
                        0.005,
                        jnp.where(ids < 11, 0.05, jnp.where(ids < 14, 0.0025, 0.000125)),
                    ),
                )
            params, first, second = params_ref[rows, span], first_ref[rows, span], second_ref[rows, span]
            seen = jnp.broadcast_to(counts, params.shape) > 0.0
            first_new = 0.9 * first + 0.1 * gradient
            second_new = 0.999 * second + 0.001 * gradient * gradient
            stride = rates * first_new / (jnp.sqrt(second_new * scale_two) + 1e-08)
            new_ref[rows, span] = jnp.where(seen, params - stride, params)
            new_first_ref[rows, span] = jnp.where(seen, first_new, first)
            new_second_ref[rows, span] = jnp.where(seen, second_new, second)
        if (b + 1) % group == 0:
            wave = b // group
            span = slice(wave * group * LANES, (wave + 1) * group * LANES)
            for i, (source, dest) in enumerate(
                ((new_ref, new_out), (new_first_ref, new_first_out), (new_second_ref, new_second_out))
            ):
                copy = pltpu.make_async_copy(source.at[:, span], dest.at[:, span], sems.at[i, wave])
                copy.start()
                copies.append(copy)
    for copy in copies:
        copy.wait()


def fused_shards(params, first_moment, second_moment, cameras, visible, send_plan, tile_lists, target):
    cells, views = lax.axis_size("cells"), lax.axis_size("views")
    count, block = params.shape
    blocks = block // LANES
    plan = send_plan[0, 0]
    lists = tile_lists[0]
    tiles, entries = lists.shape
    capacity = plan.shape[1]
    halves = capacity // LANES
    slots = cells * halves
    f32, bf16 = jnp.float32, jnp.bfloat16
    packet = pltpu.VMEM((cells, FEATS * halves, LANES), f32)
    dma = pltpu.SemaphoreType.DMA
    vmem = pl.BlockSpec(memory_space=pltpu.VMEM)
    grads = pl.pallas_call(
        main_kernel,
        out_shape=jax.ShapeDtypeStruct((blocks * PAD_ROWS + blocks, LANES), f32),
        in_specs=[pl.BlockSpec(memory_space=pltpu.HBM)] * 6,
        out_specs=vmem,
        scratch_shapes=[
            pltpu.VMEM((count, block), f32),
            pltpu.VMEM(cameras.shape, f32),
            pltpu.VMEM(plan.shape, jnp.int32),
            pltpu.VMEM(visible.shape, jnp.int32),
            pltpu.VMEM(lists.shape, jnp.int32),
            pltpu.VMEM((3, 1, target.shape[2]), f32),
            pltpu.VMEM((blocks * PAD_ROWS, LANES), f32),
            pltpu.VMEM((blocks * 8, LANES), f32),
            pltpu.VMEM((blocks, LANES), f32),
            pltpu.VMEM((slots, LANES), jnp.int32),
            packet, packet, packet, packet,
            pltpu.VMEM((3 * blocks + 8, LANES), f32),
            pltpu.VMEM((views, 3 * blocks + 8, LANES), f32),
            pltpu.VMEM((views, cells, FEATS * halves, LANES), f32),
            pltpu.VMEM((slots, LANES), f32),
            pltpu.VMEM((tiles * entries // LANES, LANES), jnp.int32),
            pltpu.VMEM((24, LANES), f32),
            pltpu.VMEM((LANES, 6 * LANES), f32),
            pltpu.VMEM((entries, LANES), f32),
            pltpu.VMEM((6, entries, LANES), f32),
            pltpu.VMEM((entries * 8, LANES), f32),
            pltpu.VMEM((entries * 8, LANES), f32),
            [pltpu.VMEM((8 * LANES, LANES), f32)] * 2,
            pltpu.VMEM((16 * LANES, entries + LANES), bf16),
            pltpu.VMEM((16 * LANES, entries + LANES), bf16),
            pltpu.VMEM((48, 16 * LANES), bf16),
            pltpu.VMEM((48, 16 * LANES), bf16),
            pltpu.VMEM((48, entries), f32),
            pltpu.VMEM((48, entries), f32),
            pltpu.VMEM((entries // LANES * 8, LANES), f32),
            pltpu.VMEM((tiles * entries // LANES * 16, LANES), f32),
            pltpu.VMEM((cells * 18, tiles * entries), bf16),
            pltpu.VMEM((capacity, tiles * entries), bf16),
            pltpu.VMEM((16, slots * LANES), bf16),
            pltpu.VMEM((2 * LANES, slots * LANES), bf16),
            dma((cells - 1,)), dma((cells,)), dma((cells - 1,)), dma((cells,)),
            dma((cells, views - 1)), dma((cells, views - 1)), dma((views - 1,)), dma((views - 1,)),
            dma((6,)),
        ],
        compiler_params=pltpu.CompilerParams(
            collective_id=0,
            has_side_effects=True,
            vmem_limit_bytes=MAIN_VMEM,
        ),
        cost_estimate=pl.CostEstimate(
            flops=4096 * tiles * 256 * entries,
            bytes_accessed=4 * count * block,
            transcendentals=tiles * 256 * entries,
        ),
    )(
        *[
            pltpu.with_memory_space_constraint(item, pltpu.HBM)
            for item in (params, cameras, plan, visible, lists, jnp.transpose(target, (1, 0, 2)))
        ]
    )
    like = jax.ShapeDtypeStruct(params.shape, f32)
    return tuple(
        pl.pallas_call(
            update_kernel,
            out_shape=(like, like, like),
            out_specs=(pl.BlockSpec(memory_space=pl.ANY),) * 3,
            scratch_shapes=[
                pltpu.VMEM(params.shape, f32),
                pltpu.VMEM(params.shape, f32),
                pltpu.VMEM(params.shape, f32),
                dma((3, WAVES)),
            ],
            compiler_params=pltpu.CompilerParams(vmem_limit_bytes=UPDATE_VMEM),
        )(params, first_moment, second_moment, grads)
    )


def local_shards(params, first_moment, second_moment, cameras, visible, send_plan, tile_lists, target):
    capacity = send_plan.shape[3]
    tiles, entries = tile_lists.shape[1:]
    halves = capacity // LANES
    fits = (
        capacity % LANES == 0
        and params.shape[1] == 16 * LANES
        and entries % (2 * LANES) == 0
        and 8 % max(halves, 1) == 0
        and lax.axis_size("cells") == 8
        and lax.axis_size("views") == 4
        and tiles * entries <= 4096
        and tiles == 4
    )
    body = fused_shards if fits else shards
    return body(params, first_moment, second_moment, cameras, visible, send_plan, tile_lists, target)


def solution(mesh):
    in_specs = (
        P(None, "cells"),
        P(None, "cells"),
        P(None, "cells"),
        P("views", None),
        P("views", "cells"),
        P("views", "cells", None, None),
        P("views", "cells", None),
        P("views", None, "cells"),
    )
    out_specs = (P(None, "cells"), P(None, "cells"), P(None, "cells"))
    return jax.shard_map(local_shards, mesh=mesh, in_specs=in_specs, out_specs=out_specs, check_vma=False)
```

```python
import functools

import jax
import jax.numpy as jnp
from jax import lax
from jax.experimental import pallas as pl
from jax.experimental.pallas import tpu as pltpu
from jax.sharding import PartitionSpec as P

TILE_COLS = 32
ADAM_STEP = 1000


harmonic_zero = 0.28209479177387814
harmonic_one = 0.4886025119029199
harmonic_two = (
    1.0925484305920792,
    -1.0925484305920792,
    0.31539156525252005,
    -1.0925484305920792,
    0.5462742152960396,
)
harmonic_three = (
    -0.5900435899266435,
    2.890611442640554,
    -0.4570457994644658,
    0.3731763325901154,
    -0.4570457994644658,
    1.445305721320277,
    -0.5900435899266435,
)


def harmonics(across, upward, onward):
    across_sq = across * across
    upward_sq = upward * upward
    onward_sq = onward * onward
    return jnp.stack(
        [
            harmonic_zero * jnp.ones_like(across),
            -harmonic_one * upward,
            harmonic_one * onward,
            -harmonic_one * across,
            harmonic_two[0] * across * upward,
            harmonic_two[1] * upward * onward,
            harmonic_two[2] * (2.0 * onward_sq - across_sq - upward_sq),
            harmonic_two[3] * across * onward,
            harmonic_two[4] * (across_sq - upward_sq),
            harmonic_three[0] * upward * (3.0 * across_sq - upward_sq),
            harmonic_three[1] * across * upward * onward,
            harmonic_three[2] * upward * (4.0 * onward_sq - across_sq - upward_sq),
            harmonic_three[3] * onward * (2.0 * onward_sq - 3.0 * across_sq - 3.0 * upward_sq),
            harmonic_three[4] * across * (4.0 * onward_sq - across_sq - upward_sq),
            harmonic_three[5] * onward * (across_sq - upward_sq),
            harmonic_three[6] * across * (across_sq - 3.0 * upward_sq),
        ]
    )


def camera_rotation(angles):
    cos_roll, sin_roll = (jnp.cos(angles[0]), jnp.sin(angles[0]))
    cos_pitch, sin_pitch = (jnp.cos(angles[1]), jnp.sin(angles[1]))
    cos_yaw, sin_yaw = (jnp.cos(angles[2]), jnp.sin(angles[2]))
    naught = jnp.zeros_like(cos_roll)
    unit_one = jnp.ones_like(cos_roll)
    roll = jnp.stack(
        [
            jnp.stack([unit_one, naught, naught]),
            jnp.stack([naught, cos_roll, -sin_roll]),
            jnp.stack([naught, sin_roll, cos_roll]),
        ]
    )
    pitch = jnp.stack(
        [
            jnp.stack([cos_pitch, naught, sin_pitch]),
            jnp.stack([naught, unit_one, naught]),
            jnp.stack([-sin_pitch, naught, cos_pitch]),
        ]
    )
    yawing = jnp.stack(
        [
            jnp.stack([cos_yaw, -sin_yaw, naught]),
            jnp.stack([sin_yaw, cos_yaw, naught]),
            jnp.stack([naught, naught, unit_one]),
        ]
    )
    inner_turn = jnp.dot(pitch, roll, precision=lax.Precision.HIGHEST)
    return jnp.dot(yawing, inner_turn, precision=lax.Precision.HIGHEST)


def project(values, camera):
    turn = camera_rotation(camera[0:3])
    offset = values[0:3] - camera[3:6][:, None]
    in_view = jnp.dot(turn, offset, precision=lax.Precision.HIGHEST)
    inv_depth = 1.0 / in_view[2]
    screen_col = in_view[0] * inv_depth
    screen_row = in_view[1] * inv_depth
    scales = jnp.exp(values[3:6])
    quat = values[6:10] / jnp.sqrt(jnp.sum(values[6:10] * values[6:10], axis=0, keepdims=True))
    quat_w, quat_x, quat_y, quat_z = (quat[0], quat[1], quat[2], quat[3])
    spin = [
        [
            1.0 - 2.0 * (quat_y * quat_y + quat_z * quat_z),
            2.0 * (quat_x * quat_y - quat_w * quat_z),
            2.0 * (quat_x * quat_z + quat_w * quat_y),
        ],
        [
            2.0 * (quat_x * quat_y + quat_w * quat_z),
            1.0 - 2.0 * (quat_x * quat_x + quat_z * quat_z),
            2.0 * (quat_y * quat_z - quat_w * quat_x),
        ],
        [
            2.0 * (quat_x * quat_z - quat_w * quat_y),
            2.0 * (quat_y * quat_z + quat_w * quat_x),
            1.0 - 2.0 * (quat_x * quat_x + quat_y * quat_y),
        ],
    ]
    basis_cam = []
    for outer_index in range(3):
        row_terms = []
        for col_index in range(3):
            entry = turn[outer_index, 0] * spin[0][col_index]
            for mid_index in range(1, 3):
                entry = entry + turn[outer_index, mid_index] * spin[mid_index][col_index]
            row_terms.append(entry * scales[col_index])
        basis_cam.append(row_terms)
    jac_top = [
        (basis_cam[0][col_index] - screen_col * basis_cam[2][col_index]) * inv_depth
        for col_index in range(3)
    ]
    jac_low = [
        (basis_cam[1][col_index] - screen_row * basis_cam[2][col_index]) * inv_depth
        for col_index in range(3)
    ]
    sigma_a = jac_top[0] * jac_top[0] + jac_top[1] * jac_top[1] + jac_top[2] * jac_top[2]
    sigma_b = jac_top[0] * jac_low[0] + jac_top[1] * jac_low[1] + jac_top[2] * jac_low[2]
    sigma_c = jac_low[0] * jac_low[0] + jac_low[1] * jac_low[1] + jac_low[2] * jac_low[2]
    determinant = sigma_a * sigma_c - sigma_b * sigma_b
    opacity = jax.nn.sigmoid(values[10])
    distance = jnp.sqrt(jnp.sum(offset * offset, axis=0))
    unit_dir = offset / distance
    basis = harmonics(unit_dir[0], unit_dir[1], unit_dir[2])
    coeffs = values[11:59].reshape(16, 3, values.shape[1])
    colors = 0.5 + jnp.sum(basis[:, None, :] * coeffs, axis=0)
    screen = jnp.stack(
        [
            screen_col,
            screen_row,
            sigma_c / determinant,
            -sigma_b / determinant,
            sigma_a / determinant,
            opacity,
        ]
    )
    return jnp.concatenate([screen, colors], axis=0)


def group_loss(pieces):
    features, live_mask, pixel_column, pixel_row, target_tile = pieces
    entries = live_mask.shape[1]
    delta_col = pixel_column[:, :, None] - features[0][:, None, :]
    delta_row = pixel_row[:, :, None] - features[1][:, None, :]
    power = -0.5 * (
        features[2][:, None, :] * delta_col * delta_col
        + 2.0 * features[3][:, None, :] * delta_col * delta_row
        + features[4][:, None, :] * delta_row * delta_row
    )
    alphas = features[5][:, None, :] * jnp.exp(power) * live_mask[:, None, :]
    log_keep = jnp.log(1.0 - alphas)
    earlier = (
        lax.broadcasted_iota(jnp.int32, (entries, entries), 0)
        < lax.broadcasted_iota(jnp.int32, (entries, entries), 1)
    ).astype(jnp.float32)
    transmit = jnp.exp(
        jnp.einsum("bpl,lm->bpm", log_keep, earlier, precision=lax.Precision.HIGHEST)
    )
    weights = alphas * transmit
    image = jnp.einsum("bpl,kbl->kbp", weights, features[6:9], precision=lax.Precision.HIGHEST)
    error = image - target_tile
    return jnp.sum(error * error)


def render_tiles(picked, live_mask, pixel_column, pixel_row, target_tile):
    groups = live_mask.shape[0] // 4
    entries = live_mask.shape[1]
    pixels = pixel_column.shape[1]
    stacked = (
        jnp.transpose(picked.reshape(picked.shape[0], groups, 4, entries), (1, 0, 2, 3)),
        live_mask.reshape(groups, 4, entries),
        pixel_column.reshape(groups, 4, pixels),
        pixel_row.reshape(groups, 4, pixels),
        jnp.transpose(target_tile.reshape(3, groups, 4, pixels), (1, 0, 2, 3)),
    )
    return jnp.sum(lax.map(jax.checkpoint(group_loss), stacked))


def pixel_grid(first_tile, count, tiles_dev, rows_pix):
    tile_ids = first_tile + jnp.arange(count, dtype=jnp.int32)
    pixel_ids = jnp.arange(256, dtype=jnp.int32)
    block_cols = TILE_COLS // 4
    owner_ids = tile_ids // tiles_dev
    local_ids = tile_ids % tiles_dev
    tile_col = 4 * (owner_ids % block_cols) + local_ids % 4
    tile_row = tiles_dev // 4 * (owner_ids // block_cols) + local_ids // 4
    half_width = TILE_COLS * 8.0
    column = (tile_col[:, None] * 16 + pixel_ids[None, :] % 16).astype(jnp.float32)
    row_pos = (tile_row[:, None] * 16 + pixel_ids[None, :] // 16).astype(jnp.float32)
    return ((column + 0.5 - half_width) / half_width, (row_pos + 0.5 - rows_pix * 0.5) / half_width)


def adam_update(params, first_moment, second_moment, gradient, counts):
    row_ids = lax.broadcasted_iota(jnp.int32, params.shape, 0)
    rates = jnp.where(
        row_ids < 6,
        0.01,
        jnp.where(
            row_ids < 10,
            0.005,
            jnp.where(row_ids < 11, 0.05, jnp.where(row_ids < 14, 0.0025, 0.000125)),
        ),
    )
    first_new = 0.9 * first_moment + 0.1 * gradient
    second = 0.999 * second_moment + 0.001 * gradient * gradient
    bias_one = 1.0 - 0.9**ADAM_STEP
    bias_two = 1.0 - 0.999**ADAM_STEP
    stride = rates * (first_new / bias_one) / (jnp.sqrt(second / bias_two) + 1e-08)
    seen_mask = counts > 0.0
    return (
        jnp.where(seen_mask, params - stride, params),
        jnp.where(seen_mask, first_new, first_moment),
        jnp.where(seen_mask, second, second_moment),
    )


def shards(params, first_moment, second_moment, cameras, visible, send_plan, tile_lists, target):
    cells = lax.axis_size("cells")
    camera = cameras[0]
    plan_rows = send_plan[0, 0]
    capacity = plan_rows.shape[1]
    sent_live = (plan_rows >= 0)[None]
    sent_rows = jnp.maximum(plan_rows, 0)
    lists = tile_lists[0]
    tiles_here = lists.shape[0]
    live_mask = (lists >= 0).astype(jnp.float32)
    slot_ids = jnp.maximum(lists, 0)
    rows_pix = tiles_here * cells // TILE_COLS * 16
    pixel_column, pixel_row = pixel_grid(
        lax.axis_index("cells") * tiles_here, tiles_here, tiles_here, rows_pix
    )
    target_tile = target[0].reshape(3, tiles_here, 256)
    block = params.shape[1]

    def image_loss(table):
        picked = jnp.take(table, slot_ids, axis=1)
        return render_tiles(picked, live_mask, pixel_column, pixel_row, target_tile)

    def own_projection(values):
        return project(values, camera)

    features, project_pull = jax.vjp(own_projection, params)
    outgoing = jnp.take(features, sent_rows, axis=1)
    incoming = lax.all_to_all(outgoing, "cells", split_axis=1, concat_axis=1, tiled=True)
    loss_value, pullback = jax.vjp(
        image_loss, incoming.reshape(features.shape[0], cells * capacity)
    )
    table_grad = pullback(jnp.ones((), jnp.float32))[0]
    returned = lax.all_to_all(
        table_grad.reshape(features.shape[0], cells, capacity),
        "cells",
        split_axis=1,
        concat_axis=1,
        tiled=True,
    )
    kept = jnp.where(sent_live, returned, 0.0)
    gradient = project_pull(
        jnp.zeros((features.shape[0], block), jnp.float32).at[:, sent_rows].add(kept)
    )[0]
    seen_here = visible.astype(jnp.float32)
    total_grad, counts = lax.psum((gradient, seen_here), "views")
    new_params, new_first, new_second = adam_update(
        params, first_moment, second_moment, total_grad, counts
    )
    return (new_params, new_first, new_second)

LANES = 128
PAD_ROWS = 64
FEATS = 9


def project_rows(rows, turn, centre):
    offset = [rows[i] - centre[i] for i in range(3)]
    in_view = [
        turn[i][0] * offset[0] + turn[i][1] * offset[1] + turn[i][2] * offset[2] for i in range(3)
    ]
    inv_depth = 1.0 / in_view[2]
    screen_col = in_view[0] * inv_depth
    screen_row = in_view[1] * inv_depth
    scales = [jnp.exp(rows[3 + i]) for i in range(3)]
    raw = rows[6:10]
    norm = jnp.sqrt(raw[0] * raw[0] + raw[1] * raw[1] + raw[2] * raw[2] + raw[3] * raw[3])
    inv_norm = 1.0 / norm
    quat_w, quat_x, quat_y, quat_z = [item * inv_norm for item in raw]
    spin = [
        [
            1.0 - 2.0 * (quat_y * quat_y + quat_z * quat_z),
            2.0 * (quat_x * quat_y - quat_w * quat_z),
            2.0 * (quat_x * quat_z + quat_w * quat_y),
        ],
        [
            2.0 * (quat_x * quat_y + quat_w * quat_z),
            1.0 - 2.0 * (quat_x * quat_x + quat_z * quat_z),
            2.0 * (quat_y * quat_z - quat_w * quat_x),
        ],
        [
            2.0 * (quat_x * quat_z - quat_w * quat_y),
            2.0 * (quat_y * quat_z + quat_w * quat_x),
            1.0 - 2.0 * (quat_x * quat_x + quat_y * quat_y),
        ],
    ]
    basis_cam = [
        [
            (turn[i][0] * spin[0][j] + turn[i][1] * spin[1][j] + turn[i][2] * spin[2][j])
            * scales[j]
            for j in range(3)
        ]
        for i in range(3)
    ]
    top = [(basis_cam[0][j] - screen_col * basis_cam[2][j]) * inv_depth for j in range(3)]
    low = [(basis_cam[1][j] - screen_row * basis_cam[2][j]) * inv_depth for j in range(3)]
    sigma_a = top[0] * top[0] + top[1] * top[1] + top[2] * top[2]
    sigma_b = top[0] * low[0] + top[1] * low[1] + top[2] * low[2]
    sigma_c = low[0] * low[0] + low[1] * low[1] + low[2] * low[2]
    inv_det = 1.0 / (sigma_a * sigma_c - sigma_b * sigma_b)
    opacity = 1.0 / (1.0 + jnp.exp(-rows[10]))
    inv_dist = 1.0 / jnp.sqrt(offset[0] * offset[0] + offset[1] * offset[1] + offset[2] * offset[2])
    x, y, z = [item * inv_dist for item in offset]
    xx, yy, zz = x * x, y * y, z * z
    basis = [
        None,
        -harmonic_one * y,
        harmonic_one * z,
        -harmonic_one * x,
        harmonic_two[0] * x * y,
        harmonic_two[1] * y * z,
        harmonic_two[2] * (2.0 * zz - xx - yy),
        harmonic_two[3] * x * z,
        harmonic_two[4] * (xx - yy),
        harmonic_three[0] * y * (3.0 * xx - yy),
        harmonic_three[1] * x * y * z,
        harmonic_three[2] * y * (4.0 * zz - xx - yy),
        harmonic_three[3] * z * (2.0 * zz - 3.0 * xx - 3.0 * yy),
        harmonic_three[4] * x * (4.0 * zz - xx - yy),
        harmonic_three[5] * z * (xx - yy),
        harmonic_three[6] * x * (xx - 3.0 * yy),
    ]
    colors = []
    for k in range(3):
        total = harmonic_zero * rows[11 + k]
        for j in range(1, 16):
            total = total + basis[j] * rows[11 + 3 * j + k]
        colors.append(0.5 + total)
    return (
        screen_col,
        screen_row,
        sigma_c * inv_det,
        -sigma_b * inv_det,
        sigma_a * inv_det,
        opacity,
        *colors,
    )


def static_terms(rows):
    scales = [jnp.exp(item) for item in rows[3:6]]
    raw = rows[6:10]
    inv_norm = 1.0 / jnp.sqrt(
        raw[0] * raw[0] + raw[1] * raw[1] + raw[2] * raw[2] + raw[3] * raw[3]
    )
    quat = [item * inv_norm for item in raw]
    w, x, y, z = quat
    spin = [
        [1.0 - 2.0 * (y * y + z * z), 2.0 * (x * y - w * z), 2.0 * (x * z + w * y)],
        [2.0 * (x * y + w * z), 1.0 - 2.0 * (x * x + z * z), 2.0 * (y * z - w * x)],
        [2.0 * (x * z - w * y), 2.0 * (y * z + w * x), 1.0 - 2.0 * (x * x + y * y)],
    ]
    frame = [[spin[m][j] * scales[j] for j in range(3)] for m in range(3)]
    fade = 1.0 - 1.0 / (1.0 + jnp.exp(-rows[10]))
    return scales, inv_norm, quat, frame, fade


def moving_terms(rows, frame, turn, centre):
    offset = [rows[i] - centre[i] for i in range(3)]
    in_view = [
        turn[i][0] * offset[0] + turn[i][1] * offset[1] + turn[i][2] * offset[2] for i in range(3)
    ]
    inv = 1.0 / in_view[2]
    col, row = in_view[0] * inv, in_view[1] * inv
    cam = [
        [
            turn[i][0] * frame[0][j] + turn[i][1] * frame[1][j] + turn[i][2] * frame[2][j]
            for j in range(3)
        ]
        for i in range(3)
    ]
    top = [(cam[0][j] - col * cam[2][j]) * inv for j in range(3)]
    low = [(cam[1][j] - row * cam[2][j]) * inv for j in range(3)]
    sigma_a = top[0] * top[0] + top[1] * top[1] + top[2] * top[2]
    sigma_b = top[0] * low[0] + top[1] * low[1] + top[2] * low[2]
    sigma_c = low[0] * low[0] + low[1] * low[1] + low[2] * low[2]
    inv_det = 1.0 / (sigma_a * sigma_c - sigma_b * sigma_b)
    conic = (sigma_c * inv_det, -sigma_b * inv_det, sigma_a * inv_det)
    inv_dist = 1.0 / jnp.sqrt(offset[0] * offset[0] + offset[1] * offset[1] + offset[2] * offset[2])
    ray = [item * inv_dist for item in offset]
    return inv, col, row, cam[2], top, low, conic, inv_dist, ray


def shade_basis(ray):
    x, y, z = ray
    xx, yy, zz = x * x, y * y, z * z
    xy, yz, xz = x * y, y * z, x * z
    h1, h2, h3 = harmonic_one, harmonic_two, harmonic_three
    outer = 4.0 * zz - xx - yy
    return [
        harmonic_zero,
        -h1 * y,
        h1 * z,
        -h1 * x,
        h2[0] * xy,
        h2[1] * yz,
        h2[2] * (2.0 * zz - xx - yy),
        h2[3] * xz,
        h2[4] * (xx - yy),
        h3[0] * y * (3.0 * xx - yy),
        h3[1] * xy * z,
        h3[2] * y * outer,
        h3[3] * z * (2.0 * zz - 3.0 * xx - 3.0 * yy),
        h3[4] * x * outer,
        h3[5] * z * (xx - yy),
        h3[6] * x * (xx - 3.0 * yy),
    ]


def pull_moving(rows, terms, turn, got):
    inv, col, row, deep, top, low, conic, inv_dist, ray = terms
    k0, k1, k2 = conic
    g0, half, g2 = -0.5 * got[3], -0.5 * got[4], -0.5 * got[5]
    p00, p01 = g0 * k0 + half * k1, g0 * k1 + half * k2
    p10, p11 = half * k0 + g2 * k1, half * k1 + g2 * k2
    d00 = -2.0 * (k0 * p00 + k1 * p10)
    d01 = -2.0 * (k0 * p01 + k1 * p11)
    d11 = -2.0 * (k1 * p01 + k2 * p11)
    d_top = [(d00 * top[j] + d01 * low[j]) * inv for j in range(3)]
    d_low = [(d01 * top[j] + d11 * low[j]) * inv for j in range(3)]
    d_cam = [d_top, d_low, [-(col * d_top[j] + row * d_low[j]) for j in range(3)]]
    d_col = k0 * got[1] + k1 * got[2]
    d_row = k1 * got[1] + k2 * got[2]
    d_depth = 0.0
    for j in range(3):
        d_col = d_col - d_top[j] * deep[j]
        d_row = d_row - d_low[j] * deep[j]
        d_depth = d_depth - (d_top[j] * top[j] + d_low[j] * low[j])
    d_view = [d_col * inv, d_row * inv]
    d_view.append(d_depth - (col * d_view[0] + row * d_view[1]))
    d_frame = [
        [turn[0][m] * d_cam[0][j] + turn[1][m] * d_cam[1][j] + turn[2][m] * d_cam[2][j] for j in range(3)]
        for m in range(3)
    ]
    x, y, z = ray
    xx, yy, zz = x * x, y * y, z * z
    yz, xz = y * z, x * z
    h1, h2, h3 = harmonic_one, harmonic_two, harmonic_three
    outer = 4.0 * zz - xx - yy
    tint = got[6:9]
    e = [None] + [
        tint[0] * rows[11 + 3 * j] + tint[1] * rows[12 + 3 * j] + tint[2] * rows[13 + 3 * j]
        for j in range(1, 16)
    ]
    gx = (
        -h1 * e[3]
        + y * (h2[0] * e[4] + (6.0 * h3[0]) * (x * e[9]) - (2.0 * h3[2]) * (x * e[11]))
        + z * (h2[3] * e[7] + h3[1] * (y * e[10]))
        + x * ((-2.0 * h2[2]) * e[6] + (2.0 * h2[4]) * e[8])
        + xz * ((-6.0 * h3[3]) * e[12] + (2.0 * h3[5]) * e[14])
        + (h3[4] * (outer - 2.0 * xx)) * e[13]
        + ((3.0 * h3[6]) * (xx - yy)) * e[15]
    )
    gy = (
        -h1 * e[1]
        + x * (h2[0] * e[4] - (2.0 * h3[4]) * (y * e[13]) - (6.0 * h3[6]) * (y * e[15]))
        + z * (h2[1] * e[5] + h3[1] * (x * e[10]))
        + y * ((-2.0 * h2[2]) * e[6] - (2.0 * h2[4]) * e[8])
        + yz * ((-6.0 * h3[3]) * e[12] - (2.0 * h3[5]) * e[14])
        + ((3.0 * h3[0]) * (xx - yy)) * e[9]
        + (h3[2] * (outer - 2.0 * yy)) * e[11]
    )
    gz = (
        h1 * e[2]
        + y * (h2[1] * e[5] + h3[1] * (x * e[10]) + (8.0 * h3[2]) * (z * e[11]))
        + x * (h2[3] * e[7] + (8.0 * h3[4]) * (z * e[13]))
        + (4.0 * h2[2]) * (z * e[6])
        + ((3.0 * h3[3]) * (2.0 * zz - xx - yy)) * e[12]
        + (h3[5] * (xx - yy)) * e[14]
    )
    along = x * gx + y * gy + z * gz
    d_ray = [(gx - x * along) * inv_dist, (gy - y * along) * inv_dist, (gz - z * along) * inv_dist]
    d_place = [
        turn[0][i] * d_view[0] + turn[1][i] * d_view[1] + turn[2][i] * d_view[2] + d_ray[i]
        for i in range(3)
    ]
    return [*d_place, *d_frame[0], *d_frame[1], *d_frame[2], got[0]]


def pull_static(static, sums):
    scales, inv_norm, quat, frame, fade = static
    d_frame = [sums[3:6], sums[6:9], sums[9:12]]
    d_scale = [
        d_frame[0][j] * frame[0][j] + d_frame[1][j] * frame[1][j] + d_frame[2][j] * frame[2][j]
        for j in range(3)
    ]
    d = [[d_frame[m][j] * scales[j] for j in range(3)] for m in range(3)]
    w, x, y, z = quat
    d_quat = [
        2.0 * (z * (d[1][0] - d[0][1]) + y * (d[0][2] - d[2][0]) + x * (d[2][1] - d[1][2])),
        2.0 * (y * (d[0][1] + d[1][0]) + z * (d[0][2] + d[2][0]) + w * (d[2][1] - d[1][2]) - 2.0 * x * (d[1][1] + d[2][2])),
        2.0 * (x * (d[0][1] + d[1][0]) + w * (d[0][2] - d[2][0]) + z * (d[1][2] + d[2][1]) - 2.0 * y * (d[0][0] + d[2][2])),
        2.0 * (w * (d[1][0] - d[0][1]) + x * (d[0][2] + d[2][0]) + y * (d[1][2] + d[2][1]) - 2.0 * z * (d[0][0] + d[1][1])),
    ]
    along = w * d_quat[0] + x * d_quat[1] + y * d_quat[2] + z * d_quat[3]
    d_raw = [(d_quat[i] - quat[i] * along) * inv_norm for i in range(4)]
    return [*sums[0:3], *d_scale, *d_raw, fade * sums[12]]


def camera_terms(cam):
    cosines, sines = jnp.cos(cam), jnp.sin(cam)
    cr, cp, cy = [cosines[:, i : i + 1] for i in range(3)]
    sr, sp, sy = [sines[:, i : i + 1] for i in range(3)]
    turn = [
        [cy * cp, cy * sp * sr - sy * cr, cy * sp * cr + sy * sr],
        [sy * cp, sy * sp * sr + cy * cr, sy * sp * cr - cy * sr],
        [-sp, cp * sr, cp * cr],
    ]
    centre = [cam[:, 3 + i : 4 + i] for i in range(3)]
    return turn, centre

MAIN_VMEM = 40 * 2**20
UPDATE_VMEM = 16 * 2**20
WAVES = 4


def fill_dense(params_ref, dense):
    count, block = params_ref.shape
    for b in range(block // LANES):
        part, line = divmod(b, 8)
        for r in range(0, count, 8):
            size = min(8, count - r)
            where = pl.ds((part * PAD_ROWS + r) * 8 + line, size, stride=8)
            dense[where, :] = params_ref[r : r + size, b * LANES : (b + 1) * LANES]


def dense_rows(dense, part, count):
    return [
        dense[(part * PAD_ROWS + r) * 8 : (part * PAD_ROWS + r) * 8 + 8, :] for r in range(count)
    ]


def lane_pick(source, lanes):
    return jnp.take_along_axis(source, lanes, axis=1, mode="promise_in_bounds")


def gather_eight(load, blocks, index):
    index = jnp.maximum(index, 0)
    lanes, block = index & (LANES - 1), index >> 7
    total = lane_pick(load(0), lanes)
    for b in range(1, blocks):
        total = jnp.where(block == b, lane_pick(load(b), lanes), total)
    return total


def split_three(x):
    first = x.astype(jnp.bfloat16).astype(jnp.float32)
    rest = x - first
    second = rest.astype(jnp.bfloat16).astype(jnp.float32)
    return first, second, rest - second


def fill_hot(hot, index, start, bits):
    shape = (hot.shape[0], LANES)
    row_ids = lax.broadcasted_iota(jnp.int32, shape, 0).astype(jnp.float32).astype(jnp.bfloat16)
    low = (index & ((1 << bits) - 1)).astype(jnp.float32).astype(jnp.bfloat16)
    one, none = jnp.ones(shape, jnp.bfloat16), jnp.zeros(shape, jnp.bfloat16)
    hot[:, start : start + LANES] = jnp.where(row_ids == jnp.broadcast_to(low, shape), one, none)


def split_two(x):
    first = x.astype(jnp.bfloat16).astype(jnp.float32)
    return first, x - first


def fill_values(lhs, main, last, index, start, bits):
    groups = lhs.shape[0] // 18
    span = slice(start, start + LANES)
    parts = jnp.concatenate(split_two(main), axis=0)
    tips = [jnp.broadcast_to(item, (8, LANES)) for item in split_two(last)]
    high = jnp.broadcast_to(index >> bits, (16, LANES))
    sub = lax.broadcasted_iota(jnp.int32, (8, LANES), 0)
    for b in range(groups):
        lhs[16 * b : 16 * b + 16, span] = jnp.where(high == b, parts, 0.0).astype(jnp.bfloat16)
    for g in range(groups // 8):
        here = high[0:8] == sub + 8 * g
        rows = jnp.concatenate([jnp.where(here, item, 0.0) for item in tips], axis=0)
        row = 16 * groups + 16 * g
        lhs[row : row + 16, span] = rows.astype(jnp.bfloat16)


def scatter_dot(lhs, hot, rows):
    return lax.dot_general(
        lhs[rows], hot[...], (((1,), (1,)), ((), ())), preferred_element_type=jnp.float32
    )


def scatter_main(lhs, hot, first, last):
    out = scatter_dot(lhs, hot, slice(16 * first, 16 * last))
    return [out[16 * b : 16 * b + 8] + out[16 * b + 8 : 16 * b + 16] for b in range(last - first)]


def scatter_tips(lhs, hot):
    groups = lhs.shape[0] // 18
    out = scatter_dot(lhs, hot, slice(16 * groups, 18 * groups))
    return [
        out[16 * (b // 8) + b % 8 : 16 * (b // 8) + b % 8 + 1]
        + out[16 * (b // 8) + 8 + b % 8 : 16 * (b // 8) + 9 + b % 8]
        for b in range(groups)
    ]


def stage_features(feat_parts, plan_ref, table, last, order, tips):
    halves = plan_ref.shape[1] // LANES
    blocks = last.shape[0]
    for part, feats in enumerate(feat_parts):
        for f in range(8):
            table[pl.ds(part * 64 + f, 8, stride=8), :] = feats[f]
        last[part * 8 : part * 8 + 8, :] = feats[8]
    slots = plan_ref.shape[0] * halves
    for o in range(slots):
        d, h = divmod(o, halves)
        order[o : o + 1, :] = plan_ref[d : d + 1, h * LANES : (h + 1) * LANES]
    for p in range(slots // 8):
        tips[8 * p : 8 * p + 8, :] = gather_eight(
            lambda b: jnp.broadcast_to(last[b : b + 1, :], (8, LANES)),
            blocks,
            order[8 * p : 8 * p + 8, :],
        )


def pack_features(d, halves, table, order, tips, out_ref):
    blocks = table.shape[0] // 8
    for h in range(halves):
        row = pl.ds(d * halves + h, 1)
        out_ref[d, 8 * h : 8 * h + 8, :] = gather_eight(
            lambda b: table[8 * b : 8 * b + 8, :],
            blocks,
            jnp.broadcast_to(order[row, :], (8, LANES)),
        )
        out_ref[d, 8 * halves + h : 8 * halves + h + 1, :] = tips[row, :]


def pixel_terms():
    lane = lax.broadcasted_iota(jnp.int32, (8, LANES), 1)
    inner = lane & 31
    tile = lane >> 5
    x = (inner & 15).astype(jnp.float32) - 7.5
    step = (inner >> 4).astype(jnp.float32) - 0.5
    return tile, x, step


def render_setup(lists_ref, target_ref, order, wanted, basis, plan_sums, hot, bits):
    tiles, entries = lists_ref.shape
    quarters = entries // LANES
    for q in range(quarters):
        order[q * tiles : (q + 1) * tiles, :] = lists_ref[:, q * LANES : (q + 1) * LANES]
    sub = lax.broadcasted_iota(jnp.int32, (8, LANES), 0)
    lane = lax.broadcasted_iota(jnp.int32, (8, LANES), 1)
    tile, x, step = pixel_terms()
    shifted = 32 * (sub & 3) + (lane & 31)
    for k in range(3):
        total = jnp.zeros((8, LANES), jnp.float32)
        for r in range(8):
            row = jnp.broadcast_to(target_ref[k, :, r * LANES : (r + 1) * LANES], (8, LANES))
            here = (tile == r // 2) & ((sub >> 2) == r % 2)
            total = jnp.where(here, lane_pick(row, shifted), total)
        wanted[8 * k : 8 * k + 8, :] = total
    for g in range(LANES // 8):
        row = sub + 8 * g
        coef = (row * 43) >> 9
        mine = tile == (row & 3)

        def column(j, *terms):
            total = jnp.zeros((8, LANES), jnp.float32)
            for c, value in terms:
                total = jnp.where(coef == c, value, total)
            total = jnp.where(mine, total, 0.0)
            basis[8 * g : 8 * g + 8, j * LANES : (j + 1) * LANES] = total

        column(0, (0, x * x), (1, x * step), (2, step * step), (3, x), (4, step), (5, 1.0))
        column(1, (1, x), (2, 2.0 * step), (4, 1.0))
    mine = tile == (sub & 3)
    for s in range(8):
        y = step + (2.0 * s - 7.0)
        rows = [jnp.ones_like(x), x, y, x * x, x * y, y * y]
        rows = jnp.concatenate([jnp.where(mine, item, 0.0) for item in rows], axis=0)
        for part in range(2):
            start = (part * 8 + s) * LANES
            plan_sums[:, start : start + LANES] = rows.astype(jnp.bfloat16)
    for o in range(tiles * quarters):
        fill_hot(hot, order[o : o + 1, :], o * LANES, bits)


def render_rest(
    cells, others, receive, recv_ref, order, wanted, back_ref,
    coefs, turned_s, tables, basis, alpha_s, weight_s, stages, joint_g, joint_w, plan_sums, error_sums,
    turned, tinted, moved, pairs, lhs, hot, bits,
):
    owners, packed, _ = recv_ref.shape
    halves = packed // FEATS
    blocks = owners * halves
    tiles = 4
    quarters = order.shape[0] // tiles
    entries = quarters * LANES
    me = lax.axis_index("cells")
    rows_pix = tiles * cells // TILE_COLS * 16
    half_width = TILE_COLS * 8.0
    inv_width = 1.0 / half_width
    log_two = 1.4426950408889634
    sub = lax.broadcasted_iota(jnp.int32, (8, LANES), 0)
    local = sub & 3
    tile_col = 4 * lax.rem(me, TILE_COLS // 4) + local
    tile_row = lax.div(me, TILE_COLS // 4)
    centre_col = (16 * tile_col + 8).astype(jnp.float32) - half_width
    centre_row = (jnp.full((8, LANES), 16 * tile_row + 8, jnp.int32)).astype(
        jnp.float32
    ) - rows_pix * 0.5

    picked = [[None] * FEATS for _ in range(quarters // 2)]
    for k in range(owners):
        origin = others[-k] if k else me
        if k:
            receive(origin)
        for p in range(quarters // 2):
            index = jnp.maximum(order[8 * p : 8 * p + 8, :], 0)
            lanes, block = index & (LANES - 1), index >> 7
            for h in range(halves):
                here = block == origin * halves + h
                for f in range(FEATS):
                    r = 8 * h + f if f < 8 else 8 * halves + h
                    row = jnp.broadcast_to(recv_ref[origin, r : r + 1, :], (8, LANES))
                    item = lane_pick(row, lanes)
                    old = picked[p][f]
                    picked[p][f] = item if old is None else jnp.where(here, item, old)

    for p in range(quarters // 2):
        index = order[8 * p : 8 * p + 8, :]
        feats = picked[p]
        off_col = feats[0] * half_width - centre_col
        off_row = feats[1] * half_width - centre_row
        moved[16 * p : 16 * p + 8, :] = off_col
        moved[16 * p + 8 : 16 * p + 16, :] = off_row
        square = feats[2] * (-0.5 * log_two * inv_width * inv_width)
        cross = feats[3] * (-log_two * inv_width * inv_width)
        bend = feats[4] * (-0.5 * log_two * inv_width * inv_width)
        faint = jnp.maximum(jnp.log(feats[5]) * log_two, -1e30)
        along = square * off_col + cross * off_row
        level = along * off_col + bend * off_row * off_row + jnp.where(index >= 0, faint, -1e30)
        terms = [
            square,
            cross,
            bend,
            -(along + square * off_col),
            -(2.0 * bend * off_row + cross * off_col),
            level,
        ]
        for m, term in enumerate((terms[2], *feats[6:9])):
            row = 72 + m * tiles
            for q in range(2):
                start = (2 * p + q) * LANES
                coefs[start + row : start + row + tiles, :] = term[4 * q : 4 * q + 4]
        for c, term in enumerate(terms):
            for i, piece in enumerate(split_three(term)):
                row = (3 * c + i) * tiles
                for q in range(2):
                    start = (2 * p + q) * LANES
                    coefs[start + row : start + row + tiles, :] = piece[4 * q : 4 * q + 4]
    for q in range(quarters):
        coefs[q * LANES + 88 : (q + 1) * LANES, :] = jnp.zeros((LANES - 88, LANES), jnp.float32)
    weights = basis[...].astype(jnp.bfloat16)
    picks = [pixel_terms()[0] + (72 + tiles * m) for m in range(4)]
    for q in range(quarters):
        span = slice(q * LANES, (q + 1) * LANES)
        columns = jnp.transpose(coefs[span, :])
        turned_s[span, :] = columns.astype(jnp.bfloat16)
        for m in range(4):
            for g in range(LANES // 8):
                row = q * LANES + 8 * g
                tables[2 + m, row : row + 8, :] = lane_pick(columns[8 * g : 8 * g + 8], picks[m])
    result = jnp.dot(turned_s[...], weights, preferred_element_type=jnp.float32)
    for j in range(2):
        tables[j] = result[:, j * LANES : (j + 1) * LANES]

    height = (2 * sub - 7).astype(jnp.float32)

    def table(l, j):
        return jnp.broadcast_to(tables[j, pl.ds(l, 1), :], (8, LANES))

    def keep(stage, c, i, item):
        tile = (c * 16 + i // 8 * 8) * 8
        stage[pl.ds(tile + i % 8, 8, stride=8), :] = item

    def turn_over(stage, joint, q, s):
        item = jnp.transpose(
            jnp.concatenate([stage[t * 64 + s * 8 : t * 64 + s * 8 + 8, :] for t in range(16)], axis=0)
        )
        top = item.astype(jnp.bfloat16)
        span = pl.ds(pl.multiple_of(q * LANES, LANES), LANES)
        joint[s * LANES : (s + 1) * LANES, span] = top
        joint[(8 + s) * LANES : (9 + s) * LANES, span] = (
            item - top.astype(jnp.float32)
        ).astype(jnp.bfloat16)

    chunks = LANES // 16

    def forward(q, carry, stage, other):
        trans, red, green, blue = carry
        first = pl.multiple_of(q * LANES, LANES)
        base = pl.multiple_of(q * 8 * LANES, 8 * LANES)
        for c in range(chunks):
            for i in range(16):
                l = first + (c * 16 + i)
                where = pl.ds(base + (c * 16 + i) * 8, 8)
                power = table(l, 0) + height * (table(l, 1) + height * table(l, 2))
                alpha = jnp.exp2(power)
                weight = alpha * trans
                alpha_s[where, :] = alpha
                weight_s[where, :] = weight
                keep(stage, c, i, weight)
                trans = trans - weight
                red = red + weight * table(l, 3)
                green = green + weight * table(l, 4)
                blue = blue + weight * table(l, 5)
            turn_over(other, joint_w, q, c)
        return trans, red, green, blue

    zero = jnp.zeros((8, LANES), jnp.float32)
    even, odd = stages

    def forward_pair(i, carry):
        carry = forward(2 * i, carry, even, odd)
        return forward(2 * i + 1, carry, odd, even)

    carry = lax.fori_loop(
        0, quarters // 2, forward_pair, (jnp.ones((8, LANES), jnp.float32), zero, zero, zero)
    )
    for c in range(chunks):
        turn_over(odd, joint_w, quarters, c)
    red, green, blue = carry[1:]
    errors = [2.0 * (item - wanted[8 * k : 8 * k + 8, :]) for k, item in enumerate((red, green, blue))]
    wanted[0:8, :], wanted[8:16, :], wanted[16:24, :] = errors
    tile, _, _ = pixel_terms()
    mine = tile == local
    for s in range(8):
        tops, lows = [], []
        for k in range(3):
            row = jnp.broadcast_to(wanted[8 * k + s : 8 * k + s + 1, :], (8, LANES))
            row = jnp.where(mine, row, 0.0)
            top = row.astype(jnp.bfloat16).astype(jnp.float32)
            tops.append(top)
            lows.append(row - top)
        blank = [jnp.zeros((24, LANES), jnp.float32)]
        start = s * LANES
        error_sums[:, start : start + LANES] = jnp.concatenate(tops + lows, axis=0).astype(jnp.bfloat16)
        start = (8 + s) * LANES
        error_sums[:, start : start + LANES] = jnp.concatenate(tops + blank, axis=0).astype(jnp.bfloat16)

    def backward(q, behind, stage, other):
        first = pl.multiple_of(q * LANES, LANES)
        tinted[:, pl.ds(first, LANES)] = jnp.dot(
            error_sums[...],
            joint_w[:, pl.ds(first + LANES, LANES)],
            preferred_element_type=jnp.float32,
        )
        base = pl.multiple_of(q * 8 * LANES, 8 * LANES)
        for c in range(chunks - 1, -1, -1):
            for i in range(15, -1, -1):
                l = first + (c * 16 + i)
                where = pl.ds(base + (c * 16 + i) * 8, 8)
                slope = errors[0] * table(l, 3) + errors[1] * table(l, 4) + errors[2] * table(l, 5)
                alpha = alpha_s[where, :]
                keep(stage, c, i, weight_s[where, :] * (slope - behind))
                behind = (1.0 - alpha) * behind + alpha * slope
            turn_over(other, joint_g, q + 1, chunks - 1 - c)
        return behind

    def backward_pair(i, behind):
        q = quarters - 1 - 2 * i
        behind = backward(q, behind, odd, even)
        return backward(q - 1, behind, even, odd)

    lax.fori_loop(0, quarters // 2, backward_pair, zero)
    for c in range(chunks):
        turn_over(even, joint_g, 0, c)
    turned[...] = jnp.dot(
        plan_sums[...], joint_g[:, 0:entries], preferred_element_type=jnp.float32
    )
    for p in range(quarters // 2):
        off_col = moved[16 * p : 16 * p + 8, :]
        off_row = moved[16 * p + 8 : 16 * p + 16, :]

        def quantity(j):
            source, r = (turned, j) if j < 6 else (tinted, j - 6)
            rows = slice(8 * r, 8 * r + 8)
            start = 2 * p * LANES
            return jnp.where(
                sub < 4,
                source[rows, start : start + LANES],
                source[rows, start + LANES : start + 2 * LANES],
            )

        plain, across, down = quantity(0), quantity(1), quantity(2)
        near_col = across - off_col * plain
        near_row = down - off_row * plain
        rows = [
            plain,
            near_col * inv_width,
            near_row * inv_width,
            (quantity(3) - off_col * (across + near_col)) * (inv_width * inv_width),
            (quantity(4) - off_col * down - off_row * near_col) * (inv_width * inv_width),
            (quantity(5) - off_row * (down + near_row)) * (inv_width * inv_width),
            *[quantity(6 + k) + quantity(9 + k) for k in range(3)],
        ]
        for f, item in enumerate(rows):
            pairs[pl.ds(p * 128 + f, 8, stride=16), :] = item
    for o in range(tiles * quarters):
        fill_values(
            lhs,
            pairs[o * 16 : o * 16 + 8, :],
            pairs[o * 16 + 8 : o * 16 + 9, :],
            order[o : o + 1, :],
            o * LANES,
            bits,
        )
    for s, (main, last) in enumerate(zip(scatter_main(lhs, hot, 0, owners), scatter_tips(lhs, hot))):
        for h in range(halves):
            span = slice(h * LANES, (h + 1) * LANES)
            back_ref[s, 8 * h : 8 * h + 8, :] = main[:, span]
            back_ref[s, 8 * halves + h : 8 * halves + h + 1, :] = last[:, span]


def main_kernel(
    params_in, cam_in, plan_in, visible_in, lists_in, target_in, out_ref,
    params_ref, cam_ref, plan_ref, visible_ref, lists_ref, target_ref, dense, table, last, plan_order, outgoing, incoming, back, returned, extra, extras, relayed, tips,
    order, wanted, basis, coefs, turned_s, tables, alpha_s, weight_s, stages, joint_g, joint_w,
    plan_sums, error_sums, turned, tinted, moved, pairs, lhs, hot, own_lhs, own_hot,
    send_one, recv_one, send_two, recv_two, send_three, recv_three, send_four, recv_four, local_sem,
):
    cells, views = lax.axis_size("cells"), lax.axis_size("views")
    cell, view = lax.axis_index("cells"), lax.axis_index("views")
    count, block = params_ref.shape
    blocks = block // LANES
    capacity = plan_ref.shape[1]
    halves = capacity // LANES
    bits = capacity.bit_length() - 1
    barrier = pltpu.get_barrier_semaphore()

    far = lax.div(cell, 4)
    depth, side = lax.div(cell, 2), lax.rem(cell, 2)
    others = [
        2 * d + e
        for d in (3 - 3 * far, 2 - far, 1 - depth + 4 * far)
        for e in (1 - side, side)
    ] + [2 * depth + 1 - side]
    twin = view + 1 - 2 * lax.rem(view, 2)
    across = lax.rem(view + 2, views)
    mates = [twin, across, lax.rem(twin + 2, views)]

    def send(axis, peer, source, dest, send_sem, recv_sem):
        copy = pltpu.make_async_remote_copy(
            src_ref=source,
            dst_ref=dest,
            send_sem=send_sem,
            recv_sem=recv_sem,
            device_id={axis: peer},
            device_id_type=pl.DeviceIdType.MESH,
        )
        copy.start()
        return copy

    def receiver(buffer, sems):
        def receive(origin):
            pltpu.make_async_remote_copy(
                src_ref=buffer.at[origin],
                dst_ref=buffer.at[origin],
                send_sem=sems.at[origin],
                recv_sem=sems.at[origin],
                device_id={"cells": origin},
                device_id_type=pl.DeviceIdType.MESH,
            ).wait_recv()

        return receive

    receive_one = receiver(incoming, recv_one)
    receive_two = receiver(returned, recv_two)
    def greet(axis, peer):
        pl.semaphore_signal(
            barrier, inc=1, device_id={axis: peer}, device_id_type=pl.DeviceIdType.MESH
        )

    for peer in others:
        greet("cells", peer)
    fetches = [
        pltpu.make_async_copy(source, dest, local_sem.at[i])
        for i, (source, dest) in enumerate(
            (
                (params_in, params_ref),
                (cam_in, cam_ref),
                (plan_in, plan_ref),
                (visible_in, visible_ref),
                (lists_in, lists_ref),
                (target_in, target_ref),
            )
        )
    ]
    for fetch in fetches:
        fetch.start()
    for mate in mates:
        greet("views", mate)
    fetches[1].wait()
    turn, centre = camera_terms(cam_ref[...])
    known = [*turn[0], *turn[1], *turn[2], *centre]
    lane = lax.broadcasted_iota(jnp.int32, (8, LANES), 1)
    line = jnp.zeros((8, LANES), jnp.float32)
    for i, item in enumerate(known):
        line = jnp.where(lane == i, jnp.broadcast_to(item, (8, LANES)), line)
    extra[blocks : blocks + 8, :] = line
    fetches[3].wait()
    for b in range(blocks):
        extra[b : b + 1, :] = visible_ref[:, b * LANES : (b + 1) * LANES].astype(jnp.float32)
    fetches[0].wait()
    fill_dense(params_ref, dense)
    feat_parts = [
        project_rows(dense_rows(dense, part, count), turn, centre) for part in range(blocks // 8)
    ]
    fetches[2].wait()
    stage_features(feat_parts, plan_ref, table, last, plan_order, tips)
    for peer in others:
        pack_features(peer, halves, table, plan_order, tips, outgoing)
    pl.semaphore_wait(barrier, cells + views - 2)
    sent = [
        send(
            "cells", peer, outgoing.at[peer], incoming.at[cell], send_one.at[i], recv_one.at[cell]
        )
        for i, peer in enumerate(others)
    ]
    pack_features(cell, halves, table, plan_order, tips, incoming)
    fetches[4].wait()
    fetches[5].wait()
    render_setup(lists_ref, target_ref, order, wanted, basis, plan_sums, hot, bits)
    wide = own_hot.shape[0].bit_length() - 1
    arrivals = [cell] + others[::-1]
    slots = cells * halves
    sub = lax.broadcasted_iota(jnp.int32, (8, LANES), 0)
    count_lanes = lane.astype(jnp.float32)
    for o in range(slots):
        row = plan_order[o : o + 1, :]
        fill_hot(own_hot, row, o * LANES, wide)
        here = jnp.broadcast_to(row >> wide, (8, LANES)) == sub
        own_lhs[:, o * LANES : (o + 1) * LANES] = jnp.concatenate(
            [jnp.where(here, o + 1.0, 0.0), jnp.where(here, count_lanes, 0.0)], axis=0
        ).astype(jnp.bfloat16)
    inverse = lax.dot_general(
        own_lhs[...], own_hot[...], (((1,), (1,)), ((), ())), preferred_element_type=jnp.float32
    )
    for i in range(2):
        span = slice(i * LANES, (i + 1) * LANES)
        extra[pl.ds(blocks + 8 + i, 8, stride=2), :] = inverse[0:8, span]
        extra[pl.ds(2 * blocks + 8 + i, 8, stride=2), :] = inverse[8:16, span]
    early = [
        send("views", mate, extra, extras.at[view], send_four.at[j], recv_four.at[j])
        for j, mate in enumerate(mates)
    ]
    render_rest(
        cells, others, receive_one, incoming, order, wanted, back,
        coefs, turned_s, tables, basis, alpha_s, weight_s, stages, joint_g, joint_w, plan_sums, error_sums,
        turned, tinted, moved, pairs, lhs, hot, bits,
    )
    sent += [
        send(
            "cells", peer, back.at[peer], returned.at[cell], send_two.at[i], recv_two.at[cell]
        )
        for i, peer in enumerate(others)
    ]

    def forward(k, source, origin):
        return [
            send(
                "views", mate, source, relayed.at[view, origin],
                send_three.at[k, j], recv_three.at[k, j],
            )
            for j, mate in enumerate(mates)
        ]

    relays = [forward(0, back.at[cell], cell)]
    for copy in early:
        copy.wait()
    counts = extra[0:blocks, :]
    for mate in mates:
        counts = counts + extras[mate, 0:blocks, :]
    grads = blocks * PAD_ROWS
    out_ref[grads : grads + blocks, :] = counts
    parts = blocks // 8
    seen = [extra] + [extras.at[mate] for mate in mates]
    rows_of = [dense_rows(dense, part, count) for part in range(parts)]
    statics = [static_terms(rows) for rows in rows_of]
    turns, terms = [], []
    for source in seen:
        known = [
            jnp.broadcast_to(source[blocks : blocks + 1, i : i + 1], (8, LANES)) for i in range(12)
        ]
        turns.append([known[0:3], known[3:6], known[6:9]])
        terms.append(
            [
                moving_terms(rows_of[part], statics[part][3], turns[-1], known[9:12])
                for part in range(parts)
            ]
        )
    for k in range(1, cells):
        receive_two(arrivals[k])
        relays.append(forward(k, returned.at[arrivals[k]], arrivals[k]))

    def collect(v, got, packet, origin):
        for part in range(parts):
            start = blocks + 8 + 8 * part
            block = seen[v][start : start + 8, :].astype(jnp.int32)
            lanes = seen[v][blocks + start : blocks + start + 8, :].astype(jnp.int32)
            for h in range(halves):
                here = block == origin * halves + h + 1
                for f in range(FEATS):
                    r = 8 * h + f if f < 8 else 8 * halves + h
                    item = lane_pick(jnp.broadcast_to(packet[r : r + 1, :], (8, LANES)), lanes)
                    got[part][f] = jnp.where(here, item, got[part][f])

    def nothing():
        return [[jnp.zeros((8, LANES), jnp.float32)] * FEATS for _ in range(parts)]

    totals = [None] * parts

    def pull_group(group, gots, last):
        for part in range(parts):
            base = part * PAD_ROWS
            rows = dense_rows(dense, part, count)
            sums = totals[part]
            for v, got in zip(group, gots):
                moved_part = pull_moving(rows, terms[v][part], turns[v], got[part])
                sums = (
                    moved_part if sums is None else [a + b for a, b in zip(sums, moved_part)]
                )
                if last:
                    sent.pop(0).wait_send()
            bases = [shade_basis(terms[v][part][8]) for v in group]
            for j in range(16):
                for k in range(3):
                    r = base + 11 + 3 * j + k
                    where = slice(r * 8, (r + 1) * 8)
                    total = None if totals[part] is None else out_ref[where, :]
                    for basis_of, got in zip(bases, gots):
                        item = basis_of[j] * got[part][6 + k]
                        total = item if total is None else total + item
                    out_ref[where, :] = total
            totals[part] = sums
            if last:
                sent.pop(0).wait_send()
                for r, item in enumerate(pull_static(statics[part], sums)):
                    out_ref[(base + r) * 8 : (base + r + 1) * 8, :] = item
                sent.pop(0).wait_send()

    got = nothing()
    for k in range(cells):
        collect(0, got, returned.at[arrivals[k]] if k else back.at[cell], arrivals[k])
    pull_group((0,), (got,), False)
    for group in ((1,), (2, 3)):
        gots = [nothing() for _ in group]
        for k in range(cells):
            for v, got in zip(group, gots):
                relays[k][v - 1].wait()
                collect(v, got, relayed.at[mates[v - 1], arrivals[k]], arrivals[k])
        pull_group(group, gots, 3 in group)
    for copy in sent:
        copy.wait_send()


def update_kernel(
    params_ref, first_ref, second_ref, grads_ref, new_out, new_first_out, new_second_out,
    new_ref, new_first_ref, new_second_ref, sems,
):
    count, block = params_ref.shape
    blocks = block // LANES
    row_ids = lax.broadcasted_iota(jnp.int32, (8, LANES), 0)
    scale_one = 1.0 / (1.0 - 0.9**ADAM_STEP)
    scale_two = 1.0 / (1.0 - 0.999**ADAM_STEP)
    copies = []
    group = blocks // WAVES
    for b in range(blocks):
        span = slice(b * LANES, (b + 1) * LANES)
        part, line = divmod(b, 8)
        counts = grads_ref[blocks * PAD_ROWS + b : blocks * PAD_ROWS + b + 1, :]
        for r in range(0, count, 8):
            size = min(8, count - r)
            rows = slice(r, r + size)
            gradient = grads_ref[pl.ds((part * PAD_ROWS + r) * 8 + line, size, stride=8), :]
            if r >= 16:
                rates = 0.000125 * scale_one
            else:
                ids = row_ids[0:size] + r
                rates = scale_one * jnp.where(
                    ids < 6,
                    0.01,
                    jnp.where(
                        ids < 10,
                        0.005,
                        jnp.where(ids < 11, 0.05, jnp.where(ids < 14, 0.0025, 0.000125)),
                    ),
                )
            params, first, second = params_ref[rows, span], first_ref[rows, span], second_ref[rows, span]
            seen = jnp.broadcast_to(counts, params.shape) > 0.0
            first_new = 0.9 * first + 0.1 * gradient
            second_new = 0.999 * second + 0.001 * gradient * gradient
            stride = rates * first_new / (jnp.sqrt(second_new * scale_two) + 1e-08)
            new_ref[rows, span] = jnp.where(seen, params - stride, params)
            new_first_ref[rows, span] = jnp.where(seen, first_new, first)
            new_second_ref[rows, span] = jnp.where(seen, second_new, second)
        if (b + 1) % group == 0:
            wave = b // group
            span = slice(wave * group * LANES, (wave + 1) * group * LANES)
            for i, (source, dest) in enumerate(
                ((new_ref, new_out), (new_first_ref, new_first_out), (new_second_ref, new_second_out))
            ):
                copy = pltpu.make_async_copy(source.at[:, span], dest.at[:, span], sems.at[i, wave])
                copy.start()
                copies.append(copy)
    for copy in copies:
        copy.wait()


def fused_shards(params, first_moment, second_moment, cameras, visible, send_plan, tile_lists, target):
    cells, views = lax.axis_size("cells"), lax.axis_size("views")
    count, block = params.shape
    blocks = block // LANES
    plan = send_plan[0, 0]
    lists = tile_lists[0]
    tiles, entries = lists.shape
    capacity = plan.shape[1]
    halves = capacity // LANES
    slots = cells * halves
    f32, bf16 = jnp.float32, jnp.bfloat16
    packet = pltpu.VMEM((cells, FEATS * halves, LANES), f32)
    dma = pltpu.SemaphoreType.DMA
    vmem = pl.BlockSpec(memory_space=pltpu.VMEM)
    grads = pl.pallas_call(
        main_kernel,
        out_shape=jax.ShapeDtypeStruct((blocks * PAD_ROWS + blocks, LANES), f32),
        in_specs=[pl.BlockSpec(memory_space=pltpu.HBM)] * 6,
        out_specs=vmem,
        scratch_shapes=[
            pltpu.VMEM((count, block), f32),
            pltpu.VMEM(cameras.shape, f32),
            pltpu.VMEM(plan.shape, jnp.int32),
            pltpu.VMEM(visible.shape, jnp.int32),
            pltpu.VMEM(lists.shape, jnp.int32),
            pltpu.VMEM((3, 1, target.shape[2]), f32),
            pltpu.VMEM((blocks * PAD_ROWS, LANES), f32),
            pltpu.VMEM((blocks * 8, LANES), f32),
            pltpu.VMEM((blocks, LANES), f32),
            pltpu.VMEM((slots, LANES), jnp.int32),
            packet, packet, packet, packet,
            pltpu.VMEM((3 * blocks + 8, LANES), f32),
            pltpu.VMEM((views, 3 * blocks + 8, LANES), f32),
            pltpu.VMEM((views, cells, FEATS * halves, LANES), f32),
            pltpu.VMEM((slots, LANES), f32),
            pltpu.VMEM((tiles * entries // LANES, LANES), jnp.int32),
            pltpu.VMEM((24, LANES), f32),
            pltpu.VMEM((LANES, 2 * LANES), f32),
            pltpu.VMEM((entries, LANES), f32),
            pltpu.VMEM((entries, LANES), bf16),
            pltpu.VMEM((6, entries, LANES), f32),
            pltpu.VMEM((entries * 8, LANES), f32),
            pltpu.VMEM((entries * 8, LANES), f32),
            [pltpu.VMEM((8 * LANES, LANES), f32)] * 2,
            pltpu.VMEM((16 * LANES, entries + LANES), bf16),
            pltpu.VMEM((16 * LANES, entries + LANES), bf16),
            pltpu.VMEM((48, 16 * LANES), bf16),
            pltpu.VMEM((48, 16 * LANES), bf16),
            pltpu.VMEM((48, entries), f32),
            pltpu.VMEM((48, entries), f32),
            pltpu.VMEM((entries // LANES * 8, LANES), f32),
            pltpu.VMEM((tiles * entries // LANES * 16, LANES), f32),
            pltpu.VMEM((cells * 18, tiles * entries), bf16),
            pltpu.VMEM((capacity, tiles * entries), bf16),
            pltpu.VMEM((16, slots * LANES), bf16),
            pltpu.VMEM((2 * LANES, slots * LANES), bf16),
            dma((cells - 1,)), dma((cells,)), dma((cells - 1,)), dma((cells,)),
            dma((cells, views - 1)), dma((cells, views - 1)), dma((views - 1,)), dma((views - 1,)),
            dma((6,)),
        ],
        compiler_params=pltpu.CompilerParams(
            collective_id=0,
            has_side_effects=True,
            vmem_limit_bytes=MAIN_VMEM,
        ),
        cost_estimate=pl.CostEstimate(
            flops=4096 * tiles * 256 * entries,
            bytes_accessed=4 * count * block,
            transcendentals=tiles * 256 * entries,
        ),
    )(
        *[
            pltpu.with_memory_space_constraint(item, pltpu.HBM)
            for item in (params, cameras, plan, visible, lists, jnp.transpose(target, (1, 0, 2)))
        ]
    )
    like = jax.ShapeDtypeStruct(params.shape, f32)
    return tuple(
        pl.pallas_call(
            update_kernel,
            out_shape=(like, like, like),
            out_specs=(pl.BlockSpec(memory_space=pl.ANY),) * 3,
            scratch_shapes=[
                pltpu.VMEM(params.shape, f32),
                pltpu.VMEM(params.shape, f32),
                pltpu.VMEM(params.shape, f32),
                dma((3, WAVES)),
            ],
            compiler_params=pltpu.CompilerParams(vmem_limit_bytes=UPDATE_VMEM),
        )(params, first_moment, second_moment, grads)
    )


def local_shards(params, first_moment, second_moment, cameras, visible, send_plan, tile_lists, target):
    capacity = send_plan.shape[3]
    tiles, entries = tile_lists.shape[1:]
    halves = capacity // LANES
    fits = (
        capacity % LANES == 0
        and params.shape[1] == 16 * LANES
        and entries % (2 * LANES) == 0
        and 8 % max(halves, 1) == 0
        and lax.axis_size("cells") == 8
        and lax.axis_size("views") == 4
        and tiles * entries <= 4096
        and tiles == 4
    )
    body = fused_shards if fits else shards
    return body(params, first_moment, second_moment, cameras, visible, send_plan, tile_lists, target)


def solution(mesh):
    in_specs = (
        P(None, "cells"),
        P(None, "cells"),
        P(None, "cells"),
        P("views", None),
        P("views", "cells"),
        P("views", "cells", None, None),
        P("views", "cells", None),
        P("views", None, "cells"),
    )
    out_specs = (P(None, "cells"), P(None, "cells"), P(None, "cells"))
    return jax.shard_map(local_shards, mesh=mesh, in_specs=in_specs, out_specs=out_specs, check_vma=False)
```

```python
import functools

import jax
import jax.numpy as jnp
from jax import lax
from jax.experimental import pallas as pl
from jax.experimental.pallas import tpu as pltpu
from jax.sharding import PartitionSpec as P

TILE_COLS = 32
ADAM_STEP = 1000


harmonic_zero = 0.28209479177387814
harmonic_one = 0.4886025119029199
harmonic_two = (
    1.0925484305920792,
    -1.0925484305920792,
    0.31539156525252005,
    -1.0925484305920792,
    0.5462742152960396,
)
harmonic_three = (
    -0.5900435899266435,
    2.890611442640554,
    -0.4570457994644658,
    0.3731763325901154,
    -0.4570457994644658,
    1.445305721320277,
    -0.5900435899266435,
)


def harmonics(across, upward, onward):
    across_sq = across * across
    upward_sq = upward * upward
    onward_sq = onward * onward
    return jnp.stack(
        [
            harmonic_zero * jnp.ones_like(across),
            -harmonic_one * upward,
            harmonic_one * onward,
            -harmonic_one * across,
            harmonic_two[0] * across * upward,
            harmonic_two[1] * upward * onward,
            harmonic_two[2] * (2.0 * onward_sq - across_sq - upward_sq),
            harmonic_two[3] * across * onward,
            harmonic_two[4] * (across_sq - upward_sq),
            harmonic_three[0] * upward * (3.0 * across_sq - upward_sq),
            harmonic_three[1] * across * upward * onward,
            harmonic_three[2] * upward * (4.0 * onward_sq - across_sq - upward_sq),
            harmonic_three[3] * onward * (2.0 * onward_sq - 3.0 * across_sq - 3.0 * upward_sq),
            harmonic_three[4] * across * (4.0 * onward_sq - across_sq - upward_sq),
            harmonic_three[5] * onward * (across_sq - upward_sq),
            harmonic_three[6] * across * (across_sq - 3.0 * upward_sq),
        ]
    )


def camera_rotation(angles):
    cos_roll, sin_roll = (jnp.cos(angles[0]), jnp.sin(angles[0]))
    cos_pitch, sin_pitch = (jnp.cos(angles[1]), jnp.sin(angles[1]))
    cos_yaw, sin_yaw = (jnp.cos(angles[2]), jnp.sin(angles[2]))
    naught = jnp.zeros_like(cos_roll)
    unit_one = jnp.ones_like(cos_roll)
    roll = jnp.stack(
        [
            jnp.stack([unit_one, naught, naught]),
            jnp.stack([naught, cos_roll, -sin_roll]),
            jnp.stack([naught, sin_roll, cos_roll]),
        ]
    )
    pitch = jnp.stack(
        [
            jnp.stack([cos_pitch, naught, sin_pitch]),
            jnp.stack([naught, unit_one, naught]),
            jnp.stack([-sin_pitch, naught, cos_pitch]),
        ]
    )
    yawing = jnp.stack(
        [
            jnp.stack([cos_yaw, -sin_yaw, naught]),
            jnp.stack([sin_yaw, cos_yaw, naught]),
            jnp.stack([naught, naught, unit_one]),
        ]
    )
    inner_turn = jnp.dot(pitch, roll, precision=lax.Precision.HIGHEST)
    return jnp.dot(yawing, inner_turn, precision=lax.Precision.HIGHEST)


def project(values, camera):
    turn = camera_rotation(camera[0:3])
    offset = values[0:3] - camera[3:6][:, None]
    in_view = jnp.dot(turn, offset, precision=lax.Precision.HIGHEST)
    inv_depth = 1.0 / in_view[2]
    screen_col = in_view[0] * inv_depth
    screen_row = in_view[1] * inv_depth
    scales = jnp.exp(values[3:6])
    quat = values[6:10] / jnp.sqrt(jnp.sum(values[6:10] * values[6:10], axis=0, keepdims=True))
    quat_w, quat_x, quat_y, quat_z = (quat[0], quat[1], quat[2], quat[3])
    spin = [
        [
            1.0 - 2.0 * (quat_y * quat_y + quat_z * quat_z),
            2.0 * (quat_x * quat_y - quat_w * quat_z),
            2.0 * (quat_x * quat_z + quat_w * quat_y),
        ],
        [
            2.0 * (quat_x * quat_y + quat_w * quat_z),
            1.0 - 2.0 * (quat_x * quat_x + quat_z * quat_z),
            2.0 * (quat_y * quat_z - quat_w * quat_x),
        ],
        [
            2.0 * (quat_x * quat_z - quat_w * quat_y),
            2.0 * (quat_y * quat_z + quat_w * quat_x),
            1.0 - 2.0 * (quat_x * quat_x + quat_y * quat_y),
        ],
    ]
    basis_cam = []
    for outer_index in range(3):
        row_terms = []
        for col_index in range(3):
            entry = turn[outer_index, 0] * spin[0][col_index]
            for mid_index in range(1, 3):
                entry = entry + turn[outer_index, mid_index] * spin[mid_index][col_index]
            row_terms.append(entry * scales[col_index])
        basis_cam.append(row_terms)
    jac_top = [
        (basis_cam[0][col_index] - screen_col * basis_cam[2][col_index]) * inv_depth
        for col_index in range(3)
    ]
    jac_low = [
        (basis_cam[1][col_index] - screen_row * basis_cam[2][col_index]) * inv_depth
        for col_index in range(3)
    ]
    sigma_a = jac_top[0] * jac_top[0] + jac_top[1] * jac_top[1] + jac_top[2] * jac_top[2]
    sigma_b = jac_top[0] * jac_low[0] + jac_top[1] * jac_low[1] + jac_top[2] * jac_low[2]
    sigma_c = jac_low[0] * jac_low[0] + jac_low[1] * jac_low[1] + jac_low[2] * jac_low[2]
    determinant = sigma_a * sigma_c - sigma_b * sigma_b
    opacity = jax.nn.sigmoid(values[10])
    distance = jnp.sqrt(jnp.sum(offset * offset, axis=0))
    unit_dir = offset / distance
    basis = harmonics(unit_dir[0], unit_dir[1], unit_dir[2])
    coeffs = values[11:59].reshape(16, 3, values.shape[1])
    colors = 0.5 + jnp.sum(basis[:, None, :] * coeffs, axis=0)
    screen = jnp.stack(
        [
            screen_col,
            screen_row,
            sigma_c / determinant,
            -sigma_b / determinant,
            sigma_a / determinant,
            opacity,
        ]
    )
    return jnp.concatenate([screen, colors], axis=0)


def group_loss(pieces):
    features, live_mask, pixel_column, pixel_row, target_tile = pieces
    entries = live_mask.shape[1]
    delta_col = pixel_column[:, :, None] - features[0][:, None, :]
    delta_row = pixel_row[:, :, None] - features[1][:, None, :]
    power = -0.5 * (
        features[2][:, None, :] * delta_col * delta_col
        + 2.0 * features[3][:, None, :] * delta_col * delta_row
        + features[4][:, None, :] * delta_row * delta_row
    )
    alphas = features[5][:, None, :] * jnp.exp(power) * live_mask[:, None, :]
    log_keep = jnp.log(1.0 - alphas)
    earlier = (
        lax.broadcasted_iota(jnp.int32, (entries, entries), 0)
        < lax.broadcasted_iota(jnp.int32, (entries, entries), 1)
    ).astype(jnp.float32)
    transmit = jnp.exp(
        jnp.einsum("bpl,lm->bpm", log_keep, earlier, precision=lax.Precision.HIGHEST)
    )
    weights = alphas * transmit
    image = jnp.einsum("bpl,kbl->kbp", weights, features[6:9], precision=lax.Precision.HIGHEST)
    error = image - target_tile
    return jnp.sum(error * error)


def render_tiles(picked, live_mask, pixel_column, pixel_row, target_tile):
    groups = live_mask.shape[0] // 4
    entries = live_mask.shape[1]
    pixels = pixel_column.shape[1]
    stacked = (
        jnp.transpose(picked.reshape(picked.shape[0], groups, 4, entries), (1, 0, 2, 3)),
        live_mask.reshape(groups, 4, entries),
        pixel_column.reshape(groups, 4, pixels),
        pixel_row.reshape(groups, 4, pixels),
        jnp.transpose(target_tile.reshape(3, groups, 4, pixels), (1, 0, 2, 3)),
    )
    return jnp.sum(lax.map(jax.checkpoint(group_loss), stacked))


def pixel_grid(first_tile, count, tiles_dev, rows_pix):
    tile_ids = first_tile + jnp.arange(count, dtype=jnp.int32)
    pixel_ids = jnp.arange(256, dtype=jnp.int32)
    block_cols = TILE_COLS // 4
    owner_ids = tile_ids // tiles_dev
    local_ids = tile_ids % tiles_dev
    tile_col = 4 * (owner_ids % block_cols) + local_ids % 4
    tile_row = tiles_dev // 4 * (owner_ids // block_cols) + local_ids // 4
    half_width = TILE_COLS * 8.0
    column = (tile_col[:, None] * 16 + pixel_ids[None, :] % 16).astype(jnp.float32)
    row_pos = (tile_row[:, None] * 16 + pixel_ids[None, :] // 16).astype(jnp.float32)
    return ((column + 0.5 - half_width) / half_width, (row_pos + 0.5 - rows_pix * 0.5) / half_width)


def adam_update(params, first_moment, second_moment, gradient, counts):
    row_ids = lax.broadcasted_iota(jnp.int32, params.shape, 0)
    rates = jnp.where(
        row_ids < 6,
        0.01,
        jnp.where(
            row_ids < 10,
            0.005,
            jnp.where(row_ids < 11, 0.05, jnp.where(row_ids < 14, 0.0025, 0.000125)),
        ),
    )
    first_new = 0.9 * first_moment + 0.1 * gradient
    second = 0.999 * second_moment + 0.001 * gradient * gradient
    bias_one = 1.0 - 0.9**ADAM_STEP
    bias_two = 1.0 - 0.999**ADAM_STEP
    stride = rates * (first_new / bias_one) / (jnp.sqrt(second / bias_two) + 1e-08)
    seen_mask = counts > 0.0
    return (
        jnp.where(seen_mask, params - stride, params),
        jnp.where(seen_mask, first_new, first_moment),
        jnp.where(seen_mask, second, second_moment),
    )


def shards(params, first_moment, second_moment, cameras, visible, send_plan, tile_lists, target):
    cells = lax.axis_size("cells")
    camera = cameras[0]
    plan_rows = send_plan[0, 0]
    capacity = plan_rows.shape[1]
    sent_live = (plan_rows >= 0)[None]
    sent_rows = jnp.maximum(plan_rows, 0)
    lists = tile_lists[0]
    tiles_here = lists.shape[0]
    live_mask = (lists >= 0).astype(jnp.float32)
    slot_ids = jnp.maximum(lists, 0)
    rows_pix = tiles_here * cells // TILE_COLS * 16
    pixel_column, pixel_row = pixel_grid(
        lax.axis_index("cells") * tiles_here, tiles_here, tiles_here, rows_pix
    )
    target_tile = target[0].reshape(3, tiles_here, 256)
    block = params.shape[1]

    def image_loss(table):
        picked = jnp.take(table, slot_ids, axis=1)
        return render_tiles(picked, live_mask, pixel_column, pixel_row, target_tile)

    def own_projection(values):
        return project(values, camera)

    features, project_pull = jax.vjp(own_projection, params)
    outgoing = jnp.take(features, sent_rows, axis=1)
    incoming = lax.all_to_all(outgoing, "cells", split_axis=1, concat_axis=1, tiled=True)
    loss_value, pullback = jax.vjp(
        image_loss, incoming.reshape(features.shape[0], cells * capacity)
    )
    table_grad = pullback(jnp.ones((), jnp.float32))[0]
    returned = lax.all_to_all(
        table_grad.reshape(features.shape[0], cells, capacity),
        "cells",
        split_axis=1,
        concat_axis=1,
        tiled=True,
    )
    kept = jnp.where(sent_live, returned, 0.0)
    gradient = project_pull(
        jnp.zeros((features.shape[0], block), jnp.float32).at[:, sent_rows].add(kept)
    )[0]
    seen_here = visible.astype(jnp.float32)
    total_grad, counts = lax.psum((gradient, seen_here), "views")
    new_params, new_first, new_second = adam_update(
        params, first_moment, second_moment, total_grad, counts
    )
    return (new_params, new_first, new_second)

LANES = 128
PAD_ROWS = 64
FEATS = 9


def project_rows(rows, turn, centre):
    offset = [rows[i] - centre[i] for i in range(3)]
    in_view = [
        turn[i][0] * offset[0] + turn[i][1] * offset[1] + turn[i][2] * offset[2] for i in range(3)
    ]
    inv_depth = 1.0 / in_view[2]
    screen_col = in_view[0] * inv_depth
    screen_row = in_view[1] * inv_depth
    scales = [jnp.exp(rows[3 + i]) for i in range(3)]
    raw = rows[6:10]
    norm = jnp.sqrt(raw[0] * raw[0] + raw[1] * raw[1] + raw[2] * raw[2] + raw[3] * raw[3])
    inv_norm = 1.0 / norm
    quat_w, quat_x, quat_y, quat_z = [item * inv_norm for item in raw]
    spin = [
        [
            1.0 - 2.0 * (quat_y * quat_y + quat_z * quat_z),
            2.0 * (quat_x * quat_y - quat_w * quat_z),
            2.0 * (quat_x * quat_z + quat_w * quat_y),
        ],
        [
            2.0 * (quat_x * quat_y + quat_w * quat_z),
            1.0 - 2.0 * (quat_x * quat_x + quat_z * quat_z),
            2.0 * (quat_y * quat_z - quat_w * quat_x),
        ],
        [
            2.0 * (quat_x * quat_z - quat_w * quat_y),
            2.0 * (quat_y * quat_z + quat_w * quat_x),
            1.0 - 2.0 * (quat_x * quat_x + quat_y * quat_y),
        ],
    ]
    basis_cam = [
        [
            (turn[i][0] * spin[0][j] + turn[i][1] * spin[1][j] + turn[i][2] * spin[2][j])
            * scales[j]
            for j in range(3)
        ]
        for i in range(3)
    ]
    top = [(basis_cam[0][j] - screen_col * basis_cam[2][j]) * inv_depth for j in range(3)]
    low = [(basis_cam[1][j] - screen_row * basis_cam[2][j]) * inv_depth for j in range(3)]
    sigma_a = top[0] * top[0] + top[1] * top[1] + top[2] * top[2]
    sigma_b = top[0] * low[0] + top[1] * low[1] + top[2] * low[2]
    sigma_c = low[0] * low[0] + low[1] * low[1] + low[2] * low[2]
    inv_det = 1.0 / (sigma_a * sigma_c - sigma_b * sigma_b)
    opacity = 1.0 / (1.0 + jnp.exp(-rows[10]))
    inv_dist = 1.0 / jnp.sqrt(offset[0] * offset[0] + offset[1] * offset[1] + offset[2] * offset[2])
    x, y, z = [item * inv_dist for item in offset]
    xx, yy, zz = x * x, y * y, z * z
    basis = [
        None,
        -harmonic_one * y,
        harmonic_one * z,
        -harmonic_one * x,
        harmonic_two[0] * x * y,
        harmonic_two[1] * y * z,
        harmonic_two[2] * (2.0 * zz - xx - yy),
        harmonic_two[3] * x * z,
        harmonic_two[4] * (xx - yy),
        harmonic_three[0] * y * (3.0 * xx - yy),
        harmonic_three[1] * x * y * z,
        harmonic_three[2] * y * (4.0 * zz - xx - yy),
        harmonic_three[3] * z * (2.0 * zz - 3.0 * xx - 3.0 * yy),
        harmonic_three[4] * x * (4.0 * zz - xx - yy),
        harmonic_three[5] * z * (xx - yy),
        harmonic_three[6] * x * (xx - 3.0 * yy),
    ]
    colors = []
    for k in range(3):
        total = harmonic_zero * rows[11 + k]
        for j in range(1, 16):
            total = total + basis[j] * rows[11 + 3 * j + k]
        colors.append(0.5 + total)
    return (
        screen_col,
        screen_row,
        sigma_c * inv_det,
        -sigma_b * inv_det,
        sigma_a * inv_det,
        opacity,
        *colors,
    )


def static_terms(rows):
    scales = [jnp.exp(item) for item in rows[3:6]]
    raw = rows[6:10]
    inv_norm = 1.0 / jnp.sqrt(
        raw[0] * raw[0] + raw[1] * raw[1] + raw[2] * raw[2] + raw[3] * raw[3]
    )
    quat = [item * inv_norm for item in raw]
    w, x, y, z = quat
    spin = [
        [1.0 - 2.0 * (y * y + z * z), 2.0 * (x * y - w * z), 2.0 * (x * z + w * y)],
        [2.0 * (x * y + w * z), 1.0 - 2.0 * (x * x + z * z), 2.0 * (y * z - w * x)],
        [2.0 * (x * z - w * y), 2.0 * (y * z + w * x), 1.0 - 2.0 * (x * x + y * y)],
    ]
    frame = [[spin[m][j] * scales[j] for j in range(3)] for m in range(3)]
    fade = 1.0 - 1.0 / (1.0 + jnp.exp(-rows[10]))
    return scales, inv_norm, quat, frame, fade


def moving_terms(rows, frame, turn, centre):
    offset = [rows[i] - centre[i] for i in range(3)]
    in_view = [
        turn[i][0] * offset[0] + turn[i][1] * offset[1] + turn[i][2] * offset[2] for i in range(3)
    ]
    inv = 1.0 / in_view[2]
    col, row = in_view[0] * inv, in_view[1] * inv
    cam = [
        [
            turn[i][0] * frame[0][j] + turn[i][1] * frame[1][j] + turn[i][2] * frame[2][j]
            for j in range(3)
        ]
        for i in range(3)
    ]
    top = [(cam[0][j] - col * cam[2][j]) * inv for j in range(3)]
    low = [(cam[1][j] - row * cam[2][j]) * inv for j in range(3)]
    sigma_a = top[0] * top[0] + top[1] * top[1] + top[2] * top[2]
    sigma_b = top[0] * low[0] + top[1] * low[1] + top[2] * low[2]
    sigma_c = low[0] * low[0] + low[1] * low[1] + low[2] * low[2]
    inv_det = 1.0 / (sigma_a * sigma_c - sigma_b * sigma_b)
    conic = (sigma_c * inv_det, -sigma_b * inv_det, sigma_a * inv_det)
    inv_dist = 1.0 / jnp.sqrt(offset[0] * offset[0] + offset[1] * offset[1] + offset[2] * offset[2])
    ray = [item * inv_dist for item in offset]
    return inv, col, row, cam[2], top, low, conic, inv_dist, ray


def shade_basis(ray):
    x, y, z = ray
    xx, yy, zz = x * x, y * y, z * z
    xy, yz, xz = x * y, y * z, x * z
    h1, h2, h3 = harmonic_one, harmonic_two, harmonic_three
    outer = 4.0 * zz - xx - yy
    return [
        harmonic_zero,
        -h1 * y,
        h1 * z,
        -h1 * x,
        h2[0] * xy,
        h2[1] * yz,
        h2[2] * (2.0 * zz - xx - yy),
        h2[3] * xz,
        h2[4] * (xx - yy),
        h3[0] * y * (3.0 * xx - yy),
        h3[1] * xy * z,
        h3[2] * y * outer,
        h3[3] * z * (2.0 * zz - 3.0 * xx - 3.0 * yy),
        h3[4] * x * outer,
        h3[5] * z * (xx - yy),
        h3[6] * x * (xx - 3.0 * yy),
    ]


def pull_moving(rows, terms, turn, got):
    inv, col, row, deep, top, low, conic, inv_dist, ray = terms
    k0, k1, k2 = conic
    g0, half, g2 = -0.5 * got[3], -0.5 * got[4], -0.5 * got[5]
    p00, p01 = g0 * k0 + half * k1, g0 * k1 + half * k2
    p10, p11 = half * k0 + g2 * k1, half * k1 + g2 * k2
    d00 = -2.0 * (k0 * p00 + k1 * p10)
    d01 = -2.0 * (k0 * p01 + k1 * p11)
    d11 = -2.0 * (k1 * p01 + k2 * p11)
    d_top = [(d00 * top[j] + d01 * low[j]) * inv for j in range(3)]
    d_low = [(d01 * top[j] + d11 * low[j]) * inv for j in range(3)]
    d_cam = [d_top, d_low, [-(col * d_top[j] + row * d_low[j]) for j in range(3)]]
    d_col = k0 * got[1] + k1 * got[2]
    d_row = k1 * got[1] + k2 * got[2]
    d_depth = 0.0
    for j in range(3):
        d_col = d_col - d_top[j] * deep[j]
        d_row = d_row - d_low[j] * deep[j]
        d_depth = d_depth - (d_top[j] * top[j] + d_low[j] * low[j])
    d_view = [d_col * inv, d_row * inv]
    d_view.append(d_depth - (col * d_view[0] + row * d_view[1]))
    d_frame = [
        [turn[0][m] * d_cam[0][j] + turn[1][m] * d_cam[1][j] + turn[2][m] * d_cam[2][j] for j in range(3)]
        for m in range(3)
    ]
    x, y, z = ray
    xx, yy, zz = x * x, y * y, z * z
    yz, xz = y * z, x * z
    h1, h2, h3 = harmonic_one, harmonic_two, harmonic_three
    outer = 4.0 * zz - xx - yy
    tint = got[6:9]
    e = [None] + [
        tint[0] * rows[11 + 3 * j] + tint[1] * rows[12 + 3 * j] + tint[2] * rows[13 + 3 * j]
        for j in range(1, 16)
    ]
    gx = (
        -h1 * e[3]
        + y * (h2[0] * e[4] + (6.0 * h3[0]) * (x * e[9]) - (2.0 * h3[2]) * (x * e[11]))
        + z * (h2[3] * e[7] + h3[1] * (y * e[10]))
        + x * ((-2.0 * h2[2]) * e[6] + (2.0 * h2[4]) * e[8])
        + xz * ((-6.0 * h3[3]) * e[12] + (2.0 * h3[5]) * e[14])
        + (h3[4] * (outer - 2.0 * xx)) * e[13]
        + ((3.0 * h3[6]) * (xx - yy)) * e[15]
    )
    gy = (
        -h1 * e[1]
        + x * (h2[0] * e[4] - (2.0 * h3[4]) * (y * e[13]) - (6.0 * h3[6]) * (y * e[15]))
        + z * (h2[1] * e[5] + h3[1] * (x * e[10]))
        + y * ((-2.0 * h2[2]) * e[6] - (2.0 * h2[4]) * e[8])
        + yz * ((-6.0 * h3[3]) * e[12] - (2.0 * h3[5]) * e[14])
        + ((3.0 * h3[0]) * (xx - yy)) * e[9]
        + (h3[2] * (outer - 2.0 * yy)) * e[11]
    )
    gz = (
        h1 * e[2]
        + y * (h2[1] * e[5] + h3[1] * (x * e[10]) + (8.0 * h3[2]) * (z * e[11]))
        + x * (h2[3] * e[7] + (8.0 * h3[4]) * (z * e[13]))
        + (4.0 * h2[2]) * (z * e[6])
        + ((3.0 * h3[3]) * (2.0 * zz - xx - yy)) * e[12]
        + (h3[5] * (xx - yy)) * e[14]
    )
    along = x * gx + y * gy + z * gz
    d_ray = [(gx - x * along) * inv_dist, (gy - y * along) * inv_dist, (gz - z * along) * inv_dist]
    d_place = [
        turn[0][i] * d_view[0] + turn[1][i] * d_view[1] + turn[2][i] * d_view[2] + d_ray[i]
        for i in range(3)
    ]
    return [*d_place, *d_frame[0], *d_frame[1], *d_frame[2], got[0]]


def pull_static(static, sums):
    scales, inv_norm, quat, frame, fade = static
    d_frame = [sums[3:6], sums[6:9], sums[9:12]]
    d_scale = [
        d_frame[0][j] * frame[0][j] + d_frame[1][j] * frame[1][j] + d_frame[2][j] * frame[2][j]
        for j in range(3)
    ]
    d = [[d_frame[m][j] * scales[j] for j in range(3)] for m in range(3)]
    w, x, y, z = quat
    d_quat = [
        2.0 * (z * (d[1][0] - d[0][1]) + y * (d[0][2] - d[2][0]) + x * (d[2][1] - d[1][2])),
        2.0 * (y * (d[0][1] + d[1][0]) + z * (d[0][2] + d[2][0]) + w * (d[2][1] - d[1][2]) - 2.0 * x * (d[1][1] + d[2][2])),
        2.0 * (x * (d[0][1] + d[1][0]) + w * (d[0][2] - d[2][0]) + z * (d[1][2] + d[2][1]) - 2.0 * y * (d[0][0] + d[2][2])),
        2.0 * (w * (d[1][0] - d[0][1]) + x * (d[0][2] + d[2][0]) + y * (d[1][2] + d[2][1]) - 2.0 * z * (d[0][0] + d[1][1])),
    ]
    along = w * d_quat[0] + x * d_quat[1] + y * d_quat[2] + z * d_quat[3]
    d_raw = [(d_quat[i] - quat[i] * along) * inv_norm for i in range(4)]
    return [*sums[0:3], *d_scale, *d_raw, fade * sums[12]]


def camera_terms(cam):
    cosines, sines = jnp.cos(cam), jnp.sin(cam)
    cr, cp, cy = [cosines[:, i : i + 1] for i in range(3)]
    sr, sp, sy = [sines[:, i : i + 1] for i in range(3)]
    turn = [
        [cy * cp, cy * sp * sr - sy * cr, cy * sp * cr + sy * sr],
        [sy * cp, sy * sp * sr + cy * cr, sy * sp * cr - cy * sr],
        [-sp, cp * sr, cp * cr],
    ]
    centre = [cam[:, 3 + i : 4 + i] for i in range(3)]
    return turn, centre

MAIN_VMEM = 40 * 2**20
UPDATE_VMEM = 16 * 2**20
WAVES = 4


def fill_dense(params_ref, dense):
    count, block = params_ref.shape
    for b in range(block // LANES):
        part, line = divmod(b, 8)
        for r in range(0, count, 8):
            size = min(8, count - r)
            where = pl.ds((part * PAD_ROWS + r) * 8 + line, size, stride=8)
            dense[where, :] = params_ref[r : r + size, b * LANES : (b + 1) * LANES]


def dense_rows(dense, part, count):
    return [
        dense[(part * PAD_ROWS + r) * 8 : (part * PAD_ROWS + r) * 8 + 8, :] for r in range(count)
    ]


def lane_pick(source, lanes):
    return jnp.take_along_axis(source, lanes, axis=1, mode="promise_in_bounds")


def gather_eight(load, blocks, index):
    index = jnp.maximum(index, 0)
    lanes, block = index & (LANES - 1), index >> 7
    total = lane_pick(load(0), lanes)
    for b in range(1, blocks):
        total = jnp.where(block == b, lane_pick(load(b), lanes), total)
    return total


def split_three(x):
    first = x.astype(jnp.bfloat16).astype(jnp.float32)
    rest = x - first
    second = rest.astype(jnp.bfloat16).astype(jnp.float32)
    return first, second, rest - second


def fill_hot(hot, index, start, bits):
    shape = (hot.shape[0], LANES)
    row_ids = lax.broadcasted_iota(jnp.int32, shape, 0).astype(jnp.float32).astype(jnp.bfloat16)
    low = (index & ((1 << bits) - 1)).astype(jnp.float32).astype(jnp.bfloat16)
    one, none = jnp.ones(shape, jnp.bfloat16), jnp.zeros(shape, jnp.bfloat16)
    hot[:, start : start + LANES] = jnp.where(row_ids == jnp.broadcast_to(low, shape), one, none)


def split_two(x):
    first = x.astype(jnp.bfloat16).astype(jnp.float32)
    return first, x - first


def fill_values(lhs, main, last, index, start, bits):
    groups = lhs.shape[0] // 18
    span = slice(start, start + LANES)
    parts = jnp.concatenate(split_two(main), axis=0)
    tips = [jnp.broadcast_to(item, (8, LANES)) for item in split_two(last)]
    high = jnp.broadcast_to(index >> bits, (16, LANES))
    sub = lax.broadcasted_iota(jnp.int32, (8, LANES), 0)
    for b in range(groups):
        lhs[16 * b : 16 * b + 16, span] = jnp.where(high == b, parts, 0.0).astype(jnp.bfloat16)
    for g in range(groups // 8):
        here = high[0:8] == sub + 8 * g
        rows = jnp.concatenate([jnp.where(here, item, 0.0) for item in tips], axis=0)
        row = 16 * groups + 16 * g
        lhs[row : row + 16, span] = rows.astype(jnp.bfloat16)


def scatter_dot(lhs, hot, rows):
    return lax.dot_general(
        lhs[rows], hot[...], (((1,), (1,)), ((), ())), preferred_element_type=jnp.float32
    )


def scatter_main(lhs, hot, first, last):
    out = scatter_dot(lhs, hot, slice(16 * first, 16 * last))
    return [out[16 * b : 16 * b + 8] + out[16 * b + 8 : 16 * b + 16] for b in range(last - first)]


def scatter_tips(lhs, hot):
    groups = lhs.shape[0] // 18
    out = scatter_dot(lhs, hot, slice(16 * groups, 18 * groups))
    return [
        out[16 * (b // 8) + b % 8 : 16 * (b // 8) + b % 8 + 1]
        + out[16 * (b // 8) + 8 + b % 8 : 16 * (b // 8) + 9 + b % 8]
        for b in range(groups)
    ]


def stage_features(feat_parts, plan_ref, table, last, order, tips):
    halves = plan_ref.shape[1] // LANES
    blocks = last.shape[0]
    for part, feats in enumerate(feat_parts):
        for f in range(8):
            table[pl.ds(part * 64 + f, 8, stride=8), :] = feats[f]
        last[part * 8 : part * 8 + 8, :] = feats[8]
    slots = plan_ref.shape[0] * halves
    for o in range(slots):
        d, h = divmod(o, halves)
        order[o : o + 1, :] = plan_ref[d : d + 1, h * LANES : (h + 1) * LANES]
    for p in range(slots // 8):
        tips[8 * p : 8 * p + 8, :] = gather_eight(
            lambda b: jnp.broadcast_to(last[b : b + 1, :], (8, LANES)),
            blocks,
            order[8 * p : 8 * p + 8, :],
        )


def pack_features(d, halves, table, order, tips, out_ref):
    blocks = table.shape[0] // 8
    for h in range(halves):
        row = pl.ds(d * halves + h, 1)
        out_ref[d, 8 * h : 8 * h + 8, :] = gather_eight(
            lambda b: table[8 * b : 8 * b + 8, :],
            blocks,
            jnp.broadcast_to(order[row, :], (8, LANES)),
        )
        out_ref[d, 8 * halves + h : 8 * halves + h + 1, :] = tips[row, :]


def pixel_terms():
    lane = lax.broadcasted_iota(jnp.int32, (8, LANES), 1)
    inner = lane & 31
    tile = lane >> 5
    x = (inner & 15).astype(jnp.float32) - 7.5
    step = (inner >> 4).astype(jnp.float32) - 0.5
    return tile, x, step


def render_setup(lists_ref, target_ref, order, wanted, basis, plan_sums, hot, bits):
    tiles, entries = lists_ref.shape
    quarters = entries // LANES
    for q in range(quarters):
        order[q * tiles : (q + 1) * tiles, :] = lists_ref[:, q * LANES : (q + 1) * LANES]
    sub = lax.broadcasted_iota(jnp.int32, (8, LANES), 0)
    lane = lax.broadcasted_iota(jnp.int32, (8, LANES), 1)
    tile, x, step = pixel_terms()
    shifted = 32 * (sub & 3) + (lane & 31)
    for k in range(3):
        total = jnp.zeros((8, LANES), jnp.float32)
        for r in range(8):
            row = jnp.broadcast_to(target_ref[k, :, r * LANES : (r + 1) * LANES], (8, LANES))
            here = (tile == r // 2) & ((sub >> 2) == r % 2)
            total = jnp.where(here, lane_pick(row, shifted), total)
        wanted[8 * k : 8 * k + 8, :] = total
    for g in range(LANES // 8):
        row = sub + 8 * g
        coef = (row * 43) >> 9
        mine = tile == (row & 3)

        def column(j, *terms):
            total = jnp.zeros((8, LANES), jnp.float32)
            for c, value in terms:
                total = jnp.where(coef == c, value, total)
            total = jnp.where(mine, total, 0.0)
            basis[8 * g : 8 * g + 8, j * LANES : (j + 1) * LANES] = total

        column(0, (0, x * x), (1, x * step), (2, step * step), (3, x), (4, step), (5, 1.0))
        column(1, (1, x), (2, 2.0 * step), (4, 1.0))
    mine = tile == (sub & 3)
    for s in range(8):
        y = step + (2.0 * s - 7.0)
        rows = [jnp.ones_like(x), x, y, x * x, x * y, y * y]
        rows = jnp.concatenate([jnp.where(mine, item, 0.0) for item in rows], axis=0)
        for part in range(2):
            start = (part * 8 + s) * LANES
            plan_sums[:, start : start + LANES] = rows.astype(jnp.bfloat16)
    for o in range(tiles * quarters):
        fill_hot(hot, order[o : o + 1, :], o * LANES, bits)


def render_rest(
    cells, others, receive, pause, recv_ref, order, wanted, back_ref,
    coefs, turned_s, tables, basis, alpha_s, weight_s, stages, joint_g, joint_w, plan_sums, error_sums,
    turned, tinted, moved, pairs, lhs, hot, bits,
):
    owners, packed, _ = recv_ref.shape
    halves = packed // FEATS
    blocks = owners * halves
    tiles = 4
    quarters = order.shape[0] // tiles
    entries = quarters * LANES
    me = lax.axis_index("cells")
    rows_pix = tiles * cells // TILE_COLS * 16
    half_width = TILE_COLS * 8.0
    inv_width = 1.0 / half_width
    log_two = 1.4426950408889634
    sub = lax.broadcasted_iota(jnp.int32, (8, LANES), 0)
    local = sub & 3
    tile_col = 4 * lax.rem(me, TILE_COLS // 4) + local
    tile_row = lax.div(me, TILE_COLS // 4)
    centre_col = (16 * tile_col + 8).astype(jnp.float32) - half_width
    centre_row = (jnp.full((8, LANES), 16 * tile_row + 8, jnp.int32)).astype(
        jnp.float32
    ) - rows_pix * 0.5

    picked = [[None] * FEATS for _ in range(quarters // 2)]
    for k in range(owners):
        origin = others[-k] if k else me
        if k:
            receive(origin)
        for p in range(quarters // 2):
            index = jnp.maximum(order[8 * p : 8 * p + 8, :], 0)
            lanes, block = index & (LANES - 1), index >> 7
            for h in range(halves):
                here = block == origin * halves + h
                for f in range(FEATS):
                    r = 8 * h + f if f < 8 else 8 * halves + h
                    row = jnp.broadcast_to(recv_ref[origin, r : r + 1, :], (8, LANES))
                    item = lane_pick(row, lanes)
                    old = picked[p][f]
                    picked[p][f] = item if old is None else jnp.where(here, item, old)

    for p in range(quarters // 2):
        index = order[8 * p : 8 * p + 8, :]
        feats = picked[p]
        off_col = feats[0] * half_width - centre_col
        off_row = feats[1] * half_width - centre_row
        moved[16 * p : 16 * p + 8, :] = off_col
        moved[16 * p + 8 : 16 * p + 16, :] = off_row
        square = feats[2] * (-0.5 * log_two * inv_width * inv_width)
        cross = feats[3] * (-log_two * inv_width * inv_width)
        bend = feats[4] * (-0.5 * log_two * inv_width * inv_width)
        faint = jnp.maximum(jnp.log(feats[5]) * log_two, -1e30)
        along = square * off_col + cross * off_row
        level = along * off_col + bend * off_row * off_row + jnp.where(index >= 0, faint, -1e30)
        terms = [
            square,
            cross,
            bend,
            -(along + square * off_col),
            -(2.0 * bend * off_row + cross * off_col),
            level,
        ]
        for m, term in enumerate((terms[2], *feats[6:9])):
            row = 72 + m * tiles
            for q in range(2):
                start = (2 * p + q) * LANES
                coefs[start + row : start + row + tiles, :] = term[4 * q : 4 * q + 4]
        for c, term in enumerate(terms):
            for i, piece in enumerate(split_three(term)):
                row = (3 * c + i) * tiles
                for q in range(2):
                    start = (2 * p + q) * LANES
                    coefs[start + row : start + row + tiles, :] = piece[4 * q : 4 * q + 4]
        pause()
    for q in range(quarters):
        coefs[q * LANES + 88 : (q + 1) * LANES, :] = jnp.zeros((LANES - 88, LANES), jnp.float32)
    weights = basis[...].astype(jnp.bfloat16)
    picks = [pixel_terms()[0] + (72 + tiles * m) for m in range(4)]
    for q in range(quarters):
        span = slice(q * LANES, (q + 1) * LANES)
        columns = jnp.transpose(coefs[span, :])
        turned_s[span, :] = columns.astype(jnp.bfloat16)
        for m in range(4):
            for g in range(LANES // 8):
                row = q * LANES + 8 * g
                tables[2 + m, row : row + 8, :] = lane_pick(columns[8 * g : 8 * g + 8], picks[m])
    result = jnp.dot(turned_s[...], weights, preferred_element_type=jnp.float32)
    for j in range(2):
        tables[j] = result[:, j * LANES : (j + 1) * LANES]

    height = (2 * sub - 7).astype(jnp.float32)

    def table(l, j):
        return jnp.broadcast_to(tables[j, pl.ds(l, 1), :], (8, LANES))

    def keep(stage, c, i, item):
        tile = (c * 16 + i // 8 * 8) * 8
        stage[pl.ds(tile + i % 8, 8, stride=8), :] = item

    def turn_over(stage, joint, q, s):
        item = jnp.transpose(
            jnp.concatenate([stage[t * 64 + s * 8 : t * 64 + s * 8 + 8, :] for t in range(16)], axis=0)
        )
        top = item.astype(jnp.bfloat16)
        span = pl.ds(pl.multiple_of(q * LANES, LANES), LANES)
        joint[s * LANES : (s + 1) * LANES, span] = top
        joint[(8 + s) * LANES : (9 + s) * LANES, span] = (
            item - top.astype(jnp.float32)
        ).astype(jnp.bfloat16)

    chunks = LANES // 16

    def forward(q, carry, stage, other):
        trans, red, green, blue = carry
        first = pl.multiple_of(q * LANES, LANES)
        base = pl.multiple_of(q * 8 * LANES, 8 * LANES)
        for c in range(chunks):
            for i in range(16):
                l = first + (c * 16 + i)
                where = pl.ds(base + (c * 16 + i) * 8, 8)
                power = table(l, 0) + height * (table(l, 1) + height * table(l, 2))
                alpha = jnp.exp2(power)
                weight = alpha * trans
                alpha_s[where, :] = alpha
                weight_s[where, :] = weight
                keep(stage, c, i, weight)
                trans = trans - weight
                red = red + weight * table(l, 3)
                green = green + weight * table(l, 4)
                blue = blue + weight * table(l, 5)
            turn_over(other, joint_w, q, c)
        return trans, red, green, blue

    zero = jnp.zeros((8, LANES), jnp.float32)
    even, odd = stages

    def forward_pair(i, carry):
        carry = forward(2 * i, carry, even, odd)
        return forward(2 * i + 1, carry, odd, even)

    carry = lax.fori_loop(
        0, quarters // 2, forward_pair, (jnp.ones((8, LANES), jnp.float32), zero, zero, zero)
    )
    for c in range(chunks):
        turn_over(odd, joint_w, quarters, c)
    red, green, blue = carry[1:]
    errors = [2.0 * (item - wanted[8 * k : 8 * k + 8, :]) for k, item in enumerate((red, green, blue))]
    wanted[0:8, :], wanted[8:16, :], wanted[16:24, :] = errors
    tile, _, _ = pixel_terms()
    mine = tile == local
    for s in range(8):
        tops, lows = [], []
        for k in range(3):
            row = jnp.broadcast_to(wanted[8 * k + s : 8 * k + s + 1, :], (8, LANES))
            row = jnp.where(mine, row, 0.0)
            top = row.astype(jnp.bfloat16).astype(jnp.float32)
            tops.append(top)
            lows.append(row - top)
        blank = [jnp.zeros((24, LANES), jnp.float32)]
        start = s * LANES
        error_sums[:, start : start + LANES] = jnp.concatenate(tops + lows, axis=0).astype(jnp.bfloat16)
        start = (8 + s) * LANES
        error_sums[:, start : start + LANES] = jnp.concatenate(tops + blank, axis=0).astype(jnp.bfloat16)

    def backward(q, behind, stage, other):
        first = pl.multiple_of(q * LANES, LANES)
        tinted[:, pl.ds(first, LANES)] = jnp.dot(
            error_sums[...],
            joint_w[:, pl.ds(first + LANES, LANES)],
            preferred_element_type=jnp.float32,
        )
        base = pl.multiple_of(q * 8 * LANES, 8 * LANES)
        for c in range(chunks - 1, -1, -1):
            for i in range(15, -1, -1):
                l = first + (c * 16 + i)
                where = pl.ds(base + (c * 16 + i) * 8, 8)
                slope = errors[0] * table(l, 3) + errors[1] * table(l, 4) + errors[2] * table(l, 5)
                alpha = alpha_s[where, :]
                keep(stage, c, i, weight_s[where, :] * (slope - behind))
                behind = (1.0 - alpha) * behind + alpha * slope
            turn_over(other, joint_g, q + 1, chunks - 1 - c)
        return behind

    def backward_pair(i, behind):
        q = quarters - 1 - 2 * i
        behind = backward(q, behind, odd, even)
        return backward(q - 1, behind, even, odd)

    lax.fori_loop(0, quarters // 2, backward_pair, zero)
    for c in range(chunks):
        turn_over(even, joint_g, 0, c)
    turned[...] = jnp.dot(
        plan_sums[...], joint_g[:, 0:entries], preferred_element_type=jnp.float32
    )
    for p in range(quarters // 2):
        off_col = moved[16 * p : 16 * p + 8, :]
        off_row = moved[16 * p + 8 : 16 * p + 16, :]

        def quantity(j):
            source, r = (turned, j) if j < 6 else (tinted, j - 6)
            rows = slice(8 * r, 8 * r + 8)
            start = 2 * p * LANES
            return jnp.where(
                sub < 4,
                source[rows, start : start + LANES],
                source[rows, start + LANES : start + 2 * LANES],
            )

        plain, across, down = quantity(0), quantity(1), quantity(2)
        near_col = across - off_col * plain
        near_row = down - off_row * plain
        rows = [
            plain,
            near_col * inv_width,
            near_row * inv_width,
            (quantity(3) - off_col * (across + near_col)) * (inv_width * inv_width),
            (quantity(4) - off_col * down - off_row * near_col) * (inv_width * inv_width),
            (quantity(5) - off_row * (down + near_row)) * (inv_width * inv_width),
            *[quantity(6 + k) + quantity(9 + k) for k in range(3)],
        ]
        for f, item in enumerate(rows):
            pairs[pl.ds(p * 128 + f, 8, stride=16), :] = item
        pause()
    for o in range(tiles * quarters):
        if o == tiles * quarters // 2:
            pause()
        fill_values(
            lhs,
            pairs[o * 16 : o * 16 + 8, :],
            pairs[o * 16 + 8 : o * 16 + 9, :],
            order[o : o + 1, :],
            o * LANES,
            bits,
        )
    for s, (main, last) in enumerate(zip(scatter_main(lhs, hot, 0, owners), scatter_tips(lhs, hot))):
        for h in range(halves):
            span = slice(h * LANES, (h + 1) * LANES)
            back_ref[s, 8 * h : 8 * h + 8, :] = main[:, span]
            back_ref[s, 8 * halves + h : 8 * halves + h + 1, :] = last[:, span]


def main_kernel(
    params_in, cam_in, plan_in, visible_in, lists_in, target_in, out_ref,
    params_ref, cam_ref, plan_ref, visible_ref, lists_ref, target_ref, dense, table, last, plan_order, outgoing, incoming, back, returned, extra, extras, relayed, tips,
    order, wanted, basis, coefs, turned_s, tables, alpha_s, weight_s, stages, joint_g, joint_w,
    plan_sums, error_sums, turned, tinted, moved, pairs, lhs, hot, own_lhs, own_hot,
    send_one, recv_one, send_two, recv_two, send_three, recv_three, send_four, recv_four, local_sem,
):
    cells, views = lax.axis_size("cells"), lax.axis_size("views")
    cell, view = lax.axis_index("cells"), lax.axis_index("views")
    count, block = params_ref.shape
    blocks = block // LANES
    capacity = plan_ref.shape[1]
    halves = capacity // LANES
    bits = capacity.bit_length() - 1
    barrier = pltpu.get_barrier_semaphore()

    far = lax.div(cell, 4)
    depth, side = lax.div(cell, 2), lax.rem(cell, 2)
    others = [
        2 * d + e
        for d in (3 - 3 * far, 2 - far, 1 - depth + 4 * far)
        for e in (1 - side, side)
    ] + [2 * depth + 1 - side]
    twin = view + 1 - 2 * lax.rem(view, 2)
    across = lax.rem(view + 2, views)
    mates = [twin, across, lax.rem(twin + 2, views)]

    def send(axis, peer, source, dest, send_sem, recv_sem):
        copy = pltpu.make_async_remote_copy(
            src_ref=source,
            dst_ref=dest,
            send_sem=send_sem,
            recv_sem=recv_sem,
            device_id={axis: peer},
            device_id_type=pl.DeviceIdType.MESH,
        )
        copy.start()
        return copy

    def receiver(buffer, sems):
        def receive(origin):
            pltpu.make_async_remote_copy(
                src_ref=buffer.at[origin],
                dst_ref=buffer.at[origin],
                send_sem=sems.at[origin],
                recv_sem=sems.at[origin],
                device_id={"cells": origin},
                device_id_type=pl.DeviceIdType.MESH,
            ).wait_recv()

        return receive

    receive_one = receiver(incoming, recv_one)
    receive_two = receiver(returned, recv_two)
    def greet(axis, peer):
        pl.semaphore_signal(
            barrier, inc=1, device_id={axis: peer}, device_id_type=pl.DeviceIdType.MESH
        )

    for peer in others:
        greet("cells", peer)
    fetches = [
        pltpu.make_async_copy(source, dest, local_sem.at[i])
        for i, (source, dest) in enumerate(
            (
                (params_in, params_ref),
                (cam_in, cam_ref),
                (plan_in, plan_ref),
                (visible_in, visible_ref),
                (lists_in, lists_ref),
                (target_in, target_ref),
            )
        )
    ]
    for fetch in fetches:
        fetch.start()
    for mate in mates:
        greet("views", mate)
    fetches[1].wait()
    turn, centre = camera_terms(cam_ref[...])
    known = [*turn[0], *turn[1], *turn[2], *centre]
    lane = lax.broadcasted_iota(jnp.int32, (8, LANES), 1)
    line = jnp.zeros((8, LANES), jnp.float32)
    for i, item in enumerate(known):
        line = jnp.where(lane == i, jnp.broadcast_to(item, (8, LANES)), line)
    extra[blocks : blocks + 8, :] = line
    fetches[3].wait()
    for b in range(blocks):
        extra[b : b + 1, :] = visible_ref[:, b * LANES : (b + 1) * LANES].astype(jnp.float32)
    fetches[0].wait()
    fill_dense(params_ref, dense)
    feat_parts = [
        project_rows(dense_rows(dense, part, count), turn, centre) for part in range(blocks // 8)
    ]
    fetches[2].wait()
    stage_features(feat_parts, plan_ref, table, last, plan_order, tips)
    for peer in others:
        pack_features(peer, halves, table, plan_order, tips, outgoing)
    pl.semaphore_wait(barrier, cells + views - 2)
    sent = [
        send(
            "cells", peer, outgoing.at[peer], incoming.at[cell], send_one.at[i], recv_one.at[cell]
        )
        for i, peer in enumerate(others)
    ]
    pack_features(cell, halves, table, plan_order, tips, incoming)
    fetches[4].wait()
    fetches[5].wait()
    render_setup(lists_ref, target_ref, order, wanted, basis, plan_sums, hot, bits)
    wide = own_hot.shape[0].bit_length() - 1
    arrivals = [cell] + others[::-1]
    slots = cells * halves
    sub = lax.broadcasted_iota(jnp.int32, (8, LANES), 0)
    count_lanes = lane.astype(jnp.float32)
    for o in range(slots):
        row = plan_order[o : o + 1, :]
        fill_hot(own_hot, row, o * LANES, wide)
        here = jnp.broadcast_to(row >> wide, (8, LANES)) == sub
        own_lhs[:, o * LANES : (o + 1) * LANES] = jnp.concatenate(
            [jnp.where(here, o + 1.0, 0.0), jnp.where(here, count_lanes, 0.0)], axis=0
        ).astype(jnp.bfloat16)
    inverse = lax.dot_general(
        own_lhs[...], own_hot[...], (((1,), (1,)), ((), ())), preferred_element_type=jnp.float32
    )
    for i in range(2):
        span = slice(i * LANES, (i + 1) * LANES)
        extra[pl.ds(blocks + 8 + i, 8, stride=2), :] = inverse[0:8, span]
        extra[pl.ds(2 * blocks + 8 + i, 8, stride=2), :] = inverse[8:16, span]
    early = [
        send("views", mate, extra, extras.at[view], send_four.at[j], recv_four.at[j])
        for j, mate in enumerate(mates)
    ]
    render_rest(
        cells, others, receive_one, lambda: sent.pop(0).wait_send(), incoming, order, wanted, back,
        coefs, turned_s, tables, basis, alpha_s, weight_s, stages, joint_g, joint_w, plan_sums, error_sums,
        turned, tinted, moved, pairs, lhs, hot, bits,
    )
    sent += [
        send(
            "cells", peer, back.at[peer], returned.at[cell], send_two.at[i], recv_two.at[cell]
        )
        for i, peer in enumerate(others)
    ]

    def forward(k, source, origin):
        return [
            send(
                "views", mate, source, relayed.at[view, origin],
                send_three.at[k, j], recv_three.at[k, j],
            )
            for j, mate in enumerate(mates)
        ]

    relays = [forward(0, back.at[cell], cell)]
    for copy in early:
        copy.wait()
    counts = extra[0:blocks, :]
    for mate in mates:
        counts = counts + extras[mate, 0:blocks, :]
    grads = blocks * PAD_ROWS
    out_ref[grads : grads + blocks, :] = counts
    parts = blocks // 8
    seen = [extra] + [extras.at[mate] for mate in mates]
    rows_of = [dense_rows(dense, part, count) for part in range(parts)]
    statics = [static_terms(rows) for rows in rows_of]
    turns, terms = [], []
    for source in seen:
        known = [
            jnp.broadcast_to(source[blocks : blocks + 1, i : i + 1], (8, LANES)) for i in range(12)
        ]
        turns.append([known[0:3], known[3:6], known[6:9]])
        terms.append(
            [
                moving_terms(rows_of[part], statics[part][3], turns[-1], known[9:12])
                for part in range(parts)
            ]
        )
    for k in range(1, cells):
        receive_two(arrivals[k])
        relays.append(forward(k, returned.at[arrivals[k]], arrivals[k]))

    def collect(v, got, packet, origin):
        for part in range(parts):
            start = blocks + 8 + 8 * part
            block = seen[v][start : start + 8, :].astype(jnp.int32)
            lanes = seen[v][blocks + start : blocks + start + 8, :].astype(jnp.int32)
            for h in range(halves):
                here = block == origin * halves + h + 1
                for f in range(FEATS):
                    r = 8 * h + f if f < 8 else 8 * halves + h
                    item = lane_pick(jnp.broadcast_to(packet[r : r + 1, :], (8, LANES)), lanes)
                    got[part][f] = jnp.where(here, item, got[part][f])

    def nothing():
        return [[jnp.zeros((8, LANES), jnp.float32)] * FEATS for _ in range(parts)]

    totals = [None] * parts

    def pull_group(group, gots, last):
        for part in range(parts):
            base = part * PAD_ROWS
            rows = dense_rows(dense, part, count)
            sums = totals[part]
            for v, got in zip(group, gots):
                moved_part = pull_moving(rows, terms[v][part], turns[v], got[part])
                sums = (
                    moved_part if sums is None else [a + b for a, b in zip(sums, moved_part)]
                )
                if last:
                    sent.pop(0).wait_send()
            bases = [shade_basis(terms[v][part][8]) for v in group]
            for j in range(16):
                for k in range(3):
                    r = base + 11 + 3 * j + k
                    where = slice(r * 8, (r + 1) * 8)
                    total = None if totals[part] is None else out_ref[where, :]
                    for basis_of, got in zip(bases, gots):
                        item = basis_of[j] * got[part][6 + k]
                        total = item if total is None else total + item
                    out_ref[where, :] = total
            totals[part] = sums
            if last:
                sent.pop(0).wait_send()
                for r, item in enumerate(pull_static(statics[part], sums)):
                    out_ref[(base + r) * 8 : (base + r + 1) * 8, :] = item
                sent.pop(0).wait_send()

    for group in relays:
        sent += group
    got = nothing()
    for k in range(cells):
        collect(0, got, returned.at[arrivals[k]] if k else back.at[cell], arrivals[k])
    pull_group((0,), (got,), False)
    for group in ((1,), (2, 3)):
        gots = [nothing() for _ in group]
        for k in range(cells):
            for v, got in zip(group, gots):
                relays[k][v - 1].wait_recv()
                collect(v, got, relayed.at[mates[v - 1], arrivals[k]], arrivals[k])
        pull_group(group, gots, 3 in group)
    for copy in sent:
        copy.wait_send()


def update_kernel(
    params_ref, first_ref, second_ref, grads_ref, new_out, new_first_out, new_second_out,
    new_ref, new_first_ref, new_second_ref, sems,
):
    count, block = params_ref.shape
    blocks = block // LANES
    row_ids = lax.broadcasted_iota(jnp.int32, (8, LANES), 0)
    scale_one = 1.0 / (1.0 - 0.9**ADAM_STEP)
    scale_two = 1.0 / (1.0 - 0.999**ADAM_STEP)
    copies = []
    group = blocks // WAVES
    for b in range(blocks):
        span = slice(b * LANES, (b + 1) * LANES)
        part, line = divmod(b, 8)
        counts = grads_ref[blocks * PAD_ROWS + b : blocks * PAD_ROWS + b + 1, :]
        for r in range(0, count, 8):
            size = min(8, count - r)
            rows = slice(r, r + size)
            gradient = grads_ref[pl.ds((part * PAD_ROWS + r) * 8 + line, size, stride=8), :]
            if r >= 16:
                rates = 0.000125 * scale_one
            else:
                ids = row_ids[0:size] + r
                rates = scale_one * jnp.where(
                    ids < 6,
                    0.01,
                    jnp.where(
                        ids < 10,
                        0.005,
                        jnp.where(ids < 11, 0.05, jnp.where(ids < 14, 0.0025, 0.000125)),
                    ),
                )
            params, first, second = params_ref[rows, span], first_ref[rows, span], second_ref[rows, span]
            seen = jnp.broadcast_to(counts, params.shape) > 0.0
            first_new = 0.9 * first + 0.1 * gradient
            second_new = 0.999 * second + 0.001 * gradient * gradient
            stride = rates * first_new / (jnp.sqrt(second_new * scale_two) + 1e-08)
            new_ref[rows, span] = jnp.where(seen, params - stride, params)
            new_first_ref[rows, span] = jnp.where(seen, first_new, first)
            new_second_ref[rows, span] = jnp.where(seen, second_new, second)
        if (b + 1) % group == 0:
            wave = b // group
            span = slice(wave * group * LANES, (wave + 1) * group * LANES)
            for i, (source, dest) in enumerate(
                ((new_ref, new_out), (new_first_ref, new_first_out), (new_second_ref, new_second_out))
            ):
                copy = pltpu.make_async_copy(source.at[:, span], dest.at[:, span], sems.at[i, wave])
                copy.start()
                copies.append(copy)
    for copy in copies:
        copy.wait()


def fused_shards(params, first_moment, second_moment, cameras, visible, send_plan, tile_lists, target):
    cells, views = lax.axis_size("cells"), lax.axis_size("views")
    count, block = params.shape
    blocks = block // LANES
    plan = send_plan[0, 0]
    lists = tile_lists[0]
    tiles, entries = lists.shape
    capacity = plan.shape[1]
    halves = capacity // LANES
    slots = cells * halves
    f32, bf16 = jnp.float32, jnp.bfloat16
    packet = pltpu.VMEM((cells, FEATS * halves, LANES), f32)
    dma = pltpu.SemaphoreType.DMA
    vmem = pl.BlockSpec(memory_space=pltpu.VMEM)
    grads = pl.pallas_call(
        main_kernel,
        out_shape=jax.ShapeDtypeStruct((blocks * PAD_ROWS + blocks, LANES), f32),
        in_specs=[pl.BlockSpec(memory_space=pltpu.HBM)] * 6,
        out_specs=vmem,
        scratch_shapes=[
            pltpu.VMEM((count, block), f32),
            pltpu.VMEM(cameras.shape, f32),
            pltpu.VMEM(plan.shape, jnp.int32),
            pltpu.VMEM(visible.shape, jnp.int32),
            pltpu.VMEM(lists.shape, jnp.int32),
            pltpu.VMEM((3, 1, target.shape[2]), f32),
            pltpu.VMEM((blocks * PAD_ROWS, LANES), f32),
            pltpu.VMEM((blocks * 8, LANES), f32),
            pltpu.VMEM((blocks, LANES), f32),
            pltpu.VMEM((slots, LANES), jnp.int32),
            packet, packet, packet, packet,
            pltpu.VMEM((3 * blocks + 8, LANES), f32),
            pltpu.VMEM((views, 3 * blocks + 8, LANES), f32),
            pltpu.VMEM((views, cells, FEATS * halves, LANES), f32),
            pltpu.VMEM((slots, LANES), f32),
            pltpu.VMEM((tiles * entries // LANES, LANES), jnp.int32),
            pltpu.VMEM((24, LANES), f32),
            pltpu.VMEM((LANES, 2 * LANES), f32),
            pltpu.VMEM((entries, LANES), f32),
            pltpu.VMEM((entries, LANES), bf16),
            pltpu.VMEM((6, entries, LANES), f32),
            pltpu.VMEM((entries * 8, LANES), f32),
            pltpu.VMEM((entries * 8, LANES), f32),
            [pltpu.VMEM((8 * LANES, LANES), f32)] * 2,
            pltpu.VMEM((16 * LANES, entries + LANES), bf16),
            pltpu.VMEM((16 * LANES, entries + LANES), bf16),
            pltpu.VMEM((48, 16 * LANES), bf16),
            pltpu.VMEM((48, 16 * LANES), bf16),
            pltpu.VMEM((48, entries), f32),
            pltpu.VMEM((48, entries), f32),
            pltpu.VMEM((entries // LANES * 8, LANES), f32),
            pltpu.VMEM((tiles * entries // LANES * 16, LANES), f32),
            pltpu.VMEM((cells * 18, tiles * entries), bf16),
            pltpu.VMEM((capacity, tiles * entries), bf16),
            pltpu.VMEM((16, slots * LANES), bf16),
            pltpu.VMEM((2 * LANES, slots * LANES), bf16),
            dma((cells - 1,)), dma((cells,)), dma((cells - 1,)), dma((cells,)),
            dma((cells, views - 1)), dma((cells, views - 1)), dma((views - 1,)), dma((views - 1,)),
            dma((6,)),
        ],
        compiler_params=pltpu.CompilerParams(
            collective_id=0,
            has_side_effects=True,
            vmem_limit_bytes=MAIN_VMEM,
        ),
        cost_estimate=pl.CostEstimate(
            flops=4096 * tiles * 256 * entries,
            bytes_accessed=4 * count * block,
            transcendentals=tiles * 256 * entries,
        ),
    )(
        *[
            pltpu.with_memory_space_constraint(item, pltpu.HBM)
            for item in (params, cameras, plan, visible, lists, jnp.transpose(target, (1, 0, 2)))
        ]
    )
    like = jax.ShapeDtypeStruct(params.shape, f32)
    return tuple(
        pl.pallas_call(
            update_kernel,
            out_shape=(like, like, like),
            out_specs=(pl.BlockSpec(memory_space=pl.ANY),) * 3,
            scratch_shapes=[
                pltpu.VMEM(params.shape, f32),
                pltpu.VMEM(params.shape, f32),
                pltpu.VMEM(params.shape, f32),
                dma((3, WAVES)),
            ],
            compiler_params=pltpu.CompilerParams(vmem_limit_bytes=UPDATE_VMEM),
        )(params, first_moment, second_moment, grads)
    )


def local_shards(params, first_moment, second_moment, cameras, visible, send_plan, tile_lists, target):
    capacity = send_plan.shape[3]
    tiles, entries = tile_lists.shape[1:]
    halves = capacity // LANES
    fits = (
        capacity % LANES == 0
        and params.shape[1] == 16 * LANES
        and entries % (2 * LANES) == 0
        and 8 % max(halves, 1) == 0
        and lax.axis_size("cells") == 8
        and lax.axis_size("views") == 4
        and tiles * entries <= 4096
        and tiles == 4
    )
    body = fused_shards if fits else shards
    return body(params, first_moment, second_moment, cameras, visible, send_plan, tile_lists, target)


def solution(mesh):
    in_specs = (
        P(None, "cells"),
        P(None, "cells"),
        P(None, "cells"),
        P("views", None),
        P("views", "cells"),
        P("views", "cells", None, None),
        P("views", "cells", None),
        P("views", None, "cells"),
    )
    out_specs = (P(None, "cells"), P(None, "cells"), P(None, "cells"))
    return jax.shard_map(local_shards, mesh=mesh, in_specs=in_specs, out_specs=out_specs, check_vma=False)
```
